128 devices in a mesh: pairs: 1, cols: 2 (over core), rows: 64 (over z, y, x).
Axes of the slice: x: 4, y: 4, z: 4, core: 2. Of those that a mesh axis runs over, the one named last changes fastest.
Arguments:
- C1: float32 [512, 512], P(('pairs', 'rows'), 'cols')
- C2: float32 [8192, 8192], P(('pairs', 'rows'), 'cols')
- T0: float32 [512, 8192], P(('pairs', 'rows'), 'cols')
- p: float32 [512], P(('pairs', 'rows'))
- q: float32 [8192], P(('pairs', 'cols'))
- eps: float32 [6], P('pairs')
Outputs:
- output 1: float32 [512, 8192], P(('pairs', 'rows'), 'cols')
- output 2: float32 [1], P('pairs')
All inputs are finite; a program needn't handle non-finite values.
Results may differ from the reference program's by a relative error of at most 0.001.
Values are sent between devices in bfloat16 or wider.
A program may use at most 1 GiB of HBM per device.

```python
import jax
import jax.numpy as jnp
from jax import lax

N = 512
M = 8192
DX = 128
DY = 128
OUTER = 6
SWEEPS = 10
CLUSTERS = 8
PROBE = 256


def cloud_dists(key, count, dim):
    subkeys = jax.random.split(key, 4)
    labels = jax.random.randint(subkeys[0], (count,), 0, CLUSTERS)
    centers = jax.random.normal(subkeys[1], (CLUSTERS, dim), jnp.float32)
    widths = jax.random.uniform(subkeys[2], (CLUSTERS, 1), jnp.float32, 0.2, 0.6)
    points = centers[labels] + widths[labels] * jax.random.normal(subkeys[3], (count, dim), jnp.float32)
    sq_norm = jnp.sum(points * points, axis=1)
    dists = jnp.maximum(sq_norm[:, None] + sq_norm[None, :] - 2.0 * jnp.dot(points, points.T), 0.0)
    dists = 0.5 * (dists + dists.T) * (1.0 - jnp.eye(count, dtype=jnp.float32))
    return points, dists / jnp.max(dists)


def point_features(key, points):
    projection = jax.random.normal(key, (points.shape[1], 4), jnp.float32)
    embedded = jnp.dot(points, projection)
    embedded = embedded - jnp.mean(embedded, axis=0)
    return embedded / jnp.std(embedded, axis=0)


def eps_schedule(key, C1, C2, T0, p, q):
    probe_rows = min(N, PROBE)
    c1_probe = C1[:probe_rows]
    lead_mat = jnp.dot(c1_probe, T0)
    cost_mat = jnp.dot(c1_probe * c1_probe, p)[:, None] + jnp.dot(C2 * C2, q)[None, :] - 2.0 * jnp.dot(lead_mat, C2)
    spread = jnp.mean(jnp.max(cost_mat, axis=1) - jnp.min(cost_mat, axis=1))
    ratios = jax.random.uniform(key, (OUTER,), jnp.float32, 6.0, 14.0)
    return spread / ratios


def setup_inputs(seed: int = 0, part: int = 0) -> dict:
    key = jax.random.fold_in(jax.random.key(seed), part)
    subkeys = jax.random.split(key, 7)
    points_x, C1 = cloud_dists(subkeys[0], N, DX)
    points_y, C2 = cloud_dists(subkeys[1], M, DY)
    p_raw = jax.random.uniform(subkeys[2], (N,), jnp.float32, 0.25, 1.75)
    q_raw = jax.random.uniform(subkeys[3], (M,), jnp.float32, 0.25, 1.75)
    p = p_raw / jnp.sum(p_raw)
    q = q_raw / jnp.sum(q_raw)
    feat_x = point_features(subkeys[4], points_x)
    feat_y = point_features(subkeys[5], points_y)
    tilt_map = 1.0 + 0.8 * jnp.tanh(0.5 * jnp.dot(feat_x, feat_y.T))
    T0 = p[:, None] * q[None, :] * tilt_map
    T0 = T0 / jnp.sum(T0)
    eps = eps_schedule(subkeys[6], C1, C2, T0, p, q)
    return {"C1": C1, "C2": C2, "T0": T0, "p": p, "q": q, "eps": eps}


def reference(C1, C2, T0, p, q, eps):
    c1_half = C1.astype(jnp.bfloat16)
    c2_half = C2.astype(jnp.bfloat16)
    const_c = jnp.dot(C1 * C1, p)[:, None] + jnp.dot(C2 * C2, q)[None, :]

    def cost_of(plan_mat):
        lead_mat = jnp.dot(c1_half, plan_mat.astype(jnp.bfloat16), preferred_element_type=jnp.float32)
        cross_mat = jnp.dot(lead_mat.astype(jnp.bfloat16), c2_half, preferred_element_type=jnp.float32)
        return const_c - 2.0 * cross_mat

    def outer_step(plan_mat, eps_step):
        cost_mat = cost_of(plan_mat)
        kernel = jnp.exp(-(cost_mat - jnp.min(cost_mat, axis=1, keepdims=True)) / eps_step)

        def sweep(sweep_idx, scales):
            row_scale = p / jnp.sum(kernel * scales[1][None, :], axis=1)
            col_scale = q / jnp.sum(kernel * row_scale[:, None], axis=0)
            return row_scale, col_scale

        row_scale, col_scale = lax.fori_loop(0, SWEEPS, sweep, (jnp.ones_like(p), jnp.ones_like(q)))
        return row_scale[:, None] * kernel * col_scale[None, :], eps_step

    plan_mat = lax.scan(outer_step, T0, eps)[0]
    loss_val = jnp.sum(cost_of(plan_mat) * plan_mat)
    return plan_mat, loss_val.reshape(1)
```

```python
import heapq
import itertools
import math

import jax
import jax.numpy as jnp
from jax import lax
from jax.experimental import pallas as pl
from jax.experimental.pallas import tpu as pltpu
from jax.sharding import PartitionSpec as P

SWEEPS = 10
MESH = pl.DeviceIdType.MESH
JB = 64
JT = JB // 8
F32, BF16 = jnp.float32, jnp.bfloat16
ORDERS = ((0, 1, 2), (1, 2, 0), (2, 0, 1))


def torus_of(chips):
    return {64: (4, 4, 4), 8: (4, 2, 1), 16: (4, 4, 1)}[chips]


def split3(n):
    cuts = [0, (n + 2) // 3, (2 * n + 2) // 3, n]
    return [(cuts[k], cuts[k + 1]) for k in range(3)]


def tree_plan(dims, tiles, tile_us, lat_us=2.0):
    rings = {1: (), 2: ((1, "f", 1),), 4: ((1, "f", 1), (3, "f", -1), (2, "a", 1), (2, "b", -1))}
    msgs = []
    for color, order in enumerate(ORDERS):
        lo, hi = split3(tiles)[color]
        mid = lo + (hi - lo + 1) // 2
        for dst in itertools.product(*(range(n) for n in dims)):
            used = [k for k in range(3) if dst[order[k]]]
            if not used or lo == hi:
                continue
            d = order[used[-1]]
            for at, part, sign in rings[dims[d]]:
                a, b = {"f": (lo, hi), "a": (lo, mid), "b": (mid, hi)}[part]
                if at != dst[d] or a == b:
                    continue
                src = list(dst)
                src[d] = (src[d] - sign) % dims[d]
                msgs.append(dict(id=len(msgs), color=color, src=tuple(src), dst=dst, link=(d, sign), lo=a, hi=b))
    into = {}
    for m in msgs:
        into.setdefault((m["color"], m["dst"]), []).append(m)
    users = {m["id"]: [] for m in msgs}
    for m in msgs:
        m["deps"] = [
            e["id"] for e in into.get((m["color"], m["src"]), []) if e["lo"] < m["hi"] and m["lo"] < e["hi"]
        ]
        for e in m["deps"]:
            users[e].append(m)
    depth = {}

    def depth_of(m):
        if m["id"] not in depth:
            depth[m["id"]] = 1 + max([depth_of(u) for u in users[m["id"]]], default=0)
        return depth[m["id"]]

    ops, free, arrivals, missing = [], {}, [], {m["id"]: len(m["deps"]) for m in msgs}
    left = {}
    for m in msgs:
        left[m["dst"]] = left.get(m["dst"], 0) + 1

    def send(ready, now):
        for m in sorted(ready, key=lambda m: (-depth_of(m), m["color"], m["id"])):
            ops.append(("send", m))
            end = max(now, free.get(m["link"], 0.0)) + (m["hi"] - m["lo"]) * tile_us
            free[m["link"]] = end
            heapq.heappush(arrivals, (end + lat_us, m["id"]))

    send([m for m in msgs if not m["deps"]], 0.0)
    now = 0.0
    while arrivals:
        now, k = heapq.heappop(arrivals)
        m = msgs[k]
        ops.append(("wait", m))
        ready = []
        for u in users[k]:
            missing[u["id"]] -= 1
            if not missing[u["id"]]:
                ready.append(u)
        send(ready, now)
        left[m["dst"]] -= 1
        if not left[m["dst"]]:
            ops.append(("slot", m["dst"]))
    links = sorted({m["link"] for m in msgs})
    totals = {k: sum(m["hi"] - m["lo"] for m in msgs if m["link"] == k) for k in links}
    return dict(msgs=msgs, ops=ops, links=links, totals=totals, end=now)


def make_kernel(dims, n_rows, n_cols, steps, sweeps):
    X, Y, Z = dims
    CH = X * Y * Z
    NR = n_rows // CH
    G = NR // 8
    NT = n_rows // 128
    TB = JT * NT
    HB = CH // 2
    JN = n_cols // 2 // 128
    JW = JN // 2
    NT0 = G * JW
    TT0 = NT0 + 2 * G
    KJ = CH * JB
    CK = min(512, KJ)
    GS = min(8, CH // 2)
    NG = CH // GS
    assert NT == 4 and n_cols == CH * 128 and JN == HB
    plan0 = tree_plan(dims, TT0, 4096 / 46.6e3)
    plan = tree_plan(dims, TB, 4096 / 46.6e3)
    links = plan["links"]
    NL = len(links)
    peers = [(d, k) for d in range(3) for k in range(1, dims[d])]
    strides = (1, X, X * Y)

    def slot_of(offset):
        return offset[0] + X * offset[1] + X * Y * offset[2]

    def kernel(
        eps_ref, p_ref, c1_ref, c2_ref, t0_ref, q_ref,
        out_ref, loss_ref,
        land, kbuf, g0, tt, c1f, c1b, c2n, c2p, bacc, lp, lprecv, bp, qf, qrep, vbuf, cbuf,
        mb, sb, fb, ub, ap, xs, xr, mss, msr, pv, ars, arr, arps, arpr, obuf, orecv, trb,
        send_sem, recv_sem, credit, x_ssem, x_rsem, ms_sem, lp_sem, c1_sem, c2_sem, q_sem, ar_ssem, ar_rsem, arp_sem, o_sem,
    ):
        chip = lax.axis_index("rows")
        core = lax.axis_index("cols")
        other = 1 - core
        pos = (lax.rem(chip, X), lax.rem(lax.div(chip, X), Y), lax.div(chip, X * Y))

        def moved(d, k):
            return chip + (lax.rem(pos[d] + k + dims[d], dims[d]) - pos[d]) * strides[d]

        near = {link: moved(*link) for link in links}

        def source_of(slot):
            off = (lax.rem(slot, X), lax.rem(lax.div(slot, X), Y), lax.div(slot, X * Y))
            at = [lax.rem(pos[d] + dims[d] - off[d], dims[d]) for d in range(3)]
            return at[0] + X * at[1] + X * Y * at[2]

        def to_partner(src, dst, ssem, rsem):
            return pltpu.make_async_remote_copy(
                src_ref=src, dst_ref=dst, send_sem=ssem, recv_sem=rsem,
                device_id={"cols": other}, device_id_type=MESH,
            )

        def tree_copy(buf, width, m):
            n = m["hi"] - m["lo"]
            return pltpu.make_async_remote_copy(
                src_ref=buf.at[pl.ds(slot_of(m["src"]) * width + m["lo"], n)],
                dst_ref=buf.at[pl.ds(slot_of(m["dst"]) * width + m["lo"], n)],
                send_sem=send_sem.at[links.index(m["link"])],
                recv_sem=recv_sem.at[m["id"]],
                device_id={"rows": near[m["link"]]},
                device_id_type=MESH,
            )

        def tree(buf, width, the_plan, before_send=None, on_slot=None, fillers=()):
            fillers, ready, sends = list(fillers), [], 0
            for op, m in the_plan["ops"]:
                if op == "send":
                    if before_send is not None:
                        before_send(m)
                    tree_copy(buf, width, m).start()
                elif op == "wait":
                    tree_copy(buf, width, m).wait_recv()
                    sends += 1
                    if ready:
                        on_slot(ready.pop(0))
                    elif fillers and sends >= fillers[0][0]:
                        fillers.pop(0)[1]()
                elif on_slot is not None:
                    ready.append(slot_of(m))
            for s in ready:
                on_slot(s)
            for _, f in fillers:
                f()

        def tree_sent(buf, the_plan):
            for k, link in enumerate(links):
                n = the_plan["totals"][link]
                ref = buf.at[pl.ds(0, n)]
                pltpu.make_async_copy(ref, ref, send_sem.at[k]).wait()

        def give_credit():
            for d, sign in links:
                pl.semaphore_signal(credit, inc=1, device_id={"rows": moved(d, -sign)}, device_id_type=MESH)

        def all_sum_send(use, stage):
            for n, k in enumerate(range(1, dims[stage])):
                pltpu.make_async_remote_copy(
                    src_ref=ars.at[use, stage], dst_ref=arr.at[use, stage, n],
                    send_sem=ar_ssem.at[use, stage, n], recv_sem=ar_rsem.at[use, stage, n],
                    device_id={"rows": moved(stage, k)}, device_id_type=MESH,
                ).start()

        def all_sum_get(use, stage):
            total = ars[use, stage]
            for n, k in enumerate(range(1, dims[stage])):
                pltpu.make_async_remote_copy(
                    src_ref=ars.at[use, stage], dst_ref=arr.at[use, stage, n],
                    send_sem=ar_ssem.at[use, stage, n], recv_sem=ar_rsem.at[use, stage, n],
                    device_id={"rows": moved(stage, k)}, device_id_type=MESH,
                ).wait()
                total = total + arr[use, stage, n]
            return total

        def all_sum_step(use, stage):
            total = all_sum_get(use, stage)
            if stage < 2:
                ars[use, stage + 1] = total
                all_sum_send(use, stage + 1)
            else:
                arps[use] = total
                to_partner(arps.at[use], arpr.at[use], arp_sem.at[use, 0], arp_sem.at[use, 1]).start()

        barrier = pltpu.get_barrier_semaphore()
        for d, k in peers:
            pl.semaphore_signal(barrier, inc=1, device_id={"rows": moved(d, k)}, device_id_type=MESH)
        pl.semaphore_signal(barrier, inc=1, device_id={"cols": other}, device_id_type=MESH)

        row = lax.broadcasted_iota(jnp.int32, (8, 128), 0)
        lane = lax.broadcasted_iota(jnp.int32, (8, 128), 1)

        for g in range(G):
            rows = slice(g * 8, g * 8 + 8)
            pair = jnp.concatenate([c1_ref[rows, :128], c1_ref[rows, 128:]], axis=0)
            g0[NT0 + core * G + g] = pair.astype(BF16)
        c1_copy = to_partner(
            g0.at[pl.ds(NT0 + core * G, G)], g0.at[pl.ds(NT0 + core * G, G)], c1_sem.at[0], c1_sem.at[1]
        )
        q_copy = to_partner(q_ref, qf.at[pl.ds(core * HB, HB)], q_sem.at[0], q_sem.at[1])

        tile = jnp.zeros((8, 128), F32)
        for t in range(2):
            part = jnp.zeros((1, 128), F32)
            for k in range(NR):
                entry = c1_ref[k : k + 1, t * 128 : t * 128 + 128]
                part = part + entry * entry * p_ref[k]
            tile = jnp.where(row == 2 * core + t, jnp.broadcast_to(part, (8, 128)), tile)
        where = (row - 4) * 128 + lane
        for k in range(NR):
            tile = jnp.where(where == chip * NR + k, p_ref[k], tile)
        ars[0, 0] = tile
        for g in range(G):
            rows = slice(g * 8, g * 8 + 8)
            for t in range(JW):
                a, b = t0_ref[rows, 256 * t : 256 * t + 128], t0_ref[rows, 256 * t + 128 : 256 * t + 256]
                g0[g * JW + t] = jnp.concatenate([a, b], axis=0).astype(BF16)
        qf[pl.ds(core * HB, HB)] = q_ref[...]

        pl.semaphore_wait(barrier, len(peers) + 1)
        give_credit()
        c1_copy.start()
        q_copy.start()
        all_sum_send(0, 0)

        c2_copy = to_partner(c2n.at[pl.ds(core * HB, HB)], c2n.at[pl.ds(core * HB, HB)], c2_sem.at[0], c2_sem.at[1])
        bp[...] = jnp.zeros_like(bp)

        def round_c2(first, last):
            for t in range(first, last):
                blk = c2_ref[:, t * 128 : t * 128 + 128]
                c2n[core * HB + t] = blk.astype(BF16)
                bp[...] += blk * blk * q_ref[t : t + 1, :]

        def finish_b():
            bp[...] = jnp.broadcast_to(jnp.sum(bp[...], axis=1, keepdims=True), (128, 128))

        src = lax.broadcasted_iota(jnp.int32, (128, 128), 0)
        dst = lax.broadcasted_iota(jnp.int32, (128, 128), 1)
        picks = [
            jnp.where((src - core * JB == dst - h * JB) & (dst >= h * JB) & (dst < h * JB + JB), 1.0, 0.0).astype(BF16)
            for h in range(2)
        ]

        def order_c2(first, last):
            for t in range(first, last):
                a = jnp.dot(c2n[source_of(2 * t)], picks[0], preferred_element_type=F32)
                b = jnp.dot(c2n[source_of(2 * t + 1)], picks[1], preferred_element_type=F32)
                c2p[:, t * 128 : t * 128 + 128] = (a + b).astype(BF16)

        def order_q(first, last):
            def one(s, carry):
                line = jnp.broadcast_to(qf[pl.ds(source_of(s), 1), :], (8, 128))
                for jt in range(JT):
                    own = jnp.where(lane == core * JB + jt * 8 + row, line, 0.0)
                    qrep[s, jt] = jnp.broadcast_to(jnp.sum(own, axis=1, keepdims=True), (8, 128))
                return carry

            lax.fori_loop(first, last, one, 0)

        def span(n, parts, f):
            cuts = [n * k // parts for k in range(parts + 1)]
            return [lambda a=a, b=b: f(a, b) for a, b in zip(cuts, cuts[1:])]

        fillers = span(HB, 8, round_c2)
        fillers += [finish_b, lambda: c2_copy.start(), lambda: all_sum_step(0, 0)]
        fillers += [lambda: q_copy.wait()] + span(CH, 8, order_q)
        fillers += [lambda: all_sum_step(0, 1), lambda: c2_copy.wait()] + span(CH // 2, 16, order_c2)
        fillers += [lambda: all_sum_step(0, 2)]
        waited = []

        def before_send(m):
            if not waited and m["hi"] > NT0:
                waited.append(1)
                c1_copy.wait()

        tree(g0, TT0, plan0, before_send=before_send, fillers=[(0, f) for f in fillers])
        tree_sent(g0, plan0)
        to_partner(arps.at[0], arpr.at[0], arp_sem.at[0, 0], arp_sem.at[0, 1]).wait()
        ap[...] = jnp.where(row < 4, arps[0] + arpr[0], arps[0])
        for t in range(NT):
            pv[t] = jnp.broadcast_to(ap[4 + t : 5 + t, :], (8, 128))

        def unpack(s, carry):
            chip_s = source_of(s)
            for g in range(G):
                for t in range(JW):
                    pair = g0[s * TT0 + g * JW + t].astype(F32)
                    kbuf[(chip_s * G + g) * JN + 2 * t] = pair[:8]
                    kbuf[(chip_s * G + g) * JN + 2 * t + 1] = pair[8:]
                for h in range(2):
                    pair = g0[s * TT0 + NT0 + h * G + g].astype(F32)
                    at = pl.ds(pl.multiple_of(chip_s * NR + g * 8, 8), 8)
                    c1f[at, 256 * h : 256 * h + 128] = pair[:8]
                    c1f[at, 256 * h + 128 : 256 * h + 256] = pair[8:]
            return carry

        lax.fori_loop(0, CH, unpack, 0)
        c1b[...] = c1f[...].astype(BF16)

        def finish_lp():
            lp[...] = jnp.concatenate([bp[...]] * NT, axis=1) - 2.0 * bacc[...]

        bacc[...] = jnp.zeros_like(bacc)
        JC = CK // 128

        def first_chunk(n, carry):
            cols = []
            for t in range(JC):
                tiles = [kbuf[g * JN + n * JC + t] for g in range(CH * G)]
                cols.append(jnp.concatenate(tiles, axis=0))
            plan_c = jnp.concatenate(cols, axis=1).astype(BF16)
            lead = jnp.dot(c1b[...], plan_c, preferred_element_type=F32).astype(BF16)
            c2c = jnp.concatenate([c2n[core * HB + n * JC + t] for t in range(JC)], axis=1)
            bacc[...] += lax.dot_general(c2c, lead, (((1,), (1,)), ((), ())), preferred_element_type=F32)
            return carry

        lax.fori_loop(0, KJ // CK, first_chunk, 0)
        finish_lp()

        def chunk(n, carry):
            at = pl.ds(pl.multiple_of(n * CK, CK), CK)
            lead = jnp.dot(tt[at, :], c1b[...], preferred_element_type=F32).astype(BF16)
            bacc[...] += jnp.dot(c2p[:, at], lead, preferred_element_type=F32)
            return carry

        def costs():
            copy = to_partner(lp.at[pl.ds(other * JB, JB)], lprecv, lp_sem.at[0], lp_sem.at[1])
            copy.start()
            copy.wait()
            own = lp[pl.ds(pl.multiple_of(core * JB, JB), JB), :] + lprecv[...]
            return own + jnp.concatenate([ap[t : t + 1, :] for t in range(NT)], axis=1)

        def block(s):
            return kbuf[pl.ds(s * TB, TB)].reshape(JT, NT, 8, 128)

        def weighted(kk, u):
            w = (kk[:, 0] * u[0] + kk[:, 1] * u[1]) + (kk[:, 2] * u[2] + kk[:, 3] * u[3])
            return jnp.sum(w, axis=2, keepdims=True)

        def passes(u, rescale=False, last=False):
            def one(g, buf):
                for k in range(GS):
                    s = g * GS + k
                    kk = block(s)
                    if rescale:
                        kk = kk * fb[:, pl.ds(s, 1), :][None]
                        kbuf[pl.ds(s * TB, TB)] = kk.reshape(TB, 8, 128)
                    cbuf[buf, k] = jnp.broadcast_to(weighted(kk, u), (JT, 8, 128))

            def two(g, buf, acc):
                for k in range(GS):
                    s = g * GS + k
                    v = qrep[s] / cbuf[buf, k]
                    kk = block(s)
                    if last:
                        vbuf[s] = v
                        t = (kk * u[None]) * v[:, None]
                        flat = jnp.concatenate([t[:, i].reshape(JB, 128) for i in range(NT)], axis=1)
                        tt[pl.ds(pl.multiple_of(s * JB, JB), JB), :] = flat.astype(BF16)
                    else:
                        acc = acc + jnp.sum(kk * v[:, None], axis=0)
                return acc

            def both(g, acc):
                acc = two(g - 1, lax.rem(g - 1, 2), acc)
                one(g, lax.rem(g, 2))
                return acc

            one(0, 0)
            acc = lax.fori_loop(1, NG, both, jnp.zeros((NT, 8, 128), F32))
            return two(NG - 1, (NG - 1) % 2, acc)

        def row_scale(acc, par):
            xs[par] = acc
            copy = to_partner(xs.at[par], xr.at[par], x_ssem.at[par], x_rsem.at[par])
            copy.start()
            copy.wait()
            total = jnp.sum(acc + xr[par], axis=1, keepdims=True)
            return pv[...] / jnp.broadcast_to(total, (NT, 8, 128))

        def outer(r, carry):
            scale = 1.4426950408889634 / eps_ref[r]
            cost = costs()
            for jt in range(JT):
                for t in range(NT):
                    land[jt * NT + t] = cost[jt * 8 : jt * 8 + 8, t * 128 : t * 128 + 128]

            def exps(s):
                ll = land[s * TB : s * TB + TB].reshape(JT, NT, 8, 128)
                low = jnp.min(jnp.min(ll, axis=0), axis=1, keepdims=True)
                kk = jnp.exp2((low[None] - ll) * scale)
                kbuf[s * TB : s * TB + TB] = kk.reshape(TB, 8, 128)
                mb[:, s : s + 1, :] = low
                sb[:, s : s + 1, :] = jnp.sum(jnp.sum(kk, axis=0), axis=1, keepdims=True)

            pl.semaphore_wait(credit, NL)
            tree(land, TB, plan, on_slot=exps, fillers=[(0, lambda: exps(0))])
            tree_sent(land, plan)
            give_credit()

            low = jnp.min(mb[...], axis=1, keepdims=True)
            part = jnp.sum(sb[...] * jnp.exp2((low - mb[...]) * scale), axis=1, keepdims=True)
            mss[0] = jnp.broadcast_to(low, (NT, 8, 128))
            mss[1] = jnp.broadcast_to(part, (NT, 8, 128))
            copy = to_partner(mss, msr, ms_sem.at[0], ms_sem.at[1])
            copy.start()
            copy.wait()
            least = jnp.minimum(mss[0], msr[0])
            total = mss[1] * jnp.exp2((least - mss[0]) * scale) + msr[1] * jnp.exp2((least - msr[0]) * scale)
            fb[...] = jnp.exp2((least[:, :1] - mb[...]) * scale)
            u = pv[...] / total

            u = row_scale(passes(u, rescale=True), 1)

            def sweep(t, u):
                return row_scale(passes(u), lax.rem(t, 2))

            u = lax.fori_loop(2, sweeps, sweep, u)
            passes(u, last=True)
            ub[...] = u
            bacc[...] = jnp.zeros_like(bacc)
            lax.fori_loop(0, KJ // CK, chunk, 0)
            finish_lp()
            return carry

        lax.fori_loop(0, steps, outer, 0)

        pl.semaphore_wait(credit, NL)
        cost = costs()
        plan_own = (block(0) * ub[...][None]) * vbuf[0][:, None]
        total = jnp.zeros((8, 128), F32)
        for jt in range(JT):
            for t in range(NT):
                total = total + cost[jt * 8 : jt * 8 + 8, t * 128 : t * 128 + 128] * plan_own[jt, t]
        ars[1, 0] = total
        all_sum_send(1, 0)

        it = lax.div(chip * NR, 128)
        inside = pl.multiple_of(lax.rem(chip * NR, 128), 8)

        def rows_of(s, carry):
            kk = jnp.concatenate([kbuf[s * TB + jt * NT + it] for jt in range(JT)], axis=0)
            uu = jnp.concatenate([ub[it]] * JT, axis=0)
            t = (kk * uu) * vbuf[s].reshape(JB, 128)
            none = jnp.zeros_like(t)
            both = jnp.where(core == 0, jnp.concatenate([t, none], axis=0), jnp.concatenate([none, t], axis=0))
            trb[...] = both.T
            obuf[source_of(s)] = trb[pl.ds(inside, NR), :]
            return carry

        lax.fori_loop(0, CH, rows_of, 0)
        o_copy = to_partner(obuf.at[pl.ds(other * HB, HB)], orecv, o_sem.at[0], o_sem.at[1])
        o_copy.start()
        all_sum_step(1, 0)
        o_copy.wait()
        for b in range(HB):
            out_ref[:, b * 128 : b * 128 + 128] = obuf[core * HB + b] + orecv[b]
        all_sum_step(1, 1)
        all_sum_step(1, 2)
        to_partner(arps.at[1], arpr.at[1], arp_sem.at[1, 0], arp_sem.at[1, 1]).wait()
        loss_ref[0] = jnp.sum(arps[1] + arpr[1])

    vm = pltpu.VMEM
    dma = pltpu.SemaphoreType.DMA
    scratch = [
        vm((CH * TB, 8, 128), F32),
        vm((CH * TB, 8, 128), F32),
        vm((CH * TT0, 16, 128), BF16),
        vm((KJ, n_rows), BF16),
        vm((n_rows, n_rows), F32),
        vm((n_rows, n_rows), BF16),
        vm((CH, 128, 128), BF16),
        vm((128, KJ), BF16),
        vm((128, n_rows), F32),
        vm((128, n_rows), F32),
        vm((JB, n_rows), F32),
        vm((128, 128), F32),
        vm((CH, 128), F32),
        vm((CH, JT, 8, 128), F32),
        vm((CH, JT, 8, 128), F32),
        vm((2, GS, JT, 8, 128), F32),
        vm((NT, CH, 128), F32),
        vm((NT, CH, 128), F32),
        vm((NT, CH, 128), F32),
        vm((NT, 8, 128), F32),
        vm((8, 128), F32),
        vm((2, NT, 8, 128), F32),
        vm((2, NT, 8, 128), F32),
        vm((2, NT, 8, 128), F32),
        vm((2, NT, 8, 128), F32),
        vm((NT, 8, 128), F32),
        vm((2, 3, 8, 128), F32),
        vm((2, 3, 3, 8, 128), F32),
        vm((2, 8, 128), F32),
        vm((2, 8, 128), F32),
        vm((CH, NR, 128), F32),
        vm((HB, NR, 128), F32),
        vm((128, 128), F32),
        dma((NL,)),
        dma((max(len(plan["msgs"]), len(plan0["msgs"])),)),
        pltpu.SemaphoreType.REGULAR,
        dma((2,)),
        dma((2,)),
        dma((2,)),
        dma((2,)),
        dma((2,)),
        dma((2,)),
        dma((2,)),
        dma((2, 3, 3)),
        dma((2, 3, 3)),
        dma((2, 2)),
        dma((2,)),
    ]
    return kernel, scratch


def solution(mesh):
    chips = mesh.shape["rows"]
    dims = torus_of(chips)
    grid_spec = P(("pairs", "rows"), "cols")

    def local_fn(c1, c2, t0, p, q, eps):
        n_rows, n_cols = p.shape[0] * chips, q.shape[0] * mesh.shape["cols"]
        kernel, scratch = make_kernel(dims, n_rows, n_cols, eps.shape[0], SWEEPS)
        vmem = pl.BlockSpec(memory_space=pltpu.VMEM)
        smem = pl.BlockSpec(memory_space=pltpu.SMEM)
        return pl.pallas_call(
            kernel,
            name="gromov",
            out_shape=(jax.ShapeDtypeStruct(t0.shape, F32), jax.ShapeDtypeStruct((1,), F32)),
            in_specs=[smem, smem, vmem, vmem, vmem, vmem],
            out_specs=(vmem, smem),
            scratch_shapes=scratch,
            compiler_params=pltpu.CompilerParams(
                collective_id=0, has_side_effects=True, vmem_limit_bytes=60 * 1024 * 1024
            ),
        )(eps, p, c1, c2, t0, q.reshape(chips // 2, 128))

    return jax.shard_map(
        local_fn,
        mesh=mesh,
        in_specs=(grid_spec, grid_spec, grid_spec, P(("pairs", "rows")), P(("pairs", "cols")), P("pairs")),
        out_specs=(grid_spec, P("pairs")),
        check_vma=False,
    )
```

```python
import heapq
import itertools
import math

import jax
import jax.numpy as jnp
from jax import lax
from jax.experimental import pallas as pl
from jax.experimental.pallas import tpu as pltpu
from jax.sharding import PartitionSpec as P

SWEEPS = 10
MESH = pl.DeviceIdType.MESH
JB = 64
JT = JB // 8
F32, BF16 = jnp.float32, jnp.bfloat16
ORDERS = ((0, 1, 2), (1, 2, 0), (2, 0, 1))


def torus_of(chips):
    return {64: (4, 4, 4), 8: (4, 2, 1), 16: (4, 4, 1)}[chips]


def split3(n):
    cuts = [0, (n + 2) // 3, (2 * n + 2) // 3, n]
    return [(cuts[k], cuts[k + 1]) for k in range(3)]


def tree_plan(dims, tiles, tile_us, lat_us=2.0):
    rings = {1: (), 2: ((1, "f", 1),), 4: ((1, "f", 1), (3, "f", -1), (2, "a", 1), (2, "b", -1))}
    msgs = []
    for color, order in enumerate(ORDERS):
        lo, hi = split3(tiles)[color]
        mid = lo + (hi - lo + 1) // 2
        for dst in itertools.product(*(range(n) for n in dims)):
            used = [k for k in range(3) if dst[order[k]]]
            if not used or lo == hi:
                continue
            d = order[used[-1]]
            for at, part, sign in rings[dims[d]]:
                a, b = {"f": (lo, hi), "a": (lo, mid), "b": (mid, hi)}[part]
                if at != dst[d] or a == b:
                    continue
                src = list(dst)
                src[d] = (src[d] - sign) % dims[d]
                msgs.append(dict(id=len(msgs), color=color, src=tuple(src), dst=dst, link=(d, sign), lo=a, hi=b))
    into = {}
    for m in msgs:
        into.setdefault((m["color"], m["dst"]), []).append(m)
    users = {m["id"]: [] for m in msgs}
    for m in msgs:
        m["deps"] = [
            e["id"] for e in into.get((m["color"], m["src"]), []) if e["lo"] < m["hi"] and m["lo"] < e["hi"]
        ]
        for e in m["deps"]:
            users[e].append(m)
    depth = {}

    def depth_of(m):
        if m["id"] not in depth:
            depth[m["id"]] = 1 + max([depth_of(u) for u in users[m["id"]]], default=0)
        return depth[m["id"]]

    ops, free, arrivals, missing = [], {}, [], {m["id"]: len(m["deps"]) for m in msgs}
    left = {}
    for m in msgs:
        left[m["dst"]] = left.get(m["dst"], 0) + 1

    def send(ready, now):
        for m in sorted(ready, key=lambda m: (-depth_of(m), m["color"], m["id"])):
            ops.append(("send", m))
            end = max(now, free.get(m["link"], 0.0)) + (m["hi"] - m["lo"]) * tile_us
            free[m["link"]] = end
            heapq.heappush(arrivals, (end + lat_us, m["id"]))

    send([m for m in msgs if not m["deps"]], 0.0)
    now = 0.0
    while arrivals:
        now, k = heapq.heappop(arrivals)
        m = msgs[k]
        ops.append(("wait", m))
        ready = []
        for u in users[k]:
            missing[u["id"]] -= 1
            if not missing[u["id"]]:
                ready.append(u)
        send(ready, now)
        left[m["dst"]] -= 1
        if not left[m["dst"]]:
            ops.append(("slot", m["dst"]))
    links = sorted({m["link"] for m in msgs})
    totals = {k: sum(m["hi"] - m["lo"] for m in msgs if m["link"] == k) for k in links}
    return dict(msgs=msgs, ops=ops, links=links, totals=totals, end=now)


def make_kernel(dims, n_rows, n_cols, steps, sweeps):
    X, Y, Z = dims
    CH = X * Y * Z
    NR = n_rows // CH
    G = NR // 8
    NT = n_rows // 128
    TB = JT * NT
    HB = CH // 2
    JN = n_cols // 2 // 128
    JW = JN // 2
    NT0 = G * JW
    TT0 = NT0 + 2 * G
    KJ = CH * JB
    CK = min(512, KJ)
    GS = min(4, CH // 2)
    NG = CH // GS
    assert NT == 4 and n_cols == CH * 128 and JN == HB
    plan0 = tree_plan(dims, TT0, 4096 / 46.6e3)
    plan = tree_plan(dims, TB, 4096 / 46.6e3)
    links = plan["links"]
    NL = len(links)
    peers = [(d, k) for d in range(3) for k in range(1, dims[d])]
    strides = (1, X, X * Y)

    def slot_of(offset):
        return offset[0] + X * offset[1] + X * Y * offset[2]

    def kernel(
        eps_ref, p_ref, c1_ref, c2_ref, t0_ref, q_ref,
        out_ref, loss_ref,
        land, kbuf, g0, tt, c1f, c1b, c2n, c2p, bacc, lp, lprecv, bp, qf, qrep, vbuf, cbuf,
        mb, sb, fb, ub, ap, xs, xr, mss, msr, pv, ars, arr, arps, arpr, obuf, orecv, trb,
        send_sem, recv_sem, credit, x_ssem, x_rsem, ms_sem, lp_sem, c1_sem, c2_sem, q_sem, ar_ssem, ar_rsem, arp_sem, o_sem,
    ):
        chip = lax.axis_index("rows")
        core = lax.axis_index("cols")
        other = 1 - core
        pos = (lax.rem(chip, X), lax.rem(lax.div(chip, X), Y), lax.div(chip, X * Y))

        def moved(d, k):
            return chip + (lax.rem(pos[d] + k + dims[d], dims[d]) - pos[d]) * strides[d]

        near = {link: moved(*link) for link in links}

        def source_of(slot):
            off = (lax.rem(slot, X), lax.rem(lax.div(slot, X), Y), lax.div(slot, X * Y))
            at = [lax.rem(pos[d] + dims[d] - off[d], dims[d]) for d in range(3)]
            return at[0] + X * at[1] + X * Y * at[2]

        def to_partner(src, dst, ssem, rsem):
            return pltpu.make_async_remote_copy(
                src_ref=src, dst_ref=dst, send_sem=ssem, recv_sem=rsem,
                device_id={"cols": other}, device_id_type=MESH,
            )

        def tree_copy(buf, width, m):
            n = m["hi"] - m["lo"]
            return pltpu.make_async_remote_copy(
                src_ref=buf.at[pl.ds(slot_of(m["src"]) * width + m["lo"], n)],
                dst_ref=buf.at[pl.ds(slot_of(m["dst"]) * width + m["lo"], n)],
                send_sem=send_sem.at[links.index(m["link"])],
                recv_sem=recv_sem.at[m["id"]],
                device_id={"rows": near[m["link"]]},
                device_id_type=MESH,
            )

        def tree(buf, width, the_plan, before_send=None, on_slot=None, fillers=()):
            fillers, ready, sends = list(fillers), [], 0
            for op, m in the_plan["ops"]:
                if op == "send":
                    if before_send is not None:
                        before_send(m)
                    tree_copy(buf, width, m).start()
                elif op == "wait":
                    tree_copy(buf, width, m).wait_recv()
                    sends += 1
                    if ready:
                        on_slot(ready.pop(0))
                    elif fillers and sends >= fillers[0][0]:
                        fillers.pop(0)[1]()
                elif on_slot is not None:
                    ready.append(slot_of(m))
            for s in ready:
                on_slot(s)
            for _, f in fillers:
                f()

        def tree_sent(buf, the_plan):
            for k, link in enumerate(links):
                n = the_plan["totals"][link]
                ref = buf.at[pl.ds(0, n)]
                pltpu.make_async_copy(ref, ref, send_sem.at[k]).wait()

        def give_credit():
            for d, sign in links:
                pl.semaphore_signal(credit, inc=1, device_id={"rows": moved(d, -sign)}, device_id_type=MESH)

        def all_sum_send(use, stage):
            for n, k in enumerate(range(1, dims[stage])):
                pltpu.make_async_remote_copy(
                    src_ref=ars.at[use, stage], dst_ref=arr.at[use, stage, n],
                    send_sem=ar_ssem.at[use, stage, n], recv_sem=ar_rsem.at[use, stage, n],
                    device_id={"rows": moved(stage, k)}, device_id_type=MESH,
                ).start()

        def all_sum_get(use, stage):
            total = ars[use, stage]
            for n, k in enumerate(range(1, dims[stage])):
                pltpu.make_async_remote_copy(
                    src_ref=ars.at[use, stage], dst_ref=arr.at[use, stage, n],
                    send_sem=ar_ssem.at[use, stage, n], recv_sem=ar_rsem.at[use, stage, n],
                    device_id={"rows": moved(stage, k)}, device_id_type=MESH,
                ).wait()
                total = total + arr[use, stage, n]
            return total

        def all_sum_step(use, stage):
            total = all_sum_get(use, stage)
            if stage < 2:
                ars[use, stage + 1] = total
                all_sum_send(use, stage + 1)
            else:
                arps[use] = total
                to_partner(arps.at[use], arpr.at[use], arp_sem.at[use, 0], arp_sem.at[use, 1]).start()

        barrier = pltpu.get_barrier_semaphore()
        for d, k in peers:
            pl.semaphore_signal(barrier, inc=1, device_id={"rows": moved(d, k)}, device_id_type=MESH)
        pl.semaphore_signal(barrier, inc=1, device_id={"cols": other}, device_id_type=MESH)

        row = lax.broadcasted_iota(jnp.int32, (8, 128), 0)
        lane = lax.broadcasted_iota(jnp.int32, (8, 128), 1)

        for g in range(G):
            rows = slice(g * 8, g * 8 + 8)
            pair = jnp.concatenate([c1_ref[rows, :128], c1_ref[rows, 128:]], axis=0)
            g0[NT0 + core * G + g] = pair.astype(BF16)
        c1_copy = to_partner(
            g0.at[pl.ds(NT0 + core * G, G)], g0.at[pl.ds(NT0 + core * G, G)], c1_sem.at[0], c1_sem.at[1]
        )
        q_copy = to_partner(q_ref, qf.at[pl.ds(core * HB, HB)], q_sem.at[0], q_sem.at[1])

        tile = jnp.zeros((8, 128), F32)
        for t in range(2):
            part = jnp.zeros((1, 128), F32)
            for k in range(NR):
                entry = c1_ref[k : k + 1, t * 128 : t * 128 + 128]
                part = part + entry * entry * p_ref[k]
            tile = jnp.where(row == 2 * core + t, jnp.broadcast_to(part, (8, 128)), tile)
        where = (row - 4) * 128 + lane
        for k in range(NR):
            tile = jnp.where(where == chip * NR + k, p_ref[k], tile)
        ars[0, 0] = tile
        for g in range(G):
            rows = slice(g * 8, g * 8 + 8)
            for t in range(JW):
                a, b = t0_ref[rows, 256 * t : 256 * t + 128], t0_ref[rows, 256 * t + 128 : 256 * t + 256]
                g0[g * JW + t] = jnp.concatenate([a, b], axis=0).astype(BF16)
        qf[pl.ds(core * HB, HB)] = q_ref[...]

        pl.semaphore_wait(barrier, len(peers) + 1)
        give_credit()
        c1_copy.start()
        q_copy.start()
        all_sum_send(0, 0)

        c2_copy = to_partner(c2n.at[pl.ds(core * HB, HB)], c2n.at[pl.ds(core * HB, HB)], c2_sem.at[0], c2_sem.at[1])
        bp[...] = jnp.zeros_like(bp)

        def round_c2(first, last):
            for t in range(first, last):
                blk = c2_ref[:, t * 128 : t * 128 + 128]
                c2n[core * HB + t] = blk.astype(BF16)
                bp[...] += blk * blk * q_ref[t : t + 1, :]

        def finish_b():
            bp[...] = jnp.broadcast_to(jnp.sum(bp[...], axis=1, keepdims=True), (128, 128))

        src = lax.broadcasted_iota(jnp.int32, (128, 128), 0)
        dst = lax.broadcasted_iota(jnp.int32, (128, 128), 1)
        picks = [
            jnp.where((src - core * JB == dst - h * JB) & (dst >= h * JB) & (dst < h * JB + JB), 1.0, 0.0).astype(BF16)
            for h in range(2)
        ]

        def order_c2(first, last):
            for t in range(first, last):
                a = jnp.dot(c2n[source_of(2 * t)], picks[0], preferred_element_type=F32)
                b = jnp.dot(c2n[source_of(2 * t + 1)], picks[1], preferred_element_type=F32)
                c2p[:, t * 128 : t * 128 + 128] = (a + b).astype(BF16)

        def order_q(first, last):
            def one(s, carry):
                line = jnp.broadcast_to(qf[pl.ds(source_of(s), 1), :], (8, 128))
                for jt in range(JT):
                    own = jnp.where(lane == core * JB + jt * 8 + row, line, 0.0)
                    qrep[s, jt] = jnp.broadcast_to(jnp.sum(own, axis=1, keepdims=True), (8, 128))
                return carry

            lax.fori_loop(first, last, one, 0)

        def span(n, parts, f):
            cuts = [n * k // parts for k in range(parts + 1)]
            return [lambda a=a, b=b: f(a, b) for a, b in zip(cuts, cuts[1:])]

        fillers = span(HB, 8, round_c2)
        fillers += [finish_b, lambda: c2_copy.start(), lambda: all_sum_step(0, 0)]
        fillers += [lambda: q_copy.wait()] + span(CH, 8, order_q)
        fillers += [lambda: all_sum_step(0, 1), lambda: c2_copy.wait()] + span(CH // 2, 16, order_c2)
        fillers += [lambda: all_sum_step(0, 2)]
        waited = []

        def before_send(m):
            if not waited and m["hi"] > NT0:
                waited.append(1)
                c1_copy.wait()

        tree(g0, TT0, plan0, before_send=before_send, fillers=[(0, f) for f in fillers])
        tree_sent(g0, plan0)
        to_partner(arps.at[0], arpr.at[0], arp_sem.at[0, 0], arp_sem.at[0, 1]).wait()
        ap[...] = jnp.where(row < 4, arps[0] + arpr[0], arps[0])
        for t in range(NT):
            pv[t] = jnp.broadcast_to(ap[4 + t : 5 + t, :], (8, 128))

        def unpack(s, carry):
            chip_s = source_of(s)
            for g in range(G):
                for t in range(JW):
                    pair = g0[s * TT0 + g * JW + t].astype(F32)
                    kbuf[(chip_s * G + g) * JN + 2 * t] = pair[:8]
                    kbuf[(chip_s * G + g) * JN + 2 * t + 1] = pair[8:]
                for h in range(2):
                    pair = g0[s * TT0 + NT0 + h * G + g].astype(F32)
                    at = pl.ds(pl.multiple_of(chip_s * NR + g * 8, 8), 8)
                    c1f[at, 256 * h : 256 * h + 128] = pair[:8]
                    c1f[at, 256 * h + 128 : 256 * h + 256] = pair[8:]
            return carry

        lax.fori_loop(0, CH, unpack, 0)
        c1b[...] = c1f[...].astype(BF16)

        def finish_lp():
            lp[...] = jnp.concatenate([bp[...]] * NT, axis=1) - 2.0 * bacc[...]

        bacc[...] = jnp.zeros_like(bacc)
        JC = CK // 128

        def first_chunk(n, carry):
            cols = []
            for t in range(JC):
                tiles = [kbuf[g * JN + n * JC + t] for g in range(CH * G)]
                cols.append(jnp.concatenate(tiles, axis=0))
            plan_c = jnp.concatenate(cols, axis=1).astype(BF16)
            lead = jnp.dot(c1b[...], plan_c, preferred_element_type=F32).astype(BF16)
            c2c = jnp.concatenate([c2n[core * HB + n * JC + t] for t in range(JC)], axis=1)
            bacc[...] += lax.dot_general(c2c, lead, (((1,), (1,)), ((), ())), preferred_element_type=F32)
            return carry

        lax.fori_loop(0, KJ // CK, first_chunk, 0)
        finish_lp()

        def chunk(n, carry):
            at = pl.ds(pl.multiple_of(n * CK, CK), CK)
            lead = jnp.dot(tt[at, :], c1b[...], preferred_element_type=F32).astype(BF16)
            bacc[...] += jnp.dot(c2p[:, at], lead, preferred_element_type=F32)
            return carry

        def costs():
            copy = to_partner(lp.at[pl.ds(other * JB, JB)], lprecv, lp_sem.at[0], lp_sem.at[1])
            copy.start()
            copy.wait()
            own = lp[pl.ds(pl.multiple_of(core * JB, JB), JB), :] + lprecv[...]
            return own + jnp.concatenate([ap[t : t + 1, :] for t in range(NT)], axis=1)

        def block(s):
            return kbuf[pl.ds(s * TB, TB)].reshape(JT, NT, 8, 128)

        def weighted(kk, u):
            w = (kk[:, 0] * u[0] + kk[:, 1] * u[1]) + (kk[:, 2] * u[2] + kk[:, 3] * u[3])
            return jnp.sum(w, axis=2, keepdims=True)

        def passes(u, rescale=False, last=False):
            def one(g, buf):
                for k in range(GS):
                    s = g * GS + k
                    kk = block(s)
                    if rescale:
                        kk = kk * fb[:, pl.ds(s, 1), :][None]
                        kbuf[pl.ds(s * TB, TB)] = kk.reshape(TB, 8, 128)
                    cbuf[buf, k] = qrep[s] / jnp.broadcast_to(weighted(kk, u), (JT, 8, 128))

            def two(g, buf, acc):
                for k in range(GS):
                    s = g * GS + k
                    v = cbuf[buf, k]
                    kk = block(s)
                    if last:
                        vbuf[s] = v
                        t = (kk * u[None]) * v[:, None]
                        flat = jnp.concatenate([t[:, i].reshape(JB, 128) for i in range(NT)], axis=1)
                        tt[pl.ds(pl.multiple_of(s * JB, JB), JB), :] = flat.astype(BF16)
                    else:
                        acc = acc + jnp.sum(kk * v[:, None], axis=0)
                return acc

            def both(n, acc):
                one(2 * n + 1, 1)
                acc = two(2 * n, 0, acc)
                one(2 * n + 2, 0)
                return two(2 * n + 1, 1, acc)

            one(0, 0)
            acc = lax.fori_loop(0, (NG - 1) // 2, both, jnp.zeros((NT, 8, 128), F32))
            if NG % 2 == 0:
                one(NG - 1, 1)
                acc = two(NG - 2, 0, acc)
            return two(NG - 1, (NG - 1) % 2, acc)

        def row_scale(acc, par):
            xs[par] = acc
            copy = to_partner(xs.at[par], xr.at[par], x_ssem.at[par], x_rsem.at[par])
            copy.start()
            copy.wait()
            total = jnp.sum(acc + xr[par], axis=1, keepdims=True)
            return pv[...] / jnp.broadcast_to(total, (NT, 8, 128))

        def outer(r, carry):
            scale = 1.4426950408889634 / eps_ref[r]
            cost = costs()
            for jt in range(JT):
                for t in range(NT):
                    land[jt * NT + t] = cost[jt * 8 : jt * 8 + 8, t * 128 : t * 128 + 128]

            def exps(s):
                ll = land[s * TB : s * TB + TB].reshape(JT, NT, 8, 128)
                low = jnp.min(jnp.min(ll, axis=0), axis=1, keepdims=True)
                kk = jnp.exp2((low[None] - ll) * scale)
                kbuf[s * TB : s * TB + TB] = kk.reshape(TB, 8, 128)
                mb[:, s : s + 1, :] = low
                sb[:, s : s + 1, :] = jnp.sum(jnp.sum(kk, axis=0), axis=1, keepdims=True)

            pl.semaphore_wait(credit, NL)
            tree(land, TB, plan, on_slot=exps, fillers=[(0, lambda: exps(0))])
            tree_sent(land, plan)
            give_credit()

            low = jnp.min(mb[...], axis=1, keepdims=True)
            part = jnp.sum(sb[...] * jnp.exp2((low - mb[...]) * scale), axis=1, keepdims=True)
            mss[0] = jnp.broadcast_to(low, (NT, 8, 128))
            mss[1] = jnp.broadcast_to(part, (NT, 8, 128))
            copy = to_partner(mss, msr, ms_sem.at[0], ms_sem.at[1])
            copy.start()
            copy.wait()
            least = jnp.minimum(mss[0], msr[0])
            total = mss[1] * jnp.exp2((least - mss[0]) * scale) + msr[1] * jnp.exp2((least - msr[0]) * scale)
            fb[...] = jnp.exp2((least[:, :1] - mb[...]) * scale)
            u = pv[...] / total

            u = row_scale(passes(u, rescale=True), 1)

            def sweep(t, u):
                return row_scale(passes(u), lax.rem(t, 2))

            u = lax.fori_loop(2, sweeps, sweep, u)
            passes(u, last=True)
            ub[...] = u
            bacc[...] = jnp.zeros_like(bacc)
            lax.fori_loop(0, KJ // CK, chunk, 0)
            finish_lp()
            return carry

        lax.fori_loop(0, steps, outer, 0)

        pl.semaphore_wait(credit, NL)
        cost = costs()
        plan_own = (block(0) * ub[...][None]) * vbuf[0][:, None]
        total = jnp.zeros((8, 128), F32)
        for jt in range(JT):
            for t in range(NT):
                total = total + cost[jt * 8 : jt * 8 + 8, t * 128 : t * 128 + 128] * plan_own[jt, t]
        ars[1, 0] = total
        all_sum_send(1, 0)

        it = lax.div(chip * NR, 128)
        inside = pl.multiple_of(lax.rem(chip * NR, 128), 8)

        def rows_of(s, carry):
            kk = jnp.concatenate([kbuf[s * TB + jt * NT + it] for jt in range(JT)], axis=0)
            uu = jnp.concatenate([ub[it]] * JT, axis=0)
            t = (kk * uu) * vbuf[s].reshape(JB, 128)
            none = jnp.zeros_like(t)
            both = jnp.where(core == 0, jnp.concatenate([t, none], axis=0), jnp.concatenate([none, t], axis=0))
            trb[...] = both.T
            obuf[source_of(s)] = trb[pl.ds(inside, NR), :]
            return carry

        lax.fori_loop(0, CH, rows_of, 0)
        o_copy = to_partner(obuf.at[pl.ds(other * HB, HB)], orecv, o_sem.at[0], o_sem.at[1])
        o_copy.start()
        all_sum_step(1, 0)
        o_copy.wait()
        for b in range(HB):
            out_ref[:, b * 128 : b * 128 + 128] = obuf[core * HB + b] + orecv[b]
        all_sum_step(1, 1)
        all_sum_step(1, 2)
        to_partner(arps.at[1], arpr.at[1], arp_sem.at[1, 0], arp_sem.at[1, 1]).wait()
        loss_ref[0] = jnp.sum(arps[1] + arpr[1])

    vm = pltpu.VMEM
    dma = pltpu.SemaphoreType.DMA
    scratch = [
        vm((CH * TB, 8, 128), F32),
        vm((CH * TB, 8, 128), F32),
        vm((CH * TT0, 16, 128), BF16),
        vm((KJ, n_rows), BF16),
        vm((n_rows, n_rows), F32),
        vm((n_rows, n_rows), BF16),
        vm((CH, 128, 128), BF16),
        vm((128, KJ), BF16),
        vm((128, n_rows), F32),
        vm((128, n_rows), F32),
        vm((JB, n_rows), F32),
        vm((128, 128), F32),
        vm((CH, 128), F32),
        vm((CH, JT, 8, 128), F32),
        vm((CH, JT, 8, 128), F32),
        vm((2, GS, JT, 8, 128), F32),
        vm((NT, CH, 128), F32),
        vm((NT, CH, 128), F32),
        vm((NT, CH, 128), F32),
        vm((NT, 8, 128), F32),
        vm((8, 128), F32),
        vm((2, NT, 8, 128), F32),
        vm((2, NT, 8, 128), F32),
        vm((2, NT, 8, 128), F32),
        vm((2, NT, 8, 128), F32),
        vm((NT, 8, 128), F32),
        vm((2, 3, 8, 128), F32),
        vm((2, 3, 3, 8, 128), F32),
        vm((2, 8, 128), F32),
        vm((2, 8, 128), F32),
        vm((CH, NR, 128), F32),
        vm((HB, NR, 128), F32),
        vm((128, 128), F32),
        dma((NL,)),
        dma((max(len(plan["msgs"]), len(plan0["msgs"])),)),
        pltpu.SemaphoreType.REGULAR,
        dma((2,)),
        dma((2,)),
        dma((2,)),
        dma((2,)),
        dma((2,)),
        dma((2,)),
        dma((2,)),
        dma((2, 3, 3)),
        dma((2, 3, 3)),
        dma((2, 2)),
        dma((2,)),
    ]
    return kernel, scratch


def solution(mesh):
    chips = mesh.shape["rows"]
    dims = torus_of(chips)
    grid_spec = P(("pairs", "rows"), "cols")

    def local_fn(c1, c2, t0, p, q, eps):
        n_rows, n_cols = p.shape[0] * chips, q.shape[0] * mesh.shape["cols"]
        kernel, scratch = make_kernel(dims, n_rows, n_cols, eps.shape[0], SWEEPS)
        vmem = pl.BlockSpec(memory_space=pltpu.VMEM)
        smem = pl.BlockSpec(memory_space=pltpu.SMEM)
        return pl.pallas_call(
            kernel,
            name="gromov",
            out_shape=(jax.ShapeDtypeStruct(t0.shape, F32), jax.ShapeDtypeStruct((1,), F32)),
            in_specs=[smem, smem, vmem, vmem, vmem, vmem],
            out_specs=(vmem, smem),
            scratch_shapes=scratch,
            compiler_params=pltpu.CompilerParams(
                collective_id=0, has_side_effects=True, vmem_limit_bytes=60 * 1024 * 1024
            ),
        )(eps, p, c1, c2, t0, q.reshape(chips // 2, 128))

    return jax.shard_map(
        local_fn,
        mesh=mesh,
        in_specs=(grid_spec, grid_spec, grid_spec, P(("pairs", "rows")), P(("pairs", "cols")), P("pairs")),
        out_specs=(grid_spec, P("pairs")),
        check_vma=False,
    )
```

```python
import heapq
import itertools
import math

import jax
import jax.numpy as jnp
from jax import lax
from jax.experimental import pallas as pl
from jax.experimental.pallas import tpu as pltpu
from jax.sharding import PartitionSpec as P

SWEEPS = 10
MESH = pl.DeviceIdType.MESH
L, S = 128, 8
JB = 64
JT = JB // S
F32, BF16 = jnp.float32, jnp.bfloat16
ORDERS = ((0, 1, 2), (1, 2, 0), (2, 0, 1))
TILE_RATE = 11.4
HOP_US = 2.6
AHEAD_US = 1.0
LATE = 100


def torus_of(chips):
    return {64: (4, 4, 4), S: (4, 2, 1), 16: (4, 4, 1)}[chips]


def split3(n):
    cuts = [0, (n + 2) // 3, (2 * n + 2) // 3, n]
    return [(cuts[k], cuts[k + 1]) for k in range(3)]


def tree_plan(dims, tiles, rate, lat_us, ahead_us):
    rings = {1: (), 2: ((1, "f", 1),), 4: ((1, "f", 1), (3, "f", -1), (2, "a", 1), (2, "b", -1))}
    msgs = []
    for color, order in enumerate(ORDERS):
        lo, hi = split3(tiles)[color]
        for dst in itertools.product(*(range(n) for n in dims)):
            used = [k for k in range(3) if dst[order[k]]]
            if not used or lo == hi:
                continue
            d = order[used[-1]]
            mid = lo + (hi - lo + (sum(dst) + color) % 2) // 2
            for at, part, sign in rings[dims[d]]:
                a, b = {"f": (lo, hi), "a": (lo, mid), "b": (mid, hi)}[part]
                if at != dst[d] or a == b:
                    continue
                src = list(dst)
                src[d] = (src[d] - sign) % dims[d]
                m = dict(id=len(msgs), color=color, src=tuple(src), dst=dst, link=(d, sign), lo=a, hi=b)
                m["us"] = (b - a) / rate
                msgs.append(m)
    into = {}
    for m in msgs:
        into.setdefault((m["color"], m["dst"]), []).append(m)
    users = [[] for _ in msgs]
    missing = []
    for m in msgs:
        deps = [e for e in into.get((m["color"], m["src"]), []) if e["lo"] < m["hi"] and m["lo"] < e["hi"]]
        missing.append(len(deps))
        for e in deps:
            users[e["id"]].append(m)
    way = {}

    def way_of(m):
        if m["id"] not in way:
            way[m["id"]] = m["us"] + lat_us + max([way_of(u) for u in users[m["id"]]], default=0.0)
        return way[m["id"]]

    links = sorted({m["link"] for m in msgs})
    queue = {k: [] for k in links}
    idle = dict.fromkeys(links, True)
    ready, events, ops = {}, [], []

    def put(m, now):
        ready[m["id"]] = now
        heapq.heappush(queue[m["link"]], (-way_of(m), m["id"]))

    def start(link, now):
        if idle[link] and queue[link]:
            k = heapq.heappop(queue[link])[1]
            idle[link] = False
            ops.append((max(ready[k], now - ahead_us), 1, "send", msgs[k]))
            heapq.heappush(events, (now + msgs[k]["us"], 0, k))
            heapq.heappush(events, (now + msgs[k]["us"] + lat_us, 1, k))

    for m in msgs:
        if not missing[m["id"]]:
            put(m, 0.0)
    for link in links:
        start(link, 0.0)
    left = {}
    for m in msgs:
        left[m["dst"]] = left.get(m["dst"], 0) + 1
    now = 0.0
    while events:
        now, arrived, k = heapq.heappop(events)
        m = msgs[k]
        if not arrived:
            idle[m["link"]] = True
            start(m["link"], now)
            continue
        ops.append((now, 0, "wait", m))
        for u in users[k]:
            missing[u["id"]] -= 1
            if not missing[u["id"]]:
                put(u, now)
                start(u["link"], now)
        left[m["dst"]] -= 1
        if not left[m["dst"]]:
            ops.append((now, 0, "slot", m["dst"]))
    ops.sort(key=lambda op: op[:2])
    totals = {k: sum(m["hi"] - m["lo"] for m in msgs if m["link"] == k) for k in links}
    return dict(msgs=msgs, ops=[op[2:] for op in ops], links=links, totals=totals, end=now)


def make_kernel(dims, n_rows, n_cols, steps, sweeps):
    X, Y, Z = dims
    CH = X * Y * Z
    NR = n_rows // CH
    G = NR // S
    NT = n_rows // L
    TB = JT * NT
    HB = CH // 2
    JN = n_cols // 2 // L
    JW = JN // 2
    NT0 = G * JW
    TT0 = NT0 + 2 * G
    KJ = CH * JB
    CK = min(512, KJ)
    GS = min(4, CH // 2)
    NG = CH // GS
    assert NT == 4 and n_cols == CH * L and JN == HB
    plan0 = tree_plan(dims, TT0, TILE_RATE, HOP_US, AHEAD_US)
    plan = tree_plan(dims, TB, TILE_RATE, HOP_US, AHEAD_US)
    links = plan["links"]
    NL = len(links)
    peers = [(d, k) for d in range(3) for k in range(1, dims[d])]
    strides = (1, X, X * Y)

    def slot_of(offset):
        return offset[0] + X * offset[1] + X * Y * offset[2]

    def kernel(
        eps_ref, p_ref, c1_ref, c2_ref, t0_ref, q_ref,
        out_ref, loss_ref,
        land, kbuf, g0, tt, c1f, c1b, c2n, c2p, bacc, lp, lprecv, bp, qf, qrep, vbuf, cbuf,
        mb, sb, fb, ub, ap, xs, xr, mss, msr, pv, ars, arr, arps, arpr, obuf, orecv, trb,
        send_sem, recv_sem, credit, x_ssem, x_rsem, ms_sem, lp_sem, c1_sem, c2_sem, q_sem, ar_ssem, ar_rsem, arp_sem, o_sem,
    ):
        chip = lax.axis_index("rows")
        core = lax.axis_index("cols")
        other = 1 - core
        pos = (lax.rem(chip, X), lax.rem(lax.div(chip, X), Y), lax.div(chip, X * Y))

        def moved(d, k):
            return chip + (lax.rem(pos[d] + k + dims[d], dims[d]) - pos[d]) * strides[d]

        near = {link: moved(*link) for link in links}

        def source_of(slot):
            off = (lax.rem(slot, X), lax.rem(lax.div(slot, X), Y), lax.div(slot, X * Y))
            at = [lax.rem(pos[d] + dims[d] - off[d], dims[d]) for d in range(3)]
            return at[0] + X * at[1] + X * Y * at[2]

        def to_partner(src, dst, ssem, rsem):
            return pltpu.make_async_remote_copy(
                src_ref=src, dst_ref=dst, send_sem=ssem, recv_sem=rsem,
                device_id={"cols": other}, device_id_type=MESH,
            )

        def tree_copy(buf, width, m):
            n = m["hi"] - m["lo"]
            return pltpu.make_async_remote_copy(
                src_ref=buf.at[pl.ds(slot_of(m["src"]) * width + m["lo"], n)],
                dst_ref=buf.at[pl.ds(slot_of(m["dst"]) * width + m["lo"], n)],
                send_sem=send_sem.at[links.index(m["link"])],
                recv_sem=recv_sem.at[m["id"]],
                device_id={"rows": near[m["link"]]},
                device_id_type=MESH,
            )

        def tree(buf, width, the_plan, before_send=None, on_slot=None, fillers=()):
            fillers, ready, waits = list(fillers), [], 0
            for op, m in the_plan["ops"]:
                if op == "send":
                    if before_send is not None:
                        before_send(m)
                    tree_copy(buf, width, m).start()
                elif op == "wait":
                    while fillers and not fillers[0][0]:
                        fillers.pop(0)[1]()
                    tree_copy(buf, width, m).wait_recv()
                    waits += 1
                    if ready:
                        on_slot(ready.pop(0))
                    elif fillers and waits >= fillers[0][0]:
                        fillers.pop(0)[1]()
                elif on_slot is not None:
                    ready.append(slot_of(m))
            for s in ready:
                on_slot(s)
            for _, f in fillers:
                f()

        def tree_sent(buf, the_plan):
            for k, link in enumerate(links):
                n = the_plan["totals"][link]
                ref = buf.at[pl.ds(0, n)]
                pltpu.make_async_copy(ref, ref, send_sem.at[k]).wait()

        def give_credit():
            for d, sign in links:
                pl.semaphore_signal(credit, inc=1, device_id={"rows": moved(d, -sign)}, device_id_type=MESH)

        def all_sum_send(use, stage):
            for n, k in enumerate(range(1, dims[stage])):
                pltpu.make_async_remote_copy(
                    src_ref=ars.at[use, stage], dst_ref=arr.at[use, stage, n],
                    send_sem=ar_ssem.at[use, stage, n], recv_sem=ar_rsem.at[use, stage, n],
                    device_id={"rows": moved(stage, k)}, device_id_type=MESH,
                ).start()

        def all_sum_get(use, stage):
            total = ars[use, stage]
            for n, k in enumerate(range(1, dims[stage])):
                pltpu.make_async_remote_copy(
                    src_ref=ars.at[use, stage], dst_ref=arr.at[use, stage, n],
                    send_sem=ar_ssem.at[use, stage, n], recv_sem=ar_rsem.at[use, stage, n],
                    device_id={"rows": moved(stage, k)}, device_id_type=MESH,
                ).wait()
                total = total + arr[use, stage, n]
            return total

        def all_sum_step(use, stage):
            total = all_sum_get(use, stage)
            if stage < 2:
                ars[use, stage + 1] = total
                all_sum_send(use, stage + 1)
            else:
                arps[use] = total
                to_partner(arps.at[use], arpr.at[use], arp_sem.at[use, 0], arp_sem.at[use, 1]).start()

        barrier = pltpu.get_barrier_semaphore()
        for d, k in peers:
            pl.semaphore_signal(barrier, inc=1, device_id={"rows": moved(d, k)}, device_id_type=MESH)
        pl.semaphore_signal(barrier, inc=1, device_id={"cols": other}, device_id_type=MESH)

        row = lax.broadcasted_iota(jnp.int32, (S, L), 0)
        lane = lax.broadcasted_iota(jnp.int32, (S, L), 1)

        for g in range(G):
            rows = slice(g * S, g * S + S)
            pair = jnp.concatenate([c1_ref[rows, :L], c1_ref[rows, L:]], axis=0)
            g0[NT0 + core * G + g] = pair.astype(BF16)
        c1_copy = to_partner(
            g0.at[pl.ds(NT0 + core * G, G)], g0.at[pl.ds(NT0 + core * G, G)], c1_sem.at[0], c1_sem.at[1]
        )
        q_copy = to_partner(q_ref, qf.at[pl.ds(core * HB, HB)], q_sem.at[0], q_sem.at[1])

        tile = jnp.zeros((S, L), F32)
        for t in range(2):
            part = jnp.zeros((1, L), F32)
            for k in range(NR):
                entry = c1_ref[k : k + 1, t * L : t * L + L]
                part = part + entry * entry * p_ref[k]
            tile = jnp.where(row == 2 * core + t, jnp.broadcast_to(part, (S, L)), tile)
        where = (row - 4) * L + lane
        for k in range(NR):
            tile = jnp.where(where == chip * NR + k, p_ref[k], tile)
        ars[0, 0] = tile
        for g in range(G):
            rows = slice(g * S, g * S + S)
            for t in range(JW):
                a, b = t0_ref[rows, (2 * L) * t : (2 * L) * t + L], t0_ref[rows, (2 * L) * t + L : (2 * L) * t + (2 * L)]
                g0[g * JW + t] = jnp.concatenate([a, b], axis=0).astype(BF16)
        qf[pl.ds(core * HB, HB)] = q_ref[...]

        with jax.named_scope("barrier"):
            pl.semaphore_wait(barrier, len(peers) + 1)
        give_credit()
        c1_copy.start()
        q_copy.start()
        all_sum_send(0, 0)

        c2_copy = to_partner(c2n.at[pl.ds(core * HB, HB)], c2n.at[pl.ds(core * HB, HB)], c2_sem.at[0], c2_sem.at[1])
        bp[...] = jnp.zeros_like(bp)

        def round_c2(first, last):
            for t in range(first, last):
                blk = c2_ref[:, t * L : t * L + L]
                c2n[core * HB + t] = blk.astype(BF16)
                bp[...] += blk * blk * q_ref[t : t + 1, :]

        def finish_b():
            bp[...] = jnp.broadcast_to(jnp.sum(bp[...], axis=1, keepdims=True), (L, L))

        src = lax.broadcasted_iota(jnp.int32, (L, L), 0)
        dst = lax.broadcasted_iota(jnp.int32, (L, L), 1)
        picks = [
            jnp.where((src - core * JB == dst - h * JB) & (dst >= h * JB) & (dst < h * JB + JB), 1.0, 0.0).astype(BF16)
            for h in range(2)
        ]

        def order_c2(first, last):
            for t in range(first, last):
                a = jnp.dot(c2n[source_of(2 * t)], picks[0], preferred_element_type=F32)
                b = jnp.dot(c2n[source_of(2 * t + 1)], picks[1], preferred_element_type=F32)
                c2p[:, t * L : t * L + L] = (a + b).astype(BF16)

        def order_q(first, last):
            def one(s, carry):
                line = jnp.broadcast_to(qf[pl.ds(source_of(s), 1), :], (S, L))
                for jt in range(JT):
                    own = jnp.where(lane == core * JB + jt * S + row, line, 0.0)
                    qrep[s, jt] = jnp.broadcast_to(jnp.sum(own, axis=1, keepdims=True), (S, L))
                return carry

            lax.fori_loop(first, last, one, 0)

        def span(n, parts, f):
            cuts = [n * k // parts for k in range(parts + 1)]
            return [lambda a=a, b=b: f(a, b) for a, b in zip(cuts, cuts[1:])]

        now = [*span(HB, S, round_c2), finish_b, lambda: c2_copy.start()]
        fillers = [(0, f) for f in now] + [(len(now), lambda: q_copy.wait())]
        fillers += [(2 * JB // 4 + 4 * n, f) for n, f in enumerate(span(CH, 2 * S, order_q))]
        fillers += [(LATE - 1, lambda: all_sum_step(0, 0)), (LATE, lambda: c2_copy.wait())]
        fillers += [(LATE + 4 * n, f) for n, f in enumerate(span(CH // 2, 2 * S, order_c2))]
        fillers += [(LATE + JB, lambda: all_sum_step(0, 1))]
        waited = []

        def before_send(m):
            if not waited and m["hi"] > NT0:
                waited.append(1)
                c1_copy.wait()

        with jax.named_scope("gather0"):
            tree(g0, TT0, plan0, before_send=before_send, fillers=fillers)
            tree_sent(g0, plan0)
        def unpack(s, carry):
            chip_s = source_of(s)
            for g in range(G):
                for t in range(JW):
                    pair = g0[s * TT0 + g * JW + t].astype(F32)
                    kbuf[(chip_s * G + g) * JN + 2 * t] = pair[:S]
                    kbuf[(chip_s * G + g) * JN + 2 * t + 1] = pair[S:]
                for h in range(2):
                    pair = g0[s * TT0 + NT0 + h * G + g].astype(F32)
                    at = pl.ds(pl.multiple_of(chip_s * NR + g * S, S), S)
                    c1f[at, (2 * L) * h : (2 * L) * h + L] = pair[:S]
                    c1f[at, (2 * L) * h + L : (2 * L) * h + (2 * L)] = pair[S:]
            return carry

        with jax.named_scope("unpack"):
            lax.fori_loop(0, CH, unpack, 0)
            c1b[...] = c1f[...].astype(BF16)
            all_sum_step(0, 2)

        def finish_lp():
            lp[...] = jnp.concatenate([bp[...]] * NT, axis=1) - 2.0 * bacc[...]

        bacc[...] = jnp.zeros_like(bacc)
        JC = CK // L

        def first_chunk(n, carry):
            cols = []
            for t in range(JC):
                tiles = [kbuf[g * JN + n * JC + t] for g in range(CH * G)]
                cols.append(jnp.concatenate(tiles, axis=0))
            plan_c = jnp.concatenate(cols, axis=1).astype(BF16)
            lead = jnp.dot(c1b[...], plan_c, preferred_element_type=F32).astype(BF16)
            c2c = jnp.concatenate([c2n[core * HB + n * JC + t] for t in range(JC)], axis=1)
            bacc[...] += lax.dot_general(c2c, lead, (((1,), (1,)), ((), ())), preferred_element_type=F32)
            return carry

        with jax.named_scope("firstmm"):
            lax.fori_loop(0, KJ // CK, first_chunk, 0)
            finish_lp()
        to_partner(arps.at[0], arpr.at[0], arp_sem.at[0, 0], arp_sem.at[0, 1]).wait()
        ap[...] = jnp.where(row < 4, arps[0] + arpr[0], arps[0])
        for t in range(NT):
            pv[t] = jnp.broadcast_to(ap[4 + t : 5 + t, :], (S, L))


        def chunk(n, carry):
            at = pl.ds(pl.multiple_of(n * CK, CK), CK)
            lead = jnp.dot(tt[at, :], c1b[...], preferred_element_type=F32).astype(BF16)
            bacc[...] += jnp.dot(c2p[:, at], lead, preferred_element_type=F32)
            return carry

        def costs():
            copy = to_partner(lp.at[pl.ds(other * JB, JB)], lprecv, lp_sem.at[0], lp_sem.at[1])
            copy.start()
            copy.wait()
            own = lp[pl.ds(pl.multiple_of(core * JB, JB), JB), :] + lprecv[...]
            return own + jnp.concatenate([ap[t : t + 1, :] for t in range(NT)], axis=1)

        def block(s):
            return kbuf[pl.ds(s * TB, TB)].reshape(JT, NT, S, L)

        def weighted(kk, u):
            w = (kk[:, 0] * u[0] + kk[:, 1] * u[1]) + (kk[:, 2] * u[2] + kk[:, 3] * u[3])
            return jnp.sum(w, axis=2, keepdims=True)

        def passes(u, rescale=False, last=False):
            def one(g, buf):
                for k in range(GS):
                    s = g * GS + k
                    kk = block(s)
                    if rescale:
                        kk = kk * fb[:, pl.ds(s, 1), :][None]
                        kbuf[pl.ds(s * TB, TB)] = kk.reshape(TB, S, L)
                    cbuf[buf, k] = qrep[s] / jnp.broadcast_to(weighted(kk, u), (JT, S, L))

            def two(g, buf, acc):
                for k in range(GS):
                    s = g * GS + k
                    v = cbuf[buf, k]
                    kk = block(s)
                    if last:
                        vbuf[s] = v
                        t = (kk * u[None]) * v[:, None]
                        flat = jnp.concatenate([t[:, i].reshape(JB, L) for i in range(NT)], axis=1)
                        tt[pl.ds(pl.multiple_of(s * JB, JB), JB), :] = flat.astype(BF16)
                    else:
                        acc = acc + jnp.sum(kk * v[:, None], axis=0)
                return acc

            def both(n, acc):
                one(2 * n + 1, 1)
                acc = two(2 * n, 0, acc)
                one(2 * n + 2, 0)
                return two(2 * n + 1, 1, acc)

            one(0, 0)
            acc = lax.fori_loop(0, (NG - 1) // 2, both, jnp.zeros((NT, S, L), F32))
            if NG % 2 == 0:
                one(NG - 1, 1)
                acc = two(NG - 2, 0, acc)
            return two(NG - 1, (NG - 1) % 2, acc)

        def row_scale(acc, par):
            xs[par] = acc
            copy = to_partner(xs.at[par], xr.at[par], x_ssem.at[par], x_rsem.at[par])
            copy.start()
            copy.wait()
            total = jnp.sum(acc + xr[par], axis=1, keepdims=True)
            return pv[...] / jnp.broadcast_to(total, (NT, S, L))

        def outer(r, carry):
            scale = 1.4426950408889634 / eps_ref[r]
            cost = costs()
            for jt in range(JT):
                for t in range(NT):
                    land[jt * NT + t] = cost[jt * S : jt * S + S, t * L : t * L + L]

            def exps(s):
                ll = land[s * TB : s * TB + TB].reshape(JT, NT, S, L)
                low = jnp.min(jnp.min(ll, axis=0), axis=1, keepdims=True)
                kk = jnp.exp2((low[None] - ll) * scale)
                kbuf[s * TB : s * TB + TB] = kk.reshape(TB, S, L)
                mb[:, s : s + 1, :] = low
                sb[:, s : s + 1, :] = jnp.sum(jnp.sum(kk, axis=0), axis=1, keepdims=True)

            with jax.named_scope("gather"):
                pl.semaphore_wait(credit, NL)
                tree(land, TB, plan, on_slot=exps, fillers=[(0, lambda: exps(0))])
                tree_sent(land, plan)
                give_credit()

            with jax.named_scope("minx"):
                low = jnp.min(mb[...], axis=1, keepdims=True)
                part = jnp.sum(sb[...] * jnp.exp2((low - mb[...]) * scale), axis=1, keepdims=True)
                mss[0] = jnp.broadcast_to(low, (NT, S, L))
                mss[1] = jnp.broadcast_to(part, (NT, S, L))
                copy = to_partner(mss, msr, ms_sem.at[0], ms_sem.at[1])
                copy.start()
                copy.wait()
                least = jnp.minimum(mss[0], msr[0])
                total = mss[1] * jnp.exp2((least - mss[0]) * scale) + msr[1] * jnp.exp2((least - msr[0]) * scale)
                fb[...] = jnp.exp2((least[:, :1] - mb[...]) * scale)
                u = pv[...] / total

            with jax.named_scope("pass1"):
                u = row_scale(passes(u, rescale=True), 1)

            def sweep(t, u):
                return row_scale(passes(u), lax.rem(t, 2))

            with jax.named_scope("sweeps"):
                u = lax.fori_loop(2, sweeps, sweep, u)
            with jax.named_scope("lastpass"):
                passes(u, last=True)
            ub[...] = u
            bacc[...] = jnp.zeros_like(bacc)
            with jax.named_scope("mm"):
                lax.fori_loop(0, KJ // CK, chunk, 0)
                finish_lp()
            return carry

        lax.fori_loop(0, steps, outer, 0)

        pl.semaphore_wait(credit, NL)
        cost = costs()
        plan_own = (block(0) * ub[...][None]) * vbuf[0][:, None]
        total = jnp.zeros((S, L), F32)
        for jt in range(JT):
            for t in range(NT):
                total = total + cost[jt * S : jt * S + S, t * L : t * L + L] * plan_own[jt, t]
        ars[1, 0] = total
        all_sum_send(1, 0)

        it = lax.div(chip * NR, L)
        inside = pl.multiple_of(lax.rem(chip * NR, L), S)

        def rows_of(n, carry):
            for k in range(4):
                s = 4 * n + k
                kk = jnp.concatenate([kbuf[s * TB + jt * NT + it] for jt in range(JT)], axis=0)
                uu = jnp.concatenate([ub[it]] * JT, axis=0)
                t = (kk * uu) * vbuf[s].reshape(JB, L)
                none = jnp.zeros_like(t)
                both = jnp.where(core == 0, jnp.concatenate([t, none], axis=0), jnp.concatenate([none, t], axis=0))
                trb[k] = both.T
                obuf[source_of(s)] = trb[k, pl.ds(inside, NR), :]
            return carry

        with jax.named_scope("tail"):
            lax.fori_loop(0, CH // 8, rows_of, 0)
            all_sum_step(1, 0)
            lax.fori_loop(CH // 8, CH // 4, rows_of, 0)
            o_copy = to_partner(obuf.at[pl.ds(other * HB, HB)], orecv, o_sem.at[0], o_sem.at[1])
            o_copy.start()
            all_sum_step(1, 1)
            o_copy.wait()
            for b in range(HB):
                out_ref[:, b * L : b * L + L] = obuf[core * HB + b] + orecv[b]
            all_sum_step(1, 2)
            to_partner(arps.at[1], arpr.at[1], arp_sem.at[1, 0], arp_sem.at[1, 1]).wait()
        loss_ref[0] = jnp.sum(arps[1] + arpr[1])

    vm = pltpu.VMEM
    dma = pltpu.SemaphoreType.DMA
    scratch = [
        vm((CH * TB, S, L), F32),
        vm((CH * TB, S, L), F32),
        vm((CH * TT0, 16, L), BF16),
        vm((KJ, n_rows), BF16),
        vm((n_rows, n_rows), F32),
        vm((n_rows, n_rows), BF16),
        vm((CH, L, L), BF16),
        vm((L, KJ), BF16),
        vm((L, n_rows), F32),
        vm((L, n_rows), F32),
        vm((JB, n_rows), F32),
        vm((L, L), F32),
        vm((CH, L), F32),
        vm((CH, JT, S, L), F32),
        vm((CH, JT, S, L), F32),
        vm((2, GS, JT, S, L), F32),
        vm((NT, CH, L), F32),
        vm((NT, CH, L), F32),
        vm((NT, CH, L), F32),
        vm((NT, S, L), F32),
        vm((S, L), F32),
        vm((2, NT, S, L), F32),
        vm((2, NT, S, L), F32),
        vm((2, NT, S, L), F32),
        vm((2, NT, S, L), F32),
        vm((NT, S, L), F32),
        vm((2, 3, S, L), F32),
        vm((2, 3, 3, S, L), F32),
        vm((2, S, L), F32),
        vm((2, S, L), F32),
        vm((CH, NR, L), F32),
        vm((HB, NR, L), F32),
        vm((4, L, L), F32),
        dma((NL,)),
        dma((max(len(plan["msgs"]), len(plan0["msgs"])),)),
        pltpu.SemaphoreType.REGULAR,
        dma((2,)),
        dma((2,)),
        dma((2,)),
        dma((2,)),
        dma((2,)),
        dma((2,)),
        dma((2,)),
        dma((2, 3, 3)),
        dma((2, 3, 3)),
        dma((2, 2)),
        dma((2,)),
    ]
    return kernel, scratch


def solution(mesh):
    chips = mesh.shape["rows"]
    dims = torus_of(chips)
    grid_spec = P(("pairs", "rows"), "cols")

    def local_fn(c1, c2, t0, p, q, eps):
        n_rows, n_cols = p.shape[0] * chips, q.shape[0] * mesh.shape["cols"]
        kernel, scratch = make_kernel(dims, n_rows, n_cols, eps.shape[0], SWEEPS)
        vmem = pl.BlockSpec(memory_space=pltpu.VMEM)
        smem = pl.BlockSpec(memory_space=pltpu.SMEM)
        return pl.pallas_call(
            kernel,
            name="gromov",
            out_shape=(jax.ShapeDtypeStruct(t0.shape, F32), jax.ShapeDtypeStruct((1,), F32)),
            in_specs=[smem, smem, vmem, vmem, vmem, vmem],
            out_specs=(vmem, smem),
            scratch_shapes=scratch,
            compiler_params=pltpu.CompilerParams(
                collective_id=0, has_side_effects=True, vmem_limit_bytes=60 * 1024 * 1024
            ),
        )(eps, p, c1, c2, t0, q.reshape(chips // 2, L))

    return jax.shard_map(
        local_fn,
        mesh=mesh,
        in_specs=(grid_spec, grid_spec, grid_spec, P(("pairs", "rows")), P(("pairs", "cols")), P("pairs")),
        out_specs=(grid_spec, P("pairs")),
        check_vma=False,
    )
```

```python
import heapq
import itertools
import math

import jax
import jax.numpy as jnp
from jax import lax
from jax.experimental import pallas as pl
from jax.experimental.pallas import tpu as pltpu
from jax.sharding import PartitionSpec as P

SWEEPS = 10
FLAT = pl.DeviceIdType.LOGICAL
L, S = 128, 8
JB = 64
JT = JB // S
F32, BF16 = jnp.float32, jnp.bfloat16
ORDERS = ((0, 1, 2), (1, 2, 0), (2, 0, 1))
TILE_RATE = 11.4
HOP_US = 2.6
AHEAD_US = 1.0
PARTNER_US = 4.0
LATE = 165


def torus_of(chips):
    return {64: (4, 4, 4), S: (4, 2, 1), 16: (4, 4, 1)}[chips]


def split3(n):
    cuts = [0, (n + 2) // 3, (2 * n + 2) // 3, n]
    return [(cuts[k], cuts[k + 1]) for k in range(3)]


def tree_plan(dims, tiles, rate, lat_us, ahead_us, shared=0):
    rings = {1: (), 2: ((1, "f", 1),), 4: ((1, "f", 1), (3, "f", -1), (2, "a", 1), (2, "b", -1))}
    msgs = []
    for color, order in enumerate(ORDERS):
        lo, hi = split3(tiles)[color]
        for dst in itertools.product(*(range(n) for n in dims)):
            used = [k for k in range(3) if dst[order[k]]]
            if not used or lo == hi:
                continue
            d = order[used[-1]]
            mid = lo + (hi - lo + (sum(dst) + color) % 2) // 2
            for at, part, sign in rings[dims[d]]:
                a, b = {"f": (lo, hi), "a": (lo, mid), "b": (mid, hi)}[part]
                if at != dst[d] or a == b:
                    continue
                src = list(dst)
                src[d] = (src[d] - sign) % dims[d]
                m = dict(id=len(msgs), color=color, src=tuple(src), dst=dst, link=(d, sign), lo=a, hi=b)
                m["us"] = (b - a) / rate
                msgs.append(m)
    into = {}
    for m in msgs:
        into.setdefault((m["color"], m["dst"]), []).append(m)
    users = [[] for _ in msgs]
    missing = []
    for m in msgs:
        deps = [e for e in into.get((m["color"], m["src"]), []) if e["lo"] < m["hi"] and m["lo"] < e["hi"]]
        missing.append(len(deps))
        for e in deps:
            users[e["id"]].append(m)
    way = {}

    def way_of(m):
        if m["id"] not in way:
            way[m["id"]] = m["us"] + lat_us + max([way_of(u) for u in users[m["id"]]], default=0.0)
        return way[m["id"]]

    links = sorted({m["link"] for m in msgs})
    queue = {k: [] for k in links}
    idle = dict.fromkeys(links, True)
    ready, events, ops = {}, [], []

    def put(m, now):
        ready[m["id"]] = now
        heapq.heappush(queue[m["link"]], (-way_of(m), m["id"]))

    def start(link, now):
        if idle[link] and queue[link]:
            k = heapq.heappop(queue[link])[1]
            idle[link] = False
            ops.append((max(ready[k], now - ahead_us), 1, "send", msgs[k]))
            heapq.heappush(events, (now + msgs[k]["us"], 0, k))
            heapq.heappush(events, (now + msgs[k]["us"] + lat_us, 1, k))

    for m in msgs:
        if not missing[m["id"]]:
            put(m, 0.0)
    for link in links:
        start(link, 0.0)
    left = {}
    for m in msgs:
        left[m["dst"]] = left.get(m["dst"], 0) + 1
    now = 0.0
    while events:
        now, arrived, k = heapq.heappop(events)
        m = msgs[k]
        if not arrived:
            idle[m["link"]] = True
            start(m["link"], now)
            continue
        ops.append((now, 0, "wait", m))
        for u in users[k]:
            missing[u["id"]] -= 1
            if not missing[u["id"]]:
                put(u, now)
                start(u["link"], now)
        left[m["dst"]] -= 1
        if not left[m["dst"]]:
            slot = m["dst"][0] + dims[0] * (m["dst"][1] + dims[1] * m["dst"][2])
            ops.append((now, 0, "slot", slot))
            if slot < shared:
                ops.append((now + PARTNER_US, 0, "partner", slot))
    ops.sort(key=lambda op: op[:2])
    totals = {k: sum(m["hi"] - m["lo"] for m in msgs if m["link"] == k) for k in links}
    return dict(msgs=msgs, ops=[op[2:] for op in ops], links=links, totals=totals, end=now)


def make_kernel(dims, n_rows, n_cols, steps, sweeps):
    X, Y, Z = dims
    CH = X * Y * Z
    NR = n_rows // CH
    G = NR // S
    NT = n_rows // L
    TB = JT * NT
    HB = CH // 2
    JN = n_cols // 2 // L
    JW = JN // 2
    NT0 = G * JW
    TT0 = NT0 + 2 * G
    KJ = CH * JB
    CK = min(1024, KJ)
    CM = min(2048, KJ)
    GS = min(4, CH // 2)
    CS = max(CH * 3 // 8 // GS * GS, GS)
    NP = CH + CS
    NE, NC = (CH - CS) // GS, 2 * CS // GS
    assert NT == 4 and n_cols == CH * L and JN == HB
    plan0 = tree_plan(dims, TT0, TILE_RATE, HOP_US, 2 * AHEAD_US)
    plan = tree_plan(dims, TB, TILE_RATE, HOP_US, AHEAD_US, CS)
    links = plan["links"]
    NL = len(links)
    peers = [(d, k) for d in range(3) for k in range(1, dims[d])]
    strides = (1, X, X * Y)

    def slot_of(offset):
        return offset[0] + X * offset[1] + X * Y * offset[2]

    def kernel(
        eps_ref, p_ref, c1_ref, c2_ref, t0_ref, q_ref,
        out_ref, loss_ref,
        land, kbuf, g0, tt, c1f, c1b, c2n, c2p, bacc, lp, lprecv, bp, qf, qrep, vbuf, cbuf,
        mb, sb, fb, ub, ap, xs, xr, mss, msr, pv, ars, arr, arps, arpr, obuf, orecv, trb, loss_rows, loss_two,
        send_sem, recv_sem, fwd_ssem, fwd_rsem, credit, x_ssem, x_rsem, ms_sem, lp_sem, c1_sem, c2_sem, q_sem, ar_ssem, ar_rsem, arp_sem, o_sem, loss_sem,
    ):
        chip = lax.axis_index("rows")
        core = lax.axis_index("cols")
        other = 1 - core
        pos = (lax.rem(chip, X), lax.rem(lax.div(chip, X), Y), lax.div(chip, X * Y))

        me = core * CH + chip
        partner = other * CH + chip

        def moved(d, k):
            return me + (lax.rem(pos[d] + k + dims[d], dims[d]) - pos[d]) * strides[d]

        near = {link: moved(*link) for link in links}

        def source_of(slot):
            off = (lax.rem(slot, X), lax.rem(lax.div(slot, X), Y), lax.div(slot, X * Y))
            at = [lax.rem(pos[d] + dims[d] - off[d], dims[d]) for d in range(3)]
            return at[0] + X * at[1] + X * Y * at[2]

        def to_partner(src, dst, ssem, rsem):
            return pltpu.make_async_remote_copy(
                src_ref=src, dst_ref=dst, send_sem=ssem, recv_sem=rsem,
                device_id=partner, device_id_type=FLAT,
            )

        def tree_copy(buf, width, first, m):
            n = m["hi"] - m["lo"]
            return pltpu.make_async_remote_copy(
                src_ref=buf.at[pl.ds((first + slot_of(m["src"])) * width + m["lo"], n)],
                dst_ref=buf.at[pl.ds((first + slot_of(m["dst"])) * width + m["lo"], n)],
                send_sem=send_sem.at[links.index(m["link"])],
                recv_sem=recv_sem.at[m["id"]],
                device_id=near[m["link"]],
                device_id_type=FLAT,
            )

        def tree(buf, width, first, the_plan, before_send=None, on_slot=None, fillers=()):
            fillers, ready, waits = list(fillers), [], 0
            for op, m in the_plan["ops"]:
                if op == "send":
                    if before_send is not None:
                        before_send(m)
                    tree_copy(buf, width, first, m).start()
                elif op == "wait":
                    while fillers and not fillers[0][0]:
                        fillers.pop(0)[1]()
                    ref = buf.at[pl.ds((first + slot_of(m["dst"])) * width + m["lo"], m["hi"] - m["lo"])]
                    pltpu.make_async_copy(ref, ref, recv_sem.at[m["id"]]).wait()
                    waits += 1
                    if ready:
                        on_slot(*ready.pop(0))
                    elif fillers and waits >= fillers[0][0]:
                        fillers.pop(0)[1]()
                elif on_slot is not None:
                    ready.append((op, m))
            for at in ready:
                on_slot(*at)
            for _, f in fillers:
                f()

        def tree_sent(buf, the_plan):
            for k, link in enumerate(links):
                n = the_plan["totals"][link]
                ref = buf.at[pl.ds(0, n)]
                pltpu.make_async_copy(ref, ref, send_sem.at[k]).wait()

        def give_credit():
            for d, sign in links:
                pl.semaphore_signal(credit, inc=1, device_id=moved(d, -sign), device_id_type=FLAT)

        def all_sum_send(stage):
            for n, k in enumerate(range(1, dims[stage])):
                pltpu.make_async_remote_copy(
                    src_ref=ars.at[stage], dst_ref=arr.at[stage, n],
                    send_sem=ar_ssem.at[stage, n], recv_sem=ar_rsem.at[stage, n],
                    device_id=moved(stage, k), device_id_type=FLAT,
                ).start()

        def all_sum_get(stage):
            total = ars[stage]
            for n, k in enumerate(range(1, dims[stage])):
                pltpu.make_async_remote_copy(
                    src_ref=ars.at[stage], dst_ref=arr.at[stage, n],
                    send_sem=ar_ssem.at[stage, n], recv_sem=ar_rsem.at[stage, n],
                    device_id=moved(stage, k), device_id_type=FLAT,
                ).wait()
                total = total + arr[stage, n]
            return total

        def all_sum_step(stage):
            total = all_sum_get(stage)
            if stage < 2:
                ars[stage + 1] = total
                all_sum_send(stage + 1)
            else:
                arps[...] = total
                to_partner(arps, arpr, arp_sem.at[0], arp_sem.at[1]).start()

        barrier = pltpu.get_barrier_semaphore()
        for d, k in peers:
            pl.semaphore_signal(barrier, inc=1, device_id=moved(d, k), device_id_type=FLAT)
        pl.semaphore_signal(barrier, inc=1, device_id=partner, device_id_type=FLAT)

        row = lax.broadcasted_iota(jnp.int32, (S, L), 0)
        lane = lax.broadcasted_iota(jnp.int32, (S, L), 1)

        for g in range(G):
            rows = slice(g * S, g * S + S)
            pair = jnp.concatenate([c1_ref[rows, :L], c1_ref[rows, L:]], axis=0)
            g0[NT0 + core * G + g] = pair.astype(BF16)
        c1_copy = to_partner(
            g0.at[pl.ds(NT0 + core * G, G)], g0.at[pl.ds(NT0 + core * G, G)], c1_sem.at[0], c1_sem.at[1]
        )
        q_copy = to_partner(q_ref, qf.at[pl.ds(core * HB, HB)], q_sem.at[0], q_sem.at[1])

        tile = jnp.zeros((S, L), F32)
        for t in range(2):
            part = jnp.zeros((1, L), F32)
            for k in range(NR):
                entry = c1_ref[k : k + 1, t * L : t * L + L]
                part = part + entry * entry * p_ref[k]
            tile = jnp.where(row == 2 * core + t, jnp.broadcast_to(part, (S, L)), tile)
        where = (row - 4) * L + lane
        for k in range(NR):
            tile = jnp.where(where == chip * NR + k, p_ref[k], tile)
        ars[0] = tile
        for g in range(G):
            rows = slice(g * S, g * S + S)
            for t in range(JW):
                a, b = t0_ref[rows, (2 * L) * t : (2 * L) * t + L], t0_ref[rows, (2 * L) * t + L : (2 * L) * t + (2 * L)]
                g0[g * JW + t] = jnp.concatenate([a, b], axis=0).astype(BF16)
        qf[pl.ds(core * HB, HB)] = q_ref[...]

        c2_copy = to_partner(c2n.at[pl.ds(core * HB, HB)], c2n.at[pl.ds(core * HB, HB)], c2_sem.at[0], c2_sem.at[1])
        bp[...] = jnp.zeros_like(bp)

        def round_c2(first, last):
            for t in range(first, last):
                blk = c2_ref[:, t * L : t * L + L]
                c2n[core * HB + t] = blk.astype(BF16)
                bp[...] += blk * blk * q_ref[t : t + 1, :]

        def finish_b():
            bp[...] = jnp.broadcast_to(jnp.sum(bp[...], axis=1, keepdims=True), (L, L))

        round_c2(0, HB)
        finish_b()
        with jax.named_scope("barrier"):
            pl.semaphore_wait(barrier, len(peers) + 1)
        give_credit()
        c1_copy.start()
        q_copy.start()
        all_sum_send(0)

        c2_copy.start()

        src = lax.broadcasted_iota(jnp.int32, (L, L), 0)
        dst = lax.broadcasted_iota(jnp.int32, (L, L), 1)
        picks = [
            jnp.where((src - core * JB == dst - h * JB) & (dst >= h * JB) & (dst < h * JB + JB), 1.0, 0.0).astype(BF16)
            for h in range(2)
        ]

        def order_c2(first, last):
            for t in range(first, last):
                a = jnp.dot(c2n[source_of(2 * t)], picks[0], preferred_element_type=F32)
                b = jnp.dot(c2n[source_of(2 * t + 1)], picks[1], preferred_element_type=F32)
                c2p[:, t * L : t * L + L] = (a + b).astype(BF16)

        def order_q(first, last):
            def four(n, carry):
                for k in range(4):
                    p = 4 * n + k
                    shared = p < CS
                    half = jnp.where(shared, other, core)
                    line = jnp.broadcast_to(qf[pl.ds(source_of(jnp.where(shared, p, p - CS)), 1), :], (S, L))
                    for jt in range(JT):
                        own = jnp.where(lane == half * JB + jt * S + row, line, 0.0)
                        qrep[p, jt] = jnp.broadcast_to(jnp.sum(own, axis=1, keepdims=True), (S, L))
                return carry

            lax.fori_loop(first // 4, last // 4, four, 0)

        def span(n, parts, f):
            cuts = [n * k // parts for k in range(parts + 1)]
            return [lambda a=a, b=b: f(a, b) for a, b in zip(cuts, cuts[1:])]

        fillers = [(0, lambda: q_copy.wait()), (0, lambda: order_q(0, NP)), (LATE // 2, lambda: all_sum_step(0))]
        fillers += [(LATE, lambda: c2_copy.wait())]
        fillers += [(LATE + 4 * n, f) for n, f in enumerate(span(CH // 2, S, order_c2))]
        fillers += [(LATE + JB // 2, lambda: all_sum_step(1))]
        waited = []

        def before_send(m):
            if not waited and m["hi"] > NT0:
                waited.append(1)
                c1_copy.wait()

        def unpack(op, s):
            chip_s = source_of(s)
            for g in range(G):
                tiles = g0[s * TT0 + g * JW : s * TT0 + g * JW + JW].astype(F32).reshape(JN, S, L)
                kbuf[pl.ds((chip_s * G + g) * JN, JN)] = tiles
                at = pl.ds(pl.multiple_of(chip_s * NR + g * S, S), S)
                for h in range(2):
                    pair = g0[s * TT0 + NT0 + h * G + g].astype(F32)
                    c1f[at, 2 * L * h : 2 * L * h + L] = pair[:S]
                    c1f[at, 2 * L * h + L : 2 * L * h + 2 * L] = pair[S:]

        with jax.named_scope("gather0"):
            first = [(0, lambda: unpack("slot", 0))]
            tree(g0, TT0, 0, plan0, before_send=before_send, on_slot=unpack, fillers=first + fillers)
            tree_sent(g0, plan0)
            c1b[...] = c1f[...].astype(BF16)
            all_sum_step(2)

        def finish_lp():
            lp[...] = jnp.concatenate([bp[...]] * NT, axis=1) - 2.0 * bacc[...]

        bacc[...] = jnp.zeros_like(bacc)
        JC = CK // L

        def first_chunk(n, carry):
            cols = []
            for t in range(JC):
                cols.append(kbuf[pl.ds(n * JC + t, CH * G, stride=JN)].reshape(n_rows, L))
            plan_c = jnp.concatenate(cols, axis=1).astype(BF16)
            lead = jnp.dot(c1b[...], plan_c, preferred_element_type=F32).astype(BF16)
            c2c = jnp.concatenate([c2n[core * HB + n * JC + t] for t in range(JC)], axis=1)
            bacc[...] += lax.dot_general(c2c, lead, (((1,), (1,)), ((), ())), preferred_element_type=F32)
            return carry

        with jax.named_scope("firstmm"):
            lax.fori_loop(0, KJ // CK, first_chunk, 0)
            finish_lp()
        to_partner(arps, arpr, arp_sem.at[0], arp_sem.at[1]).wait()
        ap[...] = jnp.where(row < 4, arps[...] + arpr[...], arps[...])
        for t in range(NT):
            pv[t] = jnp.broadcast_to(ap[4 + t : 5 + t, :], (S, L))


        def chunk(n, carry):
            at = pl.ds(pl.multiple_of(n * CM, CM), CM)
            lead = jnp.dot(tt[at, :], c1b[...], preferred_element_type=F32).astype(BF16)
            bacc[...] += jnp.dot(c2p[:, at], lead, preferred_element_type=F32)
            return carry

        def costs():
            copy = to_partner(lp.at[pl.ds(other * JB, JB)], lprecv, lp_sem.at[0], lp_sem.at[1])
            copy.start()
            copy.wait()
            own = lp[pl.ds(pl.multiple_of(core * JB, JB), JB), :] + lprecv[...]
            return own + jnp.concatenate([ap[t : t + 1, :] for t in range(NT)], axis=1)

        def block(s):
            return kbuf[pl.ds(s * TB, TB)].reshape(JT, NT, S, L)

        def weighted(kk, u):
            w = (kk[:, 0] * u[0] + kk[:, 1] * u[1]) + (kk[:, 2] * u[2] + kk[:, 3] * u[3])
            return jnp.sum(w, axis=2, keepdims=True)

        def passes(u, rescale=False, last=False, par=0):
            def place(g):
                if last:
                    return g * GS + CS
                return g * GS + 2 * CS if not isinstance(g, int) or g < NE else (g - NE) * GS

            def one(at, buf):
                for k in range(GS):
                    p = at + k
                    kk = block(p)
                    if rescale:
                        kk = kk * fb[:, pl.ds(p, 1), :][None]
                        kbuf[pl.ds(p * TB, TB)] = kk.reshape(TB, S, L)
                    cbuf[buf, k] = qrep[p] / jnp.broadcast_to(weighted(kk, u), (JT, S, L))

            def two(at, buf, acc):
                for k in range(GS):
                    p = at + k
                    v = cbuf[buf, k]
                    kk = block(p)
                    if last:
                        vbuf[p - CS] = v
                        t = (kk * u[None]) * v[:, None]
                        flat = jnp.concatenate([t[:, i].reshape(JB, L) for i in range(NT)], axis=1)
                        tt[pl.ds(pl.multiple_of((p - CS) * JB, JB), JB), :] = flat.astype(BF16)
                    else:
                        acc = acc + jnp.sum(kk * v[:, None], axis=0)
                return acc

            def run(a, b, end):
                shift = place(a) - a * GS
                even, odd = a % 2, (a + 1) % 2
                pairs = max(0, (b - a - 1) // 2)

                def both(n, acc):
                    at = (a + 2 * n) * GS + shift
                    one(at + GS, odd)
                    acc = two(at, even, acc)
                    one(at + 2 * GS, even)
                    return two(at + GS, odd, acc)

                acc = lax.fori_loop(0, pairs, both, jnp.zeros((NT, S, L), F32))
                for g in range(a + 2 * pairs, b):
                    if g + 1 < end:
                        one(place(g + 1), (g + 1) % 2)
                    acc = two(place(g), g % 2, acc)
                return acc

            one(place(0), 0)
            if last:
                run(0, CH // GS, CH // GS)
                return None
            xs[par] = run(0, NE, NE + NC)
            copy = to_partner(xs.at[par], xr.at[par], x_ssem.at[par], x_rsem.at[par])
            copy.start()
            acc = run(NE, NE + NC, NE + NC)
            copy.wait()
            total = jnp.sum((xs[par] + xr[par]) + acc, axis=1, keepdims=True)
            return pv[...] / jnp.broadcast_to(total, (NT, S, L))

        def outer(r, carry):
            scale = 1.4426950408889634 / eps_ref[r]
            cost = costs()
            for jt in range(JT):
                for t in range(NT):
                    land[CS * TB + jt * NT + t] = cost[jt * S : jt * S + S, t * L : t * L + L]

            def exps(p):
                ll = land[p * TB : p * TB + TB].reshape(JT, NT, S, L)
                low = jnp.min(jnp.min(ll, axis=0), axis=1, keepdims=True)
                kk = jnp.exp2((low[None] - ll) * scale)
                kbuf[p * TB : p * TB + TB] = kk.reshape(TB, S, L)
                mb[:, p : p + 1, :] = low
                sb[:, p : p + 1, :] = jnp.sum(jnp.sum(kk, axis=0), axis=1, keepdims=True)

            def passed_on(s):
                return to_partner(
                    land.at[pl.ds((CS + s) * TB, TB)], land.at[pl.ds(s * TB, TB)], fwd_ssem.at[0], fwd_rsem.at[s]
                )

            def on_slot(op, s):
                if op == "slot":
                    if s < CS:
                        passed_on(s).start()
                    exps(CS + s)
                else:
                    passed_on(s).wait_recv()
                    exps(s)

            with jax.named_scope("gather"):
                pl.semaphore_wait(credit, NL)
                first = [(0, lambda: on_slot("slot", 0)), (len(plan["msgs"]) // 4, lambda: on_slot("partner", 0))]
                tree(land, TB, CS, plan, on_slot=on_slot, fillers=first)
                tree_sent(land, plan)
                ref = land.at[pl.ds(0, CS * TB)]
                pltpu.make_async_copy(ref, ref, fwd_ssem.at[0]).wait()
                give_credit()

            with jax.named_scope("minx"):
                def least_of(a, b):
                    low = jnp.min(mb[:, a:b], axis=1, keepdims=True)
                    part = jnp.sum(sb[:, a:b] * jnp.exp2((low - mb[:, a:b]) * scale), axis=1, keepdims=True)
                    return jnp.broadcast_to(low, (NT, S, L)), jnp.broadcast_to(part, (NT, S, L))

                mss[0], mss[1] = least_of(2 * CS, NP)
                copy = to_partner(mss, msr, ms_sem.at[0], ms_sem.at[1])
                copy.start()
                low, part = least_of(0, 2 * CS)
                copy.wait()
                least = jnp.minimum(jnp.minimum(mss[0], msr[0]), low)
                total = mss[1] * jnp.exp2((least - mss[0]) * scale) + msr[1] * jnp.exp2((least - msr[0]) * scale)
                total = total + part * jnp.exp2((least - low) * scale)
                fb[...] = jnp.exp2((least[:, :1] - mb[...]) * scale)
                u = pv[...] / total

            with jax.named_scope("pass1"):
                u = passes(u, rescale=True, par=1)

            def sweep(t, u):
                return passes(u, par=lax.rem(t, 2))

            with jax.named_scope("sweeps"):
                u = lax.fori_loop(2, sweeps, sweep, u)
            with jax.named_scope("lastpass"):
                passes(u, last=True)
            ub[...] = u
            bacc[...] = jnp.zeros_like(bacc)
            with jax.named_scope("mm"):
                lax.fori_loop(0, KJ // CM, chunk, 0)
                finish_lp()
            return carry

        lax.fori_loop(0, steps, outer, 0)

        pl.semaphore_wait(credit, NL)
        cost = costs()
        plan_own = (block(CS) * ub[...][None]) * vbuf[0][:, None]
        total = jnp.zeros((S, L), F32)
        for jt in range(JT):
            for t in range(NT):
                total = total + cost[jt * S : jt * S + S, t * L : t * L + L] * plan_own[jt, t]
        loss_rows[0:1] = jnp.sum(total, axis=0, keepdims=True)

        def to_chip(n):
            o = CH - n
            off = (lax.rem(o, X), lax.rem(lax.div(o, X), Y), lax.div(o, X * Y))
            at = [lax.rem(pos[d] + off[d], dims[d]) for d in range(3)]
            return pltpu.make_async_remote_copy(
                src_ref=loss_rows.at[pl.ds(0, 1)], dst_ref=loss_rows.at[pl.ds(o, 1)],
                send_sem=loss_sem.at[0], recv_sem=loss_sem.at[1],
                device_id=core * CH + at[0] + X * at[1] + X * Y * at[2], device_id_type=FLAT,
            )

        def tell(n, carry):
            to_chip(n).start()
            return carry

        lax.fori_loop(1, CH, tell, 0)

        it = lax.div(chip * NR, L)
        inside = pl.multiple_of(lax.rem(chip * NR, L), S)

        def rows_of(n, carry):
            for k in range(4):
                s = 4 * n + k
                kk = jnp.concatenate([kbuf[(CS + s) * TB + jt * NT + it] for jt in range(JT)], axis=0)
                uu = jnp.concatenate([ub[it]] * JT, axis=0)
                t = (kk * uu) * vbuf[s].reshape(JB, L)
                none = jnp.zeros_like(t)
                both = jnp.where(core == 0, jnp.concatenate([t, none], axis=0), jnp.concatenate([none, t], axis=0))
                trb[k] = both.T
                obuf[source_of(s)] = trb[k, pl.ds(inside, NR), :]
            return carry

        with jax.named_scope("tail"):
            lax.fori_loop(0, CH // 4, rows_of, 0)
            o_copy = to_partner(obuf.at[pl.ds(other * HB, HB)], orecv, o_sem.at[0], o_sem.at[1])
            o_copy.start()
            o_copy.wait()
            for b in range(HB):
                out_ref[:, b * L : b * L + L] = obuf[core * HB + b] + orecv[b]
            ref = loss_rows.at[pl.ds(1, CH - 1)]
            pltpu.make_async_copy(ref, ref, loss_sem.at[0]).wait()
            pltpu.make_async_copy(ref, ref, loss_sem.at[1]).wait()
            loss_two[0:1] = jnp.sum(loss_rows[...], axis=0, keepdims=True)
            copy = to_partner(loss_two.at[pl.ds(0, 1)], loss_two.at[pl.ds(1, 1)], loss_sem.at[2], loss_sem.at[3])
            copy.start()
            copy.wait()
            loss_ref[0] = jnp.sum(loss_two[...])

    vm = pltpu.VMEM
    dma = pltpu.SemaphoreType.DMA
    scratch = [
        vm((NP * TB, S, L), F32),
        vm((NP * TB, S, L), F32),
        vm((CH * TT0, 16, L), BF16),
        vm((KJ, n_rows), BF16),
        vm((n_rows, n_rows), F32),
        vm((n_rows, n_rows), BF16),
        vm((CH, L, L), BF16),
        vm((L, KJ), BF16),
        vm((L, n_rows), F32),
        vm((L, n_rows), F32),
        vm((JB, n_rows), F32),
        vm((L, L), F32),
        vm((CH, L), F32),
        vm((NP, JT, S, L), F32),
        vm((CH, JT, S, L), F32),
        vm((2, GS, JT, S, L), F32),
        vm((NT, NP, L), F32),
        vm((NT, NP, L), F32),
        vm((NT, NP, L), F32),
        vm((NT, S, L), F32),
        vm((S, L), F32),
        vm((2, NT, S, L), F32),
        vm((2, NT, S, L), F32),
        vm((2, NT, S, L), F32),
        vm((2, NT, S, L), F32),
        vm((NT, S, L), F32),
        vm((3, S, L), F32),
        vm((3, 3, S, L), F32),
        vm((S, L), F32),
        vm((S, L), F32),
        vm((CH, NR, L), F32),
        vm((HB, NR, L), F32),
        vm((4, L, L), F32),
        vm((CH, L), F32),
        vm((2, L), F32),
        dma((NL,)),
        dma((max(len(plan["msgs"]), len(plan0["msgs"])),)),
        dma((1,)),
        dma((CS,)),
        pltpu.SemaphoreType.REGULAR,
        dma((2,)),
        dma((2,)),
        dma((2,)),
        dma((2,)),
        dma((2,)),
        dma((2,)),
        dma((2,)),
        dma((3, 3)),
        dma((3, 3)),
        dma((2,)),
        dma((2,)),
        dma((4,)),
    ]
    return kernel, scratch


def solution(mesh):
    chips = mesh.shape["rows"]
    dims = torus_of(chips)
    grid_spec = P(("pairs", "rows"), "cols")

    def local_fn(c1, c2, t0, p, q, eps):
        n_rows, n_cols = p.shape[0] * chips, q.shape[0] * mesh.shape["cols"]
        kernel, scratch = make_kernel(dims, n_rows, n_cols, eps.shape[0], SWEEPS)
        vmem = pl.BlockSpec(memory_space=pltpu.VMEM)
        smem = pl.BlockSpec(memory_space=pltpu.SMEM)
        return pl.pallas_call(
            kernel,
            name="gromov",
            out_shape=(jax.ShapeDtypeStruct(t0.shape, F32), jax.ShapeDtypeStruct((1,), F32)),
            in_specs=[smem, smem, vmem, vmem, vmem, vmem],
            out_specs=(vmem, smem),
            scratch_shapes=scratch,
            compiler_params=pltpu.CompilerParams(
                collective_id=0, has_side_effects=True, vmem_limit_bytes=60 * 1024 * 1024
            ),
        )(eps, p, c1, c2, t0, q.reshape(chips // 2, L))

    return jax.shard_map(
        local_fn,
        mesh=mesh,
        in_specs=(grid_spec, grid_spec, grid_spec, P(("pairs", "rows")), P(("pairs", "cols")), P("pairs")),
        out_specs=(grid_spec, P("pairs")),
        check_vma=False,
    )
```

```python
import heapq
import itertools
import math

import jax
import jax.numpy as jnp
from jax import lax
from jax.experimental import pallas as pl
from jax.experimental.pallas import tpu as pltpu
from jax.sharding import PartitionSpec as P

SWEEPS = 10
FLAT = pl.DeviceIdType.LOGICAL
L, S = 128, 8
JB = 64
JT = JB // S
F32, BF16 = jnp.float32, jnp.bfloat16
ORDERS = ((0, 1, 2), (1, 2, 0), (2, 0, 1))
TILE_RATE = 11.4
HOP_US = 2.6
AHEAD_US = 1.0
HOLD = 400
PARTNER_US = 4.0
LATE = 165


def torus_of(chips):
    return {64: (4, 4, 4), S: (4, 2, 1), 16: (4, 4, 1)}[chips]


def split3(n):
    cuts = [0, (n + 2) // 3, (2 * n + 2) // 3, n]
    return [(cuts[k], cuts[k + 1]) for k in range(3)]


def tree_plan(dims, tiles, rate, lat_us, ahead_us, shared=0):
    rings = {1: (), 2: ((1, "f", 1),), 4: ((1, "f", 1), (3, "f", -1), (2, "a", 1), (2, "b", -1))}
    msgs = []
    for color, order in enumerate(ORDERS):
        lo, hi = split3(tiles)[color]
        for dst in itertools.product(*(range(n) for n in dims)):
            used = [k for k in range(3) if dst[order[k]]]
            if not used or lo == hi:
                continue
            d = order[used[-1]]
            mid = lo + (hi - lo + (sum(dst) + color) % 2) // 2
            for at, part, sign in rings[dims[d]]:
                a, b = {"f": (lo, hi), "a": (lo, mid), "b": (mid, hi)}[part]
                if at != dst[d] or a == b:
                    continue
                src = list(dst)
                src[d] = (src[d] - sign) % dims[d]
                m = dict(id=len(msgs), color=color, src=tuple(src), dst=dst, link=(d, sign), lo=a, hi=b)
                m["us"] = (b - a) / rate
                msgs.append(m)
    into = {}
    for m in msgs:
        into.setdefault((m["color"], m["dst"]), []).append(m)
    users = [[] for _ in msgs]
    missing = []
    for m in msgs:
        deps = [e for e in into.get((m["color"], m["src"]), []) if e["lo"] < m["hi"] and m["lo"] < e["hi"]]
        missing.append(len(deps))
        for e in deps:
            users[e["id"]].append(m)
    way = {}

    def way_of(m):
        if m["id"] not in way:
            way[m["id"]] = m["us"] + lat_us + max([way_of(u) for u in users[m["id"]]], default=0.0)
        return way[m["id"]]

    links = sorted({m["link"] for m in msgs})
    queue = {k: [] for k in links}
    idle = dict.fromkeys(links, True)
    ready, events, ops = {}, [], []

    def put(m, now):
        ready[m["id"]] = now
        heapq.heappush(queue[m["link"]], (-way_of(m), m["id"]))

    def start(link, now):
        if idle[link] and queue[link]:
            k = heapq.heappop(queue[link])[1]
            idle[link] = False
            ops.append((max(ready[k], now - ahead_us), 1, "send", msgs[k]))
            heapq.heappush(events, (now + msgs[k]["us"], 0, k))
            heapq.heappush(events, (now + msgs[k]["us"] + lat_us, 1, k))

    for m in msgs:
        if not missing[m["id"]]:
            put(m, 0.0)
    for link in links:
        start(link, 0.0)
    left = {}
    for m in msgs:
        left[m["dst"]] = left.get(m["dst"], 0) + 1
    now = 0.0
    while events:
        now, arrived, k = heapq.heappop(events)
        m = msgs[k]
        if not arrived:
            idle[m["link"]] = True
            start(m["link"], now)
            continue
        ops.append((now, 0, "wait", m))
        for u in users[k]:
            missing[u["id"]] -= 1
            if not missing[u["id"]]:
                put(u, now)
                start(u["link"], now)
        left[m["dst"]] -= 1
        if not left[m["dst"]]:
            slot = m["dst"][0] + dims[0] * (m["dst"][1] + dims[1] * m["dst"][2])
            ops.append((now, 0, "slot", slot))
            if slot < shared:
                ops.append((now + PARTNER_US, 0, "partner", slot))
    ops.sort(key=lambda op: op[:2])
    totals = {k: sum(m["hi"] - m["lo"] for m in msgs if m["link"] == k) for k in links}
    return dict(msgs=msgs, ops=[op[2:] for op in ops], links=links, totals=totals, end=now)


def make_kernel(dims, n_rows, n_cols, steps, sweeps):
    X, Y, Z = dims
    CH = X * Y * Z
    NR = n_rows // CH
    G = NR // S
    NT = n_rows // L
    TB = JT * NT
    HB = CH // 2
    JN = n_cols // 2 // L
    JW = JN // 2
    NT0 = G * JW
    TT0 = NT0 + 2 * G
    KJ = CH * JB
    CK = min(1024, KJ)
    CM = min(2048, KJ)
    GS = min(4, CH // 2)
    CS = max(CH * 3 // 8 // GS * GS, GS)
    NP = CH + CS
    NE, NC = (CH - CS) // GS, 2 * CS // GS
    assert NT == 4 and n_cols == CH * L and JN == HB
    plan0 = tree_plan(dims, TT0, TILE_RATE, HOP_US, 2 * AHEAD_US)
    plan = tree_plan(dims, TB, TILE_RATE, HOP_US, AHEAD_US, CS)
    links = plan["links"]
    NL = len(links)
    peers = [(d, k) for d in range(3) for k in range(1, dims[d])]
    strides = (1, X, X * Y)

    def slot_of(offset):
        return offset[0] + X * offset[1] + X * Y * offset[2]

    def kernel(
        eps_ref, p_ref, c1_ref, c2_ref, t0_ref, q_ref,
        out_ref, loss_ref,
        land, kbuf, g0, tt, c1f, c1b, c2n, c2p, bacc, lp, lprecv, bp, qf, qrep, vbuf, cbuf,
        mb, sb, fb, ub, ap, xs, xr, mss, msr, pv, ars, arr, arps, arpr, obuf, orecv, trb, loss_rows, loss_two, pad,
        send_sem, recv_sem, fwd_ssem, fwd_rsem, credit, x_ssem, x_rsem, ms_sem, lp_sem, c1_sem, c2_sem, q_sem, ar_ssem, ar_rsem, arp_sem, o_sem, loss_sem,
    ):
        chip = lax.axis_index("rows")
        core = lax.axis_index("cols")
        other = 1 - core
        pos = (lax.rem(chip, X), lax.rem(lax.div(chip, X), Y), lax.div(chip, X * Y))

        me = core * CH + chip
        partner = other * CH + chip

        def moved(d, k):
            return me + (lax.rem(pos[d] + k + dims[d], dims[d]) - pos[d]) * strides[d]

        near = {link: moved(*link) for link in links}

        def source_of(slot):
            off = (lax.rem(slot, X), lax.rem(lax.div(slot, X), Y), lax.div(slot, X * Y))
            at = [lax.rem(pos[d] + dims[d] - off[d], dims[d]) for d in range(3)]
            return at[0] + X * at[1] + X * Y * at[2]

        def to_partner(src, dst, ssem, rsem):
            return pltpu.make_async_remote_copy(
                src_ref=src, dst_ref=dst, send_sem=ssem, recv_sem=rsem,
                device_id=partner, device_id_type=FLAT,
            )

        def tree_copy(buf, width, first, m):
            n = m["hi"] - m["lo"]
            return pltpu.make_async_remote_copy(
                src_ref=buf.at[pl.ds((first + slot_of(m["src"])) * width + m["lo"], n)],
                dst_ref=buf.at[pl.ds((first + slot_of(m["dst"])) * width + m["lo"], n)],
                send_sem=send_sem.at[links.index(m["link"])],
                recv_sem=recv_sem.at[m["id"]],
                device_id=near[m["link"]],
                device_id_type=FLAT,
            )

        def tree(buf, width, first, the_plan, before_send=None, on_slot=None, fillers=()):
            fillers, ready, waits = list(fillers), [], 0
            for op, m in the_plan["ops"]:
                if op == "send":
                    if before_send is not None:
                        before_send(m)
                    tree_copy(buf, width, first, m).start()
                elif op == "wait":
                    while fillers and not fillers[0][0]:
                        fillers.pop(0)[1]()
                    ref = buf.at[pl.ds((first + slot_of(m["dst"])) * width + m["lo"], m["hi"] - m["lo"])]
                    pltpu.make_async_copy(ref, ref, recv_sem.at[m["id"]]).wait()
                    waits += 1
                    if ready:
                        on_slot(*ready.pop(0))
                    elif fillers and waits >= fillers[0][0]:
                        fillers.pop(0)[1]()
                elif on_slot is not None:
                    ready.append((op, m))
            for at in ready:
                on_slot(*at)
            for _, f in fillers:
                f()

        def tree_sent(buf, the_plan):
            for k, link in enumerate(links):
                n = the_plan["totals"][link]
                ref = buf.at[pl.ds(0, n)]
                pltpu.make_async_copy(ref, ref, send_sem.at[k]).wait()

        def give_credit():
            for d, sign in links:
                pl.semaphore_signal(credit, inc=1, device_id=moved(d, -sign), device_id_type=FLAT)

        def all_sum_send(stage):
            for n, k in enumerate(range(1, dims[stage])):
                pltpu.make_async_remote_copy(
                    src_ref=ars.at[stage], dst_ref=arr.at[stage, n],
                    send_sem=ar_ssem.at[stage, n], recv_sem=ar_rsem.at[stage, n],
                    device_id=moved(stage, k), device_id_type=FLAT,
                ).start()

        def all_sum_get(stage):
            total = ars[stage]
            for n, k in enumerate(range(1, dims[stage])):
                pltpu.make_async_remote_copy(
                    src_ref=ars.at[stage], dst_ref=arr.at[stage, n],
                    send_sem=ar_ssem.at[stage, n], recv_sem=ar_rsem.at[stage, n],
                    device_id=moved(stage, k), device_id_type=FLAT,
                ).wait()
                total = total + arr[stage, n]
            return total

        def all_sum_step(stage):
            total = all_sum_get(stage)
            if stage < 2:
                ars[stage + 1] = total
                all_sum_send(stage + 1)
            else:
                arps[...] = total
                to_partner(arps, arpr, arp_sem.at[0], arp_sem.at[1]).start()

        pad[...] = jnp.zeros_like(pad)
        barrier = pltpu.get_barrier_semaphore()
        for d, k in peers:
            pl.semaphore_signal(barrier, inc=1, device_id=moved(d, k), device_id_type=FLAT)
        pl.semaphore_signal(barrier, inc=1, device_id=partner, device_id_type=FLAT)

        row = lax.broadcasted_iota(jnp.int32, (S, L), 0)
        lane = lax.broadcasted_iota(jnp.int32, (S, L), 1)

        for g in range(G):
            rows = slice(g * S, g * S + S)
            pair = jnp.concatenate([c1_ref[rows, :L], c1_ref[rows, L:]], axis=0)
            g0[NT0 + core * G + g] = pair.astype(BF16)
        c1_copy = to_partner(
            g0.at[pl.ds(NT0 + core * G, G)], g0.at[pl.ds(NT0 + core * G, G)], c1_sem.at[0], c1_sem.at[1]
        )
        q_copy = to_partner(q_ref, qf.at[pl.ds(core * HB, HB)], q_sem.at[0], q_sem.at[1])

        tile = jnp.zeros((S, L), F32)
        for t in range(2):
            part = jnp.zeros((1, L), F32)
            for k in range(NR):
                entry = c1_ref[k : k + 1, t * L : t * L + L]
                part = part + entry * entry * p_ref[k]
            tile = jnp.where(row == 2 * core + t, jnp.broadcast_to(part, (S, L)), tile)
        where = (row - 4) * L + lane
        for k in range(NR):
            tile = jnp.where(where == chip * NR + k, p_ref[k], tile)
        ars[0] = tile
        for g in range(G):
            rows = slice(g * S, g * S + S)
            for t in range(JW):
                a, b = t0_ref[rows, (2 * L) * t : (2 * L) * t + L], t0_ref[rows, (2 * L) * t + L : (2 * L) * t + (2 * L)]
                g0[g * JW + t] = jnp.concatenate([a, b], axis=0).astype(BF16)
        qf[pl.ds(core * HB, HB)] = q_ref[...]

        c2_copy = to_partner(c2n.at[pl.ds(core * HB, HB)], c2n.at[pl.ds(core * HB, HB)], c2_sem.at[0], c2_sem.at[1])
        bp[...] = jnp.zeros_like(bp)

        def round_c2(first, last):
            for t in range(first, last):
                blk = c2_ref[:, t * L : t * L + L]
                c2n[core * HB + t] = blk.astype(BF16)
                bp[...] += blk * blk * q_ref[t : t + 1, :]

        def finish_b():
            bp[...] = jnp.broadcast_to(jnp.sum(bp[...], axis=1, keepdims=True), (L, L))

        with jax.named_scope("barrier"):
            pl.semaphore_wait(barrier, len(peers) + 1)
        give_credit()
        c1_copy.start()
        q_copy.start()
        all_sum_send(0)

        src = lax.broadcasted_iota(jnp.int32, (L, L), 0)
        dst = lax.broadcasted_iota(jnp.int32, (L, L), 1)
        picks = [
            jnp.where((src - core * JB == dst - h * JB) & (dst >= h * JB) & (dst < h * JB + JB), 1.0, 0.0).astype(BF16)
            for h in range(2)
        ]

        def order_c2(first, last):
            for t in range(first, last):
                a = jnp.dot(c2n[source_of(2 * t)], picks[0], preferred_element_type=F32)
                b = jnp.dot(c2n[source_of(2 * t + 1)], picks[1], preferred_element_type=F32)
                c2p[:, t * L : t * L + L] = (a + b).astype(BF16)

        def order_q(first, last):
            def four(n, carry):
                for k in range(4):
                    p = 4 * n + k
                    shared = p < CS
                    half = jnp.where(shared, other, core)
                    line = jnp.broadcast_to(qf[pl.ds(source_of(jnp.where(shared, p, p - CS)), 1), :], (S, L))
                    for jt in range(JT):
                        own = jnp.where(lane == half * JB + jt * S + row, line, 0.0)
                        qrep[p, jt] = jnp.broadcast_to(jnp.sum(own, axis=1, keepdims=True), (S, L))
                return carry

            lax.fori_loop(first // 4, last // 4, four, 0)

        def span(n, parts, f):
            cuts = [n * k // parts for k in range(parts + 1)]
            return [lambda a=a, b=b: f(a, b) for a, b in zip(cuts, cuts[1:])]

        fillers = [(0, lambda: round_c2(0, HB)), (0, finish_b), (0, lambda: c2_copy.start())]
        fillers += [(0, lambda: q_copy.wait()), (0, lambda: order_q(0, NP)), (LATE // 2, lambda: all_sum_step(0))]
        fillers += [(LATE, lambda: c2_copy.wait())]
        fillers += [(LATE + 4 * n, f) for n, f in enumerate(span(CH // 2, S, order_c2))]
        fillers += [(LATE + JB // 2, lambda: all_sum_step(1))]
        waited = []

        def before_send(m):
            if not waited and m["hi"] > NT0:
                waited.append(1)
                c1_copy.wait()

        def unpack(op, s):
            chip_s = source_of(s)
            for g in range(G):
                tiles = g0[s * TT0 + g * JW : s * TT0 + g * JW + JW].astype(F32).reshape(JN, S, L)
                kbuf[pl.ds((chip_s * G + g) * JN, JN)] = tiles
                at = pl.ds(pl.multiple_of(chip_s * NR + g * S, S), S)
                for h in range(2):
                    pair = g0[s * TT0 + NT0 + h * G + g].astype(F32)
                    c1f[at, 2 * L * h : 2 * L * h + L] = pair[:S]
                    c1f[at, 2 * L * h + L : 2 * L * h + 2 * L] = pair[S:]

        with jax.named_scope("gather0"):
            first = [(0, lambda: unpack("slot", 0))]
            tree(g0, TT0, 0, plan0, before_send=before_send, on_slot=unpack, fillers=first + fillers)
            tree_sent(g0, plan0)
            c1b[...] = c1f[...].astype(BF16)
            all_sum_step(2)

        def finish_lp():
            lp[...] = jnp.concatenate([bp[...]] * NT, axis=1) - 2.0 * bacc[...]

        bacc[...] = jnp.zeros_like(bacc)
        JC = CK // L

        def first_chunk(n, carry):
            cols = []
            for t in range(JC):
                cols.append(kbuf[pl.ds(n * JC + t, CH * G, stride=JN)].reshape(n_rows, L))
            plan_c = jnp.concatenate(cols, axis=1).astype(BF16)
            lead = jnp.dot(c1b[...], plan_c, preferred_element_type=F32).astype(BF16)
            c2c = jnp.concatenate([c2n[core * HB + n * JC + t] for t in range(JC)], axis=1)
            bacc[...] += lax.dot_general(c2c, lead, (((1,), (1,)), ((), ())), preferred_element_type=F32)
            return carry

        with jax.named_scope("firstmm"):
            lax.fori_loop(0, KJ // CK, first_chunk, 0)
            finish_lp()
        to_partner(arps, arpr, arp_sem.at[0], arp_sem.at[1]).wait()
        ap[...] = jnp.where(row < 4, arps[...] + arpr[...], arps[...])
        for t in range(NT):
            pv[t] = jnp.broadcast_to(ap[4 + t : 5 + t, :], (S, L))


        def chunk(n, carry):
            at = pl.ds(pl.multiple_of(n * CM, CM), CM)
            lead = jnp.dot(tt[at, :], c1b[...], preferred_element_type=F32).astype(BF16)
            bacc[...] += jnp.dot(c2p[:, at], lead, preferred_element_type=F32)
            return carry

        def costs():
            copy = to_partner(lp.at[pl.ds(other * JB, JB)], lprecv, lp_sem.at[0], lp_sem.at[1])
            copy.start()
            copy.wait()
            own = lp[pl.ds(pl.multiple_of(core * JB, JB), JB), :] + lprecv[...]
            return own + jnp.concatenate([ap[t : t + 1, :] for t in range(NT)], axis=1)

        def block(s):
            return kbuf[pl.ds(s * TB, TB)].reshape(JT, NT, S, L)

        def weighted(kk, u):
            w = (kk[:, 0] * u[0] + kk[:, 1] * u[1]) + (kk[:, 2] * u[2] + kk[:, 3] * u[3])
            return jnp.sum(w, axis=2, keepdims=True)

        def passes(u, rescale=False, last=False, par=0):
            def place(g):
                if last:
                    return g * GS + CS
                return g * GS + 2 * CS if not isinstance(g, int) or g < NE else (g - NE) * GS

            def one(at, buf):
                for k in range(GS):
                    p = at + k
                    kk = block(p)
                    if rescale:
                        kk = kk * fb[:, pl.ds(p, 1), :][None]
                        kbuf[pl.ds(p * TB, TB)] = kk.reshape(TB, S, L)
                    cbuf[buf, k] = qrep[p] / jnp.broadcast_to(weighted(kk, u), (JT, S, L))

            def two(at, buf, acc):
                for k in range(GS):
                    p = at + k
                    v = cbuf[buf, k]
                    kk = block(p)
                    if last:
                        vbuf[p - CS] = v
                        t = (kk * u[None]) * v[:, None]
                        flat = jnp.concatenate([t[:, i].reshape(JB, L) for i in range(NT)], axis=1)
                        tt[pl.ds(pl.multiple_of((p - CS) * JB, JB), JB), :] = flat.astype(BF16)
                    else:
                        acc = acc + jnp.sum(kk * v[:, None], axis=0)
                return acc

            def run(a, b, end):
                shift = place(a) - a * GS
                even, odd = a % 2, (a + 1) % 2
                pairs = max(0, (b - a - 1) // 2)

                def both(n, acc):
                    at = (a + 2 * n) * GS + shift
                    one(at + GS, odd)
                    acc = two(at, even, acc)
                    one(at + 2 * GS, even)
                    return two(at + GS, odd, acc)

                acc = lax.fori_loop(0, pairs, both, jnp.zeros((NT, S, L), F32))
                for g in range(a + 2 * pairs, b):
                    if g + 1 < end:
                        one(place(g + 1), (g + 1) % 2)
                    acc = two(place(g), g % 2, acc)
                return acc

            one(place(0), 0)
            if last:
                run(0, CH // GS, CH // GS)
                return None
            xs[par] = run(0, NE, NE + NC)
            copy = to_partner(xs.at[par], xr.at[par], x_ssem.at[par], x_rsem.at[par])
            copy.start()
            acc = run(NE, NE + NC, NE + NC)
            copy.wait()
            total = jnp.sum((xs[par] + xr[par]) + acc, axis=1, keepdims=True)
            return pv[...] / jnp.broadcast_to(total, (NT, S, L))

        def outer(r, carry):
            scale = 1.4426950408889634 / eps_ref[r]
            cost = costs()
            for jt in range(JT):
                for t in range(NT):
                    land[CS * TB + jt * NT + t] = cost[jt * S : jt * S + S, t * L : t * L + L]

            def exps(p):
                ll = land[p * TB : p * TB + TB].reshape(JT, NT, S, L)
                low = jnp.min(jnp.min(ll, axis=0), axis=1, keepdims=True)
                kk = jnp.exp2((low[None] - ll) * scale)
                kbuf[p * TB : p * TB + TB] = kk.reshape(TB, S, L)
                mb[:, p : p + 1, :] = low
                sb[:, p : p + 1, :] = jnp.sum(jnp.sum(kk, axis=0), axis=1, keepdims=True)

            def passed_on(s):
                return to_partner(
                    land.at[pl.ds((CS + s) * TB, TB)], land.at[pl.ds(s * TB, TB)], fwd_ssem.at[0], fwd_rsem.at[s]
                )

            def on_slot(op, s):
                if op == "slot":
                    if s < CS:
                        passed_on(s).start()
                    exps(CS + s)
                else:
                    passed_on(s).wait_recv()
                    exps(s)

            with jax.named_scope("gather"):
                pl.semaphore_wait(credit, NL)

                def idle(n, c):
                    pad[...] = pad[...] + 1.0
                    return c

                with jax.named_scope("hold"):
                    lax.fori_loop(0, core * HOLD, idle, 0)
                first = [(0, lambda: on_slot("slot", 0)), (len(plan["msgs"]) // 4, lambda: on_slot("partner", 0))]
                tree(land, TB, CS, plan, on_slot=on_slot, fillers=first)
                tree_sent(land, plan)
                ref = land.at[pl.ds(0, CS * TB)]
                pltpu.make_async_copy(ref, ref, fwd_ssem.at[0]).wait()
                give_credit()

            with jax.named_scope("minx"):
                def least_of(a, b):
                    low = jnp.min(mb[:, a:b], axis=1, keepdims=True)
                    part = jnp.sum(sb[:, a:b] * jnp.exp2((low - mb[:, a:b]) * scale), axis=1, keepdims=True)
                    return jnp.broadcast_to(low, (NT, S, L)), jnp.broadcast_to(part, (NT, S, L))

                mss[0], mss[1] = least_of(2 * CS, NP)
                copy = to_partner(mss, msr, ms_sem.at[0], ms_sem.at[1])
                copy.start()
                low, part = least_of(0, 2 * CS)
                copy.wait()
                least = jnp.minimum(jnp.minimum(mss[0], msr[0]), low)
                total = mss[1] * jnp.exp2((least - mss[0]) * scale) + msr[1] * jnp.exp2((least - msr[0]) * scale)
                total = total + part * jnp.exp2((least - low) * scale)
                fb[...] = jnp.exp2((least[:, :1] - mb[...]) * scale)
                u = pv[...] / total

            with jax.named_scope("pass1"):
                u = passes(u, rescale=True, par=1)

            def sweep(t, u):
                return passes(u, par=lax.rem(t, 2))

            with jax.named_scope("sweeps"):
                u = lax.fori_loop(2, sweeps, sweep, u)
            with jax.named_scope("lastpass"):
                passes(u, last=True)
            ub[...] = u
            bacc[...] = jnp.zeros_like(bacc)
            with jax.named_scope("mm"):
                lax.fori_loop(0, KJ // CM, chunk, 0)
                finish_lp()
            return carry

        lax.fori_loop(0, steps, outer, 0)

        pl.semaphore_wait(credit, NL)
        cost = costs()
        plan_own = (block(CS) * ub[...][None]) * vbuf[0][:, None]
        total = jnp.zeros((S, L), F32)
        for jt in range(JT):
            for t in range(NT):
                total = total + cost[jt * S : jt * S + S, t * L : t * L + L] * plan_own[jt, t]
        loss_rows[0:1] = jnp.sum(total, axis=0, keepdims=True)

        def to_chip(n):
            o = CH - n
            off = (lax.rem(o, X), lax.rem(lax.div(o, X), Y), lax.div(o, X * Y))
            at = [lax.rem(pos[d] + off[d], dims[d]) for d in range(3)]
            return pltpu.make_async_remote_copy(
                src_ref=loss_rows.at[pl.ds(0, 1)], dst_ref=loss_rows.at[pl.ds(o, 1)],
                send_sem=loss_sem.at[0], recv_sem=loss_sem.at[1],
                device_id=core * CH + at[0] + X * at[1] + X * Y * at[2], device_id_type=FLAT,
            )

        def tell(n, carry):
            to_chip(n).start()
            return carry

        lax.fori_loop(1, CH, tell, 0)

        it = lax.div(chip * NR, L)
        inside = pl.multiple_of(lax.rem(chip * NR, L), S)

        def rows_of(n, carry):
            for k in range(4):
                s = 4 * n + k
                kk = jnp.concatenate([kbuf[(CS + s) * TB + jt * NT + it] for jt in range(JT)], axis=0)
                uu = jnp.concatenate([ub[it]] * JT, axis=0)
                t = (kk * uu) * vbuf[s].reshape(JB, L)
                none = jnp.zeros_like(t)
                both = jnp.where(core == 0, jnp.concatenate([t, none], axis=0), jnp.concatenate([none, t], axis=0))
                trb[k] = both.T
                obuf[source_of(s)] = trb[k, pl.ds(inside, NR), :]
            return carry

        with jax.named_scope("tail"):
            lax.fori_loop(0, CH // 4, rows_of, 0)
            o_copy = to_partner(obuf.at[pl.ds(other * HB, HB)], orecv, o_sem.at[0], o_sem.at[1])
            o_copy.start()
            o_copy.wait()
            for b in range(HB):
                out_ref[:, b * L : b * L + L] = obuf[core * HB + b] + orecv[b]
            ref = loss_rows.at[pl.ds(1, CH - 1)]
            pltpu.make_async_copy(ref, ref, loss_sem.at[0]).wait()
            pltpu.make_async_copy(ref, ref, loss_sem.at[1]).wait()
            loss_two[0:1] = jnp.sum(loss_rows[...], axis=0, keepdims=True)
            copy = to_partner(loss_two.at[pl.ds(0, 1)], loss_two.at[pl.ds(1, 1)], loss_sem.at[2], loss_sem.at[3])
            copy.start()
            copy.wait()
            loss_ref[0] = jnp.sum(loss_two[...])

    vm = pltpu.VMEM
    dma = pltpu.SemaphoreType.DMA
    scratch = [
        vm((NP * TB, S, L), F32),
        vm((NP * TB, S, L), F32),
        vm((CH * TT0, 16, L), BF16),
        vm((KJ, n_rows), BF16),
        vm((n_rows, n_rows), F32),
        vm((n_rows, n_rows), BF16),
        vm((CH, L, L), BF16),
        vm((L, KJ), BF16),
        vm((L, n_rows), F32),
        vm((L, n_rows), F32),
        vm((JB, n_rows), F32),
        vm((L, L), F32),
        vm((CH, L), F32),
        vm((NP, JT, S, L), F32),
        vm((CH, JT, S, L), F32),
        vm((2, GS, JT, S, L), F32),
        vm((NT, NP, L), F32),
        vm((NT, NP, L), F32),
        vm((NT, NP, L), F32),
        vm((NT, S, L), F32),
        vm((S, L), F32),
        vm((2, NT, S, L), F32),
        vm((2, NT, S, L), F32),
        vm((2, NT, S, L), F32),
        vm((2, NT, S, L), F32),
        vm((NT, S, L), F32),
        vm((3, S, L), F32),
        vm((3, 3, S, L), F32),
        vm((S, L), F32),
        vm((S, L), F32),
        vm((CH, NR, L), F32),
        vm((HB, NR, L), F32),
        vm((4, L, L), F32),
        vm((CH, L), F32),
        vm((2, L), F32),
        vm((S, L), F32),
        dma((NL,)),
        dma((max(len(plan["msgs"]), len(plan0["msgs"])),)),
        dma((1,)),
        dma((CS,)),
        pltpu.SemaphoreType.REGULAR,
        dma((2,)),
        dma((2,)),
        dma((2,)),
        dma((2,)),
        dma((2,)),
        dma((2,)),
        dma((2,)),
        dma((3, 3)),
        dma((3, 3)),
        dma((2,)),
        dma((2,)),
        dma((4,)),
    ]
    return kernel, scratch


def solution(mesh):
    chips = mesh.shape["rows"]
    dims = torus_of(chips)
    grid_spec = P(("pairs", "rows"), "cols")

    def local_fn(c1, c2, t0, p, q, eps):
        n_rows, n_cols = p.shape[0] * chips, q.shape[0] * mesh.shape["cols"]
        kernel, scratch = make_kernel(dims, n_rows, n_cols, eps.shape[0], SWEEPS)
        vmem = pl.BlockSpec(memory_space=pltpu.VMEM)
        smem = pl.BlockSpec(memory_space=pltpu.SMEM)
        return pl.pallas_call(
            kernel,
            name="gromov",
            out_shape=(jax.ShapeDtypeStruct(t0.shape, F32), jax.ShapeDtypeStruct((1,), F32)),
            in_specs=[smem, smem, vmem, vmem, vmem, vmem],
            out_specs=(vmem, smem),
            scratch_shapes=scratch,
            compiler_params=pltpu.CompilerParams(
                collective_id=0, has_side_effects=True, vmem_limit_bytes=60 * 1024 * 1024
            ),
        )(eps, p, c1, c2, t0, q.reshape(chips // 2, L))

    return jax.shard_map(
        local_fn,
        mesh=mesh,
        in_specs=(grid_spec, grid_spec, grid_spec, P(("pairs", "rows")), P(("pairs", "cols")), P("pairs")),
        out_specs=(grid_spec, P("pairs")),
        check_vma=False,
    )
```

```python
import heapq
import itertools
import math

import jax
import jax.numpy as jnp
from jax import lax
from jax.experimental import pallas as pl
from jax.experimental.pallas import tpu as pltpu
from jax.sharding import PartitionSpec as P

SWEEPS = 10
FLAT = pl.DeviceIdType.LOGICAL
L, S = 128, 8
JB = 64
JT = JB // S
F32, BF16 = jnp.float32, jnp.bfloat16
ORDERS = ((0, 1, 2), (1, 2, 0), (2, 0, 1))
TILE_RATE = 11.4
HOP_US = 3.2
AHEAD_US = 3.0
LOG2E = 1.4426950216293335
LOG2E_REST = 1.925963e-8
HOLD = 0
PARTNER_US = 4.0
LATE = 165


def torus_of(chips):
    return {64: (4, 4, 4), S: (4, 2, 1), 16: (4, 4, 1)}[chips]


def halves(x):
    c = 4097.0 * x
    high = c - (c - x)
    return high, x - high


def quotient(a, b):
    q = a / b
    return q + (a - q * b) / b


def split3(n):
    cuts = [0, (n + 2) // 3, (2 * n + 2) // 3, n]
    return [(cuts[k], cuts[k + 1]) for k in range(3)]


def tree_plan(dims, tiles, rate, lat_us, ahead_us, shared=0):
    rings = {1: (), 2: ((1, "f", 1),), 4: ((1, "f", 1), (3, "f", -1), (2, "a", 1), (2, "b", -1))}
    msgs = []
    for color, order in enumerate(ORDERS):
        lo, hi = split3(tiles)[color]
        for dst in itertools.product(*(range(n) for n in dims)):
            used = [k for k in range(3) if dst[order[k]]]
            if not used or lo == hi:
                continue
            d = order[used[-1]]
            mid = lo + (hi - lo + (sum(dst) + color) % 2) // 2
            for at, part, sign in rings[dims[d]]:
                a, b = {"f": (lo, hi), "a": (lo, mid), "b": (mid, hi)}[part]
                if at != dst[d] or a == b:
                    continue
                src = list(dst)
                src[d] = (src[d] - sign) % dims[d]
                m = dict(id=len(msgs), color=color, src=tuple(src), dst=dst, link=(d, sign), lo=a, hi=b)
                m["us"] = (b - a) / rate
                msgs.append(m)
    into = {}
    for m in msgs:
        into.setdefault((m["color"], m["dst"]), []).append(m)
    users = [[] for _ in msgs]
    missing = []
    for m in msgs:
        deps = [e for e in into.get((m["color"], m["src"]), []) if e["lo"] < m["hi"] and m["lo"] < e["hi"]]
        missing.append(len(deps))
        for e in deps:
            users[e["id"]].append(m)
    way = {}

    def way_of(m):
        if m["id"] not in way:
            way[m["id"]] = m["us"] + lat_us + max([way_of(u) for u in users[m["id"]]], default=0.0)
        return way[m["id"]]

    links = sorted({m["link"] for m in msgs})
    queue = {k: [] for k in links}
    idle = dict.fromkeys(links, True)
    ready, events, ops = {}, [], []

    def put(m, now):
        ready[m["id"]] = now
        heapq.heappush(queue[m["link"]], (-way_of(m), m["id"]))

    def start(link, now):
        if idle[link] and queue[link]:
            k = heapq.heappop(queue[link])[1]
            idle[link] = False
            ops.append((max(ready[k], now - ahead_us), 1, "send", msgs[k]))
            heapq.heappush(events, (now + msgs[k]["us"], 0, k))
            heapq.heappush(events, (now + msgs[k]["us"] + lat_us, 1, k))

    for m in msgs:
        if not missing[m["id"]]:
            put(m, 0.0)
    for link in links:
        start(link, 0.0)
    left = {}
    for m in msgs:
        left[m["dst"]] = left.get(m["dst"], 0) + 1
    now = 0.0
    while events:
        now, arrived, k = heapq.heappop(events)
        m = msgs[k]
        if not arrived:
            idle[m["link"]] = True
            start(m["link"], now)
            continue
        ops.append((now, 0, "wait", m))
        for u in users[k]:
            missing[u["id"]] -= 1
            if not missing[u["id"]]:
                put(u, now)
                start(u["link"], now)
        left[m["dst"]] -= 1
        if not left[m["dst"]]:
            slot = m["dst"][0] + dims[0] * (m["dst"][1] + dims[1] * m["dst"][2])
            ops.append((now, 0, "slot", slot))
            if slot < shared:
                ops.append((now + PARTNER_US, 0, "partner", slot))
    ops.sort(key=lambda op: op[:2])
    totals = {k: sum(m["hi"] - m["lo"] for m in msgs if m["link"] == k) for k in links}
    return dict(msgs=msgs, ops=[op[2:] for op in ops], links=links, totals=totals, end=now)


def make_kernel(dims, n_rows, n_cols, steps, sweeps):
    X, Y, Z = dims
    CH = X * Y * Z
    NR = n_rows // CH
    G = NR // S
    NT = n_rows // L
    TB = JT * NT
    HB = CH // 2
    JN = n_cols // 2 // L
    JW = JN // 2
    NT0 = G * JW
    TT0 = NT0 + 2 * G
    KJ = CH * JB
    CK = min(1024, KJ)
    CM = min(2048, KJ)
    GS = min(4, CH // 2)
    CS = max(CH * 3 // 8 // GS * GS, GS)
    NP = CH + CS
    NE, NC = (CH - CS) // GS, 2 * CS // GS
    assert NT == 4 and n_cols == CH * L and JN == HB
    plan0 = tree_plan(dims, TT0, TILE_RATE, HOP_US, AHEAD_US)
    plan = tree_plan(dims, TB, TILE_RATE, HOP_US, AHEAD_US, CS)
    links = plan["links"]
    NL = len(links)
    peers = [(d, k) for d in range(3) for k in range(1, dims[d])]
    strides = (1, X, X * Y)

    def slot_of(offset):
        return offset[0] + X * offset[1] + X * Y * offset[2]

    def kernel(
        eps_ref, p_ref, c1_ref, c2_ref, t0_ref, q_ref,
        out_ref, loss_ref,
        land, kbuf, g0, tt, c1f, c1b, c2n, c2p, bacc, lp, lprecv, bp, qf, qrep, vbuf, cbuf,
        mb, sb, fb, ub, ap, xs, xr, mss, msr, pv, ars, arr, arps, arpr, obuf, orecv, trb, loss_rows, loss_two, pad,
        send_sem, recv_sem, fwd_ssem, fwd_rsem, credit, x_ssem, x_rsem, ms_sem, lp_sem, c1_sem, c2_sem, q_sem, ar_ssem, ar_rsem, arp_sem, o_sem, loss_sem,
    ):
        chip = lax.axis_index("rows")
        core = lax.axis_index("cols")
        other = 1 - core
        pos = (lax.rem(chip, X), lax.rem(lax.div(chip, X), Y), lax.div(chip, X * Y))

        me = core * CH + chip
        partner = other * CH + chip

        def moved(d, k):
            return me + (lax.rem(pos[d] + k + dims[d], dims[d]) - pos[d]) * strides[d]

        near = {link: moved(*link) for link in links}

        def source_of(slot):
            off = (lax.rem(slot, X), lax.rem(lax.div(slot, X), Y), lax.div(slot, X * Y))
            at = [lax.rem(pos[d] + dims[d] - off[d], dims[d]) for d in range(3)]
            return at[0] + X * at[1] + X * Y * at[2]

        def to_partner(src, dst, ssem, rsem):
            return pltpu.make_async_remote_copy(
                src_ref=src, dst_ref=dst, send_sem=ssem, recv_sem=rsem,
                device_id=partner, device_id_type=FLAT,
            )

        def tree_copy(buf, width, first, m):
            n = m["hi"] - m["lo"]
            return pltpu.make_async_remote_copy(
                src_ref=buf.at[pl.ds((first + slot_of(m["src"])) * width + m["lo"], n)],
                dst_ref=buf.at[pl.ds((first + slot_of(m["dst"])) * width + m["lo"], n)],
                send_sem=send_sem.at[links.index(m["link"])],
                recv_sem=recv_sem.at[m["id"]],
                device_id=near[m["link"]],
                device_id_type=FLAT,
            )

        def tree(buf, width, first, the_plan, before_send=None, on_slot=None, fillers=()):
            fillers, ready, waits = list(fillers), [], 0
            for op, m in the_plan["ops"]:
                if op == "send":
                    if before_send is not None:
                        before_send(m)
                    tree_copy(buf, width, first, m).start()
                elif op == "wait":
                    while fillers and not fillers[0][0]:
                        fillers.pop(0)[1]()
                    ref = buf.at[pl.ds((first + slot_of(m["dst"])) * width + m["lo"], m["hi"] - m["lo"])]
                    pltpu.make_async_copy(ref, ref, recv_sem.at[m["id"]]).wait()
                    waits += 1
                    if ready:
                        on_slot(*ready.pop(0))
                    elif fillers and waits >= fillers[0][0]:
                        fillers.pop(0)[1]()
                elif on_slot is not None:
                    ready.append((op, m))
            for at in ready:
                on_slot(*at)
            for _, f in fillers:
                f()

        def tree_sent(buf, the_plan):
            for k, link in enumerate(links):
                n = the_plan["totals"][link]
                ref = buf.at[pl.ds(0, n)]
                pltpu.make_async_copy(ref, ref, send_sem.at[k]).wait()

        def give_credit():
            for d, sign in links:
                pl.semaphore_signal(credit, inc=1, device_id=moved(d, -sign), device_id_type=FLAT)

        def all_sum_send(stage):
            for n, k in enumerate(range(1, dims[stage])):
                pltpu.make_async_remote_copy(
                    src_ref=ars.at[stage], dst_ref=arr.at[stage, n],
                    send_sem=ar_ssem.at[stage, n], recv_sem=ar_rsem.at[stage, n],
                    device_id=moved(stage, k), device_id_type=FLAT,
                ).start()

        def all_sum_get(stage):
            total = ars[stage]
            for n, k in enumerate(range(1, dims[stage])):
                pltpu.make_async_remote_copy(
                    src_ref=ars.at[stage], dst_ref=arr.at[stage, n],
                    send_sem=ar_ssem.at[stage, n], recv_sem=ar_rsem.at[stage, n],
                    device_id=moved(stage, k), device_id_type=FLAT,
                ).wait()
                total = total + arr[stage, n]
            return total

        def all_sum_step(stage):
            total = all_sum_get(stage)
            if stage < 2:
                ars[stage + 1] = total
                all_sum_send(stage + 1)
            else:
                arps[...] = total
                to_partner(arps, arpr, arp_sem.at[0], arp_sem.at[1]).start()

        pad[...] = jnp.zeros_like(pad)
        barrier = pltpu.get_barrier_semaphore()
        for d, k in peers:
            pl.semaphore_signal(barrier, inc=1, device_id=moved(d, k), device_id_type=FLAT)
        pl.semaphore_signal(barrier, inc=1, device_id=partner, device_id_type=FLAT)

        row = lax.broadcasted_iota(jnp.int32, (S, L), 0)
        lane = lax.broadcasted_iota(jnp.int32, (S, L), 1)

        for g in range(G):
            rows = slice(g * S, g * S + S)
            pair = jnp.concatenate([c1_ref[rows, :L], c1_ref[rows, L:]], axis=0)
            g0[NT0 + core * G + g] = pair.astype(BF16)
        c1_copy = to_partner(
            g0.at[pl.ds(NT0 + core * G, G)], g0.at[pl.ds(NT0 + core * G, G)], c1_sem.at[0], c1_sem.at[1]
        )
        q_copy = to_partner(q_ref, qf.at[pl.ds(core * HB, HB)], q_sem.at[0], q_sem.at[1])

        tile = jnp.zeros((S, L), F32)
        for t in range(2):
            part = jnp.zeros((1, L), F32)
            for k in range(NR):
                entry = c1_ref[k : k + 1, t * L : t * L + L]
                part = part + entry * entry * p_ref[k]
            tile = jnp.where(row == 2 * core + t, jnp.broadcast_to(part, (S, L)), tile)
        where = (row - 4) * L + lane
        for k in range(NR):
            tile = jnp.where(where == chip * NR + k, p_ref[k], tile)
        ars[0] = tile
        for g in range(G):
            rows = slice(g * S, g * S + S)
            for t in range(JW):
                a, b = t0_ref[rows, (2 * L) * t : (2 * L) * t + L], t0_ref[rows, (2 * L) * t + L : (2 * L) * t + (2 * L)]
                g0[g * JW + t] = jnp.concatenate([a, b], axis=0).astype(BF16)
        qf[pl.ds(core * HB, HB)] = q_ref[...]

        c2_copy = to_partner(c2n.at[pl.ds(core * HB, HB)], c2n.at[pl.ds(core * HB, HB)], c2_sem.at[0], c2_sem.at[1])
        bp[...] = jnp.zeros_like(bp)

        def round_c2(first, last):
            for t in range(first, last):
                blk = c2_ref[:, t * L : t * L + L]
                c2n[core * HB + t] = blk.astype(BF16)
                bp[...] += blk * blk * q_ref[t : t + 1, :]

        def finish_b():
            bp[...] = jnp.broadcast_to(jnp.sum(bp[...], axis=1, keepdims=True), (L, L))

        with jax.named_scope("barrier"):
            pl.semaphore_wait(barrier, len(peers) + 1)
        give_credit()
        c1_copy.start()
        q_copy.start()
        all_sum_send(0)

        src = lax.broadcasted_iota(jnp.int32, (L, L), 0)
        dst = lax.broadcasted_iota(jnp.int32, (L, L), 1)
        picks = [
            jnp.where((src - core * JB == dst - h * JB) & (dst >= h * JB) & (dst < h * JB + JB), 1.0, 0.0).astype(BF16)
            for h in range(2)
        ]

        def order_c2(first, last):
            for t in range(first, last):
                a = jnp.dot(c2n[source_of(2 * t)], picks[0], preferred_element_type=F32)
                b = jnp.dot(c2n[source_of(2 * t + 1)], picks[1], preferred_element_type=F32)
                c2p[:, t * L : t * L + L] = (a + b).astype(BF16)

        def order_q(first, last):
            def four(n, carry):
                for k in range(4):
                    p = 4 * n + k
                    shared = p < CS
                    half = jnp.where(shared, other, core)
                    line = jnp.broadcast_to(qf[pl.ds(source_of(jnp.where(shared, p, p - CS)), 1), :], (S, L))
                    for jt in range(JT):
                        own = jnp.where(lane == half * JB + jt * S + row, line, 0.0)
                        qrep[p, jt] = jnp.broadcast_to(jnp.sum(own, axis=1, keepdims=True), (S, L))
                return carry

            lax.fori_loop(first // 4, last // 4, four, 0)

        def span(n, parts, f):
            cuts = [n * k // parts for k in range(parts + 1)]
            return [lambda a=a, b=b: f(a, b) for a, b in zip(cuts, cuts[1:])]

        fillers = [(0, lambda: round_c2(0, HB)), (0, finish_b), (0, lambda: c2_copy.start())]
        fillers += [(0, lambda: q_copy.wait()), (0, lambda: order_q(0, NP)), (LATE // 2, lambda: all_sum_step(0))]
        fillers += [(LATE, lambda: c2_copy.wait())]
        fillers += [(LATE + 4 * n, f) for n, f in enumerate(span(CH // 2, S, order_c2))]
        fillers += [(LATE + JB // 2, lambda: all_sum_step(1))]
        waited = []

        def before_send(m):
            if not waited and m["hi"] > NT0:
                waited.append(1)
                c1_copy.wait()

        def unpack(op, s):
            chip_s = source_of(s)
            for g in range(G):
                tiles = g0[s * TT0 + g * JW : s * TT0 + g * JW + JW].astype(F32).reshape(JN, S, L)
                kbuf[pl.ds((chip_s * G + g) * JN, JN)] = tiles
                at = pl.ds(pl.multiple_of(chip_s * NR + g * S, S), S)
                for h in range(2):
                    pair = g0[s * TT0 + NT0 + h * G + g].astype(F32)
                    c1f[at, 2 * L * h : 2 * L * h + L] = pair[:S]
                    c1f[at, 2 * L * h + L : 2 * L * h + 2 * L] = pair[S:]

        with jax.named_scope("gather0"):
            first = [(0, lambda: unpack("slot", 0))]
            tree(g0, TT0, 0, plan0, before_send=before_send, on_slot=unpack, fillers=first + fillers)
            tree_sent(g0, plan0)
            c1b[...] = c1f[...].astype(BF16)
            all_sum_step(2)

        def finish_lp():
            lp[...] = jnp.concatenate([bp[...]] * NT, axis=1) - 2.0 * bacc[...]

        bacc[...] = jnp.zeros_like(bacc)
        JC = CK // L

        def first_chunk(n, carry):
            cols = []
            for t in range(JC):
                cols.append(kbuf[pl.ds(n * JC + t, CH * G, stride=JN)].reshape(n_rows, L))
            plan_c = jnp.concatenate(cols, axis=1).astype(BF16)
            lead = jnp.dot(c1b[...], plan_c, preferred_element_type=F32).astype(BF16)
            c2c = jnp.concatenate([c2n[core * HB + n * JC + t] for t in range(JC)], axis=1)
            bacc[...] += lax.dot_general(c2c, lead, (((1,), (1,)), ((), ())), preferred_element_type=F32)
            return carry

        with jax.named_scope("firstmm"):
            lax.fori_loop(0, KJ // CK, first_chunk, 0)
            finish_lp()
        to_partner(arps, arpr, arp_sem.at[0], arp_sem.at[1]).wait()
        ap[...] = jnp.where(row < 4, arps[...] + arpr[...], arps[...])
        for t in range(NT):
            pv[t] = jnp.broadcast_to(ap[4 + t : 5 + t, :], (S, L))


        def chunk(n, carry):
            at = pl.ds(pl.multiple_of(n * CM, CM), CM)
            lead = jnp.dot(tt[at, :], c1b[...], preferred_element_type=F32).astype(BF16)
            bacc[...] += jnp.dot(c2p[:, at], lead, preferred_element_type=F32)
            return carry

        def costs():
            copy = to_partner(lp.at[pl.ds(other * JB, JB)], lprecv, lp_sem.at[0], lp_sem.at[1])
            copy.start()
            copy.wait()
            own = lp[pl.ds(pl.multiple_of(core * JB, JB), JB), :] + lprecv[...]
            return own + jnp.concatenate([ap[t : t + 1, :] for t in range(NT)], axis=1)

        def block(s):
            return kbuf[pl.ds(s * TB, TB)].reshape(JT, NT, S, L)

        def weighted(kk, u):
            w = (kk[:, 0] * u[0] + kk[:, 1] * u[1]) + (kk[:, 2] * u[2] + kk[:, 3] * u[3])
            return jnp.sum(w, axis=2, keepdims=True)

        def passes(u, rescale=False, last=False, par=0):
            def place(g):
                if last:
                    return g * GS + CS
                return g * GS + 2 * CS if not isinstance(g, int) or g < NE else (g - NE) * GS

            def one(at, buf):
                for k in range(GS):
                    p = at + k
                    kk = block(p)
                    if rescale:
                        kk = kk * fb[:, pl.ds(p, 1), :][None]
                        kbuf[pl.ds(p * TB, TB)] = kk.reshape(TB, S, L)
                    c = jnp.broadcast_to(weighted(kk, u), (JT, S, L))
                    cbuf[buf, k] = quotient(qrep[p], c) if last else qrep[p] / c

            def two(at, buf, acc):
                for k in range(GS):
                    p = at + k
                    v = cbuf[buf, k]
                    kk = block(p)
                    if last:
                        vbuf[p - CS] = v
                        t = (kk * u[None]) * v[:, None]
                        flat = jnp.concatenate([t[:, i].reshape(JB, L) for i in range(NT)], axis=1)
                        tt[pl.ds(pl.multiple_of((p - CS) * JB, JB), JB), :] = flat.astype(BF16)
                    else:
                        acc = acc + jnp.sum(kk * v[:, None], axis=0)
                return acc

            def run(a, b, end):
                shift = place(a) - a * GS
                even, odd = a % 2, (a + 1) % 2
                pairs = max(0, (b - a - 1) // 2)

                def both(n, acc):
                    at = (a + 2 * n) * GS + shift
                    one(at + GS, odd)
                    acc = two(at, even, acc)
                    one(at + 2 * GS, even)
                    return two(at + GS, odd, acc)

                acc = lax.fori_loop(0, pairs, both, jnp.zeros((NT, S, L), F32))
                for g in range(a + 2 * pairs, b):
                    if g + 1 < end:
                        one(place(g + 1), (g + 1) % 2)
                    acc = two(place(g), g % 2, acc)
                return acc

            one(place(0), 0)
            if last:
                run(0, CH // GS, CH // GS)
                return None
            xs[par] = run(0, NE, NE + NC)
            copy = to_partner(xs.at[par], xr.at[par], x_ssem.at[par], x_rsem.at[par])
            copy.start()
            acc = run(NE, NE + NC, NE + NC)
            copy.wait()
            total = jnp.sum((xs[par] + xr[par]) + acc, axis=1, keepdims=True)
            return quotient(pv[...], jnp.broadcast_to(total, (NT, S, L)))

        def outer(r, carry):
            eps = eps_ref[r]
            inv = 1.0 / eps
            inv = inv * (2.0 - eps * inv)
            main = LOG2E * inv
            (e0, e1), (m0, m1) = halves(eps), halves(main)
            prod = eps * main
            low_part = ((e0 * m0 - prod) + (e0 * m1 + e1 * m0)) + e1 * m1
            rest = (((LOG2E - prod) - low_part) + LOG2E_REST) * inv

            def decay(x):
                return jnp.exp2(x * main + x * rest)

            cost = costs()
            for jt in range(JT):
                for t in range(NT):
                    land[CS * TB + jt * NT + t] = cost[jt * S : jt * S + S, t * L : t * L + L]

            def exps(p):
                ll = land[p * TB : p * TB + TB].reshape(JT, NT, S, L)
                low = jnp.min(jnp.min(ll, axis=0), axis=1, keepdims=True)
                kk = decay(low[None] - ll)
                kbuf[p * TB : p * TB + TB] = kk.reshape(TB, S, L)
                mb[:, p : p + 1, :] = low
                sb[:, p : p + 1, :] = jnp.sum(jnp.sum(kk, axis=0), axis=1, keepdims=True)

            def passed_on(s):
                return to_partner(
                    land.at[pl.ds((CS + s) * TB, TB)], land.at[pl.ds(s * TB, TB)], fwd_ssem.at[0], fwd_rsem.at[s]
                )

            def on_slot(op, s):
                if op == "slot":
                    if s < CS:
                        passed_on(s).start()
                    exps(CS + s)
                else:
                    passed_on(s).wait_recv()
                    exps(s)

            with jax.named_scope("gather"):
                pl.semaphore_wait(credit, NL)

                def idle(n, c):
                    pad[...] = pad[...] + 1.0
                    return c

                with jax.named_scope("hold"):
                    lax.fori_loop(0, core * HOLD, idle, 0)
                first = [(0, lambda: on_slot("slot", 0)), (len(plan["msgs"]) // 4, lambda: on_slot("partner", 0))]
                tree(land, TB, CS, plan, on_slot=on_slot, fillers=first)
                tree_sent(land, plan)
                ref = land.at[pl.ds(0, CS * TB)]
                pltpu.make_async_copy(ref, ref, fwd_ssem.at[0]).wait()
                give_credit()

            with jax.named_scope("minx"):
                def least_of(a, b):
                    low = jnp.min(mb[:, a:b], axis=1, keepdims=True)
                    part = jnp.sum(sb[:, a:b] * decay(low - mb[:, a:b]), axis=1, keepdims=True)
                    return jnp.broadcast_to(low, (NT, S, L)), jnp.broadcast_to(part, (NT, S, L))

                mss[0], mss[1] = least_of(2 * CS, NP)
                copy = to_partner(mss, msr, ms_sem.at[0], ms_sem.at[1])
                copy.start()
                low, part = least_of(0, 2 * CS)
                copy.wait()
                least = jnp.minimum(jnp.minimum(mss[0], msr[0]), low)
                total = mss[1] * decay(least - mss[0]) + msr[1] * decay(least - msr[0])
                total = total + part * decay(least - low)
                fb[...] = decay(least[:, :1] - mb[...])
                u = quotient(pv[...], total)

            with jax.named_scope("pass1"):
                u = passes(u, rescale=True, par=1)

            def sweep(t, u):
                return passes(u, par=lax.rem(t, 2))

            with jax.named_scope("sweeps"):
                u = lax.fori_loop(2, sweeps, sweep, u)
            with jax.named_scope("lastpass"):
                passes(u, last=True)
            ub[...] = u
            bacc[...] = jnp.zeros_like(bacc)
            with jax.named_scope("mm"):
                lax.fori_loop(0, KJ // CM, chunk, 0)
                finish_lp()
            return carry

        lax.fori_loop(0, steps, outer, 0)

        pl.semaphore_wait(credit, NL)
        cost = costs()
        plan_own = (block(CS) * ub[...][None]) * vbuf[0][:, None]
        total = jnp.zeros((S, L), F32)
        for jt in range(JT):
            for t in range(NT):
                total = total + cost[jt * S : jt * S + S, t * L : t * L + L] * plan_own[jt, t]
        loss_rows[0:1] = jnp.sum(total, axis=0, keepdims=True)

        def to_chip(n):
            o = CH - n
            off = (lax.rem(o, X), lax.rem(lax.div(o, X), Y), lax.div(o, X * Y))
            at = [lax.rem(pos[d] + off[d], dims[d]) for d in range(3)]
            return pltpu.make_async_remote_copy(
                src_ref=loss_rows.at[pl.ds(0, 1)], dst_ref=loss_rows.at[pl.ds(o, 1)],
                send_sem=loss_sem.at[0], recv_sem=loss_sem.at[1],
                device_id=core * CH + at[0] + X * at[1] + X * Y * at[2], device_id_type=FLAT,
            )

        def tell(n, carry):
            to_chip(n).start()
            return carry

        lax.fori_loop(1, CH, tell, 0)

        it = lax.div(chip * NR, L)
        inside = pl.multiple_of(lax.rem(chip * NR, L), S)

        def rows_of(n, carry):
            for k in range(4):
                s = 4 * n + k
                kk = jnp.concatenate([kbuf[(CS + s) * TB + jt * NT + it] for jt in range(JT)], axis=0)
                uu = jnp.concatenate([ub[it]] * JT, axis=0)
                t = (kk * uu) * vbuf[s].reshape(JB, L)
                none = jnp.zeros_like(t)
                both = jnp.where(core == 0, jnp.concatenate([t, none], axis=0), jnp.concatenate([none, t], axis=0))
                trb[k] = both.T
                obuf[source_of(s)] = trb[k, pl.ds(inside, NR), :]
            return carry

        with jax.named_scope("tail"):
            lax.fori_loop(0, CH // 4, rows_of, 0)
            o_copy = to_partner(obuf.at[pl.ds(other * HB, HB)], orecv, o_sem.at[0], o_sem.at[1])
            o_copy.start()
            o_copy.wait()
            for b in range(HB):
                out_ref[:, b * L : b * L + L] = obuf[core * HB + b] + orecv[b]
            ref = loss_rows.at[pl.ds(1, CH - 1)]
            pltpu.make_async_copy(ref, ref, loss_sem.at[0]).wait()
            pltpu.make_async_copy(ref, ref, loss_sem.at[1]).wait()
            loss_two[0:1] = jnp.sum(loss_rows[...], axis=0, keepdims=True)
            copy = to_partner(loss_two.at[pl.ds(0, 1)], loss_two.at[pl.ds(1, 1)], loss_sem.at[2], loss_sem.at[3])
            copy.start()
            copy.wait()
            loss_ref[0] = jnp.sum(loss_two[...])

    vm = pltpu.VMEM
    dma = pltpu.SemaphoreType.DMA
    scratch = [
        vm((NP * TB, S, L), F32),
        vm((NP * TB, S, L), F32),
        vm((CH * TT0, 16, L), BF16),
        vm((KJ, n_rows), BF16),
        vm((n_rows, n_rows), F32),
        vm((n_rows, n_rows), BF16),
        vm((CH, L, L), BF16),
        vm((L, KJ), BF16),
        vm((L, n_rows), F32),
        vm((L, n_rows), F32),
        vm((JB, n_rows), F32),
        vm((L, L), F32),
        vm((CH, L), F32),
        vm((NP, JT, S, L), F32),
        vm((CH, JT, S, L), F32),
        vm((2, GS, JT, S, L), F32),
        vm((NT, NP, L), F32),
        vm((NT, NP, L), F32),
        vm((NT, NP, L), F32),
        vm((NT, S, L), F32),
        vm((S, L), F32),
        vm((2, NT, S, L), F32),
        vm((2, NT, S, L), F32),
        vm((2, NT, S, L), F32),
        vm((2, NT, S, L), F32),
        vm((NT, S, L), F32),
        vm((3, S, L), F32),
        vm((3, 3, S, L), F32),
        vm((S, L), F32),
        vm((S, L), F32),
        vm((CH, NR, L), F32),
        vm((HB, NR, L), F32),
        vm((4, L, L), F32),
        vm((CH, L), F32),
        vm((2, L), F32),
        vm((S, L), F32),
        dma((NL,)),
        dma((max(len(plan["msgs"]), len(plan0["msgs"])),)),
        dma((1,)),
        dma((CS,)),
        pltpu.SemaphoreType.REGULAR,
        dma((2,)),
        dma((2,)),
        dma((2,)),
        dma((2,)),
        dma((2,)),
        dma((2,)),
        dma((2,)),
        dma((3, 3)),
        dma((3, 3)),
        dma((2,)),
        dma((2,)),
        dma((4,)),
    ]
    return kernel, scratch


def solution(mesh):
    chips = mesh.shape["rows"]
    dims = torus_of(chips)
    grid_spec = P(("pairs", "rows"), "cols")

    def local_fn(c1, c2, t0, p, q, eps):
        n_rows, n_cols = p.shape[0] * chips, q.shape[0] * mesh.shape["cols"]
        kernel, scratch = make_kernel(dims, n_rows, n_cols, eps.shape[0], SWEEPS)
        vmem = pl.BlockSpec(memory_space=pltpu.VMEM)
        smem = pl.BlockSpec(memory_space=pltpu.SMEM)
        return pl.pallas_call(
            kernel,
            name="gromov",
            out_shape=(jax.ShapeDtypeStruct(t0.shape, F32), jax.ShapeDtypeStruct((1,), F32)),
            in_specs=[smem, smem, vmem, vmem, vmem, vmem],
            out_specs=(vmem, smem),
            scratch_shapes=scratch,
            compiler_params=pltpu.CompilerParams(
                collective_id=0, has_side_effects=True, vmem_limit_bytes=60 * 1024 * 1024
            ),
        )(eps, p, c1, c2, t0, q.reshape(chips // 2, L))

    return jax.shard_map(
        local_fn,
        mesh=mesh,
        in_specs=(grid_spec, grid_spec, grid_spec, P(("pairs", "rows")), P(("pairs", "cols")), P("pairs")),
        out_specs=(grid_spec, P("pairs")),
        check_vma=False,
    )
```

```python
import heapq
import itertools
import math

import jax
import jax.numpy as jnp
from jax import lax
from jax.experimental import pallas as pl
from jax.experimental.pallas import tpu as pltpu
from jax.sharding import PartitionSpec as P

SWEEPS = 10
FLAT = pl.DeviceIdType.LOGICAL
L, S = 128, 8
JB = 64
JT = JB // S
F32, BF16 = jnp.float32, jnp.bfloat16
ORDERS = ((0, 1, 2), (1, 2, 0), (2, 0, 1))
TILE_RATE = 11.4
HOP_US = 3.2
AHEAD_US = 8.0
LOG2E = 1.4426950216293335
LOG2E_REST = 1.925963e-8
PARTNER_US = 4.0
LATE = 165


def torus_of(chips):
    return {64: (4, 4, 4), S: (4, 2, 1), 16: (4, 4, 1)}[chips]


def halves(x):
    c = 4097.0 * x
    high = c - (c - x)
    return high, x - high


def quotient(a, b):
    q = a / b
    return q + (a - q * b) / b


def split3(n):
    cuts = [0, (n + 2) // 3, (2 * n + 2) // 3, n]
    return [(cuts[k], cuts[k + 1]) for k in range(3)]


def tree_plan(dims, tiles, rate, lat_us, ahead_us, shared=0):
    rings = {1: (), 2: ((1, "f", 1),), 4: ((1, "f", 1), (3, "f", -1), (2, "a", 1), (2, "b", -1))}
    msgs = []
    for color, order in enumerate(ORDERS):
        lo, hi = split3(tiles)[color]
        for dst in itertools.product(*(range(n) for n in dims)):
            used = [k for k in range(3) if dst[order[k]]]
            if not used or lo == hi:
                continue
            d = order[used[-1]]
            mid = lo + (hi - lo + (sum(dst) + color) % 2) // 2
            for at, part, sign in rings[dims[d]]:
                a, b = {"f": (lo, hi), "a": (lo, mid), "b": (mid, hi)}[part]
                if at != dst[d] or a == b:
                    continue
                src = list(dst)
                src[d] = (src[d] - sign) % dims[d]
                m = dict(id=len(msgs), color=color, src=tuple(src), dst=dst, link=(d, sign), lo=a, hi=b)
                m["us"] = (b - a) / rate
                msgs.append(m)
    into = {}
    for m in msgs:
        into.setdefault((m["color"], m["dst"]), []).append(m)
    users = [[] for _ in msgs]
    missing = []
    for m in msgs:
        deps = [e for e in into.get((m["color"], m["src"]), []) if e["lo"] < m["hi"] and m["lo"] < e["hi"]]
        missing.append(len(deps))
        for e in deps:
            users[e["id"]].append(m)
    way = {}

    def way_of(m):
        if m["id"] not in way:
            way[m["id"]] = m["us"] + lat_us + max([way_of(u) for u in users[m["id"]]], default=0.0)
        return way[m["id"]]

    links = sorted({m["link"] for m in msgs})
    queue = {k: [] for k in links}
    idle = dict.fromkeys(links, True)
    ready, events, ops = {}, [], []

    def put(m, now):
        ready[m["id"]] = now
        heapq.heappush(queue[m["link"]], (-way_of(m), m["id"]))

    def start(link, now):
        if idle[link] and queue[link]:
            k = heapq.heappop(queue[link])[1]
            idle[link] = False
            ops.append((max(ready[k], now - ahead_us), 1, "send", msgs[k]))
            heapq.heappush(events, (now + msgs[k]["us"], 0, k))
            heapq.heappush(events, (now + msgs[k]["us"] + lat_us, 1, k))

    for m in msgs:
        if not missing[m["id"]]:
            put(m, 0.0)
    for link in links:
        start(link, 0.0)
    left = {}
    for m in msgs:
        left[m["dst"]] = left.get(m["dst"], 0) + 1
    now = 0.0
    while events:
        now, arrived, k = heapq.heappop(events)
        m = msgs[k]
        if not arrived:
            idle[m["link"]] = True
            start(m["link"], now)
            continue
        ops.append((now, 0, "wait", m))
        for u in users[k]:
            missing[u["id"]] -= 1
            if not missing[u["id"]]:
                put(u, now)
                start(u["link"], now)
        left[m["dst"]] -= 1
        if not left[m["dst"]]:
            slot = m["dst"][0] + dims[0] * (m["dst"][1] + dims[1] * m["dst"][2])
            ops.append((now, 0, "slot", slot))
            if slot < shared:
                ops.append((now + PARTNER_US, 0, "partner", slot))
    ops.sort(key=lambda op: op[:2])
    totals = {k: sum(m["hi"] - m["lo"] for m in msgs if m["link"] == k) for k in links}
    return dict(msgs=msgs, ops=[op[2:] for op in ops], links=links, totals=totals, end=now)


def make_kernel(dims, n_rows, n_cols, steps, sweeps):
    X, Y, Z = dims
    CH = X * Y * Z
    NR = n_rows // CH
    G = NR // S
    NT = n_rows // L
    TB = JT * NT
    HB = CH // 2
    JN = n_cols // 2 // L
    JW = JN // 2
    NT0 = G * JW
    TT0 = NT0 + 2 * G
    KJ = CH * JB
    CK = min(1024, KJ)
    CM = min(2048, KJ)
    GS = min(4, CH // 2)
    CS = max(CH * 3 // 8 // GS * GS, GS)
    NP = CH + CS
    NE, NC = (CH - CS) // GS, 2 * CS // GS
    assert NT == 4 and n_cols == CH * L and JN == HB
    plan0 = tree_plan(dims, TT0, TILE_RATE, HOP_US, AHEAD_US)
    plan = tree_plan(dims, TB, TILE_RATE, HOP_US, AHEAD_US, CS)
    links = plan["links"]
    NL = len(links)
    peers = [(d, k) for d in range(3) for k in range(1, dims[d])]
    strides = (1, X, X * Y)

    def slot_of(offset):
        return offset[0] + X * offset[1] + X * Y * offset[2]

    def kernel(
        eps_ref, p_ref, c1_ref, c2_ref, t0_ref, q_ref,
        out_ref, loss_ref,
        land, kbuf, g0, tt, c1f, c1b, c2n, c2p, bacc, lp, lprecv, bp, qf, qrep, vbuf, cbuf,
        mb, sb, fb, ub, ap, xs, xr, mss, msr, pv, ars, arr, arps, arpr, obuf, orecv, trb, loss_rows, loss_two,
        send_sem, recv_sem, fwd_ssem, fwd_rsem, credit, x_ssem, x_rsem, ms_sem, lp_sem, c1_sem, c2_sem, q_sem, ar_ssem, ar_rsem, arp_sem, o_sem, loss_sem,
    ):
        chip = lax.axis_index("rows")
        core = lax.axis_index("cols")
        other = 1 - core
        pos = (lax.rem(chip, X), lax.rem(lax.div(chip, X), Y), lax.div(chip, X * Y))

        me = core * CH + chip
        partner = other * CH + chip

        def moved(d, k):
            return me + (lax.rem(pos[d] + k + dims[d], dims[d]) - pos[d]) * strides[d]

        near = {link: moved(*link) for link in links}

        def source_of(slot):
            off = (lax.rem(slot, X), lax.rem(lax.div(slot, X), Y), lax.div(slot, X * Y))
            at = [lax.rem(pos[d] + dims[d] - off[d], dims[d]) for d in range(3)]
            return at[0] + X * at[1] + X * Y * at[2]

        def to_partner(src, dst, ssem, rsem):
            return pltpu.make_async_remote_copy(
                src_ref=src, dst_ref=dst, send_sem=ssem, recv_sem=rsem,
                device_id=partner, device_id_type=FLAT,
            )

        def tree_copy(buf, width, first, m):
            n = m["hi"] - m["lo"]
            return pltpu.make_async_remote_copy(
                src_ref=buf.at[pl.ds((first + slot_of(m["src"])) * width + m["lo"], n)],
                dst_ref=buf.at[pl.ds((first + slot_of(m["dst"])) * width + m["lo"], n)],
                send_sem=send_sem.at[links.index(m["link"])],
                recv_sem=recv_sem.at[m["id"]],
                device_id=near[m["link"]],
                device_id_type=FLAT,
            )

        def tree(buf, width, first, the_plan, before_send=None, on_slot=None, fillers=()):
            fillers, ready, waits = list(fillers), [], 0
            for op, m in the_plan["ops"]:
                if op == "send":
                    if before_send is not None:
                        before_send(m)
                    tree_copy(buf, width, first, m).start()
                elif op == "wait":
                    while fillers and not fillers[0][0]:
                        fillers.pop(0)[1]()
                    ref = buf.at[pl.ds((first + slot_of(m["dst"])) * width + m["lo"], m["hi"] - m["lo"])]
                    pltpu.make_async_copy(ref, ref, recv_sem.at[m["id"]]).wait()
                    waits += 1
                    if ready:
                        on_slot(*ready.pop(0))
                    elif fillers and waits >= fillers[0][0]:
                        fillers.pop(0)[1]()
                elif on_slot is not None:
                    ready.append((op, m))
            for at in ready:
                on_slot(*at)
            for _, f in fillers:
                f()

        def tree_sent(buf, the_plan):
            for k, link in enumerate(links):
                n = the_plan["totals"][link]
                ref = buf.at[pl.ds(0, n)]
                pltpu.make_async_copy(ref, ref, send_sem.at[k]).wait()

        def give_credit():
            for d, sign in links:
                pl.semaphore_signal(credit, inc=1, device_id=moved(d, -sign), device_id_type=FLAT)

        def all_sum_send(stage):
            for n, k in enumerate(range(1, dims[stage])):
                pltpu.make_async_remote_copy(
                    src_ref=ars.at[stage], dst_ref=arr.at[stage, n],
                    send_sem=ar_ssem.at[stage, n], recv_sem=ar_rsem.at[stage, n],
                    device_id=moved(stage, k), device_id_type=FLAT,
                ).start()

        def all_sum_get(stage):
            total = ars[stage]
            for n, k in enumerate(range(1, dims[stage])):
                pltpu.make_async_remote_copy(
                    src_ref=ars.at[stage], dst_ref=arr.at[stage, n],
                    send_sem=ar_ssem.at[stage, n], recv_sem=ar_rsem.at[stage, n],
                    device_id=moved(stage, k), device_id_type=FLAT,
                ).wait()
                total = total + arr[stage, n]
            return total

        def all_sum_step(stage):
            total = all_sum_get(stage)
            if stage < 2:
                ars[stage + 1] = total
                all_sum_send(stage + 1)
            else:
                arps[...] = total
                to_partner(arps, arpr, arp_sem.at[0], arp_sem.at[1]).start()

        barrier = pltpu.get_barrier_semaphore()
        for d, k in peers:
            pl.semaphore_signal(barrier, inc=1, device_id=moved(d, k), device_id_type=FLAT)
        pl.semaphore_signal(barrier, inc=1, device_id=partner, device_id_type=FLAT)

        row = lax.broadcasted_iota(jnp.int32, (S, L), 0)
        lane = lax.broadcasted_iota(jnp.int32, (S, L), 1)

        for g in range(G):
            rows = slice(g * S, g * S + S)
            pair = jnp.concatenate([c1_ref[rows, :L], c1_ref[rows, L:]], axis=0)
            g0[NT0 + core * G + g] = pair.astype(BF16)
        c1_copy = to_partner(
            g0.at[pl.ds(NT0 + core * G, G)], g0.at[pl.ds(NT0 + core * G, G)], c1_sem.at[0], c1_sem.at[1]
        )
        q_copy = to_partner(q_ref, qf.at[pl.ds(core * HB, HB)], q_sem.at[0], q_sem.at[1])

        tile = jnp.zeros((S, L), F32)
        for t in range(2):
            part = jnp.zeros((1, L), F32)
            for k in range(NR):
                entry = c1_ref[k : k + 1, t * L : t * L + L]
                part = part + entry * entry * p_ref[k]
            tile = jnp.where(row == 2 * core + t, jnp.broadcast_to(part, (S, L)), tile)
        where = (row - 4) * L + lane
        for k in range(NR):
            tile = jnp.where(where == chip * NR + k, p_ref[k], tile)
        ars[0] = tile
        for g in range(G):
            rows = slice(g * S, g * S + S)
            for t in range(JW):
                a, b = t0_ref[rows, (2 * L) * t : (2 * L) * t + L], t0_ref[rows, (2 * L) * t + L : (2 * L) * t + (2 * L)]
                g0[g * JW + t] = jnp.concatenate([a, b], axis=0).astype(BF16)
        qf[pl.ds(core * HB, HB)] = q_ref[...]

        c2_copy = to_partner(c2n.at[pl.ds(core * HB, HB)], c2n.at[pl.ds(core * HB, HB)], c2_sem.at[0], c2_sem.at[1])
        bp[...] = jnp.zeros_like(bp)

        def round_c2(first, last):
            for t in range(first, last):
                blk = c2_ref[:, t * L : t * L + L]
                c2n[core * HB + t] = blk.astype(BF16)
                bp[...] += blk * blk * q_ref[t : t + 1, :]

        def finish_b():
            bp[...] = jnp.broadcast_to(jnp.sum(bp[...], axis=1, keepdims=True), (L, L))

        with jax.named_scope("barrier"):
            pl.semaphore_wait(barrier, len(peers) + 1)
        give_credit()
        c1_copy.start()
        q_copy.start()
        all_sum_send(0)

        src = lax.broadcasted_iota(jnp.int32, (L, L), 0)
        dst = lax.broadcasted_iota(jnp.int32, (L, L), 1)
        picks = [
            jnp.where((src - core * JB == dst - h * JB) & (dst >= h * JB) & (dst < h * JB + JB), 1.0, 0.0).astype(BF16)
            for h in range(2)
        ]

        def order_c2(first, last):
            for t in range(first, last):
                a = jnp.dot(c2n[source_of(2 * t)], picks[0], preferred_element_type=F32)
                b = jnp.dot(c2n[source_of(2 * t + 1)], picks[1], preferred_element_type=F32)
                c2p[:, t * L : t * L + L] = (a + b).astype(BF16)

        def order_q(first, last):
            def four(n, carry):
                for k in range(4):
                    p = 4 * n + k
                    shared = p < CS
                    half = jnp.where(shared, other, core)
                    line = jnp.broadcast_to(qf[pl.ds(source_of(jnp.where(shared, p, p - CS)), 1), :], (S, L))
                    for jt in range(JT):
                        own = jnp.where(lane == half * JB + jt * S + row, line, 0.0)
                        qrep[p, jt] = jnp.broadcast_to(jnp.sum(own, axis=1, keepdims=True), (S, L))
                return carry

            lax.fori_loop(first // 4, last // 4, four, 0)

        def span(n, parts, f):
            cuts = [n * k // parts for k in range(parts + 1)]
            return [lambda a=a, b=b: f(a, b) for a, b in zip(cuts, cuts[1:])]

        fillers = [(0, lambda: round_c2(0, HB)), (0, finish_b), (0, lambda: c2_copy.start())]
        fillers += [(0, lambda: q_copy.wait()), (0, lambda: order_q(0, NP)), (LATE // 2, lambda: all_sum_step(0))]
        fillers += [(LATE, lambda: c2_copy.wait())]
        fillers += [(LATE + 4 * n, f) for n, f in enumerate(span(CH // 2, S, order_c2))]
        fillers += [(LATE + JB // 2, lambda: all_sum_step(1))]
        waited = []

        def before_send(m):
            if not waited and m["hi"] > NT0:
                waited.append(1)
                c1_copy.wait()

        def unpack(op, s):
            chip_s = source_of(s)
            for g in range(G):
                tiles = g0[s * TT0 + g * JW : s * TT0 + g * JW + JW].astype(F32).reshape(JN, S, L)
                kbuf[pl.ds((chip_s * G + g) * JN, JN)] = tiles
                at = pl.ds(pl.multiple_of(chip_s * NR + g * S, S), S)
                for h in range(2):
                    pair = g0[s * TT0 + NT0 + h * G + g].astype(F32)
                    c1f[at, 2 * L * h : 2 * L * h + L] = pair[:S]
                    c1f[at, 2 * L * h + L : 2 * L * h + 2 * L] = pair[S:]

        with jax.named_scope("gather0"):
            first = [(0, lambda: unpack("slot", 0))]
            tree(g0, TT0, 0, plan0, before_send=before_send, on_slot=unpack, fillers=first + fillers)
            tree_sent(g0, plan0)
            c1b[...] = c1f[...].astype(BF16)
            all_sum_step(2)

        def finish_lp():
            lp[...] = jnp.concatenate([bp[...]] * NT, axis=1) - 2.0 * bacc[...]

        bacc[...] = jnp.zeros_like(bacc)
        JC = CK // L

        def first_chunk(n, carry):
            cols = []
            for t in range(JC):
                cols.append(kbuf[pl.ds(n * JC + t, CH * G, stride=JN)].reshape(n_rows, L))
            plan_c = jnp.concatenate(cols, axis=1).astype(BF16)
            lead = jnp.dot(c1b[...], plan_c, preferred_element_type=F32).astype(BF16)
            c2c = jnp.concatenate([c2n[core * HB + n * JC + t] for t in range(JC)], axis=1)
            bacc[...] += lax.dot_general(c2c, lead, (((1,), (1,)), ((), ())), preferred_element_type=F32)
            return carry

        with jax.named_scope("firstmm"):
            lax.fori_loop(0, KJ // CK, first_chunk, 0)
            finish_lp()
        to_partner(arps, arpr, arp_sem.at[0], arp_sem.at[1]).wait()
        ap[...] = jnp.where(row < 4, arps[...] + arpr[...], arps[...])
        for t in range(NT):
            pv[t] = jnp.broadcast_to(ap[4 + t : 5 + t, :], (S, L))


        def chunk(n, carry):
            at = pl.ds(pl.multiple_of(n * CM, CM), CM)
            lead = jnp.dot(tt[at, :], c1b[...], preferred_element_type=F32).astype(BF16)
            bacc[...] += jnp.dot(c2p[:, at], lead, preferred_element_type=F32)
            return carry

        def costs():
            copy = to_partner(lp.at[pl.ds(other * JB, JB)], lprecv, lp_sem.at[0], lp_sem.at[1])
            copy.start()
            copy.wait()
            own = lp[pl.ds(pl.multiple_of(core * JB, JB), JB), :] + lprecv[...]
            return own + jnp.concatenate([ap[t : t + 1, :] for t in range(NT)], axis=1)

        def block(s):
            return kbuf[pl.ds(s * TB, TB)].reshape(JT, NT, S, L)

        def weighted(kk, u):
            w = (kk[:, 0] * u[0] + kk[:, 1] * u[1]) + (kk[:, 2] * u[2] + kk[:, 3] * u[3])
            return jnp.sum(w, axis=2, keepdims=True)

        def passes(u, rescale=False, last=False, par=0):
            def place(g):
                if last:
                    return g * GS + CS
                return g * GS + 2 * CS if not isinstance(g, int) or g < NE else (g - NE) * GS

            def one(at, buf):
                for k in range(GS):
                    p = at + k
                    kk = block(p)
                    if rescale:
                        kk = kk * fb[:, pl.ds(p, 1), :][None]
                        kbuf[pl.ds(p * TB, TB)] = kk.reshape(TB, S, L)
                    c = jnp.broadcast_to(weighted(kk, u), (JT, S, L))
                    cbuf[buf, k] = quotient(qrep[p], c) if last else qrep[p] / c

            def two(at, buf, acc):
                for k in range(GS):
                    p = at + k
                    v = cbuf[buf, k]
                    kk = block(p)
                    if last:
                        vbuf[p - CS] = v
                        t = (kk * u[None]) * v[:, None]
                        flat = jnp.concatenate([t[:, i].reshape(JB, L) for i in range(NT)], axis=1)
                        tt[pl.ds(pl.multiple_of((p - CS) * JB, JB), JB), :] = flat.astype(BF16)
                    else:
                        acc = acc + jnp.sum(kk * v[:, None], axis=0)
                return acc

            def run(a, b, end):
                shift = place(a) - a * GS
                even, odd = a % 2, (a + 1) % 2
                pairs = max(0, (b - a - 1) // 2)

                def both(n, acc):
                    at = (a + 2 * n) * GS + shift
                    one(at + GS, odd)
                    acc = two(at, even, acc)
                    one(at + 2 * GS, even)
                    return two(at + GS, odd, acc)

                acc = lax.fori_loop(0, pairs, both, jnp.zeros((NT, S, L), F32))
                for g in range(a + 2 * pairs, b):
                    if g + 1 < end:
                        one(place(g + 1), (g + 1) % 2)
                    acc = two(place(g), g % 2, acc)
                return acc

            one(place(0), 0)
            if last:
                run(0, CH // GS, CH // GS)
                return None
            xs[par] = run(0, NE, NE + NC)
            copy = to_partner(xs.at[par], xr.at[par], x_ssem.at[par], x_rsem.at[par])
            copy.start()
            acc = run(NE, NE + NC, NE + NC)
            copy.wait()
            total = jnp.sum((xs[par] + xr[par]) + acc, axis=1, keepdims=True)
            return quotient(pv[...], jnp.broadcast_to(total, (NT, S, L)))

        def outer(r, carry):
            eps = eps_ref[r]
            inv = 1.0 / eps
            inv = inv * (2.0 - eps * inv)
            main = LOG2E * inv
            (e0, e1), (m0, m1) = halves(eps), halves(main)
            prod = eps * main
            low_part = ((e0 * m0 - prod) + (e0 * m1 + e1 * m0)) + e1 * m1
            rest = (((LOG2E - prod) - low_part) + LOG2E_REST) * inv

            def decay(x):
                return jnp.exp2(x * main + x * rest)

            cost = costs()
            for jt in range(JT):
                for t in range(NT):
                    land[CS * TB + jt * NT + t] = cost[jt * S : jt * S + S, t * L : t * L + L]

            def exps(p):
                ll = land[p * TB : p * TB + TB].reshape(JT, NT, S, L)
                low = jnp.min(jnp.min(ll, axis=0), axis=1, keepdims=True)
                kk = decay(low[None] - ll)
                kbuf[p * TB : p * TB + TB] = kk.reshape(TB, S, L)
                mb[:, p : p + 1, :] = low
                sb[:, p : p + 1, :] = jnp.sum(jnp.sum(kk, axis=0), axis=1, keepdims=True)

            def passed_on(s):
                return to_partner(
                    land.at[pl.ds((CS + s) * TB, TB)], land.at[pl.ds(s * TB, TB)], fwd_ssem.at[0], fwd_rsem.at[s]
                )

            def on_slot(op, s):
                if op == "slot":
                    if s < CS:
                        passed_on(s).start()
                    exps(CS + s)
                else:
                    passed_on(s).wait_recv()
                    exps(s)

            with jax.named_scope("gather"):
                pl.semaphore_wait(credit, NL)
                first = [(0, lambda: on_slot("slot", 0)), (len(plan["msgs"]) // 4, lambda: on_slot("partner", 0))]
                tree(land, TB, CS, plan, on_slot=on_slot, fillers=first)
                tree_sent(land, plan)
                ref = land.at[pl.ds(0, CS * TB)]
                pltpu.make_async_copy(ref, ref, fwd_ssem.at[0]).wait()
                give_credit()

            with jax.named_scope("minx"):
                def least_of(a, b):
                    low = jnp.min(mb[:, a:b], axis=1, keepdims=True)
                    part = jnp.sum(sb[:, a:b] * decay(low - mb[:, a:b]), axis=1, keepdims=True)
                    return jnp.broadcast_to(low, (NT, S, L)), jnp.broadcast_to(part, (NT, S, L))

                mss[0], mss[1] = least_of(2 * CS, NP)
                copy = to_partner(mss, msr, ms_sem.at[0], ms_sem.at[1])
                copy.start()
                low, part = least_of(0, 2 * CS)
                copy.wait()
                least = jnp.minimum(jnp.minimum(mss[0], msr[0]), low)
                total = mss[1] * decay(least - mss[0]) + msr[1] * decay(least - msr[0])
                total = total + part * decay(least - low)
                fb[...] = decay(least[:, :1] - mb[...])
                u = quotient(pv[...], total)

            with jax.named_scope("pass1"):
                u = passes(u, rescale=True, par=1)

            def sweep(t, u):
                return passes(u, par=lax.rem(t, 2))

            with jax.named_scope("sweeps"):
                u = lax.fori_loop(2, sweeps, sweep, u)
            with jax.named_scope("lastpass"):
                passes(u, last=True)
            ub[...] = u
            bacc[...] = jnp.zeros_like(bacc)
            with jax.named_scope("mm"):
                lax.fori_loop(0, KJ // CM, chunk, 0)
                finish_lp()
            return carry

        lax.fori_loop(0, steps, outer, 0)

        pl.semaphore_wait(credit, NL)
        cost = costs()
        plan_own = (block(CS) * ub[...][None]) * vbuf[0][:, None]
        total = jnp.zeros((S, L), F32)
        for jt in range(JT):
            for t in range(NT):
                total = total + cost[jt * S : jt * S + S, t * L : t * L + L] * plan_own[jt, t]
        loss_rows[0:1] = jnp.sum(total, axis=0, keepdims=True)

        def to_chip(n):
            o = CH - n
            off = (lax.rem(o, X), lax.rem(lax.div(o, X), Y), lax.div(o, X * Y))
            at = [lax.rem(pos[d] + off[d], dims[d]) for d in range(3)]
            return pltpu.make_async_remote_copy(
                src_ref=loss_rows.at[pl.ds(0, 1)], dst_ref=loss_rows.at[pl.ds(o, 1)],
                send_sem=loss_sem.at[0], recv_sem=loss_sem.at[1],
                device_id=core * CH + at[0] + X * at[1] + X * Y * at[2], device_id_type=FLAT,
            )

        def tell(n, carry):
            to_chip(n).start()
            return carry

        lax.fori_loop(1, CH, tell, 0)

        it = lax.div(chip * NR, L)
        inside = pl.multiple_of(lax.rem(chip * NR, L), S)

        def rows_of(n, carry):
            for k in range(4):
                s = 4 * n + k
                kk = jnp.concatenate([kbuf[(CS + s) * TB + jt * NT + it] for jt in range(JT)], axis=0)
                uu = jnp.concatenate([ub[it]] * JT, axis=0)
                t = (kk * uu) * vbuf[s].reshape(JB, L)
                none = jnp.zeros_like(t)
                both = jnp.where(core == 0, jnp.concatenate([t, none], axis=0), jnp.concatenate([none, t], axis=0))
                trb[k] = both.T
                obuf[source_of(s)] = trb[k, pl.ds(inside, NR), :]
            return carry

        with jax.named_scope("tail"):
            lax.fori_loop(0, CH // 4, rows_of, 0)
            o_copy = to_partner(obuf.at[pl.ds(other * HB, HB)], orecv, o_sem.at[0], o_sem.at[1])
            o_copy.start()
            o_copy.wait()
            for b in range(HB):
                out_ref[:, b * L : b * L + L] = obuf[core * HB + b] + orecv[b]
            ref = loss_rows.at[pl.ds(1, CH - 1)]
            pltpu.make_async_copy(ref, ref, loss_sem.at[0]).wait()
            pltpu.make_async_copy(ref, ref, loss_sem.at[1]).wait()
            loss_two[0:1] = jnp.sum(loss_rows[...], axis=0, keepdims=True)
            copy = to_partner(loss_two.at[pl.ds(0, 1)], loss_two.at[pl.ds(1, 1)], loss_sem.at[2], loss_sem.at[3])
            copy.start()
            copy.wait()
            loss_ref[0] = jnp.sum(loss_two[...])

    vm = pltpu.VMEM
    dma = pltpu.SemaphoreType.DMA
    scratch = [
        vm((NP * TB, S, L), F32),
        vm((NP * TB, S, L), F32),
        vm((CH * TT0, 16, L), BF16),
        vm((KJ, n_rows), BF16),
        vm((n_rows, n_rows), F32),
        vm((n_rows, n_rows), BF16),
        vm((CH, L, L), BF16),
        vm((L, KJ), BF16),
        vm((L, n_rows), F32),
        vm((L, n_rows), F32),
        vm((JB, n_rows), F32),
        vm((L, L), F32),
        vm((CH, L), F32),
        vm((NP, JT, S, L), F32),
        vm((CH, JT, S, L), F32),
        vm((2, GS, JT, S, L), F32),
        vm((NT, NP, L), F32),
        vm((NT, NP, L), F32),
        vm((NT, NP, L), F32),
        vm((NT, S, L), F32),
        vm((S, L), F32),
        vm((2, NT, S, L), F32),
        vm((2, NT, S, L), F32),
        vm((2, NT, S, L), F32),
        vm((2, NT, S, L), F32),
        vm((NT, S, L), F32),
        vm((3, S, L), F32),
        vm((3, 3, S, L), F32),
        vm((S, L), F32),
        vm((S, L), F32),
        vm((CH, NR, L), F32),
        vm((HB, NR, L), F32),
        vm((4, L, L), F32),
        vm((CH, L), F32),
        vm((2, L), F32),
        dma((NL,)),
        dma((max(len(plan["msgs"]), len(plan0["msgs"])),)),
        dma((1,)),
        dma((CS,)),
        pltpu.SemaphoreType.REGULAR,
        dma((2,)),
        dma((2,)),
        dma((2,)),
        dma((2,)),
        dma((2,)),
        dma((2,)),
        dma((2,)),
        dma((3, 3)),
        dma((3, 3)),
        dma((2,)),
        dma((2,)),
        dma((4,)),
    ]
    return kernel, scratch


def solution(mesh):
    chips = mesh.shape["rows"]
    dims = torus_of(chips)
    grid_spec = P(("pairs", "rows"), "cols")

    def local_fn(c1, c2, t0, p, q, eps):
        n_rows, n_cols = p.shape[0] * chips, q.shape[0] * mesh.shape["cols"]
        kernel, scratch = make_kernel(dims, n_rows, n_cols, eps.shape[0], SWEEPS)
        vmem = pl.BlockSpec(memory_space=pltpu.VMEM)
        smem = pl.BlockSpec(memory_space=pltpu.SMEM)
        return pl.pallas_call(
            kernel,
            name="gromov",
            out_shape=(jax.ShapeDtypeStruct(t0.shape, F32), jax.ShapeDtypeStruct((1,), F32)),
            in_specs=[smem, smem, vmem, vmem, vmem, vmem],
            out_specs=(vmem, smem),
            scratch_shapes=scratch,
            compiler_params=pltpu.CompilerParams(
                collective_id=0, has_side_effects=True, vmem_limit_bytes=60 * 1024 * 1024
            ),
        )(eps, p, c1, c2, t0, q.reshape(chips // 2, L))

    return jax.shard_map(
        local_fn,
        mesh=mesh,
        in_specs=(grid_spec, grid_spec, grid_spec, P(("pairs", "rows")), P(("pairs", "cols")), P("pairs")),
        out_specs=(grid_spec, P("pairs")),
        check_vma=False,
    )
```

```python
import heapq
import itertools
import math

import jax
import jax.numpy as jnp
from jax import lax
from jax.experimental import pallas as pl
from jax.experimental.pallas import tpu as pltpu
from jax.sharding import PartitionSpec as P

SWEEPS = 10
FLAT = pl.DeviceIdType.LOGICAL
L, S = 128, 8
JB = 64
JT = JB // S
F32, BF16 = jnp.float32, jnp.bfloat16
ORDERS = ((0, 1, 2), (1, 2, 0), (2, 0, 1))
TILE_RATE = 11.4
HOP_US = 4.0
AHEAD_US = 2.0
LOG2E = 1.4426950216293335
LOG2E_REST = 1.925963e-8
PARTNER_US = 4.0
LATE = 165


def torus_of(chips):
    return {64: (4, 4, 4), S: (4, 2, 1), 16: (4, 4, 1)}[chips]


def halves(x):
    c = 4097.0 * x
    high = c - (c - x)
    return high, x - high


def quotient(a, b):
    q = a / b
    return q + (a - q * b) / b


def split3(n):
    cuts = [0, (n + 2) // 3, (2 * n + 2) // 3, n]
    return [(cuts[k], cuts[k + 1]) for k in range(3)]


def tree_plan(dims, tiles, rate, lat_us, ahead_us, shared=0):
    rings = {1: (), 2: ((1, "f", 1),), 4: ((1, "f", 1), (3, "f", -1), (2, "a", 1), (2, "b", -1))}
    msgs = []
    for color, order in enumerate(ORDERS):
        lo, hi = split3(tiles)[color]
        for dst in itertools.product(*(range(n) for n in dims)):
            used = [k for k in range(3) if dst[order[k]]]
            if not used or lo == hi:
                continue
            d = order[used[-1]]
            mid = lo + (hi - lo + (sum(dst) + color) % 2) // 2
            for at, part, sign in rings[dims[d]]:
                a, b = {"f": (lo, hi), "a": (lo, mid), "b": (mid, hi)}[part]
                if at != dst[d] or a == b:
                    continue
                src = list(dst)
                src[d] = (src[d] - sign) % dims[d]
                m = dict(id=len(msgs), color=color, src=tuple(src), dst=dst, link=(d, sign), lo=a, hi=b)
                m["us"] = (b - a) / rate
                msgs.append(m)
    into = {}
    for m in msgs:
        into.setdefault((m["color"], m["dst"]), []).append(m)
    users = [[] for _ in msgs]
    missing = []
    for m in msgs:
        deps = [e for e in into.get((m["color"], m["src"]), []) if e["lo"] < m["hi"] and m["lo"] < e["hi"]]
        missing.append(len(deps))
        for e in deps:
            users[e["id"]].append(m)
    way = {}

    def way_of(m):
        if m["id"] not in way:
            way[m["id"]] = m["us"] + lat_us + max([way_of(u) for u in users[m["id"]]], default=0.0)
        return way[m["id"]]

    links = sorted({m["link"] for m in msgs})
    queue = {k: [] for k in links}
    idle = dict.fromkeys(links, True)
    ready, events, ops = {}, [], []

    def put(m, now):
        ready[m["id"]] = now
        heapq.heappush(queue[m["link"]], (-way_of(m), m["id"]))

    def start(link, now):
        if idle[link] and queue[link]:
            k = heapq.heappop(queue[link])[1]
            idle[link] = False
            ops.append((max(ready[k], now - ahead_us), 1, "send", msgs[k]))
            heapq.heappush(events, (now + msgs[k]["us"], 0, k))
            heapq.heappush(events, (now + msgs[k]["us"] + lat_us, 1, k))

    for m in msgs:
        if not missing[m["id"]]:
            put(m, 0.0)
    for link in links:
        start(link, 0.0)
    left = {}
    for m in msgs:
        left[m["dst"]] = left.get(m["dst"], 0) + 1
    now = 0.0
    while events:
        now, arrived, k = heapq.heappop(events)
        m = msgs[k]
        if not arrived:
            idle[m["link"]] = True
            start(m["link"], now)
            continue
        ops.append((now, 0, "wait", m))
        for u in users[k]:
            missing[u["id"]] -= 1
            if not missing[u["id"]]:
                put(u, now)
                start(u["link"], now)
        left[m["dst"]] -= 1
        if not left[m["dst"]]:
            slot = m["dst"][0] + dims[0] * (m["dst"][1] + dims[1] * m["dst"][2])
            ops.append((now, 0, "slot", slot))
            if slot < shared:
                ops.append((now + PARTNER_US, 0, "partner", slot))
    ops.sort(key=lambda op: op[:2])
    totals = {k: sum(m["hi"] - m["lo"] for m in msgs if m["link"] == k) for k in links}
    return dict(msgs=msgs, ops=[op[2:] for op in ops], links=links, totals=totals, end=now)


def make_kernel(dims, n_rows, n_cols, steps, sweeps):
    X, Y, Z = dims
    CH = X * Y * Z
    NR = n_rows // CH
    G = NR // S
    NT = n_rows // L
    TB = JT * NT
    HB = CH // 2
    JN = n_cols // 2 // L
    JW = JN // 2
    NT0 = G * JW
    TT0 = NT0 + 2 * G
    KJ = CH * JB
    CK = min(1024, KJ)
    CM = min(1024, KJ)
    GS = min(4, CH // 2)
    CS = max(CH * 3 // 8 // GS * GS, GS)
    NP = CH + CS
    NE, NC = (CH - CS) // GS, 2 * CS // GS
    GC = CM // JB // GS
    assert NT == 4 and n_cols == CH * L and JN == HB
    plan0 = tree_plan(dims, TT0, TILE_RATE, HOP_US, AHEAD_US)
    plan = tree_plan(dims, TB, TILE_RATE, HOP_US, AHEAD_US, CS)
    links = plan["links"]
    NL = len(links)
    peers = [(d, k) for d in range(3) for k in range(1, dims[d])]
    strides = (1, X, X * Y)

    def slot_of(offset):
        return offset[0] + X * offset[1] + X * Y * offset[2]

    def kernel(
        eps_ref, p_ref, c1_ref, c2_ref, t0_ref, q_ref,
        out_ref, loss_ref,
        land, kbuf, g0, tt0, tt1, c1f, c1b, c2n, c2p, bacc, lp, lprecv, bp, qf, qrep, vbuf, cbuf,
        mb, sb, fb, ub, ap, xs, xr, mss, msr, pv, ars, arr, arps, arpr, obuf, orecv, trb, loss_rows, loss_two,
        send_sem, recv_sem, fwd_ssem, fwd_rsem, credit, x_ssem, x_rsem, ms_sem, lp_sem, c1_sem, c2_sem, q_sem, ar_ssem, ar_rsem, arp_sem, o_sem, loss_sem,
    ):
        tts = (tt0, tt1)
        chip = lax.axis_index("rows")
        core = lax.axis_index("cols")
        other = 1 - core
        pos = (lax.rem(chip, X), lax.rem(lax.div(chip, X), Y), lax.div(chip, X * Y))

        me = core * CH + chip
        partner = other * CH + chip

        def moved(d, k):
            return me + (lax.rem(pos[d] + k + dims[d], dims[d]) - pos[d]) * strides[d]

        near = {link: moved(*link) for link in links}

        def source_of(slot):
            off = (lax.rem(slot, X), lax.rem(lax.div(slot, X), Y), lax.div(slot, X * Y))
            at = [lax.rem(pos[d] + dims[d] - off[d], dims[d]) for d in range(3)]
            return at[0] + X * at[1] + X * Y * at[2]

        def to_partner(src, dst, ssem, rsem):
            return pltpu.make_async_remote_copy(
                src_ref=src, dst_ref=dst, send_sem=ssem, recv_sem=rsem,
                device_id=partner, device_id_type=FLAT,
            )

        def tree_copy(buf, width, first, m):
            n = m["hi"] - m["lo"]
            return pltpu.make_async_remote_copy(
                src_ref=buf.at[pl.ds((first + slot_of(m["src"])) * width + m["lo"], n)],
                dst_ref=buf.at[pl.ds((first + slot_of(m["dst"])) * width + m["lo"], n)],
                send_sem=send_sem.at[links.index(m["link"])],
                recv_sem=recv_sem.at[m["id"]],
                device_id=near[m["link"]],
                device_id_type=FLAT,
            )

        def tree(buf, width, first, the_plan, before_send=None, on_slot=None, fillers=()):
            fillers, ready, waits = list(fillers), [], 0
            for op, m in the_plan["ops"]:
                if op == "send":
                    if before_send is not None:
                        before_send(m)
                    tree_copy(buf, width, first, m).start()
                elif op == "wait":
                    while fillers and not fillers[0][0]:
                        fillers.pop(0)[1]()
                    ref = buf.at[pl.ds((first + slot_of(m["dst"])) * width + m["lo"], m["hi"] - m["lo"])]
                    pltpu.make_async_copy(ref, ref, recv_sem.at[m["id"]]).wait()
                    waits += 1
                    if ready:
                        on_slot(*ready.pop(0))
                    elif fillers and waits >= fillers[0][0]:
                        fillers.pop(0)[1]()
                elif on_slot is not None:
                    ready.append((op, m))
            for at in ready:
                on_slot(*at)
            for _, f in fillers:
                f()

        def tree_sent(buf, the_plan):
            for k, link in enumerate(links):
                n = the_plan["totals"][link]
                ref = buf.at[pl.ds(0, n)]
                pltpu.make_async_copy(ref, ref, send_sem.at[k]).wait()

        def give_credit():
            for d, sign in links:
                pl.semaphore_signal(credit, inc=1, device_id=moved(d, -sign), device_id_type=FLAT)

        def all_sum_send(stage):
            for n, k in enumerate(range(1, dims[stage])):
                pltpu.make_async_remote_copy(
                    src_ref=ars.at[stage], dst_ref=arr.at[stage, n],
                    send_sem=ar_ssem.at[stage, n], recv_sem=ar_rsem.at[stage, n],
                    device_id=moved(stage, k), device_id_type=FLAT,
                ).start()

        def all_sum_get(stage):
            total = ars[stage]
            for n, k in enumerate(range(1, dims[stage])):
                pltpu.make_async_remote_copy(
                    src_ref=ars.at[stage], dst_ref=arr.at[stage, n],
                    send_sem=ar_ssem.at[stage, n], recv_sem=ar_rsem.at[stage, n],
                    device_id=moved(stage, k), device_id_type=FLAT,
                ).wait()
                total = total + arr[stage, n]
            return total

        def all_sum_step(stage):
            total = all_sum_get(stage)
            if stage < 2:
                ars[stage + 1] = total
                all_sum_send(stage + 1)
            else:
                arps[...] = total
                to_partner(arps, arpr, arp_sem.at[0], arp_sem.at[1]).start()

        barrier = pltpu.get_barrier_semaphore()
        for d, k in peers:
            pl.semaphore_signal(barrier, inc=1, device_id=moved(d, k), device_id_type=FLAT)
        pl.semaphore_signal(barrier, inc=1, device_id=partner, device_id_type=FLAT)

        row = lax.broadcasted_iota(jnp.int32, (S, L), 0)
        lane = lax.broadcasted_iota(jnp.int32, (S, L), 1)

        for g in range(G):
            rows = slice(g * S, g * S + S)
            pair = jnp.concatenate([c1_ref[rows, :L], c1_ref[rows, L:]], axis=0)
            g0[NT0 + core * G + g] = pair.astype(BF16)
        c1_copy = to_partner(
            g0.at[pl.ds(NT0 + core * G, G)], g0.at[pl.ds(NT0 + core * G, G)], c1_sem.at[0], c1_sem.at[1]
        )
        q_copy = to_partner(q_ref, qf.at[pl.ds(core * HB, HB)], q_sem.at[0], q_sem.at[1])

        tile = jnp.zeros((S, L), F32)
        for t in range(2):
            part = jnp.zeros((1, L), F32)
            for k in range(NR):
                entry = c1_ref[k : k + 1, t * L : t * L + L]
                part = part + entry * entry * p_ref[k]
            tile = jnp.where(row == 2 * core + t, jnp.broadcast_to(part, (S, L)), tile)
        where = (row - 4) * L + lane
        for k in range(NR):
            tile = jnp.where(where == chip * NR + k, p_ref[k], tile)
        ars[0] = tile
        for g in range(G):
            rows = slice(g * S, g * S + S)
            for t in range(JW):
                a, b = t0_ref[rows, (2 * L) * t : (2 * L) * t + L], t0_ref[rows, (2 * L) * t + L : (2 * L) * t + (2 * L)]
                g0[g * JW + t] = jnp.concatenate([a, b], axis=0).astype(BF16)
        qf[pl.ds(core * HB, HB)] = q_ref[...]

        c2_copy = to_partner(c2n.at[pl.ds(core * HB, HB)], c2n.at[pl.ds(core * HB, HB)], c2_sem.at[0], c2_sem.at[1])
        bp[...] = jnp.zeros_like(bp)

        def round_c2(first, last):
            for t in range(first, last):
                blk = c2_ref[:, t * L : t * L + L]
                c2n[core * HB + t] = blk.astype(BF16)
                bp[...] += blk * blk * q_ref[t : t + 1, :]

        def finish_b():
            bp[...] = jnp.broadcast_to(jnp.sum(bp[...], axis=1, keepdims=True), (L, L))

        with jax.named_scope("barrier"):
            pl.semaphore_wait(barrier, len(peers) + 1)
        give_credit()
        c1_copy.start()
        q_copy.start()
        all_sum_send(0)

        src = lax.broadcasted_iota(jnp.int32, (L, L), 0)
        dst = lax.broadcasted_iota(jnp.int32, (L, L), 1)
        picks = [
            jnp.where((src - core * JB == dst - h * JB) & (dst >= h * JB) & (dst < h * JB + JB), 1.0, 0.0).astype(BF16)
            for h in range(2)
        ]

        def order_c2(first, last):
            for t in range(first, last):
                a = jnp.dot(c2n[source_of(2 * t)], picks[0], preferred_element_type=F32)
                b = jnp.dot(c2n[source_of(2 * t + 1)], picks[1], preferred_element_type=F32)
                c2p[:, t * L : t * L + L] = (a + b).astype(BF16)

        def order_q(first, last):
            def four(n, carry):
                for k in range(4):
                    p = 4 * n + k
                    shared = p < CS
                    half = jnp.where(shared, other, core)
                    line = jnp.broadcast_to(qf[pl.ds(source_of(jnp.where(shared, p, p - CS)), 1), :], (S, L))
                    for jt in range(JT):
                        own = jnp.where(lane == half * JB + jt * S + row, line, 0.0)
                        qrep[p, jt] = jnp.broadcast_to(jnp.sum(own, axis=1, keepdims=True), (S, L))
                return carry

            lax.fori_loop(first // 4, last // 4, four, 0)

        def span(n, parts, f):
            cuts = [n * k // parts for k in range(parts + 1)]
            return [lambda a=a, b=b: f(a, b) for a, b in zip(cuts, cuts[1:])]

        fillers = [(0, lambda: round_c2(0, HB)), (0, finish_b), (0, lambda: c2_copy.start())]
        fillers += [(0, lambda: q_copy.wait()), (0, lambda: order_q(0, NP)), (LATE // 2, lambda: all_sum_step(0))]
        fillers += [(LATE, lambda: c2_copy.wait())]
        fillers += [(LATE + 4 * n, f) for n, f in enumerate(span(CH // 2, S, order_c2))]
        fillers += [(LATE + JB // 2, lambda: all_sum_step(1))]
        waited = []

        def before_send(m):
            if not waited and m["hi"] > NT0:
                waited.append(1)
                c1_copy.wait()

        def unpack(op, s):
            chip_s = source_of(s)
            for g in range(G):
                tiles = g0[s * TT0 + g * JW : s * TT0 + g * JW + JW].astype(F32).reshape(JN, S, L)
                kbuf[pl.ds((chip_s * G + g) * JN, JN)] = tiles
                at = pl.ds(pl.multiple_of(chip_s * NR + g * S, S), S)
                for h in range(2):
                    pair = g0[s * TT0 + NT0 + h * G + g].astype(F32)
                    c1f[at, 2 * L * h : 2 * L * h + L] = pair[:S]
                    c1f[at, 2 * L * h + L : 2 * L * h + 2 * L] = pair[S:]

        with jax.named_scope("gather0"):
            first = [(0, lambda: unpack("slot", 0))]
            tree(g0, TT0, 0, plan0, before_send=before_send, on_slot=unpack, fillers=first + fillers)
            tree_sent(g0, plan0)
            c1b[...] = c1f[...].astype(BF16)
            all_sum_step(2)

        def finish_lp():
            lp[...] = jnp.concatenate([bp[...]] * NT, axis=1) - 2.0 * bacc[...]

        bacc[...] = jnp.zeros_like(bacc)
        JC = CK // L

        def first_chunk(n, carry):
            cols = []
            for t in range(JC):
                cols.append(kbuf[pl.ds(n * JC + t, CH * G, stride=JN)].reshape(n_rows, L))
            plan_c = jnp.concatenate(cols, axis=1).astype(BF16)
            lead = jnp.dot(c1b[...], plan_c, preferred_element_type=F32).astype(BF16)
            c2c = jnp.concatenate([c2n[core * HB + n * JC + t] for t in range(JC)], axis=1)
            bacc[...] += lax.dot_general(c2c, lead, (((1,), (1,)), ((), ())), preferred_element_type=F32)
            return carry

        with jax.named_scope("firstmm"):
            lax.fori_loop(0, KJ // CK, first_chunk, 0)
            finish_lp()
        to_partner(arps, arpr, arp_sem.at[0], arp_sem.at[1]).wait()
        ap[...] = jnp.where(row < 4, arps[...] + arpr[...], arps[...])
        for t in range(NT):
            pv[t] = jnp.broadcast_to(ap[4 + t : 5 + t, :], (S, L))


        def lead_and_cross(n, plan_c):
            lead = jnp.dot(plan_c[...], c1b[...], preferred_element_type=F32).astype(BF16)
            bacc[...] += jnp.dot(c2p[:, n * CM : n * CM + CM], lead, preferred_element_type=F32)

        def costs():
            copy = to_partner(lp.at[pl.ds(other * JB, JB)], lprecv, lp_sem.at[0], lp_sem.at[1])
            copy.start()
            copy.wait()
            own = lp[pl.ds(pl.multiple_of(core * JB, JB), JB), :] + lprecv[...]
            return own + jnp.concatenate([ap[t : t + 1, :] for t in range(NT)], axis=1)

        def block(s):
            return kbuf[pl.ds(s * TB, TB)].reshape(JT, NT, S, L)

        def weighted(kk, u):
            w = (kk[:, 0] * u[0] + kk[:, 1] * u[1]) + (kk[:, 2] * u[2] + kk[:, 3] * u[3])
            return jnp.sum(w, axis=2, keepdims=True)

        def passes(u, rescale=False, par=0):
            def place(g):
                return g * GS + 2 * CS if not isinstance(g, int) or g < NE else (g - NE) * GS

            def one(at, buf):
                for k in range(GS):
                    p = at + k
                    kk = block(p)
                    if rescale:
                        kk = kk * fb[:, pl.ds(p, 1), :][None]
                        kbuf[pl.ds(p * TB, TB)] = kk.reshape(TB, S, L)
                    cbuf[buf, k] = qrep[p] / jnp.broadcast_to(weighted(kk, u), (JT, S, L))

            def two(at, buf, acc):
                for k in range(GS):
                    p = at + k
                    acc = acc + jnp.sum(block(p) * cbuf[buf, k][:, None], axis=0)
                return acc

            def run(a, b, end):
                shift = place(a) - a * GS
                even, odd = a % 2, (a + 1) % 2
                pairs = max(0, (b - a - 1) // 2)

                def both(n, acc):
                    at = (a + 2 * n) * GS + shift
                    one(at + GS, odd)
                    acc = two(at, even, acc)
                    one(at + 2 * GS, even)
                    return two(at + GS, odd, acc)

                acc = lax.fori_loop(0, pairs, both, jnp.zeros((NT, S, L), F32))
                for g in range(a + 2 * pairs, b):
                    if g + 1 < end:
                        one(place(g + 1), (g + 1) % 2)
                    acc = two(place(g), g % 2, acc)
                return acc

            one(place(0), 0)
            xs[par] = run(0, NE, NE + NC)
            copy = to_partner(xs.at[par], xr.at[par], x_ssem.at[par], x_rsem.at[par])
            copy.start()
            acc = run(NE, NE + NC, NE + NC)
            copy.wait()
            total = jnp.sum((xs[par] + xr[par]) + acc, axis=1, keepdims=True)
            return quotient(pv[...], jnp.broadcast_to(total, (NT, S, L)))

        def plan_chunk(n, dst, u):
            def one(g):
                for k in range(GS):
                    p = CS + (n * GC + g) * GS + k
                    cbuf[g % 2, k] = quotient(qrep[p], jnp.broadcast_to(weighted(block(p), u), (JT, S, L)))

            one(0)
            for g in range(GC):
                if g + 1 < GC:
                    one(g + 1)
                for k in range(GS):
                    s = (n * GC + g) * GS + k
                    v = cbuf[g % 2, k]
                    vbuf[s] = v
                    t = (block(CS + s) * u[None]) * v[:, None]
                    flat = jnp.concatenate([t[:, i].reshape(JB, L) for i in range(NT)], axis=1)
                    at = (g * GS + k) * JB
                    dst[at : at + JB, :] = flat.astype(BF16)

        def outer(r, carry):
            eps = eps_ref[r]
            inv = 1.0 / eps
            inv = inv * (2.0 - eps * inv)
            main = LOG2E * inv
            (e0, e1), (m0, m1) = halves(eps), halves(main)
            prod = eps * main
            low_part = ((e0 * m0 - prod) + (e0 * m1 + e1 * m0)) + e1 * m1
            rest = (((LOG2E - prod) - low_part) + LOG2E_REST) * inv

            def decay(x):
                return jnp.exp2(x * main + x * rest)

            cost = costs()
            for jt in range(JT):
                for t in range(NT):
                    land[CS * TB + jt * NT + t] = cost[jt * S : jt * S + S, t * L : t * L + L]

            def exps(p):
                ll = land[p * TB : p * TB + TB].reshape(JT, NT, S, L)
                low = jnp.min(jnp.min(ll, axis=0), axis=1, keepdims=True)
                kk = decay(low[None] - ll)
                kbuf[p * TB : p * TB + TB] = kk.reshape(TB, S, L)
                mb[:, p : p + 1, :] = low
                sb[:, p : p + 1, :] = jnp.sum(jnp.sum(kk, axis=0), axis=1, keepdims=True)

            def passed_on(s):
                return to_partner(
                    land.at[pl.ds((CS + s) * TB, TB)], land.at[pl.ds(s * TB, TB)], fwd_ssem.at[0], fwd_rsem.at[s]
                )

            def on_slot(op, s):
                if op == "slot":
                    if s < CS:
                        passed_on(s).start()
                    exps(CS + s)
                else:
                    passed_on(s).wait_recv()
                    exps(s)

            with jax.named_scope("gather"):
                pl.semaphore_wait(credit, NL)
                first = [(0, lambda: on_slot("slot", 0)), (len(plan["msgs"]) // 4, lambda: on_slot("partner", 0))]
                tree(land, TB, CS, plan, on_slot=on_slot, fillers=first)
                tree_sent(land, plan)
                ref = land.at[pl.ds(0, CS * TB)]
                pltpu.make_async_copy(ref, ref, fwd_ssem.at[0]).wait()
                give_credit()

            with jax.named_scope("minx"):
                def least_of(a, b):
                    low = jnp.min(mb[:, a:b], axis=1, keepdims=True)
                    part = jnp.sum(sb[:, a:b] * decay(low - mb[:, a:b]), axis=1, keepdims=True)
                    return jnp.broadcast_to(low, (NT, S, L)), jnp.broadcast_to(part, (NT, S, L))

                mss[0], mss[1] = least_of(2 * CS, NP)
                copy = to_partner(mss, msr, ms_sem.at[0], ms_sem.at[1])
                copy.start()
                low, part = least_of(0, 2 * CS)
                copy.wait()
                least = jnp.minimum(jnp.minimum(mss[0], msr[0]), low)
                total = mss[1] * decay(least - mss[0]) + msr[1] * decay(least - msr[0])
                total = total + part * decay(least - low)
                fb[...] = decay(least[:, :1] - mb[...])
                u = quotient(pv[...], total)

            with jax.named_scope("pass1"):
                u = passes(u, rescale=True, par=1)

            def sweep(t, u):
                return passes(u, par=lax.rem(t, 2))

            with jax.named_scope("sweeps"):
                u = lax.fori_loop(2, sweeps, sweep, u)
            ub[...] = u
            bacc[...] = jnp.zeros_like(bacc)
            with jax.named_scope("finish"):
                plan_chunk(0, tts[0], u)
                for n in range(KJ // CM):
                    if n + 1 < KJ // CM:
                        plan_chunk(n + 1, tts[(n + 1) % 2], u)
                    lead_and_cross(n, tts[n % 2])
                finish_lp()
            return carry

        lax.fori_loop(0, steps, outer, 0)

        pl.semaphore_wait(credit, NL)
        cost = costs()
        plan_own = (block(CS) * ub[...][None]) * vbuf[0][:, None]
        total = jnp.zeros((S, L), F32)
        for jt in range(JT):
            for t in range(NT):
                total = total + cost[jt * S : jt * S + S, t * L : t * L + L] * plan_own[jt, t]
        loss_rows[0:1] = jnp.sum(total, axis=0, keepdims=True)

        def to_chip(n):
            o = CH - n
            off = (lax.rem(o, X), lax.rem(lax.div(o, X), Y), lax.div(o, X * Y))
            at = [lax.rem(pos[d] + off[d], dims[d]) for d in range(3)]
            return pltpu.make_async_remote_copy(
                src_ref=loss_rows.at[pl.ds(0, 1)], dst_ref=loss_rows.at[pl.ds(o, 1)],
                send_sem=loss_sem.at[0], recv_sem=loss_sem.at[1],
                device_id=core * CH + at[0] + X * at[1] + X * Y * at[2], device_id_type=FLAT,
            )

        def tell(n, carry):
            to_chip(n).start()
            return carry

        lax.fori_loop(1, CH, tell, 0)

        it = lax.div(chip * NR, L)
        inside = pl.multiple_of(lax.rem(chip * NR, L), S)

        def rows_of(n, carry):
            for k in range(4):
                s = 4 * n + k
                kk = jnp.concatenate([kbuf[(CS + s) * TB + jt * NT + it] for jt in range(JT)], axis=0)
                uu = jnp.concatenate([ub[it]] * JT, axis=0)
                t = (kk * uu) * vbuf[s].reshape(JB, L)
                none = jnp.zeros_like(t)
                both = jnp.where(core == 0, jnp.concatenate([t, none], axis=0), jnp.concatenate([none, t], axis=0))
                trb[k] = both.T
                obuf[source_of(s)] = trb[k, pl.ds(inside, NR), :]
            return carry

        with jax.named_scope("tail"):
            lax.fori_loop(0, CH // 4, rows_of, 0)
            o_copy = to_partner(obuf.at[pl.ds(other * HB, HB)], orecv, o_sem.at[0], o_sem.at[1])
            o_copy.start()
            o_copy.wait()
            for b in range(HB):
                out_ref[:, b * L : b * L + L] = obuf[core * HB + b] + orecv[b]
            ref = loss_rows.at[pl.ds(1, CH - 1)]
            pltpu.make_async_copy(ref, ref, loss_sem.at[0]).wait()
            pltpu.make_async_copy(ref, ref, loss_sem.at[1]).wait()
            loss_two[0:1] = jnp.sum(loss_rows[...], axis=0, keepdims=True)
            copy = to_partner(loss_two.at[pl.ds(0, 1)], loss_two.at[pl.ds(1, 1)], loss_sem.at[2], loss_sem.at[3])
            copy.start()
            copy.wait()
            loss_ref[0] = jnp.sum(loss_two[...])

    vm = pltpu.VMEM
    dma = pltpu.SemaphoreType.DMA
    scratch = [
        vm((NP * TB, S, L), F32),
        vm((NP * TB, S, L), F32),
        vm((CH * TT0, 16, L), BF16),
        vm((CM, n_rows), BF16),
        vm((CM, n_rows), BF16),
        vm((n_rows, n_rows), F32),
        vm((n_rows, n_rows), BF16),
        vm((CH, L, L), BF16),
        vm((L, KJ), BF16),
        vm((L, n_rows), F32),
        vm((L, n_rows), F32),
        vm((JB, n_rows), F32),
        vm((L, L), F32),
        vm((CH, L), F32),
        vm((NP, JT, S, L), F32),
        vm((CH, JT, S, L), F32),
        vm((2, GS, JT, S, L), F32),
        vm((NT, NP, L), F32),
        vm((NT, NP, L), F32),
        vm((NT, NP, L), F32),
        vm((NT, S, L), F32),
        vm((S, L), F32),
        vm((2, NT, S, L), F32),
        vm((2, NT, S, L), F32),
        vm((2, NT, S, L), F32),
        vm((2, NT, S, L), F32),
        vm((NT, S, L), F32),
        vm((3, S, L), F32),
        vm((3, 3, S, L), F32),
        vm((S, L), F32),
        vm((S, L), F32),
        vm((CH, NR, L), F32),
        vm((HB, NR, L), F32),
        vm((4, L, L), F32),
        vm((CH, L), F32),
        vm((2, L), F32),
        dma((NL,)),
        dma((max(len(plan["msgs"]), len(plan0["msgs"])),)),
        dma((1,)),
        dma((CS,)),
        pltpu.SemaphoreType.REGULAR,
        dma((2,)),
        dma((2,)),
        dma((2,)),
        dma((2,)),
        dma((2,)),
        dma((2,)),
        dma((2,)),
        dma((3, 3)),
        dma((3, 3)),
        dma((2,)),
        dma((2,)),
        dma((4,)),
    ]
    return kernel, scratch


def solution(mesh):
    chips = mesh.shape["rows"]
    dims = torus_of(chips)
    grid_spec = P(("pairs", "rows"), "cols")

    def local_fn(c1, c2, t0, p, q, eps):
        n_rows, n_cols = p.shape[0] * chips, q.shape[0] * mesh.shape["cols"]
        kernel, scratch = make_kernel(dims, n_rows, n_cols, eps.shape[0], SWEEPS)
        vmem = pl.BlockSpec(memory_space=pltpu.VMEM)
        smem = pl.BlockSpec(memory_space=pltpu.SMEM)
        return pl.pallas_call(
            kernel,
            name="gromov",
            out_shape=(jax.ShapeDtypeStruct(t0.shape, F32), jax.ShapeDtypeStruct((1,), F32)),
            in_specs=[smem, smem, vmem, vmem, vmem, vmem],
            out_specs=(vmem, smem),
            scratch_shapes=scratch,
            compiler_params=pltpu.CompilerParams(
                collective_id=0, has_side_effects=True, vmem_limit_bytes=60 * 1024 * 1024
            ),
        )(eps, p, c1, c2, t0, q.reshape(chips // 2, L))

    return jax.shard_map(
        local_fn,
        mesh=mesh,
        in_specs=(grid_spec, grid_spec, grid_spec, P(("pairs", "rows")), P(("pairs", "cols")), P("pairs")),
        out_specs=(grid_spec, P("pairs")),
        check_vma=False,
    )
```

```python
import heapq
import itertools
import math

import jax
import jax.numpy as jnp
from jax import lax
from jax.experimental import pallas as pl
from jax.experimental.pallas import tpu as pltpu
from jax.sharding import PartitionSpec as P

SWEEPS = 10
FLAT = pl.DeviceIdType.LOGICAL
L, S = 128, 8
JB = 64
JT = JB // S
F32, BF16 = jnp.float32, jnp.bfloat16
ORDERS = ((0, 1, 2), (1, 2, 0), (2, 0, 1))
TILE_RATE = 11.4
HOP_US = 4.0
AHEAD_US = 2.0
LOG2E = 1.4426950216293335
LOG2E_REST = 1.925963e-8
PARTNER_US = 4.0
LATE = 165


def torus_of(chips):
    return {64: (4, 4, 4), S: (4, 2, 1), 16: (4, 4, 1)}[chips]


def halves(x):
    c = 4097.0 * x
    high = c - (c - x)
    return high, x - high


def quotient(a, b):
    q = a / b
    return q + (a - q * b) / b


def split3(n):
    cuts = [0, (n + 2) // 3, (2 * n + 2) // 3, n]
    return [(cuts[k], cuts[k + 1]) for k in range(3)]


def tree_plan(dims, tiles, rate, lat_us, ahead_us, shared=0):
    rings = {1: (), 2: ((1, "f", 1),), 4: ((1, "f", 1), (3, "f", -1), (2, "a", 1), (2, "b", -1))}
    msgs = []
    for color, order in enumerate(ORDERS):
        lo, hi = split3(tiles)[color]
        for dst in itertools.product(*(range(n) for n in dims)):
            used = [k for k in range(3) if dst[order[k]]]
            if not used or lo == hi:
                continue
            d = order[used[-1]]
            mid = lo + (hi - lo + (sum(dst) + color) % 2) // 2
            for at, part, sign in rings[dims[d]]:
                a, b = {"f": (lo, hi), "a": (lo, mid), "b": (mid, hi)}[part]
                if at != dst[d] or a == b:
                    continue
                src = list(dst)
                src[d] = (src[d] - sign) % dims[d]
                m = dict(id=len(msgs), color=color, src=tuple(src), dst=dst, link=(d, sign), lo=a, hi=b)
                m["us"] = (b - a) / rate
                msgs.append(m)
    into = {}
    for m in msgs:
        into.setdefault((m["color"], m["dst"]), []).append(m)
    users = [[] for _ in msgs]
    missing = []
    for m in msgs:
        deps = [e for e in into.get((m["color"], m["src"]), []) if e["lo"] < m["hi"] and m["lo"] < e["hi"]]
        missing.append(len(deps))
        for e in deps:
            users[e["id"]].append(m)
    way = {}

    def way_of(m):
        if m["id"] not in way:
            way[m["id"]] = m["us"] + lat_us + max([way_of(u) for u in users[m["id"]]], default=0.0)
        return way[m["id"]]

    links = sorted({m["link"] for m in msgs})
    queue = {k: [] for k in links}
    idle = dict.fromkeys(links, True)
    ready, events, ops = {}, [], []

    def put(m, now):
        ready[m["id"]] = now
        heapq.heappush(queue[m["link"]], (-way_of(m), m["id"]))

    def start(link, now):
        if idle[link] and queue[link]:
            k = heapq.heappop(queue[link])[1]
            idle[link] = False
            ops.append((max(ready[k], now - ahead_us), 1, "send", msgs[k]))
            heapq.heappush(events, (now + msgs[k]["us"], 0, k))
            heapq.heappush(events, (now + msgs[k]["us"] + lat_us, 1, k))

    for m in msgs:
        if not missing[m["id"]]:
            put(m, 0.0)
    for link in links:
        start(link, 0.0)
    left = {}
    for m in msgs:
        left[m["dst"]] = left.get(m["dst"], 0) + 1
    now = 0.0
    while events:
        now, arrived, k = heapq.heappop(events)
        m = msgs[k]
        if not arrived:
            idle[m["link"]] = True
            start(m["link"], now)
            continue
        ops.append((now, 0, "wait", m))
        for u in users[k]:
            missing[u["id"]] -= 1
            if not missing[u["id"]]:
                put(u, now)
                start(u["link"], now)
        left[m["dst"]] -= 1
        if not left[m["dst"]]:
            slot = m["dst"][0] + dims[0] * (m["dst"][1] + dims[1] * m["dst"][2])
            ops.append((now, 0, "slot", slot))
            if slot < shared:
                ops.append((now + PARTNER_US, 0, "partner", slot))
    ops.sort(key=lambda op: op[:2])
    totals = {k: sum(m["hi"] - m["lo"] for m in msgs if m["link"] == k) for k in links}
    return dict(msgs=msgs, ops=[op[2:] for op in ops], links=links, totals=totals, end=now)


def make_kernel(dims, n_rows, n_cols, steps, sweeps):
    X, Y, Z = dims
    CH = X * Y * Z
    NR = n_rows // CH
    G = NR // S
    NT = n_rows // L
    TB = JT * NT
    HB = CH // 2
    JN = n_cols // 2 // L
    JW = JN // 2
    NT0 = G * JW
    TT0 = NT0 + 2 * G
    KJ = CH * JB
    CK = min(1024, KJ)
    CM = min(1024, KJ)
    GS = min(4, CH // 2)
    CS = max(CH * 3 // 8 // GS * GS, GS)
    NP = CH + CS
    NE, NC = (CH - CS) // GS, 2 * CS // GS
    GC = CM // JB // GS
    assert NT == 4 and n_cols == CH * L and JN == HB
    plan0 = tree_plan(dims, TT0, TILE_RATE, HOP_US, AHEAD_US)
    plan = tree_plan(dims, TB, TILE_RATE, HOP_US, AHEAD_US, CS)
    links = plan["links"]
    NL = len(links)
    peers = [(d, k) for d in range(3) for k in range(1, dims[d])]
    strides = (1, X, X * Y)

    def slot_of(offset):
        return offset[0] + X * offset[1] + X * Y * offset[2]

    def kernel(
        eps_ref, p_ref, c1_ref, c2_ref, t0_ref, q_ref,
        out_ref, loss_ref,
        land, kbuf, g0, tt0, tt1, c1f, c1b, c2n, c2p, bacc, lp, lprecv, bp, qf, qrep, vbuf, cbuf,
        mb, sb, fb, ub, ap, xs, xr, mss, msr, pv, ars, arr, arps, arpr, obuf, orecv, trb, loss_rows, loss_two, c2v,
        send_sem, recv_sem, fwd_ssem, fwd_rsem, credit, x_ssem, x_rsem, ms_sem, lp_sem, c1_sem, c2_sem, q_sem, ar_ssem, ar_rsem, arp_sem, o_sem, loss_sem, in_sem,
    ):
        tts = (tt0, tt1)
        chip = lax.axis_index("rows")
        core = lax.axis_index("cols")
        other = 1 - core
        pos = (lax.rem(chip, X), lax.rem(lax.div(chip, X), Y), lax.div(chip, X * Y))

        me = core * CH + chip
        partner = other * CH + chip

        def moved(d, k):
            return me + (lax.rem(pos[d] + k + dims[d], dims[d]) - pos[d]) * strides[d]

        near = {link: moved(*link) for link in links}

        def source_of(slot):
            off = (lax.rem(slot, X), lax.rem(lax.div(slot, X), Y), lax.div(slot, X * Y))
            at = [lax.rem(pos[d] + dims[d] - off[d], dims[d]) for d in range(3)]
            return at[0] + X * at[1] + X * Y * at[2]

        def to_partner(src, dst, ssem, rsem):
            return pltpu.make_async_remote_copy(
                src_ref=src, dst_ref=dst, send_sem=ssem, recv_sem=rsem,
                device_id=partner, device_id_type=FLAT,
            )

        def tree_copy(buf, width, first, m):
            n = m["hi"] - m["lo"]
            return pltpu.make_async_remote_copy(
                src_ref=buf.at[pl.ds((first + slot_of(m["src"])) * width + m["lo"], n)],
                dst_ref=buf.at[pl.ds((first + slot_of(m["dst"])) * width + m["lo"], n)],
                send_sem=send_sem.at[links.index(m["link"])],
                recv_sem=recv_sem.at[m["id"]],
                device_id=near[m["link"]],
                device_id_type=FLAT,
            )

        def tree(buf, width, first, the_plan, before_send=None, on_slot=None, fillers=()):
            fillers, ready, waits = list(fillers), [], 0
            for op, m in the_plan["ops"]:
                if op == "send":
                    if before_send is not None:
                        before_send(m)
                    tree_copy(buf, width, first, m).start()
                elif op == "wait":
                    while fillers and not fillers[0][0]:
                        fillers.pop(0)[1]()
                    ref = buf.at[pl.ds((first + slot_of(m["dst"])) * width + m["lo"], m["hi"] - m["lo"])]
                    pltpu.make_async_copy(ref, ref, recv_sem.at[m["id"]]).wait()
                    waits += 1
                    if ready:
                        on_slot(*ready.pop(0))
                    elif fillers and waits >= fillers[0][0]:
                        fillers.pop(0)[1]()
                elif on_slot is not None:
                    ready.append((op, m))
            for at in ready:
                on_slot(*at)
            for _, f in fillers:
                f()

        def tree_sent(buf, the_plan):
            for k, link in enumerate(links):
                n = the_plan["totals"][link]
                ref = buf.at[pl.ds(0, n)]
                pltpu.make_async_copy(ref, ref, send_sem.at[k]).wait()

        def give_credit():
            for d, sign in links:
                pl.semaphore_signal(credit, inc=1, device_id=moved(d, -sign), device_id_type=FLAT)

        def all_sum_send(stage):
            for n, k in enumerate(range(1, dims[stage])):
                pltpu.make_async_remote_copy(
                    src_ref=ars.at[stage], dst_ref=arr.at[stage, n],
                    send_sem=ar_ssem.at[stage, n], recv_sem=ar_rsem.at[stage, n],
                    device_id=moved(stage, k), device_id_type=FLAT,
                ).start()

        def all_sum_get(stage):
            total = ars[stage]
            for n, k in enumerate(range(1, dims[stage])):
                pltpu.make_async_remote_copy(
                    src_ref=ars.at[stage], dst_ref=arr.at[stage, n],
                    send_sem=ar_ssem.at[stage, n], recv_sem=ar_rsem.at[stage, n],
                    device_id=moved(stage, k), device_id_type=FLAT,
                ).wait()
                total = total + arr[stage, n]
            return total

        def all_sum_step(stage):
            total = all_sum_get(stage)
            if stage < 2:
                ars[stage + 1] = total
                all_sum_send(stage + 1)
            else:
                arps[...] = total
                to_partner(arps, arpr, arp_sem.at[0], arp_sem.at[1]).start()

        c2_in = pltpu.make_async_copy(c2_ref, c2v, in_sem.at[0])
        c2_in.start()
        barrier = pltpu.get_barrier_semaphore()
        for d, k in peers:
            pl.semaphore_signal(barrier, inc=1, device_id=moved(d, k), device_id_type=FLAT)
        pl.semaphore_signal(barrier, inc=1, device_id=partner, device_id_type=FLAT)

        row = lax.broadcasted_iota(jnp.int32, (S, L), 0)
        lane = lax.broadcasted_iota(jnp.int32, (S, L), 1)

        for g in range(G):
            rows = slice(g * S, g * S + S)
            pair = jnp.concatenate([c1_ref[rows, :L], c1_ref[rows, L:]], axis=0)
            g0[NT0 + core * G + g] = pair.astype(BF16)
        c1_copy = to_partner(
            g0.at[pl.ds(NT0 + core * G, G)], g0.at[pl.ds(NT0 + core * G, G)], c1_sem.at[0], c1_sem.at[1]
        )
        q_copy = to_partner(q_ref, qf.at[pl.ds(core * HB, HB)], q_sem.at[0], q_sem.at[1])

        tile = jnp.zeros((S, L), F32)
        for t in range(2):
            part = jnp.zeros((1, L), F32)
            for k in range(NR):
                entry = c1_ref[k : k + 1, t * L : t * L + L]
                part = part + entry * entry * p_ref[k]
            tile = jnp.where(row == 2 * core + t, jnp.broadcast_to(part, (S, L)), tile)
        where = (row - 4) * L + lane
        for k in range(NR):
            tile = jnp.where(where == chip * NR + k, p_ref[k], tile)
        ars[0] = tile
        for g in range(G):
            rows = slice(g * S, g * S + S)
            for t in range(JW):
                a, b = t0_ref[rows, (2 * L) * t : (2 * L) * t + L], t0_ref[rows, (2 * L) * t + L : (2 * L) * t + (2 * L)]
                g0[g * JW + t] = jnp.concatenate([a, b], axis=0).astype(BF16)
        qf[pl.ds(core * HB, HB)] = q_ref[...]

        c2_copy = to_partner(c2n.at[pl.ds(core * HB, HB)], c2n.at[pl.ds(core * HB, HB)], c2_sem.at[0], c2_sem.at[1])
        bp[...] = jnp.zeros_like(bp)

        def round_c2(first, last):
            c2_in.wait()
            for t in range(first, last):
                blk = c2v[:, t * L : t * L + L]
                c2n[core * HB + t] = blk.astype(BF16)
                bp[...] += blk * blk * q_ref[t : t + 1, :]

        def finish_b():
            bp[...] = jnp.broadcast_to(jnp.sum(bp[...], axis=1, keepdims=True), (L, L))

        with jax.named_scope("barrier"):
            pl.semaphore_wait(barrier, len(peers) + 1)
        give_credit()
        c1_copy.start()
        q_copy.start()
        all_sum_send(0)

        src = lax.broadcasted_iota(jnp.int32, (L, L), 0)
        dst = lax.broadcasted_iota(jnp.int32, (L, L), 1)
        picks = [
            jnp.where((src - core * JB == dst - h * JB) & (dst >= h * JB) & (dst < h * JB + JB), 1.0, 0.0).astype(BF16)
            for h in range(2)
        ]

        def order_c2(first, last):
            for t in range(first, last):
                a = jnp.dot(c2n[source_of(2 * t)], picks[0], preferred_element_type=F32)
                b = jnp.dot(c2n[source_of(2 * t + 1)], picks[1], preferred_element_type=F32)
                c2p[:, t * L : t * L + L] = (a + b).astype(BF16)

        def order_q(first, last):
            def four(n, carry):
                for k in range(4):
                    p = 4 * n + k
                    shared = p < CS
                    half = jnp.where(shared, other, core)
                    line = jnp.broadcast_to(qf[pl.ds(source_of(jnp.where(shared, p, p - CS)), 1), :], (S, L))
                    for jt in range(JT):
                        own = jnp.where(lane == half * JB + jt * S + row, line, 0.0)
                        qrep[p, jt] = jnp.broadcast_to(jnp.sum(own, axis=1, keepdims=True), (S, L))
                return carry

            lax.fori_loop(first // 4, last // 4, four, 0)

        def span(n, parts, f):
            cuts = [n * k // parts for k in range(parts + 1)]
            return [lambda a=a, b=b: f(a, b) for a, b in zip(cuts, cuts[1:])]

        fillers = [(0, lambda: round_c2(0, HB)), (0, finish_b), (0, lambda: c2_copy.start())]
        fillers += [(0, lambda: q_copy.wait()), (0, lambda: order_q(0, NP)), (LATE // 2, lambda: all_sum_step(0))]
        fillers += [(LATE, lambda: all_sum_step(1))]
        waited = []

        def before_send(m):
            if not waited and m["hi"] > NT0:
                waited.append(1)
                c1_copy.wait()

        def unpack(op, s):
            chip_s = source_of(s)
            for g in range(G):
                tiles = g0[s * TT0 + g * JW : s * TT0 + g * JW + JW].astype(F32).reshape(JN, S, L)
                kbuf[pl.ds((chip_s * G + g) * JN, JN)] = tiles
                at = pl.ds(pl.multiple_of(chip_s * NR + g * S, S), S)
                for h in range(2):
                    pair = g0[s * TT0 + NT0 + h * G + g].astype(F32)
                    c1f[at, 2 * L * h : 2 * L * h + L] = pair[:S]
                    c1f[at, 2 * L * h + L : 2 * L * h + 2 * L] = pair[S:]

        with jax.named_scope("gather0"):
            first = [(0, lambda: unpack("slot", 0))]
            tree(g0, TT0, 0, plan0, before_send=before_send, on_slot=unpack, fillers=first + fillers)
            tree_sent(g0, plan0)
            c1b[...] = c1f[...].astype(BF16)
            all_sum_step(2)

        def finish_lp():
            lp[...] = jnp.concatenate([bp[...]] * NT, axis=1) - 2.0 * bacc[...]

        bacc[...] = jnp.zeros_like(bacc)
        JC = CK // L

        def first_chunk(n, carry):
            cols = []
            for t in range(JC):
                cols.append(kbuf[pl.ds(n * JC + t, CH * G, stride=JN)].reshape(n_rows, L))
            plan_c = jnp.concatenate(cols, axis=1).astype(BF16)
            lead = jnp.dot(c1b[...], plan_c, preferred_element_type=F32).astype(BF16)
            c2c = jnp.concatenate([c2n[core * HB + n * JC + t] for t in range(JC)], axis=1)
            bacc[...] += lax.dot_general(c2c, lead, (((1,), (1,)), ((), ())), preferred_element_type=F32)
            return carry

        with jax.named_scope("firstmm"):
            lax.fori_loop(0, KJ // CK, first_chunk, 0)
            finish_lp()
        to_partner(arps, arpr, arp_sem.at[0], arp_sem.at[1]).wait()
        ap[...] = jnp.where(row < 4, arps[...] + arpr[...], arps[...])
        for t in range(NT):
            pv[t] = jnp.broadcast_to(ap[4 + t : 5 + t, :], (S, L))


        def lead_and_cross(n, plan_c):
            lead = jnp.dot(plan_c[...], c1b[...], preferred_element_type=F32).astype(BF16)
            bacc[...] += jnp.dot(c2p[:, n * CM : n * CM + CM], lead, preferred_element_type=F32)

        def costs():
            copy = to_partner(lp.at[pl.ds(other * JB, JB)], lprecv, lp_sem.at[0], lp_sem.at[1])
            copy.start()
            copy.wait()
            own = lp[pl.ds(pl.multiple_of(core * JB, JB), JB), :] + lprecv[...]
            return own + jnp.concatenate([ap[t : t + 1, :] for t in range(NT)], axis=1)

        def block(s):
            return kbuf[pl.ds(s * TB, TB)].reshape(JT, NT, S, L)

        def weighted(kk, u):
            w = (kk[:, 0] * u[0] + kk[:, 1] * u[1]) + (kk[:, 2] * u[2] + kk[:, 3] * u[3])
            return jnp.sum(w, axis=2, keepdims=True)

        def passes(u, rescale=False, par=0):
            def place(g):
                return g * GS + 2 * CS if not isinstance(g, int) or g < NE else (g - NE) * GS

            def one(at, buf):
                for k in range(GS):
                    p = at + k
                    kk = block(p)
                    if rescale:
                        kk = kk * fb[:, pl.ds(p, 1), :][None]
                        kbuf[pl.ds(p * TB, TB)] = kk.reshape(TB, S, L)
                    cbuf[buf, k] = qrep[p] / jnp.broadcast_to(weighted(kk, u), (JT, S, L))

            def two(at, buf, acc):
                for k in range(GS):
                    p = at + k
                    acc = acc + jnp.sum(block(p) * cbuf[buf, k][:, None], axis=0)
                return acc

            def run(a, b, end):
                shift = place(a) - a * GS
                even, odd = a % 2, (a + 1) % 2
                pairs = max(0, (b - a - 1) // 2)

                def both(n, acc):
                    at = (a + 2 * n) * GS + shift
                    one(at + GS, odd)
                    acc = two(at, even, acc)
                    one(at + 2 * GS, even)
                    return two(at + GS, odd, acc)

                acc = lax.fori_loop(0, pairs, both, jnp.zeros((NT, S, L), F32))
                for g in range(a + 2 * pairs, b):
                    if g + 1 < end:
                        one(place(g + 1), (g + 1) % 2)
                    acc = two(place(g), g % 2, acc)
                return acc

            one(place(0), 0)
            xs[par] = run(0, NE, NE + NC)
            copy = to_partner(xs.at[par], xr.at[par], x_ssem.at[par], x_rsem.at[par])
            copy.start()
            acc = run(NE, NE + NC, NE + NC)
            copy.wait()
            total = jnp.sum((xs[par] + xr[par]) + acc, axis=1, keepdims=True)
            return quotient(pv[...], jnp.broadcast_to(total, (NT, S, L)))

        def plan_chunk(n, dst, u):
            def one(g):
                for k in range(GS):
                    p = CS + (n * GC + g) * GS + k
                    cbuf[g % 2, k] = quotient(qrep[p], jnp.broadcast_to(weighted(block(p), u), (JT, S, L)))

            one(0)
            for g in range(GC):
                if g + 1 < GC:
                    one(g + 1)
                for k in range(GS):
                    s = (n * GC + g) * GS + k
                    v = cbuf[g % 2, k]
                    vbuf[s] = v
                    t = (block(CS + s) * u[None]) * v[:, None]
                    flat = jnp.concatenate([t[:, i].reshape(JB, L) for i in range(NT)], axis=1)
                    at = (g * GS + k) * JB
                    dst[at : at + JB, :] = flat.astype(BF16)

        def outer(r, carry):
            eps = eps_ref[r]
            inv = 1.0 / eps
            inv = inv * (2.0 - eps * inv)
            main = LOG2E * inv
            (e0, e1), (m0, m1) = halves(eps), halves(main)
            prod = eps * main
            low_part = ((e0 * m0 - prod) + (e0 * m1 + e1 * m0)) + e1 * m1
            rest = (((LOG2E - prod) - low_part) + LOG2E_REST) * inv

            def decay(x):
                return jnp.exp2(x * main + x * rest)

            cost = costs()
            for jt in range(JT):
                for t in range(NT):
                    land[CS * TB + jt * NT + t] = cost[jt * S : jt * S + S, t * L : t * L + L]

            def exps(p):
                ll = land[p * TB : p * TB + TB].reshape(JT, NT, S, L)
                low = jnp.min(jnp.min(ll, axis=0), axis=1, keepdims=True)
                kk = decay(low[None] - ll)
                kbuf[p * TB : p * TB + TB] = kk.reshape(TB, S, L)
                mb[:, p : p + 1, :] = low
                sb[:, p : p + 1, :] = jnp.sum(jnp.sum(kk, axis=0), axis=1, keepdims=True)

            def passed_on(s):
                return to_partner(
                    land.at[pl.ds((CS + s) * TB, TB)], land.at[pl.ds(s * TB, TB)], fwd_ssem.at[0], fwd_rsem.at[s]
                )

            def on_slot(op, s):
                if op == "slot":
                    if s < CS:
                        passed_on(s).start()
                    exps(CS + s)
                else:
                    passed_on(s).wait_recv()
                    exps(s)

            def once(n, f):
                @pl.when(r == 0)
                def _():
                    if not n:
                        c2_copy.wait()
                    f()

            with jax.named_scope("gather"):
                pl.semaphore_wait(credit, NL)
                first = [(0, lambda: on_slot("slot", 0)), (len(plan["msgs"]) // 4, lambda: on_slot("partner", 0))]
                for n, f in enumerate(span(CH // 2, S, order_c2)):
                    first.append((LATE // 2 + 4 * n, lambda n=n, f=f: once(n, f)))
                tree(land, TB, CS, plan, on_slot=on_slot, fillers=first)
                tree_sent(land, plan)
                ref = land.at[pl.ds(0, CS * TB)]
                pltpu.make_async_copy(ref, ref, fwd_ssem.at[0]).wait()
                give_credit()

            with jax.named_scope("minx"):
                def least_of(a, b):
                    low = jnp.min(mb[:, a:b], axis=1, keepdims=True)
                    part = jnp.sum(sb[:, a:b] * decay(low - mb[:, a:b]), axis=1, keepdims=True)
                    return jnp.broadcast_to(low, (NT, S, L)), jnp.broadcast_to(part, (NT, S, L))

                mss[0], mss[1] = least_of(2 * CS, NP)
                copy = to_partner(mss, msr, ms_sem.at[0], ms_sem.at[1])
                copy.start()
                low, part = least_of(0, 2 * CS)
                copy.wait()
                least = jnp.minimum(jnp.minimum(mss[0], msr[0]), low)
                total = mss[1] * decay(least - mss[0]) + msr[1] * decay(least - msr[0])
                total = total + part * decay(least - low)
                fb[...] = decay(least[:, :1] - mb[...])
                u = quotient(pv[...], total)

            with jax.named_scope("pass1"):
                u = passes(u, rescale=True, par=1)

            def sweep(t, u):
                return passes(u, par=lax.rem(t, 2))

            with jax.named_scope("sweeps"):
                u = lax.fori_loop(2, sweeps, sweep, u)
            ub[...] = u
            bacc[...] = jnp.zeros_like(bacc)
            with jax.named_scope("finish"):
                plan_chunk(0, tts[0], u)
                for n in range(KJ // CM):
                    if n + 1 < KJ // CM:
                        plan_chunk(n + 1, tts[(n + 1) % 2], u)
                    lead_and_cross(n, tts[n % 2])
                finish_lp()
            return carry

        lax.fori_loop(0, steps, outer, 0)

        pl.semaphore_wait(credit, NL)
        cost = costs()
        plan_own = (block(CS) * ub[...][None]) * vbuf[0][:, None]
        total = jnp.zeros((S, L), F32)
        for jt in range(JT):
            for t in range(NT):
                total = total + cost[jt * S : jt * S + S, t * L : t * L + L] * plan_own[jt, t]
        loss_rows[0:1] = jnp.sum(total, axis=0, keepdims=True)

        def to_chip(n):
            o = CH - n
            off = (lax.rem(o, X), lax.rem(lax.div(o, X), Y), lax.div(o, X * Y))
            at = [lax.rem(pos[d] + off[d], dims[d]) for d in range(3)]
            return pltpu.make_async_remote_copy(
                src_ref=loss_rows.at[pl.ds(0, 1)], dst_ref=loss_rows.at[pl.ds(o, 1)],
                send_sem=loss_sem.at[0], recv_sem=loss_sem.at[1],
                device_id=core * CH + at[0] + X * at[1] + X * Y * at[2], device_id_type=FLAT,
            )

        def tell(n, carry):
            to_chip(n).start()
            return carry

        lax.fori_loop(1, CH, tell, 0)

        it = lax.div(chip * NR, L)
        inside = pl.multiple_of(lax.rem(chip * NR, L), S)

        def rows_of(n, carry):
            for k in range(4):
                s = 4 * n + k
                kk = jnp.concatenate([kbuf[(CS + s) * TB + jt * NT + it] for jt in range(JT)], axis=0)
                uu = jnp.concatenate([ub[it]] * JT, axis=0)
                t = (kk * uu) * vbuf[s].reshape(JB, L)
                none = jnp.zeros_like(t)
                both = jnp.where(core == 0, jnp.concatenate([t, none], axis=0), jnp.concatenate([none, t], axis=0))
                trb[k] = both.T
                obuf[source_of(s)] = trb[k, pl.ds(inside, NR), :]
            return carry

        with jax.named_scope("tail"):
            lax.fori_loop(0, CH // 4, rows_of, 0)
            o_copy = to_partner(obuf.at[pl.ds(other * HB, HB)], orecv, o_sem.at[0], o_sem.at[1])
            o_copy.start()
            o_copy.wait()
            orecv[...] = obuf[pl.ds(core * HB, HB)] + orecv[...]
            o_out = pltpu.make_async_copy(orecv, out_ref, in_sem.at[1])
            o_out.start()
            ref = loss_rows.at[pl.ds(1, CH - 1)]
            pltpu.make_async_copy(ref, ref, loss_sem.at[0]).wait()
            pltpu.make_async_copy(ref, ref, loss_sem.at[1]).wait()
            loss_two[0:1] = jnp.sum(loss_rows[...], axis=0, keepdims=True)
            copy = to_partner(loss_two.at[pl.ds(0, 1)], loss_two.at[pl.ds(1, 1)], loss_sem.at[2], loss_sem.at[3])
            copy.start()
            copy.wait()
            loss_ref[0] = jnp.sum(loss_two[...])
            o_out.wait()

    vm = pltpu.VMEM
    dma = pltpu.SemaphoreType.DMA
    scratch = [
        vm((NP * TB, S, L), F32),
        vm((NP * TB, S, L), F32),
        vm((CH * TT0, 16, L), BF16),
        vm((CM, n_rows), BF16),
        vm((CM, n_rows), BF16),
        vm((n_rows, n_rows), F32),
        vm((n_rows, n_rows), BF16),
        vm((CH, L, L), BF16),
        vm((L, KJ), BF16),
        vm((L, n_rows), F32),
        vm((L, n_rows), F32),
        vm((JB, n_rows), F32),
        vm((L, L), F32),
        vm((CH, L), F32),
        vm((NP, JT, S, L), F32),
        vm((CH, JT, S, L), F32),
        vm((2, GS, JT, S, L), F32),
        vm((NT, NP, L), F32),
        vm((NT, NP, L), F32),
        vm((NT, NP, L), F32),
        vm((NT, S, L), F32),
        vm((S, L), F32),
        vm((2, NT, S, L), F32),
        vm((2, NT, S, L), F32),
        vm((2, NT, S, L), F32),
        vm((2, NT, S, L), F32),
        vm((NT, S, L), F32),
        vm((3, S, L), F32),
        vm((3, 3, S, L), F32),
        vm((S, L), F32),
        vm((S, L), F32),
        vm((CH, NR, L), F32),
        vm((HB, NR, L), F32),
        vm((4, L, L), F32),
        vm((CH, L), F32),
        vm((2, L), F32),
        vm((L, n_cols // 2), F32),
        dma((NL,)),
        dma((max(len(plan["msgs"]), len(plan0["msgs"])),)),
        dma((1,)),
        dma((CS,)),
        pltpu.SemaphoreType.REGULAR,
        dma((2,)),
        dma((2,)),
        dma((2,)),
        dma((2,)),
        dma((2,)),
        dma((2,)),
        dma((2,)),
        dma((3, 3)),
        dma((3, 3)),
        dma((2,)),
        dma((2,)),
        dma((4,)),
        dma((2,)),
    ]
    return kernel, scratch


def solution(mesh):
    chips = mesh.shape["rows"]
    dims = torus_of(chips)
    grid_spec = P(("pairs", "rows"), "cols")

    def local_fn(c1, c2, t0, p, q, eps):
        n_rows, n_cols = p.shape[0] * chips, q.shape[0] * mesh.shape["cols"]
        kernel, scratch = make_kernel(dims, n_rows, n_cols, eps.shape[0], SWEEPS)
        vmem = pl.BlockSpec(memory_space=pltpu.VMEM)
        smem = pl.BlockSpec(memory_space=pltpu.SMEM)
        anywhere = pl.BlockSpec(memory_space=pl.ANY)
        plan, loss = pl.pallas_call(
            kernel,
            name="gromov",
            out_shape=(jax.ShapeDtypeStruct((chips // 2, t0.shape[0], L), F32), jax.ShapeDtypeStruct((1,), F32)),
            in_specs=[smem, smem, vmem, anywhere, vmem, vmem],
            out_specs=(anywhere, smem),
            scratch_shapes=scratch,
            compiler_params=pltpu.CompilerParams(
                collective_id=0, has_side_effects=True, vmem_limit_bytes=60 * 1024 * 1024
            ),
        )(eps, p, c1, c2, t0, q.reshape(chips // 2, L))
        return plan.transpose(1, 0, 2).reshape(t0.shape), loss

    return jax.shard_map(
        local_fn,
        mesh=mesh,
        in_specs=(grid_spec, grid_spec, grid_spec, P(("pairs", "rows")), P(("pairs", "cols")), P("pairs")),
        out_specs=(grid_spec, P("pairs")),
        check_vma=False,
    )
```

```python
import heapq
import itertools
import math

import jax
import jax.numpy as jnp
from jax import lax
from jax.experimental import pallas as pl
from jax.experimental.pallas import tpu as pltpu
from jax.sharding import PartitionSpec as P

SWEEPS = 10
FLAT = pl.DeviceIdType.LOGICAL
L, S = 128, 8
JB = 64
JT = JB // S
F32, BF16 = jnp.float32, jnp.bfloat16
ORDERS = ((0, 1, 2), (1, 2, 0), (2, 0, 1))
TILE_RATE = 11.4
HOP_US = 4.0
AHEAD_US = 2.0
LOG2E = 1.4426950216293335
LOG2E_REST = 1.925963e-8
PARTNER_US = 4.0
LATE = 100


def torus_of(chips):
    return {64: (4, 4, 4), S: (4, 2, 1), 16: (4, 4, 1)}[chips]


def halves(x):
    c = 4097.0 * x
    high = c - (c - x)
    return high, x - high


def quotient(a, b):
    q = a / b
    return q + (a - q * b) / b


def split3(n):
    cuts = [0, (n + 2) // 3, (2 * n + 2) // 3, n]
    return [(cuts[k], cuts[k + 1]) for k in range(3)]


def tree_plan(dims, tiles, rate, lat_us, ahead_us, shared=0):
    rings = {1: (), 2: ((1, "f", 1),), 4: ((1, "f", 1), (3, "f", -1), (2, "a", 1), (2, "b", -1))}
    msgs = []
    for color, order in enumerate(ORDERS):
        lo, hi = split3(tiles)[color]
        for dst in itertools.product(*(range(n) for n in dims)):
            used = [k for k in range(3) if dst[order[k]]]
            if not used or lo == hi:
                continue
            d = order[used[-1]]
            mid = lo + (hi - lo + (sum(dst) + color) % 2) // 2
            for at, part, sign in rings[dims[d]]:
                a, b = {"f": (lo, hi), "a": (lo, mid), "b": (mid, hi)}[part]
                if at != dst[d] or a == b:
                    continue
                src = list(dst)
                src[d] = (src[d] - sign) % dims[d]
                m = dict(id=len(msgs), color=color, src=tuple(src), dst=dst, link=(d, sign), lo=a, hi=b)
                m["us"] = (b - a) / rate
                msgs.append(m)
    into = {}
    for m in msgs:
        into.setdefault((m["color"], m["dst"]), []).append(m)
    users = [[] for _ in msgs]
    missing = []
    for m in msgs:
        deps = [e for e in into.get((m["color"], m["src"]), []) if e["lo"] < m["hi"] and m["lo"] < e["hi"]]
        missing.append(len(deps))
        for e in deps:
            users[e["id"]].append(m)
    sems, waiting = {}, {}
    for m in msgs:
        key = (m["color"] if users[m["id"]] else None, m["dst"])
        m["sem"] = sems.setdefault(key, len(sems))
        waiting.setdefault(m["sem"], []).append(m)
    pending = {k: len(group) for k, group in waiting.items()}
    way = {}

    def way_of(m):
        if m["id"] not in way:
            way[m["id"]] = m["us"] + lat_us + max([way_of(u) for u in users[m["id"]]], default=0.0)
        return way[m["id"]]

    links = sorted({m["link"] for m in msgs})
    queue = {k: [] for k in links}
    idle = dict.fromkeys(links, True)
    ready, events, ops = {}, [], []

    def put(m, now):
        ready[m["id"]] = now
        heapq.heappush(queue[m["link"]], (-way_of(m), m["id"]))

    def start(link, now):
        if idle[link] and queue[link]:
            k = heapq.heappop(queue[link])[1]
            idle[link] = False
            ops.append((max(ready[k], now - ahead_us), 1, "send", msgs[k]))
            heapq.heappush(events, (now + msgs[k]["us"], 0, k))
            heapq.heappush(events, (now + msgs[k]["us"] + lat_us, 1, k))

    for m in msgs:
        if not missing[m["id"]]:
            put(m, 0.0)
    for link in links:
        start(link, 0.0)
    left = {}
    for m in msgs:
        left[m["dst"]] = left.get(m["dst"], 0) + 1
    now = 0.0
    while events:
        now, arrived, k = heapq.heappop(events)
        m = msgs[k]
        if not arrived:
            idle[m["link"]] = True
            start(m["link"], now)
            continue
        pending[m["sem"]] -= 1
        if not pending[m["sem"]]:
            ops.append((now, 0, "wait", waiting[m["sem"]]))
        for u in users[k]:
            missing[u["id"]] -= 1
            if not missing[u["id"]]:
                put(u, now)
                start(u["link"], now)
        left[m["dst"]] -= 1
        if not left[m["dst"]]:
            slot = m["dst"][0] + dims[0] * (m["dst"][1] + dims[1] * m["dst"][2])
            ops.append((now, 0, "slot", slot))
            if slot < shared:
                ops.append((now + PARTNER_US, 0, "partner", slot))
    ops.sort(key=lambda op: op[:2])
    totals = {k: sum(m["hi"] - m["lo"] for m in msgs if m["link"] == k) for k in links}
    return dict(waits=len(sems), ops=[op[2:] for op in ops], links=links, totals=totals, end=now)


def make_kernel(dims, n_rows, n_cols, steps, sweeps):
    X, Y, Z = dims
    CH = X * Y * Z
    NR = n_rows // CH
    G = NR // S
    NT = n_rows // L
    TB = JT * NT
    HB = CH // 2
    JN = n_cols // 2 // L
    JW = JN // 2
    NT0 = G * JW
    TT0 = NT0 + 2 * G
    KJ = CH * JB
    CK = min(1024, KJ)
    CM = min(1024, KJ)
    GS = min(4, CH // 2)
    CS = max(CH * 3 // 8 // GS * GS, GS)
    NP = CH + CS
    NE, NC = (CH - CS) // GS, 2 * CS // GS
    GC = CM // JB // GS
    assert NT == 4 and n_cols == CH * L and JN == HB
    plan0 = tree_plan(dims, TT0, TILE_RATE, HOP_US, AHEAD_US)
    plan = tree_plan(dims, TB, TILE_RATE, HOP_US, AHEAD_US, CS)
    links = plan["links"]
    NL = len(links)
    peers = [(d, k) for d in range(3) for k in range(1, dims[d])]
    strides = (1, X, X * Y)

    def slot_of(offset):
        return offset[0] + X * offset[1] + X * Y * offset[2]

    def kernel(
        eps_ref, p_ref, c1_ref, c2_ref, t0_ref, q_ref,
        out_ref, loss_ref,
        land, kbuf, g0, tt0, tt1, c1f, c1b, c2n, c2p, bacc, lp, lprecv, bp, qf, qrep, vbuf, cbuf,
        mb, sb, fb, ub, ap, xs, xr, mss, msr, pv, ars, arr, arps, arpr, obuf, orecv, trb, loss_rows, loss_two, c2v,
        send_sem, recv_sem, fwd_ssem, fwd_rsem, credit, x_ssem, x_rsem, ms_sem, lp_sem, c1_sem, c2_sem, q_sem, ar_ssem, ar_rsem, arp_sem, o_sem, loss_sem, in_sem,
    ):
        tts = (tt0, tt1)
        chip = lax.axis_index("rows")
        core = lax.axis_index("cols")
        other = 1 - core
        pos = (lax.rem(chip, X), lax.rem(lax.div(chip, X), Y), lax.div(chip, X * Y))

        me = core * CH + chip
        partner = other * CH + chip

        def moved(d, k):
            return me + (lax.rem(pos[d] + k + dims[d], dims[d]) - pos[d]) * strides[d]

        near = {link: moved(*link) for link in links}

        def source_of(slot):
            off = (lax.rem(slot, X), lax.rem(lax.div(slot, X), Y), lax.div(slot, X * Y))
            at = [lax.rem(pos[d] + dims[d] - off[d], dims[d]) for d in range(3)]
            return at[0] + X * at[1] + X * Y * at[2]

        def to_partner(src, dst, ssem, rsem):
            return pltpu.make_async_remote_copy(
                src_ref=src, dst_ref=dst, send_sem=ssem, recv_sem=rsem,
                device_id=partner, device_id_type=FLAT,
            )

        def tree_copy(buf, width, first, m):
            n = m["hi"] - m["lo"]
            return pltpu.make_async_remote_copy(
                src_ref=buf.at[pl.ds((first + slot_of(m["src"])) * width + m["lo"], n)],
                dst_ref=buf.at[pl.ds((first + slot_of(m["dst"])) * width + m["lo"], n)],
                send_sem=send_sem.at[links.index(m["link"])],
                recv_sem=recv_sem.at[m["sem"]],
                device_id=near[m["link"]],
                device_id_type=FLAT,
            )

        def tree(buf, width, first, the_plan, before_send=None, on_slot=None, fillers=()):
            fillers, ready, waits = list(fillers), [], 0
            for op, m in the_plan["ops"]:
                if op == "send":
                    if before_send is not None:
                        before_send(m)
                    tree_copy(buf, width, first, m).start()
                elif op == "wait":
                    while fillers and not fillers[0][0]:
                        fillers.pop(0)[1]()
                    if ready:
                        on_slot(*ready.pop(0))
                    elif fillers and waits >= fillers[0][0]:
                        fillers.pop(0)[1]()
                    n = sum(e["hi"] - e["lo"] for e in m)
                    ref = buf.at[pl.ds((first + slot_of(m[0]["dst"])) * width, n)]
                    pltpu.make_async_copy(ref, ref, recv_sem.at[m[0]["sem"]]).wait()
                    waits += 1
                elif on_slot is not None:
                    ready.append((op, m))
            for at in ready:
                on_slot(*at)
            for _, f in fillers:
                f()

        def tree_sent(buf, the_plan):
            for k, link in enumerate(links):
                n = the_plan["totals"][link]
                ref = buf.at[pl.ds(0, n)]
                pltpu.make_async_copy(ref, ref, send_sem.at[k]).wait()

        def give_credit():
            for d, sign in links:
                pl.semaphore_signal(credit, inc=1, device_id=moved(d, -sign), device_id_type=FLAT)

        def all_sum_send(stage):
            for n, k in enumerate(range(1, dims[stage])):
                pltpu.make_async_remote_copy(
                    src_ref=ars.at[stage], dst_ref=arr.at[stage, n],
                    send_sem=ar_ssem.at[stage, n], recv_sem=ar_rsem.at[stage, n],
                    device_id=moved(stage, k), device_id_type=FLAT,
                ).start()

        def all_sum_get(stage):
            total = ars[stage]
            for n, k in enumerate(range(1, dims[stage])):
                pltpu.make_async_remote_copy(
                    src_ref=ars.at[stage], dst_ref=arr.at[stage, n],
                    send_sem=ar_ssem.at[stage, n], recv_sem=ar_rsem.at[stage, n],
                    device_id=moved(stage, k), device_id_type=FLAT,
                ).wait()
                total = total + arr[stage, n]
            return total

        def all_sum_step(stage):
            total = all_sum_get(stage)
            if stage < 2:
                ars[stage + 1] = total
                all_sum_send(stage + 1)
            else:
                arps[...] = total
                to_partner(arps, arpr, arp_sem.at[0], arp_sem.at[1]).start()

        c2_in = pltpu.make_async_copy(c2_ref, c2v, in_sem.at[0])
        c2_in.start()
        barrier = pltpu.get_barrier_semaphore()
        for d, k in peers:
            pl.semaphore_signal(barrier, inc=1, device_id=moved(d, k), device_id_type=FLAT)
        pl.semaphore_signal(barrier, inc=1, device_id=partner, device_id_type=FLAT)

        row = lax.broadcasted_iota(jnp.int32, (S, L), 0)
        lane = lax.broadcasted_iota(jnp.int32, (S, L), 1)

        for g in range(G):
            rows = slice(g * S, g * S + S)
            pair = jnp.concatenate([c1_ref[rows, :L], c1_ref[rows, L:]], axis=0)
            g0[NT0 + core * G + g] = pair.astype(BF16)
        c1_copy = to_partner(
            g0.at[pl.ds(NT0 + core * G, G)], g0.at[pl.ds(NT0 + core * G, G)], c1_sem.at[0], c1_sem.at[1]
        )
        q_copy = to_partner(q_ref, qf.at[pl.ds(core * HB, HB)], q_sem.at[0], q_sem.at[1])

        tile = jnp.zeros((S, L), F32)
        for t in range(2):
            part = jnp.zeros((1, L), F32)
            for k in range(NR):
                entry = c1_ref[k : k + 1, t * L : t * L + L]
                part = part + entry * entry * p_ref[k]
            tile = jnp.where(row == 2 * core + t, jnp.broadcast_to(part, (S, L)), tile)
        where = (row - 4) * L + lane
        for k in range(NR):
            tile = jnp.where(where == chip * NR + k, p_ref[k], tile)
        ars[0] = tile
        for g in range(G):
            rows = slice(g * S, g * S + S)
            for t in range(JW):
                a, b = t0_ref[rows, (2 * L) * t : (2 * L) * t + L], t0_ref[rows, (2 * L) * t + L : (2 * L) * t + (2 * L)]
                g0[g * JW + t] = jnp.concatenate([a, b], axis=0).astype(BF16)
        qf[pl.ds(core * HB, HB)] = q_ref[...]

        c2_copy = to_partner(c2n.at[pl.ds(core * HB, HB)], c2n.at[pl.ds(core * HB, HB)], c2_sem.at[0], c2_sem.at[1])
        bp[...] = jnp.zeros_like(bp)

        def round_c2(first, last):
            c2_in.wait()
            for t in range(first, last):
                blk = c2v[:, t * L : t * L + L]
                c2n[core * HB + t] = blk.astype(BF16)
                bp[...] += blk * blk * q_ref[t : t + 1, :]

        def finish_b():
            bp[...] = jnp.broadcast_to(jnp.sum(bp[...], axis=1, keepdims=True), (L, L))

        with jax.named_scope("barrier"):
            pl.semaphore_wait(barrier, len(peers) + 1)
        give_credit()
        c1_copy.start()
        q_copy.start()
        all_sum_send(0)

        src = lax.broadcasted_iota(jnp.int32, (L, L), 0)
        dst = lax.broadcasted_iota(jnp.int32, (L, L), 1)
        picks = [
            jnp.where((src - core * JB == dst - h * JB) & (dst >= h * JB) & (dst < h * JB + JB), 1.0, 0.0).astype(BF16)
            for h in range(2)
        ]

        def order_c2(first, last):
            for t in range(first, last):
                a = jnp.dot(c2n[source_of(2 * t)], picks[0], preferred_element_type=F32)
                b = jnp.dot(c2n[source_of(2 * t + 1)], picks[1], preferred_element_type=F32)
                c2p[:, t * L : t * L + L] = (a + b).astype(BF16)

        def order_q(first, last):
            def four(n, carry):
                for k in range(4):
                    p = 4 * n + k
                    shared = p < CS
                    half = jnp.where(shared, other, core)
                    line = jnp.broadcast_to(qf[pl.ds(source_of(jnp.where(shared, p, p - CS)), 1), :], (S, L))
                    for jt in range(JT):
                        own = jnp.where(lane == half * JB + jt * S + row, line, 0.0)
                        qrep[p, jt] = jnp.broadcast_to(jnp.sum(own, axis=1, keepdims=True), (S, L))
                return carry

            lax.fori_loop(first // 4, last // 4, four, 0)

        def span(n, parts, f):
            cuts = [n * k // parts for k in range(parts + 1)]
            return [lambda a=a, b=b: f(a, b) for a, b in zip(cuts, cuts[1:])]

        fillers = [(0, lambda: round_c2(0, HB)), (0, finish_b), (0, lambda: c2_copy.start())]
        fillers += [(0, lambda: q_copy.wait()), (0, lambda: order_q(0, NP)), (LATE // 2, lambda: all_sum_step(0))]
        fillers += [(LATE, lambda: all_sum_step(1))]
        waited = []

        def before_send(m):
            if not waited and m["hi"] > NT0:
                waited.append(1)
                c1_copy.wait()

        def unpack(op, s):
            chip_s = source_of(s)
            for g in range(G):
                tiles = g0[s * TT0 + g * JW : s * TT0 + g * JW + JW].astype(F32).reshape(JN, S, L)
                kbuf[pl.ds((chip_s * G + g) * JN, JN)] = tiles
                at = pl.ds(pl.multiple_of(chip_s * NR + g * S, S), S)
                for h in range(2):
                    pair = g0[s * TT0 + NT0 + h * G + g].astype(F32)
                    c1f[at, 2 * L * h : 2 * L * h + L] = pair[:S]
                    c1f[at, 2 * L * h + L : 2 * L * h + 2 * L] = pair[S:]

        with jax.named_scope("gather0"):
            first = [(0, lambda: unpack("slot", 0))]
            tree(g0, TT0, 0, plan0, before_send=before_send, on_slot=unpack, fillers=first + fillers)
            tree_sent(g0, plan0)
            c1b[...] = c1f[...].astype(BF16)
            all_sum_step(2)

        def finish_lp():
            lp[...] = jnp.concatenate([bp[...]] * NT, axis=1) - 2.0 * bacc[...]

        bacc[...] = jnp.zeros_like(bacc)
        JC = CK // L

        def first_chunk(n, carry):
            cols = []
            for t in range(JC):
                cols.append(kbuf[pl.ds(n * JC + t, CH * G, stride=JN)].reshape(n_rows, L))
            plan_c = jnp.concatenate(cols, axis=1).astype(BF16)
            lead = jnp.dot(c1b[...], plan_c, preferred_element_type=F32).astype(BF16)
            c2c = jnp.concatenate([c2n[core * HB + n * JC + t] for t in range(JC)], axis=1)
            bacc[...] += lax.dot_general(c2c, lead, (((1,), (1,)), ((), ())), preferred_element_type=F32)
            return carry

        with jax.named_scope("firstmm"):
            lax.fori_loop(0, KJ // CK, first_chunk, 0)
            finish_lp()
        to_partner(arps, arpr, arp_sem.at[0], arp_sem.at[1]).wait()
        ap[...] = jnp.where(row < 4, arps[...] + arpr[...], arps[...])
        for t in range(NT):
            pv[t] = jnp.broadcast_to(ap[4 + t : 5 + t, :], (S, L))


        def lead_and_cross(n, plan_c):
            lead = jnp.dot(plan_c[...], c1b[...], preferred_element_type=F32).astype(BF16)
            bacc[...] += jnp.dot(c2p[:, n * CM : n * CM + CM], lead, preferred_element_type=F32)

        def costs():
            copy = to_partner(lp.at[pl.ds(other * JB, JB)], lprecv, lp_sem.at[0], lp_sem.at[1])
            copy.start()
            copy.wait()
            own = lp[pl.ds(pl.multiple_of(core * JB, JB), JB), :] + lprecv[...]
            return own + jnp.concatenate([ap[t : t + 1, :] for t in range(NT)], axis=1)

        def block(s):
            return kbuf[pl.ds(s * TB, TB)].reshape(JT, NT, S, L)

        def weighted(kk, u):
            w = (kk[:, 0] * u[0] + kk[:, 1] * u[1]) + (kk[:, 2] * u[2] + kk[:, 3] * u[3])
            return jnp.sum(w, axis=2, keepdims=True)

        def passes(u, rescale=False, par=0):
            def place(g):
                return g * GS + 2 * CS if not isinstance(g, int) or g < NE else (g - NE) * GS

            def one(at, buf):
                for k in range(GS):
                    p = at + k
                    kk = block(p)
                    if rescale:
                        kk = kk * fb[:, pl.ds(p, 1), :][None]
                        kbuf[pl.ds(p * TB, TB)] = kk.reshape(TB, S, L)
                    cbuf[buf, k] = qrep[p] / jnp.broadcast_to(weighted(kk, u), (JT, S, L))

            def two(at, buf, acc):
                for k in range(GS):
                    p = at + k
                    acc = acc + jnp.sum(block(p) * cbuf[buf, k][:, None], axis=0)
                return acc

            def run(a, b, end):
                shift = place(a) - a * GS
                even, odd = a % 2, (a + 1) % 2
                pairs = max(0, (b - a - 1) // 2)

                def both(n, acc):
                    at = (a + 2 * n) * GS + shift
                    one(at + GS, odd)
                    acc = two(at, even, acc)
                    one(at + 2 * GS, even)
                    return two(at + GS, odd, acc)

                acc = lax.fori_loop(0, pairs, both, jnp.zeros((NT, S, L), F32))
                for g in range(a + 2 * pairs, b):
                    if g + 1 < end:
                        one(place(g + 1), (g + 1) % 2)
                    acc = two(place(g), g % 2, acc)
                return acc

            one(place(0), 0)
            xs[par] = run(0, NE, NE + NC)
            copy = to_partner(xs.at[par], xr.at[par], x_ssem.at[par], x_rsem.at[par])
            copy.start()
            acc = run(NE, NE + NC, NE + NC)
            copy.wait()
            total = jnp.sum((xs[par] + xr[par]) + acc, axis=1, keepdims=True)
            return quotient(pv[...], jnp.broadcast_to(total, (NT, S, L)))

        def plan_chunk(n, dst, u):
            def one(g):
                for k in range(GS):
                    p = CS + (n * GC + g) * GS + k
                    cbuf[g % 2, k] = quotient(qrep[p], jnp.broadcast_to(weighted(block(p), u), (JT, S, L)))

            one(0)
            for g in range(GC):
                if g + 1 < GC:
                    one(g + 1)
                for k in range(GS):
                    s = (n * GC + g) * GS + k
                    v = cbuf[g % 2, k]
                    vbuf[s] = v
                    t = (block(CS + s) * u[None]) * v[:, None]
                    flat = jnp.concatenate([t[:, i].reshape(JB, L) for i in range(NT)], axis=1)
                    at = (g * GS + k) * JB
                    dst[at : at + JB, :] = flat.astype(BF16)

        def outer(r, carry):
            eps = eps_ref[r]
            inv = 1.0 / eps
            inv = inv * (2.0 - eps * inv)
            main = LOG2E * inv
            (e0, e1), (m0, m1) = halves(eps), halves(main)
            prod = eps * main
            low_part = ((e0 * m0 - prod) + (e0 * m1 + e1 * m0)) + e1 * m1
            rest = (((LOG2E - prod) - low_part) + LOG2E_REST) * inv

            def decay(x):
                return jnp.exp2(x * main + x * rest)

            cost = costs()
            for jt in range(JT):
                for t in range(NT):
                    land[CS * TB + jt * NT + t] = cost[jt * S : jt * S + S, t * L : t * L + L]

            def exps(p):
                ll = land[p * TB : p * TB + TB].reshape(JT, NT, S, L)
                low = jnp.min(jnp.min(ll, axis=0), axis=1, keepdims=True)
                kk = decay(low[None] - ll)
                kbuf[p * TB : p * TB + TB] = kk.reshape(TB, S, L)
                mb[:, p : p + 1, :] = low
                sb[:, p : p + 1, :] = jnp.sum(jnp.sum(kk, axis=0), axis=1, keepdims=True)

            def passed_on(s):
                return to_partner(
                    land.at[pl.ds((CS + s) * TB, TB)], land.at[pl.ds(s * TB, TB)], fwd_ssem.at[0], fwd_rsem.at[s]
                )

            def on_slot(op, s):
                if op == "slot":
                    if s < CS:
                        passed_on(s).start()
                    exps(CS + s)
                else:
                    passed_on(s).wait_recv()
                    exps(s)

            def once(n, f):
                @pl.when(r == 0)
                def _():
                    if not n:
                        c2_copy.wait()
                    f()

            with jax.named_scope("gather"):
                pl.semaphore_wait(credit, NL)
                first = [(0, lambda: on_slot("slot", 0)), (plan["waits"] // 4, lambda: on_slot("partner", 0))]
                for n, f in enumerate(span(CH // 2, S, order_c2)):
                    first.append((LATE // 2 + 2 * n, lambda n=n, f=f: once(n, f)))
                tree(land, TB, CS, plan, on_slot=on_slot, fillers=first)
                tree_sent(land, plan)
                ref = land.at[pl.ds(0, CS * TB)]
                pltpu.make_async_copy(ref, ref, fwd_ssem.at[0]).wait()
                give_credit()

            with jax.named_scope("minx"):
                def least_of(a, b):
                    low = jnp.min(mb[:, a:b], axis=1, keepdims=True)
                    part = jnp.sum(sb[:, a:b] * decay(low - mb[:, a:b]), axis=1, keepdims=True)
                    return jnp.broadcast_to(low, (NT, S, L)), jnp.broadcast_to(part, (NT, S, L))

                mss[0], mss[1] = least_of(2 * CS, NP)
                copy = to_partner(mss, msr, ms_sem.at[0], ms_sem.at[1])
                copy.start()
                low, part = least_of(0, 2 * CS)
                copy.wait()
                least = jnp.minimum(jnp.minimum(mss[0], msr[0]), low)
                total = mss[1] * decay(least - mss[0]) + msr[1] * decay(least - msr[0])
                total = total + part * decay(least - low)
                fb[...] = decay(least[:, :1] - mb[...])
                u = quotient(pv[...], total)

            with jax.named_scope("pass1"):
                u = passes(u, rescale=True, par=1)

            def sweep(t, u):
                return passes(u, par=lax.rem(t, 2))

            with jax.named_scope("sweeps"):
                u = lax.fori_loop(2, sweeps, sweep, u)
            ub[...] = u
            bacc[...] = jnp.zeros_like(bacc)
            with jax.named_scope("finish"):
                plan_chunk(0, tts[0], u)
                for n in range(KJ // CM):
                    if n + 1 < KJ // CM:
                        plan_chunk(n + 1, tts[(n + 1) % 2], u)
                    lead_and_cross(n, tts[n % 2])
                finish_lp()
            return carry

        lax.fori_loop(0, steps, outer, 0)

        pl.semaphore_wait(credit, NL)
        cost = costs()
        plan_own = (block(CS) * ub[...][None]) * vbuf[0][:, None]
        total = jnp.zeros((S, L), F32)
        for jt in range(JT):
            for t in range(NT):
                total = total + cost[jt * S : jt * S + S, t * L : t * L + L] * plan_own[jt, t]
        loss_rows[0:1] = jnp.sum(total, axis=0, keepdims=True)

        def to_chip(n):
            o = CH - n
            off = (lax.rem(o, X), lax.rem(lax.div(o, X), Y), lax.div(o, X * Y))
            at = [lax.rem(pos[d] + off[d], dims[d]) for d in range(3)]
            return pltpu.make_async_remote_copy(
                src_ref=loss_rows.at[pl.ds(0, 1)], dst_ref=loss_rows.at[pl.ds(o, 1)],
                send_sem=loss_sem.at[0], recv_sem=loss_sem.at[1],
                device_id=core * CH + at[0] + X * at[1] + X * Y * at[2], device_id_type=FLAT,
            )

        def tell(n, carry):
            to_chip(n).start()
            return carry

        lax.fori_loop(1, CH, tell, 0)

        it = lax.div(chip * NR, L)
        inside = pl.multiple_of(lax.rem(chip * NR, L), S)

        def rows_of(n, carry):
            for k in range(4):
                s = 4 * n + k
                kk = jnp.concatenate([kbuf[(CS + s) * TB + jt * NT + it] for jt in range(JT)], axis=0)
                uu = jnp.concatenate([ub[it]] * JT, axis=0)
                t = (kk * uu) * vbuf[s].reshape(JB, L)
                none = jnp.zeros_like(t)
                both = jnp.where(core == 0, jnp.concatenate([t, none], axis=0), jnp.concatenate([none, t], axis=0))
                trb[k] = both.T
                obuf[source_of(s)] = trb[k, pl.ds(inside, NR), :]
            return carry

        with jax.named_scope("tail"):
            lax.fori_loop(0, CH // 4, rows_of, 0)
            o_copy = to_partner(obuf.at[pl.ds(other * HB, HB)], orecv, o_sem.at[0], o_sem.at[1])
            o_copy.start()
            o_copy.wait()
            orecv[...] = obuf[pl.ds(core * HB, HB)] + orecv[...]
            o_out = pltpu.make_async_copy(orecv, out_ref, in_sem.at[1])
            o_out.start()
            ref = loss_rows.at[pl.ds(1, CH - 1)]
            pltpu.make_async_copy(ref, ref, loss_sem.at[0]).wait()
            pltpu.make_async_copy(ref, ref, loss_sem.at[1]).wait()
            loss_two[0:1] = jnp.sum(loss_rows[...], axis=0, keepdims=True)
            copy = to_partner(loss_two.at[pl.ds(0, 1)], loss_two.at[pl.ds(1, 1)], loss_sem.at[2], loss_sem.at[3])
            copy.start()
            copy.wait()
            loss_ref[0] = jnp.sum(loss_two[...])
            o_out.wait()

    vm = pltpu.VMEM
    dma = pltpu.SemaphoreType.DMA
    scratch = [
        vm((NP * TB, S, L), F32),
        vm((NP * TB, S, L), F32),
        vm((CH * TT0, 16, L), BF16),
        vm((CM, n_rows), BF16),
        vm((CM, n_rows), BF16),
        vm((n_rows, n_rows), F32),
        vm((n_rows, n_rows), BF16),
        vm((CH, L, L), BF16),
        vm((L, KJ), BF16),
        vm((L, n_rows), F32),
        vm((L, n_rows), F32),
        vm((JB, n_rows), F32),
        vm((L, L), F32),
        vm((CH, L), F32),
        vm((NP, JT, S, L), F32),
        vm((CH, JT, S, L), F32),
        vm((2, GS, JT, S, L), F32),
        vm((NT, NP, L), F32),
        vm((NT, NP, L), F32),
        vm((NT, NP, L), F32),
        vm((NT, S, L), F32),
        vm((S, L), F32),
        vm((2, NT, S, L), F32),
        vm((2, NT, S, L), F32),
        vm((2, NT, S, L), F32),
        vm((2, NT, S, L), F32),
        vm((NT, S, L), F32),
        vm((3, S, L), F32),
        vm((3, 3, S, L), F32),
        vm((S, L), F32),
        vm((S, L), F32),
        vm((CH, NR, L), F32),
        vm((HB, NR, L), F32),
        vm((4, L, L), F32),
        vm((CH, L), F32),
        vm((2, L), F32),
        vm((L, n_cols // 2), F32),
        dma((NL,)),
        dma((max(plan["waits"], plan0["waits"]),)),
        dma((1,)),
        dma((CS,)),
        pltpu.SemaphoreType.REGULAR,
        dma((2,)),
        dma((2,)),
        dma((2,)),
        dma((2,)),
        dma((2,)),
        dma((2,)),
        dma((2,)),
        dma((3, 3)),
        dma((3, 3)),
        dma((2,)),
        dma((2,)),
        dma((4,)),
        dma((2,)),
    ]
    return kernel, scratch


def solution(mesh):
    chips = mesh.shape["rows"]
    dims = torus_of(chips)
    grid_spec = P(("pairs", "rows"), "cols")

    def local_fn(c1, c2, t0, p, q, eps):
        n_rows, n_cols = p.shape[0] * chips, q.shape[0] * mesh.shape["cols"]
        kernel, scratch = make_kernel(dims, n_rows, n_cols, eps.shape[0], SWEEPS)
        vmem = pl.BlockSpec(memory_space=pltpu.VMEM)
        smem = pl.BlockSpec(memory_space=pltpu.SMEM)
        anywhere = pl.BlockSpec(memory_space=pl.ANY)
        plan, loss = pl.pallas_call(
            kernel,
            name="gromov",
            out_shape=(jax.ShapeDtypeStruct((chips // 2, t0.shape[0], L), F32), jax.ShapeDtypeStruct((1,), F32)),
            in_specs=[smem, smem, vmem, anywhere, vmem, vmem],
            out_specs=(anywhere, smem),
            scratch_shapes=scratch,
            compiler_params=pltpu.CompilerParams(
                collective_id=0, has_side_effects=True, vmem_limit_bytes=60 * 1024 * 1024
            ),
        )(eps, p, c1, c2, t0, q.reshape(chips // 2, L))
        return plan.transpose(1, 0, 2).reshape(t0.shape), loss

    return jax.shard_map(
        local_fn,
        mesh=mesh,
        in_specs=(grid_spec, grid_spec, grid_spec, P(("pairs", "rows")), P(("pairs", "cols")), P("pairs")),
        out_specs=(grid_spec, P("pairs")),
        check_vma=False,
    )
```

```python
import heapq
import itertools
import math

import jax
import jax.numpy as jnp
from jax import lax
from jax.experimental import pallas as pl
from jax.experimental.pallas import tpu as pltpu
from jax.sharding import PartitionSpec as P

SWEEPS = 10
FLAT = pl.DeviceIdType.LOGICAL
L, S = 128, 8
JB = 64
JT = JB // S
F32, BF16 = jnp.float32, jnp.bfloat16
ORDERS = ((0, 1, 2), (1, 2, 0), (2, 0, 1))
TILE_RATE = 11.4
HOP_US = 4.0
AHEAD_US = 2.0
LOG2E = 1.4426950216293335
LOG2E_REST = 1.925963e-8
PARTNER_US = 4.0
LATE = 100


def torus_of(chips):
    return {64: (4, 4, 4), S: (4, 2, 1), 16: (4, 4, 1)}[chips]


def halves(x):
    c = 4097.0 * x
    high = c - (c - x)
    return high, x - high


def quotient(a, b):
    q = a / b
    return q + (a - q * b) / b


def split3(n):
    cuts = [0, (n + 2) // 3, (2 * n + 2) // 3, n]
    return [(cuts[k], cuts[k + 1]) for k in range(3)]


def tree_plan(dims, tiles, rate, lat_us, ahead_us, shared=0):
    rings = {1: (), 2: ((1, "f", 1),), 4: ((1, "f", 1), (3, "f", -1), (2, "a", 1), (2, "b", -1))}
    msgs = []
    for color, order in enumerate(ORDERS):
        lo, hi = split3(tiles)[color]
        for dst in itertools.product(*(range(n) for n in dims)):
            used = [k for k in range(3) if dst[order[k]]]
            if not used or lo == hi:
                continue
            d = order[used[-1]]
            mid = lo + (hi - lo + (sum(dst) + color) % 2) // 2
            for at, part, sign in rings[dims[d]]:
                a, b = {"f": (lo, hi), "a": (lo, mid), "b": (mid, hi)}[part]
                if at != dst[d] or a == b:
                    continue
                src = list(dst)
                src[d] = (src[d] - sign) % dims[d]
                m = dict(id=len(msgs), color=color, src=tuple(src), dst=dst, link=(d, sign), lo=a, hi=b)
                m["us"] = (b - a) / rate
                msgs.append(m)
    into = {}
    for m in msgs:
        into.setdefault((m["color"], m["dst"]), []).append(m)
    users = [[] for _ in msgs]
    missing = []
    for m in msgs:
        deps = [e for e in into.get((m["color"], m["src"]), []) if e["lo"] < m["hi"] and m["lo"] < e["hi"]]
        missing.append(len(deps))
        for e in deps:
            users[e["id"]].append(m)
    sems, waiting = {}, {}
    for m in msgs:
        key = (m["color"] if users[m["id"]] else None, m["dst"])
        m["sem"] = sems.setdefault(key, len(sems))
        waiting.setdefault(m["sem"], []).append(m)
    pending = {k: len(group) for k, group in waiting.items()}
    way = {}

    def way_of(m):
        if m["id"] not in way:
            way[m["id"]] = m["us"] + lat_us + max([way_of(u) for u in users[m["id"]]], default=0.0)
        return way[m["id"]]

    links = sorted({m["link"] for m in msgs})
    queue = {k: [] for k in links}
    idle = dict.fromkeys(links, True)
    ready, events, ops = {}, [], []

    def put(m, now):
        ready[m["id"]] = now
        heapq.heappush(queue[m["link"]], (-way_of(m), m["id"]))

    def start(link, now):
        if idle[link] and queue[link]:
            k = heapq.heappop(queue[link])[1]
            idle[link] = False
            ops.append((max(ready[k], now - ahead_us), 1, "send", msgs[k]))
            heapq.heappush(events, (now + msgs[k]["us"], 0, k))
            heapq.heappush(events, (now + msgs[k]["us"] + lat_us, 1, k))

    for m in msgs:
        if not missing[m["id"]]:
            put(m, 0.0)
    for link in links:
        start(link, 0.0)
    left = {}
    for m in msgs:
        left[m["dst"]] = left.get(m["dst"], 0) + 1
    now = 0.0
    while events:
        now, arrived, k = heapq.heappop(events)
        m = msgs[k]
        if not arrived:
            idle[m["link"]] = True
            start(m["link"], now)
            continue
        pending[m["sem"]] -= 1
        if not pending[m["sem"]]:
            ops.append((now, 0, "wait", waiting[m["sem"]]))
        for u in users[k]:
            missing[u["id"]] -= 1
            if not missing[u["id"]]:
                put(u, now)
                start(u["link"], now)
        left[m["dst"]] -= 1
        if not left[m["dst"]]:
            slot = m["dst"][0] + dims[0] * (m["dst"][1] + dims[1] * m["dst"][2])
            ops.append((now, 0, "slot", slot))
            if slot < shared:
                ops.append((now + PARTNER_US, 0, "partner", slot))
    ops.sort(key=lambda op: op[:2])
    totals = {k: sum(m["hi"] - m["lo"] for m in msgs if m["link"] == k) for k in links}
    return dict(waits=len(sems), ops=[op[2:] for op in ops], links=links, totals=totals, end=now)


def make_kernel(dims, n_rows, n_cols, steps, sweeps):
    X, Y, Z = dims
    CH = X * Y * Z
    NR = n_rows // CH
    G = NR // S
    NT = n_rows // L
    TB = JT * NT
    HB = CH // 2
    JN = n_cols // 2 // L
    JW = JN // 2
    NT0 = G * JW
    TT0 = NT0 + 2 * G
    KJ = CH * JB
    CK = min(1024, KJ)
    CM = min(1024, KJ)
    GS = min(4, CH // 2)
    CS = max(CH * 3 // 8 // GS * GS, GS)
    NP = CH + CS
    NE, NC = (CH - CS) // GS, 2 * CS // GS
    GC = CM // JB // GS
    assert NT == 4 and n_cols == CH * L and JN == HB
    plan0 = tree_plan(dims, TT0, TILE_RATE, HOP_US - 1, AHEAD_US)
    plan = tree_plan(dims, TB, TILE_RATE, HOP_US, AHEAD_US, CS)
    links = plan["links"]
    NL = len(links)
    peers = [(d, k) for d in range(3) for k in range(1, dims[d])]
    strides = (1, X, X * Y)

    def slot_of(offset):
        return offset[0] + X * offset[1] + X * Y * offset[2]

    def kernel(
        eps_ref, p_ref, c1_ref, c2_ref, t0_ref, q_ref,
        out_ref, loss_ref,
        land, kbuf, g0, tt0, tt1, c1f, c1b, c2n, c2p, bacc, lp, lprecv, bp, qf, qrep, vbuf, cbuf,
        mb, sb, fb, ub, ap, xs, xr, mss, msr, pv, ars, arr, arps, arpr, obuf, orecv, trb, loss_rows, loss_two, c2v,
        send_sem, recv_sem, fwd_ssem, fwd_rsem, credit, x_ssem, x_rsem, ms_sem, lp_sem, c1_sem, c2_sem, q_sem, ar_ssem, ar_rsem, arp_sem, o_sem, loss_sem, in_sem,
    ):
        tts = (tt0, tt1)
        chip = lax.axis_index("rows")
        core = lax.axis_index("cols")
        other = 1 - core
        pos = (lax.rem(chip, X), lax.rem(lax.div(chip, X), Y), lax.div(chip, X * Y))

        me = core * CH + chip
        partner = other * CH + chip

        def moved(d, k):
            return me + (lax.rem(pos[d] + k + dims[d], dims[d]) - pos[d]) * strides[d]

        near = {link: moved(*link) for link in links}

        def source_of(slot):
            off = (lax.rem(slot, X), lax.rem(lax.div(slot, X), Y), lax.div(slot, X * Y))
            at = [lax.rem(pos[d] + dims[d] - off[d], dims[d]) for d in range(3)]
            return at[0] + X * at[1] + X * Y * at[2]

        def to_partner(src, dst, ssem, rsem):
            return pltpu.make_async_remote_copy(
                src_ref=src, dst_ref=dst, send_sem=ssem, recv_sem=rsem,
                device_id=partner, device_id_type=FLAT,
            )

        def tree_copy(buf, width, first, m):
            n = m["hi"] - m["lo"]
            return pltpu.make_async_remote_copy(
                src_ref=buf.at[pl.ds((first + slot_of(m["src"])) * width + m["lo"], n)],
                dst_ref=buf.at[pl.ds((first + slot_of(m["dst"])) * width + m["lo"], n)],
                send_sem=send_sem.at[links.index(m["link"])],
                recv_sem=recv_sem.at[m["sem"]],
                device_id=near[m["link"]],
                device_id_type=FLAT,
            )

        def tree(buf, width, first, the_plan, before_send=None, on_slot=None, fillers=()):
            fillers, ready, waits = list(fillers), [], 0
            for op, m in the_plan["ops"]:
                if op == "send":
                    if before_send is not None:
                        before_send(m)
                    tree_copy(buf, width, first, m).start()
                elif op == "wait":
                    while fillers and not fillers[0][0]:
                        fillers.pop(0)[1]()
                    if not ready and fillers and waits >= fillers[0][0]:
                        fillers.pop(0)[1]()
                    while ready:
                        on_slot(*ready.pop(0))
                    n = sum(e["hi"] - e["lo"] for e in m)
                    ref = buf.at[pl.ds((first + slot_of(m[0]["dst"])) * width, n)]
                    pltpu.make_async_copy(ref, ref, recv_sem.at[m[0]["sem"]]).wait()
                    waits += 1
                elif on_slot is not None:
                    ready.append((op, m))
            for at in ready:
                on_slot(*at)
            for _, f in fillers:
                f()

        def tree_sent(buf, the_plan):
            for k, link in enumerate(links):
                n = the_plan["totals"][link]
                ref = buf.at[pl.ds(0, n)]
                pltpu.make_async_copy(ref, ref, send_sem.at[k]).wait()

        def give_credit():
            for d, sign in links:
                pl.semaphore_signal(credit, inc=1, device_id=moved(d, -sign), device_id_type=FLAT)

        def all_sum_send(stage):
            for n, k in enumerate(range(1, dims[stage])):
                pltpu.make_async_remote_copy(
                    src_ref=ars.at[stage], dst_ref=arr.at[stage, n],
                    send_sem=ar_ssem.at[stage, n], recv_sem=ar_rsem.at[stage, n],
                    device_id=moved(stage, k), device_id_type=FLAT,
                ).start()

        def all_sum_get(stage):
            total = ars[stage]
            for n, k in enumerate(range(1, dims[stage])):
                pltpu.make_async_remote_copy(
                    src_ref=ars.at[stage], dst_ref=arr.at[stage, n],
                    send_sem=ar_ssem.at[stage, n], recv_sem=ar_rsem.at[stage, n],
                    device_id=moved(stage, k), device_id_type=FLAT,
                ).wait()
                total = total + arr[stage, n]
            return total

        def all_sum_step(stage):
            total = all_sum_get(stage)
            if stage < 2:
                ars[stage + 1] = total
                all_sum_send(stage + 1)
            else:
                arps[...] = total
                to_partner(arps, arpr, arp_sem.at[0], arp_sem.at[1]).start()

        c2_in = pltpu.make_async_copy(c2_ref, c2v, in_sem.at[0])
        c2_in.start()
        barrier = pltpu.get_barrier_semaphore()
        for d, k in peers:
            pl.semaphore_signal(barrier, inc=1, device_id=moved(d, k), device_id_type=FLAT)
        pl.semaphore_signal(barrier, inc=1, device_id=partner, device_id_type=FLAT)

        row = lax.broadcasted_iota(jnp.int32, (S, L), 0)
        lane = lax.broadcasted_iota(jnp.int32, (S, L), 1)

        for g in range(G):
            rows = slice(g * S, g * S + S)
            pair = jnp.concatenate([c1_ref[rows, :L], c1_ref[rows, L:]], axis=0)
            g0[NT0 + core * G + g] = pair.astype(BF16)
        c1_copy = to_partner(
            g0.at[pl.ds(NT0 + core * G, G)], g0.at[pl.ds(NT0 + core * G, G)], c1_sem.at[0], c1_sem.at[1]
        )
        q_copy = to_partner(q_ref, qf.at[pl.ds(core * HB, HB)], q_sem.at[0], q_sem.at[1])

        tile = jnp.zeros((S, L), F32)
        for t in range(2):
            part = jnp.zeros((1, L), F32)
            for k in range(NR):
                entry = c1_ref[k : k + 1, t * L : t * L + L]
                part = part + entry * entry * p_ref[k]
            tile = jnp.where(row == 2 * core + t, jnp.broadcast_to(part, (S, L)), tile)
        where = (row - 4) * L + lane
        for k in range(NR):
            tile = jnp.where(where == chip * NR + k, p_ref[k], tile)
        ars[0] = tile
        for g in range(G):
            rows = slice(g * S, g * S + S)
            for t in range(JW):
                a, b = t0_ref[rows, (2 * L) * t : (2 * L) * t + L], t0_ref[rows, (2 * L) * t + L : (2 * L) * t + (2 * L)]
                g0[g * JW + t] = jnp.concatenate([a, b], axis=0).astype(BF16)
        qf[pl.ds(core * HB, HB)] = q_ref[...]

        c2_copy = to_partner(c2n.at[pl.ds(core * HB, HB)], c2n.at[pl.ds(core * HB, HB)], c2_sem.at[0], c2_sem.at[1])
        bp[...] = jnp.zeros_like(bp)

        def round_c2(first, last):
            c2_in.wait()
            for t in range(first, last):
                blk = c2v[:, t * L : t * L + L]
                c2n[core * HB + t] = blk.astype(BF16)
                bp[...] += blk * blk * q_ref[t : t + 1, :]

        def finish_b():
            bp[...] = jnp.broadcast_to(jnp.sum(bp[...], axis=1, keepdims=True), (L, L))

        with jax.named_scope("barrier"):
            pl.semaphore_wait(barrier, len(peers) + 1)
        give_credit()
        c1_copy.start()
        q_copy.start()
        all_sum_send(0)

        src = lax.broadcasted_iota(jnp.int32, (L, L), 0)
        dst = lax.broadcasted_iota(jnp.int32, (L, L), 1)
        picks = [
            jnp.where((src - core * JB == dst - h * JB) & (dst >= h * JB) & (dst < h * JB + JB), 1.0, 0.0).astype(BF16)
            for h in range(2)
        ]

        def order_c2(first, last):
            for t in range(first, last):
                a = jnp.dot(c2n[source_of(2 * t)], picks[0], preferred_element_type=F32)
                b = jnp.dot(c2n[source_of(2 * t + 1)], picks[1], preferred_element_type=F32)
                c2p[:, t * L : t * L + L] = (a + b).astype(BF16)

        def order_q(first, last):
            def four(n, carry):
                for k in range(4):
                    p = 4 * n + k
                    shared = p < CS
                    half = jnp.where(shared, other, core)
                    line = jnp.broadcast_to(qf[pl.ds(source_of(jnp.where(shared, p, p - CS)), 1), :], (S, L))
                    for jt in range(JT):
                        own = jnp.where(lane == half * JB + jt * S + row, line, 0.0)
                        qrep[p, jt] = jnp.broadcast_to(jnp.sum(own, axis=1, keepdims=True), (S, L))
                return carry

            lax.fori_loop(first // 4, last // 4, four, 0)

        def span(n, parts, f):
            cuts = [n * k // parts for k in range(parts + 1)]
            return [lambda a=a, b=b: f(a, b) for a, b in zip(cuts, cuts[1:])]

        fillers = [(0, lambda: round_c2(0, HB)), (0, finish_b), (0, lambda: c2_copy.start())]
        fillers += [(0, lambda: q_copy.wait()), (0, lambda: order_q(0, NP)), (LATE // 2, lambda: all_sum_step(0))]
        fillers += [(LATE, lambda: all_sum_step(1))]
        waited = []

        def before_send(m):
            if not waited and m["hi"] > NT0:
                waited.append(1)
                c1_copy.wait()

        def unpack(op, s):
            chip_s = source_of(s)
            for g in range(G):
                tiles = g0[s * TT0 + g * JW : s * TT0 + g * JW + JW].astype(F32).reshape(JN, S, L)
                kbuf[pl.ds((chip_s * G + g) * JN, JN)] = tiles
                at = pl.ds(pl.multiple_of(chip_s * NR + g * S, S), S)
                for h in range(2):
                    pair = g0[s * TT0 + NT0 + h * G + g].astype(F32)
                    c1f[at, 2 * L * h : 2 * L * h + L] = pair[:S]
                    c1f[at, 2 * L * h + L : 2 * L * h + 2 * L] = pair[S:]

        with jax.named_scope("gather0"):
            first = [(0, lambda: unpack("slot", 0))]
            tree(g0, TT0, 0, plan0, before_send=before_send, on_slot=unpack, fillers=first + fillers)
            tree_sent(g0, plan0)
            c1b[...] = c1f[...].astype(BF16)
            all_sum_step(2)

        def finish_lp():
            lp[...] = jnp.concatenate([bp[...]] * NT, axis=1) - 2.0 * bacc[...]

        bacc[...] = jnp.zeros_like(bacc)
        JC = CK // L

        def first_chunk(n, carry):
            cols = []
            for t in range(JC):
                cols.append(kbuf[pl.ds(n * JC + t, CH * G, stride=JN)].reshape(n_rows, L))
            plan_c = jnp.concatenate(cols, axis=1).astype(BF16)
            lead = jnp.dot(c1b[...], plan_c, preferred_element_type=F32).astype(BF16)
            c2c = jnp.concatenate([c2n[core * HB + n * JC + t] for t in range(JC)], axis=1)
            bacc[...] += lax.dot_general(c2c, lead, (((1,), (1,)), ((), ())), preferred_element_type=F32)
            return carry

        with jax.named_scope("firstmm"):
            lax.fori_loop(0, KJ // CK, first_chunk, 0)
            finish_lp()
        to_partner(arps, arpr, arp_sem.at[0], arp_sem.at[1]).wait()
        ap[...] = jnp.where(row < 4, arps[...] + arpr[...], arps[...])
        for t in range(NT):
            pv[t] = jnp.broadcast_to(ap[4 + t : 5 + t, :], (S, L))


        def lead_and_cross(n, plan_c):
            lead = jnp.dot(plan_c[...], c1b[...], preferred_element_type=F32).astype(BF16)
            bacc[...] += jnp.dot(c2p[:, n * CM : n * CM + CM], lead, preferred_element_type=F32)

        def costs():
            copy = to_partner(lp.at[pl.ds(other * JB, JB)], lprecv, lp_sem.at[0], lp_sem.at[1])
            copy.start()
            copy.wait()
            own = lp[pl.ds(pl.multiple_of(core * JB, JB), JB), :] + lprecv[...]
            return own + jnp.concatenate([ap[t : t + 1, :] for t in range(NT)], axis=1)

        def block(s):
            return kbuf[pl.ds(s * TB, TB)].reshape(JT, NT, S, L)

        def weighted(kk, u):
            w = (kk[:, 0] * u[0] + kk[:, 1] * u[1]) + (kk[:, 2] * u[2] + kk[:, 3] * u[3])
            return jnp.sum(w, axis=2, keepdims=True)

        def passes(u, rescale=False, par=0):
            def place(g):
                return g * GS + 2 * CS if not isinstance(g, int) or g < NE else (g - NE) * GS

            def one(at, buf):
                for k in range(GS):
                    p = at + k
                    kk = block(p)
                    if rescale:
                        kk = kk * fb[:, pl.ds(p, 1), :][None]
                        kbuf[pl.ds(p * TB, TB)] = kk.reshape(TB, S, L)
                    cbuf[buf, k] = qrep[p] / jnp.broadcast_to(weighted(kk, u), (JT, S, L))

            def two(at, buf, acc):
                for k in range(GS):
                    p = at + k
                    acc = acc + jnp.sum(block(p) * cbuf[buf, k][:, None], axis=0)
                return acc

            def run(a, b, end):
                shift = place(a) - a * GS
                even, odd = a % 2, (a + 1) % 2
                pairs = max(0, (b - a - 1) // 2)

                def both(n, acc):
                    at = (a + 2 * n) * GS + shift
                    one(at + GS, odd)
                    acc = two(at, even, acc)
                    one(at + 2 * GS, even)
                    return two(at + GS, odd, acc)

                acc = lax.fori_loop(0, pairs, both, jnp.zeros((NT, S, L), F32))
                for g in range(a + 2 * pairs, b):
                    if g + 1 < end:
                        one(place(g + 1), (g + 1) % 2)
                    acc = two(place(g), g % 2, acc)
                return acc

            one(place(0), 0)
            xs[par] = run(0, NE, NE + NC)
            copy = to_partner(xs.at[par], xr.at[par], x_ssem.at[par], x_rsem.at[par])
            copy.start()
            acc = run(NE, NE + NC, NE + NC)
            copy.wait()
            total = jnp.sum((xs[par] + xr[par]) + acc, axis=1, keepdims=True)
            return quotient(pv[...], jnp.broadcast_to(total, (NT, S, L)))

        def plan_chunk(n, dst, u):
            def one(g):
                for k in range(GS):
                    p = CS + (n * GC + g) * GS + k
                    cbuf[g % 2, k] = quotient(qrep[p], jnp.broadcast_to(weighted(block(p), u), (JT, S, L)))

            one(0)
            for g in range(GC):
                if g + 1 < GC:
                    one(g + 1)
                for k in range(GS):
                    s = (n * GC + g) * GS + k
                    v = cbuf[g % 2, k]
                    vbuf[s] = v
                    t = (block(CS + s) * u[None]) * v[:, None]
                    flat = jnp.concatenate([t[:, i].reshape(JB, L) for i in range(NT)], axis=1)
                    at = (g * GS + k) * JB
                    dst[at : at + JB, :] = flat.astype(BF16)

        def outer(r, carry):
            eps = eps_ref[r]
            inv = 1.0 / eps
            inv = inv * (2.0 - eps * inv)
            main = LOG2E * inv
            (e0, e1), (m0, m1) = halves(eps), halves(main)
            prod = eps * main
            low_part = ((e0 * m0 - prod) + (e0 * m1 + e1 * m0)) + e1 * m1
            rest = (((LOG2E - prod) - low_part) + LOG2E_REST) * inv

            def decay(x):
                return jnp.exp2(x * main + x * rest)

            cost = costs()
            for jt in range(JT):
                for t in range(NT):
                    land[CS * TB + jt * NT + t] = cost[jt * S : jt * S + S, t * L : t * L + L]

            def exps(p):
                ll = land[p * TB : p * TB + TB].reshape(JT, NT, S, L)
                low = jnp.min(jnp.min(ll, axis=0), axis=1, keepdims=True)
                kk = decay(low[None] - ll)
                kbuf[p * TB : p * TB + TB] = kk.reshape(TB, S, L)
                mb[:, p : p + 1, :] = low
                sb[:, p : p + 1, :] = jnp.sum(jnp.sum(kk, axis=0), axis=1, keepdims=True)

            def passed_on(s):
                return to_partner(
                    land.at[pl.ds((CS + s) * TB, TB)], land.at[pl.ds(s * TB, TB)], fwd_ssem.at[0], fwd_rsem.at[s]
                )

            def on_slot(op, s):
                if op == "slot":
                    if s < CS:
                        passed_on(s).start()
                    exps(CS + s)
                else:
                    passed_on(s).wait_recv()
                    exps(s)

            def once(n, f):
                @pl.when(r == 0)
                def _():
                    if not n:
                        c2_copy.wait()
                    f()

            with jax.named_scope("gather"):
                pl.semaphore_wait(credit, NL)
                first = [(0, lambda: on_slot("slot", 0)), (plan["waits"] // 4, lambda: on_slot("partner", 0))]
                for n, f in enumerate(span(CH // 2, S, order_c2)):
                    first.append((LATE // 2 + 2 * n, lambda n=n, f=f: once(n, f)))
                tree(land, TB, CS, plan, on_slot=on_slot, fillers=first)
                tree_sent(land, plan)
                ref = land.at[pl.ds(0, CS * TB)]
                pltpu.make_async_copy(ref, ref, fwd_ssem.at[0]).wait()
                give_credit()

            with jax.named_scope("minx"):
                def least_of(a, b):
                    low = jnp.min(mb[:, a:b], axis=1, keepdims=True)
                    part = jnp.sum(sb[:, a:b] * decay(low - mb[:, a:b]), axis=1, keepdims=True)
                    return jnp.broadcast_to(low, (NT, S, L)), jnp.broadcast_to(part, (NT, S, L))

                mss[0], mss[1] = least_of(2 * CS, NP)
                copy = to_partner(mss, msr, ms_sem.at[0], ms_sem.at[1])
                copy.start()
                low, part = least_of(0, 2 * CS)
                copy.wait()
                least = jnp.minimum(jnp.minimum(mss[0], msr[0]), low)
                total = mss[1] * decay(least - mss[0]) + msr[1] * decay(least - msr[0])
                total = total + part * decay(least - low)
                fb[...] = decay(least[:, :1] - mb[...])
                u = quotient(pv[...], total)

            with jax.named_scope("pass1"):
                u = passes(u, rescale=True, par=1)

            def sweep(t, u):
                return passes(u, par=lax.rem(t, 2))

            with jax.named_scope("sweeps"):
                u = lax.fori_loop(2, sweeps, sweep, u)
            ub[...] = u
            bacc[...] = jnp.zeros_like(bacc)
            with jax.named_scope("finish"):
                plan_chunk(0, tts[0], u)
                for n in range(KJ // CM):
                    if n + 1 < KJ // CM:
                        plan_chunk(n + 1, tts[(n + 1) % 2], u)
                    lead_and_cross(n, tts[n % 2])
                finish_lp()
            return carry

        lax.fori_loop(0, steps, outer, 0)

        pl.semaphore_wait(credit, NL)
        cost = costs()
        plan_own = (block(CS) * ub[...][None]) * vbuf[0][:, None]
        total = jnp.zeros((S, L), F32)
        for jt in range(JT):
            for t in range(NT):
                total = total + cost[jt * S : jt * S + S, t * L : t * L + L] * plan_own[jt, t]
        loss_rows[0:1] = jnp.sum(total, axis=0, keepdims=True)

        def to_chip(n):
            o = CH - n
            off = (lax.rem(o, X), lax.rem(lax.div(o, X), Y), lax.div(o, X * Y))
            at = [lax.rem(pos[d] + off[d], dims[d]) for d in range(3)]
            return pltpu.make_async_remote_copy(
                src_ref=loss_rows.at[pl.ds(0, 1)], dst_ref=loss_rows.at[pl.ds(o, 1)],
                send_sem=loss_sem.at[0], recv_sem=loss_sem.at[1],
                device_id=core * CH + at[0] + X * at[1] + X * Y * at[2], device_id_type=FLAT,
            )

        def tell(n, carry):
            to_chip(n).start()
            return carry

        lax.fori_loop(1, CH, tell, 0)

        it = lax.div(chip * NR, L)
        inside = pl.multiple_of(lax.rem(chip * NR, L), S)

        def rows_of(n, carry):
            for k in range(4):
                s = 4 * n + k
                kk = jnp.concatenate([kbuf[(CS + s) * TB + jt * NT + it] for jt in range(JT)], axis=0)
                uu = jnp.concatenate([ub[it]] * JT, axis=0)
                t = (kk * uu) * vbuf[s].reshape(JB, L)
                none = jnp.zeros_like(t)
                both = jnp.where(core == 0, jnp.concatenate([t, none], axis=0), jnp.concatenate([none, t], axis=0))
                trb[k] = both.T
                obuf[source_of(s)] = trb[k, pl.ds(inside, NR), :]
            return carry

        with jax.named_scope("tail"):
            lax.fori_loop(0, CH // 4, rows_of, 0)
            o_copy = to_partner(obuf.at[pl.ds(other * HB, HB)], orecv, o_sem.at[0], o_sem.at[1])
            o_copy.start()
            o_copy.wait()
            orecv[...] = obuf[pl.ds(core * HB, HB)] + orecv[...]
            o_out = pltpu.make_async_copy(orecv, out_ref, in_sem.at[1])
            o_out.start()
            ref = loss_rows.at[pl.ds(1, CH - 1)]
            pltpu.make_async_copy(ref, ref, loss_sem.at[0]).wait()
            pltpu.make_async_copy(ref, ref, loss_sem.at[1]).wait()
            loss_two[0:1] = jnp.sum(loss_rows[...], axis=0, keepdims=True)
            copy = to_partner(loss_two.at[pl.ds(0, 1)], loss_two.at[pl.ds(1, 1)], loss_sem.at[2], loss_sem.at[3])
            copy.start()
            copy.wait()
            loss_ref[0] = jnp.sum(loss_two[...])
            o_out.wait()

    vm = pltpu.VMEM
    dma = pltpu.SemaphoreType.DMA
    scratch = [
        vm((NP * TB, S, L), F32),
        vm((NP * TB, S, L), F32),
        vm((CH * TT0, 16, L), BF16),
        vm((CM, n_rows), BF16),
        vm((CM, n_rows), BF16),
        vm((n_rows, n_rows), F32),
        vm((n_rows, n_rows), BF16),
        vm((CH, L, L), BF16),
        vm((L, KJ), BF16),
        vm((L, n_rows), F32),
        vm((L, n_rows), F32),
        vm((JB, n_rows), F32),
        vm((L, L), F32),
        vm((CH, L), F32),
        vm((NP, JT, S, L), F32),
        vm((CH, JT, S, L), F32),
        vm((2, GS, JT, S, L), F32),
        vm((NT, NP, L), F32),
        vm((NT, NP, L), F32),
        vm((NT, NP, L), F32),
        vm((NT, S, L), F32),
        vm((S, L), F32),
        vm((2, NT, S, L), F32),
        vm((2, NT, S, L), F32),
        vm((2, NT, S, L), F32),
        vm((2, NT, S, L), F32),
        vm((NT, S, L), F32),
        vm((3, S, L), F32),
        vm((3, 3, S, L), F32),
        vm((S, L), F32),
        vm((S, L), F32),
        vm((CH, NR, L), F32),
        vm((HB, NR, L), F32),
        vm((4, L, L), F32),
        vm((CH, L), F32),
        vm((2, L), F32),
        vm((L, n_cols // 2), F32),
        dma((NL,)),
        dma((max(plan["waits"], plan0["waits"]),)),
        dma((1,)),
        dma((CS,)),
        pltpu.SemaphoreType.REGULAR,
        dma((2,)),
        dma((2,)),
        dma((2,)),
        dma((2,)),
        dma((2,)),
        dma((2,)),
        dma((2,)),
        dma((3, 3)),
        dma((3, 3)),
        dma((2,)),
        dma((2,)),
        dma((4,)),
        dma((2,)),
    ]
    return kernel, scratch


def solution(mesh):
    chips = mesh.shape["rows"]
    dims = torus_of(chips)
    grid_spec = P(("pairs", "rows"), "cols")

    def local_fn(c1, c2, t0, p, q, eps):
        n_rows, n_cols = p.shape[0] * chips, q.shape[0] * mesh.shape["cols"]
        kernel, scratch = make_kernel(dims, n_rows, n_cols, eps.shape[0], SWEEPS)
        vmem = pl.BlockSpec(memory_space=pltpu.VMEM)
        smem = pl.BlockSpec(memory_space=pltpu.SMEM)
        anywhere = pl.BlockSpec(memory_space=pl.ANY)
        plan, loss = pl.pallas_call(
            kernel,
            name="gromov",
            out_shape=(jax.ShapeDtypeStruct((chips // 2, t0.shape[0], L), F32), jax.ShapeDtypeStruct((1,), F32)),
            in_specs=[smem, smem, vmem, anywhere, vmem, vmem],
            out_specs=(anywhere, smem),
            scratch_shapes=scratch,
            compiler_params=pltpu.CompilerParams(
                collective_id=0, has_side_effects=True, vmem_limit_bytes=60 * 1024 * 1024
            ),
        )(eps, p, c1, c2, t0, q.reshape(chips // 2, L))
        return plan.transpose(1, 0, 2).reshape(t0.shape), loss

    return jax.shard_map(
        local_fn,
        mesh=mesh,
        in_specs=(grid_spec, grid_spec, grid_spec, P(("pairs", "rows")), P(("pairs", "cols")), P("pairs")),
        out_specs=(grid_spec, P("pairs")),
        check_vma=False,
    )
```

```python
import heapq
import itertools
import math

import jax
import jax.numpy as jnp
from jax import lax
from jax.experimental import pallas as pl
from jax.experimental.pallas import tpu as pltpu
from jax.sharding import PartitionSpec as P

SWEEPS = 10
FLAT = pl.DeviceIdType.LOGICAL
L, S = 128, 8
JB = 64
JT = JB // S
F32, BF16 = jnp.float32, jnp.bfloat16
ORDERS = ((0, 1, 2), (1, 2, 0), (2, 0, 1))
TILE_RATE = 11.4
HOP_US = 4.0
AHEAD_US = 2.0
LOG2E = 1.4426950216293335
LOG2E_REST = 1.925963e-8
PARTNER_US = 4.0
LATE = 100


def torus_of(chips):
    return {64: (4, 4, 4), S: (4, 2, 1), 16: (4, 4, 1)}[chips]


def halves(x):
    c = 4097.0 * x
    high = c - (c - x)
    return high, x - high


def quotient(a, b):
    q = a / b
    return q + (a - q * b) / b


def split3(n):
    cuts = [0, (n + 2) // 3, (2 * n + 2) // 3, n]
    return [(cuts[k], cuts[k + 1]) for k in range(3)]


def tree_plan(dims, tiles, rate, lat_us, ahead_us, shared=0):
    rings = {1: (), 2: ((1, "f", 1),), 4: ((1, "f", 1), (3, "f", -1), (2, "a", 1), (2, "b", -1))}
    msgs = []
    for color, order in enumerate(ORDERS):
        lo, hi = split3(tiles)[color]
        for dst in itertools.product(*(range(n) for n in dims)):
            used = [k for k in range(3) if dst[order[k]]]
            if not used or lo == hi:
                continue
            d = order[used[-1]]
            mid = lo + (hi - lo + (sum(dst) + color) % 2) // 2
            for at, part, sign in rings[dims[d]]:
                a, b = {"f": (lo, hi), "a": (lo, mid), "b": (mid, hi)}[part]
                if at != dst[d] or a == b:
                    continue
                src = list(dst)
                src[d] = (src[d] - sign) % dims[d]
                m = dict(id=len(msgs), color=color, src=tuple(src), dst=dst, link=(d, sign), lo=a, hi=b)
                m["us"] = (b - a) / rate
                msgs.append(m)
    into = {}
    for m in msgs:
        into.setdefault((m["color"], m["dst"]), []).append(m)
    users = [[] for _ in msgs]
    missing = []
    for m in msgs:
        deps = [e for e in into.get((m["color"], m["src"]), []) if e["lo"] < m["hi"] and m["lo"] < e["hi"]]
        missing.append(len(deps))
        for e in deps:
            users[e["id"]].append(m)
    sems, waiting = {}, {}
    for m in msgs:
        key = (m["color"] if users[m["id"]] else None, m["dst"])
        m["sem"] = sems.setdefault(key, len(sems))
        waiting.setdefault(m["sem"], []).append(m)
    pending = {k: len(group) for k, group in waiting.items()}
    way = {}

    def way_of(m):
        if m["id"] not in way:
            way[m["id"]] = m["us"] + lat_us + max([way_of(u) for u in users[m["id"]]], default=0.0)
        return way[m["id"]]

    links = sorted({m["link"] for m in msgs})
    queue = {k: [] for k in links}
    idle = dict.fromkeys(links, True)
    ready, events, ops = {}, [], []

    def put(m, now):
        ready[m["id"]] = now
        heapq.heappush(queue[m["link"]], (-way_of(m), m["id"]))

    def start(link, now):
        if idle[link] and queue[link]:
            k = heapq.heappop(queue[link])[1]
            idle[link] = False
            ops.append((max(ready[k], now - ahead_us), 1, "send", msgs[k]))
            heapq.heappush(events, (now + msgs[k]["us"], 0, k))
            heapq.heappush(events, (now + msgs[k]["us"] + lat_us, 1, k))

    for m in msgs:
        if not missing[m["id"]]:
            put(m, 0.0)
    for link in links:
        start(link, 0.0)
    left = {}
    for m in msgs:
        left[m["dst"]] = left.get(m["dst"], 0) + 1
    now = 0.0
    while events:
        now, arrived, k = heapq.heappop(events)
        m = msgs[k]
        if not arrived:
            idle[m["link"]] = True
            start(m["link"], now)
            continue
        pending[m["sem"]] -= 1
        if not pending[m["sem"]]:
            ops.append((now, 0, "wait", waiting[m["sem"]]))
        for u in users[k]:
            missing[u["id"]] -= 1
            if not missing[u["id"]]:
                put(u, now)
                start(u["link"], now)
        left[m["dst"]] -= 1
        if not left[m["dst"]]:
            slot = m["dst"][0] + dims[0] * (m["dst"][1] + dims[1] * m["dst"][2])
            ops.append((now, 0, "slot", slot))
            if slot < shared:
                ops.append((now + PARTNER_US, 0, "partner", slot))
    ops.sort(key=lambda op: op[:2])
    totals = {k: sum(m["hi"] - m["lo"] for m in msgs if m["link"] == k) for k in links}
    return dict(waits=len(sems), ops=[op[2:] for op in ops], links=links, totals=totals, end=now)


def make_kernel(dims, n_rows, n_cols, steps, sweeps):
    X, Y, Z = dims
    CH = X * Y * Z
    NR = n_rows // CH
    G = NR // S
    NT = n_rows // L
    TB = JT * NT
    HB = CH // 2
    JN = n_cols // 2 // L
    JW = JN // 2
    NT0 = G * JW
    TT0 = NT0 + 2 * G
    KJ = CH * JB
    CK = min(1024, KJ)
    CM = min(1024, KJ)
    GS = min(4, CH // 2)
    CS = max(CH * 3 // 8 // GS * GS, GS)
    NP = CH + CS
    NE, NC = (CH - CS) // GS, 2 * CS // GS
    GC = CM // JB // GS
    assert NT == 4 and n_cols == CH * L and JN == HB
    plan0 = tree_plan(dims, TT0, TILE_RATE, HOP_US - 1.4, AHEAD_US)
    plan = tree_plan(dims, TB, TILE_RATE, HOP_US, AHEAD_US, CS)
    links = plan["links"]
    NL = len(links)
    peers = [(d, k) for d in range(3) for k in range(1, dims[d])]
    strides = (1, X, X * Y)

    def slot_of(offset):
        return offset[0] + X * offset[1] + X * Y * offset[2]

    def kernel(
        eps_ref, p_ref, c1_ref, c2_ref, t0_ref, q_ref,
        out_ref, loss_ref,
        land, kbuf, g0, tt0, tt1, c1f, c1b, c2n, c2p, bacc, lp, lprecv, bp, qf, qrep, vbuf, cbuf,
        mb, sb, fb, ub, ap, xs, xr, mss, msr, pv, ars, arr, arps, arpr, obuf, orecv, trb, loss_rows, loss_two, c2v,
        send_sem, recv_sem, fwd_ssem, fwd_rsem, credit, x_ssem, x_rsem, ms_sem, lp_sem, c1_sem, c2_sem, q_sem, ar_ssem, ar_rsem, arp_sem, o_sem, loss_sem, in_sem,
    ):
        tts = (tt0, tt1)
        chip = lax.axis_index("rows")
        core = lax.axis_index("cols")
        other = 1 - core
        pos = (lax.rem(chip, X), lax.rem(lax.div(chip, X), Y), lax.div(chip, X * Y))

        me = core * CH + chip
        partner = other * CH + chip

        def moved(d, k):
            return me + (lax.rem(pos[d] + k + dims[d], dims[d]) - pos[d]) * strides[d]

        near = {link: moved(*link) for link in links}

        def source_of(slot):
            off = (lax.rem(slot, X), lax.rem(lax.div(slot, X), Y), lax.div(slot, X * Y))
            at = [lax.rem(pos[d] + dims[d] - off[d], dims[d]) for d in range(3)]
            return at[0] + X * at[1] + X * Y * at[2]

        def to_partner(src, dst, ssem, rsem):
            return pltpu.make_async_remote_copy(
                src_ref=src, dst_ref=dst, send_sem=ssem, recv_sem=rsem,
                device_id=partner, device_id_type=FLAT,
            )

        def tree_copy(buf, width, first, m):
            n = m["hi"] - m["lo"]
            return pltpu.make_async_remote_copy(
                src_ref=buf.at[pl.ds((first + slot_of(m["src"])) * width + m["lo"], n)],
                dst_ref=buf.at[pl.ds((first + slot_of(m["dst"])) * width + m["lo"], n)],
                send_sem=send_sem.at[links.index(m["link"])],
                recv_sem=recv_sem.at[m["sem"]],
                device_id=near[m["link"]],
                device_id_type=FLAT,
            )

        def tree(buf, width, first, the_plan, before_send=None, on_slot=None, fillers=()):
            fillers, ready, waits = list(fillers), [], 0
            for op, m in the_plan["ops"]:
                if op == "send":
                    if before_send is not None:
                        before_send(m)
                    tree_copy(buf, width, first, m).start()
                elif op == "wait":
                    while fillers and not fillers[0][0]:
                        fillers.pop(0)[1]()
                    if not ready and fillers and waits >= fillers[0][0]:
                        fillers.pop(0)[1]()
                    while ready:
                        on_slot(*ready.pop(0))
                    n = sum(e["hi"] - e["lo"] for e in m)
                    ref = buf.at[pl.ds((first + slot_of(m[0]["dst"])) * width, n)]
                    pltpu.make_async_copy(ref, ref, recv_sem.at[m[0]["sem"]]).wait()
                    waits += 1
                elif on_slot is not None:
                    ready.append((op, m))
            for at in ready:
                on_slot(*at)
            for _, f in fillers:
                f()

        def tree_sent(buf, the_plan):
            for k, link in enumerate(links):
                n = the_plan["totals"][link]
                ref = buf.at[pl.ds(0, n)]
                pltpu.make_async_copy(ref, ref, send_sem.at[k]).wait()

        def give_credit():
            for d, sign in links:
                pl.semaphore_signal(credit, inc=1, device_id=moved(d, -sign), device_id_type=FLAT)

        def all_sum_send(stage):
            for n, k in enumerate(range(1, dims[stage])):
                pltpu.make_async_remote_copy(
                    src_ref=ars.at[stage], dst_ref=arr.at[stage, n],
                    send_sem=ar_ssem.at[stage, n], recv_sem=ar_rsem.at[stage, n],
                    device_id=moved(stage, k), device_id_type=FLAT,
                ).start()

        def all_sum_get(stage):
            total = ars[stage]
            for n, k in enumerate(range(1, dims[stage])):
                pltpu.make_async_remote_copy(
                    src_ref=ars.at[stage], dst_ref=arr.at[stage, n],
                    send_sem=ar_ssem.at[stage, n], recv_sem=ar_rsem.at[stage, n],
                    device_id=moved(stage, k), device_id_type=FLAT,
                ).wait()
                total = total + arr[stage, n]
            return total

        def all_sum_step(stage):
            total = all_sum_get(stage)
            if stage < 2:
                ars[stage + 1] = total
                all_sum_send(stage + 1)
            else:
                arps[...] = total
                to_partner(arps, arpr, arp_sem.at[0], arp_sem.at[1]).start()

        c2_in = pltpu.make_async_copy(c2_ref, c2v, in_sem.at[0])
        c2_in.start()
        barrier = pltpu.get_barrier_semaphore()
        for d, k in peers:
            pl.semaphore_signal(barrier, inc=1, device_id=moved(d, k), device_id_type=FLAT)
        pl.semaphore_signal(barrier, inc=1, device_id=partner, device_id_type=FLAT)

        row = lax.broadcasted_iota(jnp.int32, (S, L), 0)
        lane = lax.broadcasted_iota(jnp.int32, (S, L), 1)

        for g in range(G):
            rows = slice(g * S, g * S + S)
            pair = jnp.concatenate([c1_ref[rows, :L], c1_ref[rows, L:]], axis=0)
            g0[NT0 + core * G + g] = pair.astype(BF16)
        c1_copy = to_partner(
            g0.at[pl.ds(NT0 + core * G, G)], g0.at[pl.ds(NT0 + core * G, G)], c1_sem.at[0], c1_sem.at[1]
        )
        q_copy = to_partner(q_ref, qf.at[pl.ds(core * HB, HB)], q_sem.at[0], q_sem.at[1])

        tile = jnp.zeros((S, L), F32)
        for t in range(2):
            part = jnp.zeros((1, L), F32)
            for k in range(NR):
                entry = c1_ref[k : k + 1, t * L : t * L + L]
                part = part + entry * entry * p_ref[k]
            tile = jnp.where(row == 2 * core + t, jnp.broadcast_to(part, (S, L)), tile)
        where = (row - 4) * L + lane
        for k in range(NR):
            tile = jnp.where(where == chip * NR + k, p_ref[k], tile)
        ars[0] = tile
        for g in range(G):
            rows = slice(g * S, g * S + S)
            for t in range(JW):
                a, b = t0_ref[rows, (2 * L) * t : (2 * L) * t + L], t0_ref[rows, (2 * L) * t + L : (2 * L) * t + (2 * L)]
                g0[g * JW + t] = jnp.concatenate([a, b], axis=0).astype(BF16)
        qf[pl.ds(core * HB, HB)] = q_ref[...]

        c2_copy = to_partner(c2n.at[pl.ds(core * HB, HB)], c2n.at[pl.ds(core * HB, HB)], c2_sem.at[0], c2_sem.at[1])
        bp[...] = jnp.zeros_like(bp)

        def round_c2(first, last):
            c2_in.wait()
            for t in range(first, last):
                blk = c2v[:, t * L : t * L + L]
                c2n[core * HB + t] = blk.astype(BF16)
                bp[...] += blk * blk * q_ref[t : t + 1, :]

        def finish_b():
            bp[...] = jnp.broadcast_to(jnp.sum(bp[...], axis=1, keepdims=True), (L, L))

        with jax.named_scope("barrier"):
            pl.semaphore_wait(barrier, len(peers) + 1)
        give_credit()
        c1_copy.start()
        q_copy.start()
        all_sum_send(0)

        src = lax.broadcasted_iota(jnp.int32, (L, L), 0)
        dst = lax.broadcasted_iota(jnp.int32, (L, L), 1)
        picks = [
            jnp.where((src - core * JB == dst - h * JB) & (dst >= h * JB) & (dst < h * JB + JB), 1.0, 0.0).astype(BF16)
            for h in range(2)
        ]

        def order_c2(first, last):
            for t in range(first, last):
                a = jnp.dot(c2n[source_of(2 * t)], picks[0], preferred_element_type=F32)
                b = jnp.dot(c2n[source_of(2 * t + 1)], picks[1], preferred_element_type=F32)
                c2p[:, t * L : t * L + L] = (a + b).astype(BF16)

        def order_q(first, last):
            def four(n, carry):
                for k in range(4):
                    p = 4 * n + k
                    shared = p < CS
                    half = jnp.where(shared, other, core)
                    line = jnp.broadcast_to(qf[pl.ds(source_of(jnp.where(shared, p, p - CS)), 1), :], (S, L))
                    for jt in range(JT):
                        own = jnp.where(lane == half * JB + jt * S + row, line, 0.0)
                        qrep[p, jt] = jnp.broadcast_to(jnp.sum(own, axis=1, keepdims=True), (S, L))
                return carry

            lax.fori_loop(first // 4, last // 4, four, 0)

        def span(n, parts, f):
            cuts = [n * k // parts for k in range(parts + 1)]
            return [lambda a=a, b=b: f(a, b) for a, b in zip(cuts, cuts[1:])]

        fillers = [(0, lambda: round_c2(0, HB)), (0, finish_b), (0, lambda: c2_copy.start())]
        fillers += [(0, lambda: q_copy.wait()), (0, lambda: order_q(0, NP)), (LATE // 2, lambda: all_sum_step(0))]
        fillers += [(LATE, lambda: all_sum_step(1))]
        waited = []

        def before_send(m):
            if not waited and m["hi"] > NT0:
                waited.append(1)
                c1_copy.wait()

        def unpack(op, s):
            chip_s = source_of(s)
            for g in range(G):
                tiles = g0[s * TT0 + g * JW : s * TT0 + g * JW + JW].astype(F32).reshape(JN, S, L)
                kbuf[pl.ds((chip_s * G + g) * JN, JN)] = tiles
                at = pl.ds(pl.multiple_of(chip_s * NR + g * S, S), S)
                for h in range(2):
                    pair = g0[s * TT0 + NT0 + h * G + g].astype(F32)
                    c1f[at, 2 * L * h : 2 * L * h + L] = pair[:S]
                    c1f[at, 2 * L * h + L : 2 * L * h + 2 * L] = pair[S:]

        with jax.named_scope("gather0"):
            first = [(0, lambda: unpack("slot", 0))]
            tree(g0, TT0, 0, plan0, before_send=before_send, on_slot=unpack, fillers=first + fillers)
            tree_sent(g0, plan0)
            c1b[...] = c1f[...].astype(BF16)
            all_sum_step(2)

        def finish_lp():
            lp[...] = jnp.concatenate([bp[...]] * NT, axis=1) - 2.0 * bacc[...]

        bacc[...] = jnp.zeros_like(bacc)
        JC = CK // L

        def first_chunk(n, carry):
            cols = []
            for t in range(JC):
                cols.append(kbuf[pl.ds(n * JC + t, CH * G, stride=JN)].reshape(n_rows, L))
            plan_c = jnp.concatenate(cols, axis=1).astype(BF16)
            lead = jnp.dot(c1b[...], plan_c, preferred_element_type=F32).astype(BF16)
            c2c = jnp.concatenate([c2n[core * HB + n * JC + t] for t in range(JC)], axis=1)
            bacc[...] += lax.dot_general(c2c, lead, (((1,), (1,)), ((), ())), preferred_element_type=F32)
            return carry

        with jax.named_scope("firstmm"):
            lax.fori_loop(0, KJ // CK, first_chunk, 0)
            finish_lp()
        to_partner(arps, arpr, arp_sem.at[0], arp_sem.at[1]).wait()
        ap[...] = jnp.where(row < 4, arps[...] + arpr[...], arps[...])
        for t in range(NT):
            pv[t] = jnp.broadcast_to(ap[4 + t : 5 + t, :], (S, L))


        def lead_and_cross(n, plan_c):
            lead = jnp.dot(plan_c[...], c1b[...], preferred_element_type=F32).astype(BF16)
            bacc[...] += jnp.dot(c2p[:, n * CM : n * CM + CM], lead, preferred_element_type=F32)

        def costs(meanwhile=None):
            copy = to_partner(lp.at[pl.ds(other * JB, JB)], lprecv, lp_sem.at[0], lp_sem.at[1])
            copy.start()
            if meanwhile is not None:
                meanwhile()
            copy.wait()
            own = lp[pl.ds(pl.multiple_of(core * JB, JB), JB), :] + lprecv[...]
            return own + jnp.concatenate([ap[t : t + 1, :] for t in range(NT)], axis=1)

        def block(s):
            return kbuf[pl.ds(s * TB, TB)].reshape(JT, NT, S, L)

        def weighted(kk, u):
            w = (kk[:, 0] * u[0] + kk[:, 1] * u[1]) + (kk[:, 2] * u[2] + kk[:, 3] * u[3])
            return jnp.sum(w, axis=2, keepdims=True)

        def passes(u, rescale=False, par=0):
            def place(g):
                return g * GS + 2 * CS if not isinstance(g, int) or g < NE else (g - NE) * GS

            def one(at, buf):
                for k in range(GS):
                    p = at + k
                    kk = block(p)
                    if rescale:
                        kk = kk * fb[:, pl.ds(p, 1), :][None]
                        kbuf[pl.ds(p * TB, TB)] = kk.reshape(TB, S, L)
                    cbuf[buf, k] = qrep[p] / jnp.broadcast_to(weighted(kk, u), (JT, S, L))

            def two(at, buf, acc):
                for k in range(GS):
                    p = at + k
                    acc = acc + jnp.sum(block(p) * cbuf[buf, k][:, None], axis=0)
                return acc

            def run(a, b, end):
                shift = place(a) - a * GS
                even, odd = a % 2, (a + 1) % 2
                pairs = max(0, (b - a - 1) // 2)

                def both(n, acc):
                    at = (a + 2 * n) * GS + shift
                    one(at + GS, odd)
                    acc = two(at, even, acc)
                    one(at + 2 * GS, even)
                    return two(at + GS, odd, acc)

                acc = lax.fori_loop(0, pairs, both, jnp.zeros((NT, S, L), F32))
                for g in range(a + 2 * pairs, b):
                    if g + 1 < end:
                        one(place(g + 1), (g + 1) % 2)
                    acc = two(place(g), g % 2, acc)
                return acc

            one(place(0), 0)
            xs[par] = run(0, NE, NE + NC)
            copy = to_partner(xs.at[par], xr.at[par], x_ssem.at[par], x_rsem.at[par])
            copy.start()
            acc = run(NE, NE + NC, NE + NC)
            copy.wait()
            total = jnp.sum((xs[par] + xr[par]) + acc, axis=1, keepdims=True)
            return quotient(pv[...], jnp.broadcast_to(total, (NT, S, L)))

        def plan_chunk(n, dst, u):
            def one(g):
                for k in range(GS):
                    p = CS + (n * GC + g) * GS + k
                    cbuf[g % 2, k] = quotient(qrep[p], jnp.broadcast_to(weighted(block(p), u), (JT, S, L)))

            one(0)
            for g in range(GC):
                if g + 1 < GC:
                    one(g + 1)
                for k in range(GS):
                    s = (n * GC + g) * GS + k
                    v = cbuf[g % 2, k]
                    vbuf[s] = v
                    t = (block(CS + s) * u[None]) * v[:, None]
                    flat = jnp.concatenate([t[:, i].reshape(JB, L) for i in range(NT)], axis=1)
                    at = (g * GS + k) * JB
                    dst[at : at + JB, :] = flat.astype(BF16)

        def outer(r, carry):
            eps = eps_ref[r]
            inv = 1.0 / eps
            inv = inv * (2.0 - eps * inv)
            main = LOG2E * inv
            (e0, e1), (m0, m1) = halves(eps), halves(main)
            prod = eps * main
            low_part = ((e0 * m0 - prod) + (e0 * m1 + e1 * m0)) + e1 * m1
            rest = (((LOG2E - prod) - low_part) + LOG2E_REST) * inv

            def decay(x):
                return jnp.exp2(x * main + x * rest)

            cost = costs()
            for jt in range(JT):
                for t in range(NT):
                    land[CS * TB + jt * NT + t] = cost[jt * S : jt * S + S, t * L : t * L + L]

            def exps(p):
                ll = land[p * TB : p * TB + TB].reshape(JT, NT, S, L)
                low = jnp.min(jnp.min(ll, axis=0), axis=1, keepdims=True)
                kk = decay(low[None] - ll)
                kbuf[p * TB : p * TB + TB] = kk.reshape(TB, S, L)
                mb[:, p : p + 1, :] = low
                sb[:, p : p + 1, :] = jnp.sum(jnp.sum(kk, axis=0), axis=1, keepdims=True)

            def passed_on(s):
                return to_partner(
                    land.at[pl.ds((CS + s) * TB, TB)], land.at[pl.ds(s * TB, TB)], fwd_ssem.at[0], fwd_rsem.at[s]
                )

            def on_slot(op, s):
                if op == "slot":
                    if s < CS:
                        passed_on(s).start()
                    exps(CS + s)
                else:
                    passed_on(s).wait_recv()
                    exps(s)

            def once(n, f):
                @pl.when(r == 0)
                def _():
                    if not n:
                        c2_copy.wait()
                    f()

            with jax.named_scope("gather"):
                pl.semaphore_wait(credit, NL)
                first = [(0, lambda: on_slot("slot", 0)), (plan["waits"] // 4, lambda: on_slot("partner", 0))]
                for n, f in enumerate(span(CH // 2, S, order_c2)):
                    first.append((LATE // 2 + 2 * n, lambda n=n, f=f: once(n, f)))
                tree(land, TB, CS, plan, on_slot=on_slot, fillers=first)
                tree_sent(land, plan)
                ref = land.at[pl.ds(0, CS * TB)]
                pltpu.make_async_copy(ref, ref, fwd_ssem.at[0]).wait()
                give_credit()

            with jax.named_scope("minx"):
                def least_of(a, b):
                    low = jnp.min(mb[:, a:b], axis=1, keepdims=True)
                    part = jnp.sum(sb[:, a:b] * decay(low - mb[:, a:b]), axis=1, keepdims=True)
                    return jnp.broadcast_to(low, (NT, S, L)), jnp.broadcast_to(part, (NT, S, L))

                mss[0], mss[1] = least_of(2 * CS, NP)
                copy = to_partner(mss, msr, ms_sem.at[0], ms_sem.at[1])
                copy.start()
                low, part = least_of(0, 2 * CS)
                copy.wait()
                least = jnp.minimum(jnp.minimum(mss[0], msr[0]), low)
                total = mss[1] * decay(least - mss[0]) + msr[1] * decay(least - msr[0])
                total = total + part * decay(least - low)
                fb[...] = decay(least[:, :1] - mb[...])
                u = quotient(pv[...], total)

            with jax.named_scope("pass1"):
                u = passes(u, rescale=True, par=1)

            def sweep(t, u):
                return passes(u, par=lax.rem(t, 2))

            with jax.named_scope("sweeps"):
                u = lax.fori_loop(2, sweeps, sweep, u)
            ub[...] = u
            bacc[...] = jnp.zeros_like(bacc)
            with jax.named_scope("finish"):
                plan_chunk(0, tts[0], u)
                for n in range(KJ // CM):
                    if n + 1 < KJ // CM:
                        plan_chunk(n + 1, tts[(n + 1) % 2], u)
                    lead_and_cross(n, tts[n % 2])
                finish_lp()
            return carry

        lax.fori_loop(0, steps, outer, 0)

        pl.semaphore_wait(credit, NL)

        it = lax.div(chip * NR, L)
        inside = pl.multiple_of(lax.rem(chip * NR, L), S)

        def rows_of(n, carry):
            for k in range(4):
                s = 4 * n + k
                kk = jnp.concatenate([kbuf[(CS + s) * TB + jt * NT + it] for jt in range(JT)], axis=0)
                uu = jnp.concatenate([ub[it]] * JT, axis=0)
                t = (kk * uu) * vbuf[s].reshape(JB, L)
                none = jnp.zeros_like(t)
                both = jnp.where(core == 0, jnp.concatenate([t, none], axis=0), jnp.concatenate([none, t], axis=0))
                trb[k] = both.T
                obuf[source_of(s)] = trb[k, pl.ds(inside, NR), :]
            return carry

        early = CH // 4 * 3 // 8
        cost = costs(lambda: lax.fori_loop(0, early, rows_of, 0))
        plan_own = (block(CS) * ub[...][None]) * vbuf[0][:, None]
        total = jnp.zeros((S, L), F32)
        for jt in range(JT):
            for t in range(NT):
                total = total + cost[jt * S : jt * S + S, t * L : t * L + L] * plan_own[jt, t]
        loss_rows[0:1] = jnp.sum(total, axis=0, keepdims=True)

        def to_chip(n):
            o = CH - n
            off = (lax.rem(o, X), lax.rem(lax.div(o, X), Y), lax.div(o, X * Y))
            at = [lax.rem(pos[d] + off[d], dims[d]) for d in range(3)]
            return pltpu.make_async_remote_copy(
                src_ref=loss_rows.at[pl.ds(0, 1)], dst_ref=loss_rows.at[pl.ds(o, 1)],
                send_sem=loss_sem.at[0], recv_sem=loss_sem.at[1],
                device_id=core * CH + at[0] + X * at[1] + X * Y * at[2], device_id_type=FLAT,
            )

        def tell(n, carry):
            to_chip(n).start()
            return carry

        lax.fori_loop(1, CH, tell, 0)

        with jax.named_scope("tail"):
            lax.fori_loop(early, CH // 4, rows_of, 0)
            o_copy = to_partner(obuf.at[pl.ds(other * HB, HB)], orecv, o_sem.at[0], o_sem.at[1])
            o_copy.start()
            ref = loss_rows.at[pl.ds(1, CH - 1)]
            pltpu.make_async_copy(ref, ref, loss_sem.at[0]).wait()
            pltpu.make_async_copy(ref, ref, loss_sem.at[1]).wait()
            loss_two[0:1] = jnp.sum(loss_rows[...], axis=0, keepdims=True)
            copy = to_partner(loss_two.at[pl.ds(0, 1)], loss_two.at[pl.ds(1, 1)], loss_sem.at[2], loss_sem.at[3])
            copy.start()
            o_copy.wait()
            orecv[...] = obuf[pl.ds(core * HB, HB)] + orecv[...]
            o_out = pltpu.make_async_copy(orecv, out_ref, in_sem.at[1])
            o_out.start()
            copy.wait()
            loss_ref[0] = jnp.sum(loss_two[...])
            o_out.wait()

    vm = pltpu.VMEM
    dma = pltpu.SemaphoreType.DMA
    scratch = [
        vm((NP * TB, S, L), F32),
        vm((NP * TB, S, L), F32),
        vm((CH * TT0, 16, L), BF16),
        vm((CM, n_rows), BF16),
        vm((CM, n_rows), BF16),
        vm((n_rows, n_rows), F32),
        vm((n_rows, n_rows), BF16),
        vm((CH, L, L), BF16),
        vm((L, KJ), BF16),
        vm((L, n_rows), F32),
        vm((L, n_rows), F32),
        vm((JB, n_rows), F32),
        vm((L, L), F32),
        vm((CH, L), F32),
        vm((NP, JT, S, L), F32),
        vm((CH, JT, S, L), F32),
        vm((2, GS, JT, S, L), F32),
        vm((NT, NP, L), F32),
        vm((NT, NP, L), F32),
        vm((NT, NP, L), F32),
        vm((NT, S, L), F32),
        vm((S, L), F32),
        vm((2, NT, S, L), F32),
        vm((2, NT, S, L), F32),
        vm((2, NT, S, L), F32),
        vm((2, NT, S, L), F32),
        vm((NT, S, L), F32),
        vm((3, S, L), F32),
        vm((3, 3, S, L), F32),
        vm((S, L), F32),
        vm((S, L), F32),
        vm((CH, NR, L), F32),
        vm((HB, NR, L), F32),
        vm((4, L, L), F32),
        vm((CH, L), F32),
        vm((2, L), F32),
        vm((L, n_cols // 2), F32),
        dma((NL,)),
        dma((max(plan["waits"], plan0["waits"]),)),
        dma((1,)),
        dma((CS,)),
        pltpu.SemaphoreType.REGULAR,
        dma((2,)),
        dma((2,)),
        dma((2,)),
        dma((2,)),
        dma((2,)),
        dma((2,)),
        dma((2,)),
        dma((3, 3)),
        dma((3, 3)),
        dma((2,)),
        dma((2,)),
        dma((4,)),
        dma((2,)),
    ]
    return kernel, scratch


def solution(mesh):
    chips = mesh.shape["rows"]
    dims = torus_of(chips)
    grid_spec = P(("pairs", "rows"), "cols")

    def local_fn(c1, c2, t0, p, q, eps):
        n_rows, n_cols = p.shape[0] * chips, q.shape[0] * mesh.shape["cols"]
        kernel, scratch = make_kernel(dims, n_rows, n_cols, eps.shape[0], SWEEPS)
        vmem = pl.BlockSpec(memory_space=pltpu.VMEM)
        smem = pl.BlockSpec(memory_space=pltpu.SMEM)
        anywhere = pl.BlockSpec(memory_space=pl.ANY)
        plan, loss = pl.pallas_call(
            kernel,
            name="gromov",
            out_shape=(jax.ShapeDtypeStruct((chips // 2, t0.shape[0], L), F32), jax.ShapeDtypeStruct((1,), F32)),
            in_specs=[smem, smem, vmem, anywhere, vmem, vmem],
            out_specs=(anywhere, smem),
            scratch_shapes=scratch,
            compiler_params=pltpu.CompilerParams(
                collective_id=0, has_side_effects=True, vmem_limit_bytes=60 * 1024 * 1024
            ),
        )(eps, p, c1, c2, t0, q.reshape(chips // 2, L))
        return plan.transpose(1, 0, 2).reshape(t0.shape), loss

    return jax.shard_map(
        local_fn,
        mesh=mesh,
        in_specs=(grid_spec, grid_spec, grid_spec, P(("pairs", "rows")), P(("pairs", "cols")), P("pairs")),
        out_specs=(grid_spec, P("pairs")),
        check_vma=False,
    )
```

```python
import heapq
import itertools
import math

import jax
import jax.numpy as jnp
from jax import lax
from jax.experimental import pallas as pl
from jax.experimental.pallas import tpu as pltpu
from jax.sharding import PartitionSpec as P

SWEEPS = 10
FLAT = pl.DeviceIdType.LOGICAL
L, S = 128, 8
JB = 64
JT = JB // S
F32, BF16 = jnp.float32, jnp.bfloat16
ORDERS = ((0, 1, 2), (1, 2, 0), (2, 0, 1))
TILE_RATE = 11.4
HOP_US = 5.0
AHEAD_US = 3.0
LOG2E = 1.4426950216293335
LOG2E_REST = 1.925963e-8
PARTNER_US = 4.0
LATE = 100


def torus_of(chips):
    return {64: (4, 4, 4), S: (4, 2, 1), 16: (4, 4, 1)}[chips]


def halves(x):
    c = 4097.0 * x
    high = c - (c - x)
    return high, x - high


def quotient(a, b):
    q = a / b
    return q + (a - q * b) / b


def split3(n):
    cuts = [0, (n + 2) // 3, (2 * n + 2) // 3, n]
    return [(cuts[k], cuts[k + 1]) for k in range(3)]


def tree_plan(dims, tiles, rate, lat_us, ahead_us, shared=0):
    rings = {1: (), 2: ((1, "f", 1),), 4: ((1, "f", 1), (3, "f", -1), (2, "a", 1), (2, "b", -1))}
    msgs = []
    for color, order in enumerate(ORDERS):
        lo, hi = split3(tiles)[color]
        for dst in itertools.product(*(range(n) for n in dims)):
            used = [k for k in range(3) if dst[order[k]]]
            if not used or lo == hi:
                continue
            d = order[used[-1]]
            mid = lo + (hi - lo + (sum(dst) + color) % 2) // 2
            for at, part, sign in rings[dims[d]]:
                a, b = {"f": (lo, hi), "a": (lo, mid), "b": (mid, hi)}[part]
                if at != dst[d] or a == b:
                    continue
                src = list(dst)
                src[d] = (src[d] - sign) % dims[d]
                m = dict(id=len(msgs), color=color, src=tuple(src), dst=dst, link=(d, sign), lo=a, hi=b)
                m["us"] = (b - a) / rate
                msgs.append(m)
    into = {}
    for m in msgs:
        into.setdefault((m["color"], m["dst"]), []).append(m)
    users = [[] for _ in msgs]
    missing = []
    for m in msgs:
        deps = [e for e in into.get((m["color"], m["src"]), []) if e["lo"] < m["hi"] and m["lo"] < e["hi"]]
        missing.append(len(deps))
        for e in deps:
            users[e["id"]].append(m)
    sems, waiting = {}, {}
    for m in msgs:
        key = (m["color"] if users[m["id"]] else None, m["dst"])
        m["sem"] = sems.setdefault(key, len(sems))
        waiting.setdefault(m["sem"], []).append(m)
    pending = {k: len(group) for k, group in waiting.items()}
    way = {}

    def way_of(m):
        if m["id"] not in way:
            way[m["id"]] = m["us"] + lat_us + max([way_of(u) for u in users[m["id"]]], default=0.0)
        return way[m["id"]]

    links = sorted({m["link"] for m in msgs})
    queue = {k: [] for k in links}
    idle = dict.fromkeys(links, True)
    ready, events, ops = {}, [], []

    def put(m, now):
        ready[m["id"]] = now
        heapq.heappush(queue[m["link"]], (-way_of(m), m["id"]))

    def start(link, now):
        if idle[link] and queue[link]:
            k = heapq.heappop(queue[link])[1]
            idle[link] = False
            ops.append((max(ready[k], now - ahead_us), 1, "send", msgs[k]))
            heapq.heappush(events, (now + msgs[k]["us"], 0, k))
            heapq.heappush(events, (now + msgs[k]["us"] + lat_us, 1, k))

    for m in msgs:
        if not missing[m["id"]]:
            put(m, 0.0)
    for link in links:
        start(link, 0.0)
    left = {}
    for m in msgs:
        left[m["dst"]] = left.get(m["dst"], 0) + 1
    now = 0.0
    while events:
        now, arrived, k = heapq.heappop(events)
        m = msgs[k]
        if not arrived:
            idle[m["link"]] = True
            start(m["link"], now)
            continue
        pending[m["sem"]] -= 1
        if not pending[m["sem"]]:
            ops.append((now, 0, "wait", waiting[m["sem"]]))
        for u in users[k]:
            missing[u["id"]] -= 1
            if not missing[u["id"]]:
                put(u, now)
                start(u["link"], now)
        left[m["dst"]] -= 1
        if not left[m["dst"]]:
            slot = m["dst"][0] + dims[0] * (m["dst"][1] + dims[1] * m["dst"][2])
            ops.append((now, 0, "slot", slot))
            if slot < shared:
                ops.append((now + PARTNER_US, 0, "partner", slot))
    ops.sort(key=lambda op: op[:2])
    totals = {k: sum(m["hi"] - m["lo"] for m in msgs if m["link"] == k) for k in links}
    return dict(waits=len(sems), ops=[op[2:] for op in ops], links=links, totals=totals, end=now)


def make_kernel(dims, n_rows, n_cols, steps, sweeps):
    X, Y, Z = dims
    CH = X * Y * Z
    NR = n_rows // CH
    G = NR // S
    NT = n_rows // L
    TB = JT * NT
    HB = CH // 2
    JN = n_cols // 2 // L
    JW = JN // 2
    NT0 = G * JW
    TT0 = NT0 + 2 * G
    KJ = CH * JB
    CK = min(1024, KJ)
    CM = min(1024, KJ)
    GS = min(4, CH // 2)
    CS = max(CH * 3 // 8 // GS * GS, GS)
    NP = CH + CS
    NE, NC = (CH - CS) // GS, 2 * CS // GS
    GC = CM // JB // GS
    assert NT == 4 and n_cols == CH * L and JN == HB
    plan0 = tree_plan(dims, TT0, TILE_RATE, HOP_US - 2, AHEAD_US - 1)
    plan = tree_plan(dims, TB, TILE_RATE, HOP_US, AHEAD_US, CS)
    links = plan["links"]
    NL = len(links)
    peers = [(d, k) for d in range(3) for k in range(1, dims[d])]
    strides = (1, X, X * Y)

    def slot_of(offset):
        return offset[0] + X * offset[1] + X * Y * offset[2]

    def kernel(
        eps_ref, p_ref, c1_ref, c2_ref, t0_ref, q_ref,
        out_ref, loss_ref,
        land, kbuf, g0, tt0, tt1, c1f, c1b, c2n, c2p, bacc, lp, lprecv, bp, qf, qrep, vbuf, cbuf,
        mb, sb, fb, ub, ap, xs, xr, mss, msr, pv, ars, arr, arps, arpr, obuf, orecv, trb, loss_rows, loss_two, c2v,
        send_sem, recv_sem, fwd_ssem, fwd_rsem, credit, x_ssem, x_rsem, ms_sem, lp_sem, c1_sem, c2_sem, q_sem, ar_ssem, ar_rsem, arp_sem, o_sem, loss_sem, in_sem,
    ):
        tts = (tt0, tt1)
        chip = lax.axis_index("rows")
        core = lax.axis_index("cols")
        other = 1 - core
        pos = (lax.rem(chip, X), lax.rem(lax.div(chip, X), Y), lax.div(chip, X * Y))

        me = core * CH + chip
        partner = other * CH + chip

        def moved(d, k):
            return me + (lax.rem(pos[d] + k + dims[d], dims[d]) - pos[d]) * strides[d]

        near = {link: moved(*link) for link in links}

        def source_of(slot):
            off = (lax.rem(slot, X), lax.rem(lax.div(slot, X), Y), lax.div(slot, X * Y))
            at = [lax.rem(pos[d] + dims[d] - off[d], dims[d]) for d in range(3)]
            return at[0] + X * at[1] + X * Y * at[2]

        def to_partner(src, dst, ssem, rsem):
            return pltpu.make_async_remote_copy(
                src_ref=src, dst_ref=dst, send_sem=ssem, recv_sem=rsem,
                device_id=partner, device_id_type=FLAT,
            )

        def tree_copy(buf, width, first, m):
            n = m["hi"] - m["lo"]
            return pltpu.make_async_remote_copy(
                src_ref=buf.at[pl.ds((first + slot_of(m["src"])) * width + m["lo"], n)],
                dst_ref=buf.at[pl.ds((first + slot_of(m["dst"])) * width + m["lo"], n)],
                send_sem=send_sem.at[links.index(m["link"])],
                recv_sem=recv_sem.at[m["sem"]],
                device_id=near[m["link"]],
                device_id_type=FLAT,
            )

        def tree(buf, width, first, the_plan, before_send=None, on_slot=None, fillers=()):
            fillers, ready, waits = list(fillers), [], 0
            for op, m in the_plan["ops"]:
                if op == "send":
                    if before_send is not None:
                        before_send(m)
                    tree_copy(buf, width, first, m).start()
                elif op == "wait":
                    while fillers and not fillers[0][0]:
                        fillers.pop(0)[1]()
                    if not ready and fillers and waits >= fillers[0][0]:
                        fillers.pop(0)[1]()
                    while ready:
                        on_slot(*ready.pop(0))
                    n = sum(e["hi"] - e["lo"] for e in m)
                    ref = buf.at[pl.ds((first + slot_of(m[0]["dst"])) * width, n)]
                    pltpu.make_async_copy(ref, ref, recv_sem.at[m[0]["sem"]]).wait()
                    waits += 1
                elif on_slot is not None:
                    ready.append((op, m))
            for at in ready:
                on_slot(*at)
            for _, f in fillers:
                f()

        def tree_sent(buf, the_plan):
            for k, link in enumerate(links):
                n = the_plan["totals"][link]
                ref = buf.at[pl.ds(0, n)]
                pltpu.make_async_copy(ref, ref, send_sem.at[k]).wait()

        def give_credit():
            for d, sign in links:
                pl.semaphore_signal(credit, inc=1, device_id=moved(d, -sign), device_id_type=FLAT)

        def all_sum_send(stage):
            for n, k in enumerate(range(1, dims[stage])):
                pltpu.make_async_remote_copy(
                    src_ref=ars.at[stage], dst_ref=arr.at[stage, n],
                    send_sem=ar_ssem.at[stage, n], recv_sem=ar_rsem.at[stage, n],
                    device_id=moved(stage, k), device_id_type=FLAT,
                ).start()

        def all_sum_get(stage):
            total = ars[stage]
            for n, k in enumerate(range(1, dims[stage])):
                pltpu.make_async_remote_copy(
                    src_ref=ars.at[stage], dst_ref=arr.at[stage, n],
                    send_sem=ar_ssem.at[stage, n], recv_sem=ar_rsem.at[stage, n],
                    device_id=moved(stage, k), device_id_type=FLAT,
                ).wait()
                total = total + arr[stage, n]
            return total

        def all_sum_step(stage):
            total = all_sum_get(stage)
            if stage < 2:
                ars[stage + 1] = total
                all_sum_send(stage + 1)
            else:
                arps[...] = total
                to_partner(arps, arpr, arp_sem.at[0], arp_sem.at[1]).start()

        c2_in = pltpu.make_async_copy(c2_ref, c2v, in_sem.at[0])
        c2_in.start()
        barrier = pltpu.get_barrier_semaphore()
        for d, k in peers:
            pl.semaphore_signal(barrier, inc=1, device_id=moved(d, k), device_id_type=FLAT)
        pl.semaphore_signal(barrier, inc=1, device_id=partner, device_id_type=FLAT)

        row = lax.broadcasted_iota(jnp.int32, (S, L), 0)
        lane = lax.broadcasted_iota(jnp.int32, (S, L), 1)

        for g in range(G):
            rows = slice(g * S, g * S + S)
            pair = jnp.concatenate([c1_ref[rows, :L], c1_ref[rows, L:]], axis=0)
            g0[NT0 + core * G + g] = pair.astype(BF16)
        c1_copy = to_partner(
            g0.at[pl.ds(NT0 + core * G, G)], g0.at[pl.ds(NT0 + core * G, G)], c1_sem.at[0], c1_sem.at[1]
        )
        q_copy = to_partner(q_ref, qf.at[pl.ds(core * HB, HB)], q_sem.at[0], q_sem.at[1])

        tile = jnp.zeros((S, L), F32)
        for t in range(2):
            part = jnp.zeros((1, L), F32)
            for k in range(NR):
                entry = c1_ref[k : k + 1, t * L : t * L + L]
                part = part + entry * entry * p_ref[k]
            tile = jnp.where(row == 2 * core + t, jnp.broadcast_to(part, (S, L)), tile)
        where = (row - 4) * L + lane
        for k in range(NR):
            tile = jnp.where(where == chip * NR + k, p_ref[k], tile)
        ars[0] = tile
        for g in range(G):
            rows = slice(g * S, g * S + S)
            for t in range(JW):
                a, b = t0_ref[rows, (2 * L) * t : (2 * L) * t + L], t0_ref[rows, (2 * L) * t + L : (2 * L) * t + (2 * L)]
                g0[g * JW + t] = jnp.concatenate([a, b], axis=0).astype(BF16)
        qf[pl.ds(core * HB, HB)] = q_ref[...]

        c2_copy = to_partner(c2n.at[pl.ds(core * HB, HB)], c2n.at[pl.ds(core * HB, HB)], c2_sem.at[0], c2_sem.at[1])
        bp[...] = jnp.zeros_like(bp)

        def round_c2(first, last):
            c2_in.wait()
            for t in range(first, last):
                blk = c2v[:, t * L : t * L + L]
                c2n[core * HB + t] = blk.astype(BF16)
                bp[...] += blk * blk * q_ref[t : t + 1, :]

        def finish_b():
            bp[...] = jnp.broadcast_to(jnp.sum(bp[...], axis=1, keepdims=True), (L, L))

        with jax.named_scope("barrier"):
            pl.semaphore_wait(barrier, len(peers) + 1)
        give_credit()
        c1_copy.start()
        q_copy.start()
        all_sum_send(0)

        src = lax.broadcasted_iota(jnp.int32, (L, L), 0)
        dst = lax.broadcasted_iota(jnp.int32, (L, L), 1)
        picks = [
            jnp.where((src - core * JB == dst - h * JB) & (dst >= h * JB) & (dst < h * JB + JB), 1.0, 0.0).astype(BF16)
            for h in range(2)
        ]

        def order_c2(first, last):
            for t in range(first, last):
                a = jnp.dot(c2n[source_of(2 * t)], picks[0], preferred_element_type=F32)
                b = jnp.dot(c2n[source_of(2 * t + 1)], picks[1], preferred_element_type=F32)
                c2p[:, t * L : t * L + L] = (a + b).astype(BF16)

        def order_q(first, last):
            def four(n, carry):
                for k in range(4):
                    p = 4 * n + k
                    shared = p < CS
                    half = jnp.where(shared, other, core)
                    line = jnp.broadcast_to(qf[pl.ds(source_of(jnp.where(shared, p, p - CS)), 1), :], (S, L))
                    for jt in range(JT):
                        own = jnp.where(lane == half * JB + jt * S + row, line, 0.0)
                        qrep[p, jt] = jnp.broadcast_to(jnp.sum(own, axis=1, keepdims=True), (S, L))
                return carry

            lax.fori_loop(first // 4, last // 4, four, 0)

        def span(n, parts, f):
            cuts = [n * k // parts for k in range(parts + 1)]
            return [lambda a=a, b=b: f(a, b) for a, b in zip(cuts, cuts[1:])]

        fillers = [(0, lambda: round_c2(0, HB)), (0, finish_b), (0, lambda: c2_copy.start())]
        fillers += [(0, lambda: q_copy.wait()), (0, lambda: order_q(0, NP)), (LATE // 2, lambda: all_sum_step(0))]
        fillers += [(LATE, lambda: all_sum_step(1))]
        waited = []

        def before_send(m):
            if not waited and m["hi"] > NT0:
                waited.append(1)
                c1_copy.wait()

        def unpack(op, s):
            chip_s = source_of(s)
            for g in range(G):
                tiles = g0[s * TT0 + g * JW : s * TT0 + g * JW + JW].astype(F32).reshape(JN, S, L)
                kbuf[pl.ds((chip_s * G + g) * JN, JN)] = tiles
                at = pl.ds(pl.multiple_of(chip_s * NR + g * S, S), S)
                for h in range(2):
                    pair = g0[s * TT0 + NT0 + h * G + g].astype(F32)
                    c1f[at, 2 * L * h : 2 * L * h + L] = pair[:S]
                    c1f[at, 2 * L * h + L : 2 * L * h + 2 * L] = pair[S:]

        with jax.named_scope("gather0"):
            first = [(0, lambda: unpack("slot", 0))]
            tree(g0, TT0, 0, plan0, before_send=before_send, on_slot=unpack, fillers=first + fillers)
            tree_sent(g0, plan0)
            c1b[...] = c1f[...].astype(BF16)
            all_sum_step(2)

        def finish_lp():
            lp[...] = jnp.concatenate([bp[...]] * NT, axis=1) - 2.0 * bacc[...]

        bacc[...] = jnp.zeros_like(bacc)
        JC = CK // L

        def first_chunk(n, carry):
            cols = []
            for t in range(JC):
                cols.append(kbuf[pl.ds(n * JC + t, CH * G, stride=JN)].reshape(n_rows, L))
            plan_c = jnp.concatenate(cols, axis=1).astype(BF16)
            lead = jnp.dot(c1b[...], plan_c, preferred_element_type=F32).astype(BF16)
            c2c = jnp.concatenate([c2n[core * HB + n * JC + t] for t in range(JC)], axis=1)
            bacc[...] += lax.dot_general(c2c, lead, (((1,), (1,)), ((), ())), preferred_element_type=F32)
            return carry

        with jax.named_scope("firstmm"):
            lax.fori_loop(0, KJ // CK, first_chunk, 0)
            finish_lp()
        to_partner(arps, arpr, arp_sem.at[0], arp_sem.at[1]).wait()
        ap[...] = jnp.where(row < 4, arps[...] + arpr[...], arps[...])
        for t in range(NT):
            pv[t] = jnp.broadcast_to(ap[4 + t : 5 + t, :], (S, L))


        def lead_and_cross(n, plan_c):
            lead = jnp.dot(plan_c[...], c1b[...], preferred_element_type=F32).astype(BF16)
            bacc[...] += jnp.dot(c2p[:, n * CM : n * CM + CM], lead, preferred_element_type=F32)

        def costs():
            copy = to_partner(lp.at[pl.ds(other * JB, JB)], lprecv, lp_sem.at[0], lp_sem.at[1])
            copy.start()
            copy.wait()
            own = lp[pl.ds(pl.multiple_of(core * JB, JB), JB), :] + lprecv[...]
            return own + jnp.concatenate([ap[t : t + 1, :] for t in range(NT)], axis=1)

        def block(s):
            return kbuf[pl.ds(s * TB, TB)].reshape(JT, NT, S, L)

        def weighted(kk, u):
            w = (kk[:, 0] * u[0] + kk[:, 1] * u[1]) + (kk[:, 2] * u[2] + kk[:, 3] * u[3])
            return jnp.sum(w, axis=2, keepdims=True)

        def passes(u, rescale=False, par=0):
            def place(g):
                return g * GS + 2 * CS if not isinstance(g, int) or g < NE else (g - NE) * GS

            def one(at, buf):
                for k in range(GS):
                    p = at + k
                    kk = block(p)
                    if rescale:
                        kk = kk * fb[:, pl.ds(p, 1), :][None]
                        kbuf[pl.ds(p * TB, TB)] = kk.reshape(TB, S, L)
                    cbuf[buf, k] = qrep[p] / jnp.broadcast_to(weighted(kk, u), (JT, S, L))

            def two(at, buf, acc):
                for k in range(GS):
                    p = at + k
                    acc = acc + jnp.sum(block(p) * cbuf[buf, k][:, None], axis=0)
                return acc

            def run(a, b, end):
                shift = place(a) - a * GS
                even, odd = a % 2, (a + 1) % 2
                pairs = max(0, (b - a - 1) // 2)

                def both(n, acc):
                    at = (a + 2 * n) * GS + shift
                    one(at + GS, odd)
                    acc = two(at, even, acc)
                    one(at + 2 * GS, even)
                    return two(at + GS, odd, acc)

                acc = lax.fori_loop(0, pairs, both, jnp.zeros((NT, S, L), F32))
                for g in range(a + 2 * pairs, b):
                    if g + 1 < end:
                        one(place(g + 1), (g + 1) % 2)
                    acc = two(place(g), g % 2, acc)
                return acc

            one(place(0), 0)
            xs[par] = run(0, NE, NE + NC)
            copy = to_partner(xs.at[par], xr.at[par], x_ssem.at[par], x_rsem.at[par])
            copy.start()
            acc = run(NE, NE + NC, NE + NC)
            copy.wait()
            total = jnp.sum((xs[par] + xr[par]) + acc, axis=1, keepdims=True)
            return quotient(pv[...], jnp.broadcast_to(total, (NT, S, L)))

        def plan_chunk(n, dst, u):
            def one(g):
                for k in range(GS):
                    p = CS + (n * GC + g) * GS + k
                    cbuf[g % 2, k] = quotient(qrep[p], jnp.broadcast_to(weighted(block(p), u), (JT, S, L)))

            one(0)
            for g in range(GC):
                if g + 1 < GC:
                    one(g + 1)
                for k in range(GS):
                    s = (n * GC + g) * GS + k
                    v = cbuf[g % 2, k]
                    vbuf[s] = v
                    t = (block(CS + s) * u[None]) * v[:, None]
                    flat = jnp.concatenate([t[:, i].reshape(JB, L) for i in range(NT)], axis=1)
                    at = (g * GS + k) * JB
                    dst[at : at + JB, :] = flat.astype(BF16)

        def outer(r, carry):
            eps = eps_ref[r]
            inv = 1.0 / eps
            inv = inv * (2.0 - eps * inv)
            main = LOG2E * inv
            (e0, e1), (m0, m1) = halves(eps), halves(main)
            prod = eps * main
            low_part = ((e0 * m0 - prod) + (e0 * m1 + e1 * m0)) + e1 * m1
            rest = (((LOG2E - prod) - low_part) + LOG2E_REST) * inv

            def decay(x):
                return jnp.exp2(x * main + x * rest)

            cost = costs()
            for jt in range(JT):
                for t in range(NT):
                    land[CS * TB + jt * NT + t] = cost[jt * S : jt * S + S, t * L : t * L + L]

            def exps(p):
                ll = land[p * TB : p * TB + TB].reshape(JT, NT, S, L)
                low = jnp.min(jnp.min(ll, axis=0), axis=1, keepdims=True)
                kk = decay(low[None] - ll)
                kbuf[p * TB : p * TB + TB] = kk.reshape(TB, S, L)
                mb[:, p : p + 1, :] = low
                sb[:, p : p + 1, :] = jnp.sum(jnp.sum(kk, axis=0), axis=1, keepdims=True)

            def passed_on(s):
                return to_partner(
                    land.at[pl.ds((CS + s) * TB, TB)], land.at[pl.ds(s * TB, TB)], fwd_ssem.at[0], fwd_rsem.at[s]
                )

            def on_slot(op, s):
                if op == "slot":
                    if s < CS:
                        passed_on(s).start()
                    exps(CS + s)
                else:
                    passed_on(s).wait_recv()
                    exps(s)

            def once(n, f):
                @pl.when(r == 0)
                def _():
                    if not n:
                        c2_copy.wait()
                    f()

            with jax.named_scope("gather"):
                pl.semaphore_wait(credit, NL)
                first = [(0, lambda: on_slot("slot", 0)), (plan["waits"] // 4, lambda: on_slot("partner", 0))]
                for n, f in enumerate(span(CH // 2, S, order_c2)):
                    first.append((LATE // 2 + 2 * n, lambda n=n, f=f: once(n, f)))
                tree(land, TB, CS, plan, on_slot=on_slot, fillers=first)
                tree_sent(land, plan)
                ref = land.at[pl.ds(0, CS * TB)]
                pltpu.make_async_copy(ref, ref, fwd_ssem.at[0]).wait()
                give_credit()

            with jax.named_scope("minx"):
                def least_of(a, b):
                    low = jnp.min(mb[:, a:b], axis=1, keepdims=True)
                    part = jnp.sum(sb[:, a:b] * decay(low - mb[:, a:b]), axis=1, keepdims=True)
                    return jnp.broadcast_to(low, (NT, S, L)), jnp.broadcast_to(part, (NT, S, L))

                mss[0], mss[1] = least_of(2 * CS, NP)
                copy = to_partner(mss, msr, ms_sem.at[0], ms_sem.at[1])
                copy.start()
                low, part = least_of(0, 2 * CS)
                copy.wait()
                least = jnp.minimum(jnp.minimum(mss[0], msr[0]), low)
                total = mss[1] * decay(least - mss[0]) + msr[1] * decay(least - msr[0])
                total = total + part * decay(least - low)
                fb[...] = decay(least[:, :1] - mb[...])
                u = quotient(pv[...], total)

            with jax.named_scope("pass1"):
                u = passes(u, rescale=True, par=1)

            def sweep(t, u):
                return passes(u, par=lax.rem(t, 2))

            with jax.named_scope("sweeps"):
                u = lax.fori_loop(2, sweeps, sweep, u)
            ub[...] = u
            bacc[...] = jnp.zeros_like(bacc)
            with jax.named_scope("finish"):
                plan_chunk(0, tts[0], u)
                for n in range(KJ // CM):
                    if n + 1 < KJ // CM:
                        plan_chunk(n + 1, tts[(n + 1) % 2], u)
                    lead_and_cross(n, tts[n % 2])
                finish_lp()
            return carry

        lax.fori_loop(0, steps, outer, 0)

        pl.semaphore_wait(credit, NL)
        cost = costs()
        plan_own = (block(CS) * ub[...][None]) * vbuf[0][:, None]
        total = jnp.zeros((S, L), F32)
        for jt in range(JT):
            for t in range(NT):
                total = total + cost[jt * S : jt * S + S, t * L : t * L + L] * plan_own[jt, t]
        loss_rows[0:1] = jnp.sum(total, axis=0, keepdims=True)

        steps_on = [[moved(d, k) - me for k in range(dims[d])] for d in range(3)]
        offsets = sorted(itertools.product(*(range(n) for n in dims)), key=lambda o: -sum(min(k, 4 - k) for k in o))
        for o in offsets[:-1]:
            pltpu.make_async_remote_copy(
                src_ref=loss_rows.at[pl.ds(0, 1)], dst_ref=loss_rows.at[pl.ds(slot_of(o), 1)],
                send_sem=loss_sem.at[0], recv_sem=loss_sem.at[1],
                device_id=me + steps_on[0][o[0]] + steps_on[1][o[1]] + steps_on[2][o[2]], device_id_type=FLAT,
            ).start()

        it = lax.div(chip * NR, L)
        inside = pl.multiple_of(lax.rem(chip * NR, L), S)

        def rows_of(n, carry):
            for k in range(4):
                s = 4 * n + k
                kk = jnp.concatenate([kbuf[(CS + s) * TB + jt * NT + it] for jt in range(JT)], axis=0)
                uu = jnp.concatenate([ub[it]] * JT, axis=0)
                t = (kk * uu) * vbuf[s].reshape(JB, L)
                none = jnp.zeros_like(t)
                both = jnp.where(core == 0, jnp.concatenate([t, none], axis=0), jnp.concatenate([none, t], axis=0))
                trb[k] = both.T
                obuf[source_of(s)] = trb[k, pl.ds(inside, NR), :]
            return carry

        with jax.named_scope("tail"):
            lax.fori_loop(0, CH // 4, rows_of, 0)
            o_copy = to_partner(obuf.at[pl.ds(other * HB, HB)], orecv, o_sem.at[0], o_sem.at[1])
            o_copy.start()
            o_copy.wait()
            orecv[...] = obuf[pl.ds(core * HB, HB)] + orecv[...]
            o_out = pltpu.make_async_copy(orecv, out_ref, in_sem.at[1])
            o_out.start()
            ref = loss_rows.at[pl.ds(1, CH - 1)]
            pltpu.make_async_copy(ref, ref, loss_sem.at[0]).wait()
            pltpu.make_async_copy(ref, ref, loss_sem.at[1]).wait()
            loss_two[0:1] = jnp.sum(loss_rows[...], axis=0, keepdims=True)
            copy = to_partner(loss_two.at[pl.ds(0, 1)], loss_two.at[pl.ds(1, 1)], loss_sem.at[2], loss_sem.at[3])
            copy.start()
            copy.wait()
            loss_ref[0] = jnp.sum(loss_two[...])
            o_out.wait()

    vm = pltpu.VMEM
    dma = pltpu.SemaphoreType.DMA
    scratch = [
        vm((NP * TB, S, L), F32),
        vm((NP * TB, S, L), F32),
        vm((CH * TT0, 16, L), BF16),
        vm((CM, n_rows), BF16),
        vm((CM, n_rows), BF16),
        vm((n_rows, n_rows), F32),
        vm((n_rows, n_rows), BF16),
        vm((CH, L, L), BF16),
        vm((L, KJ), BF16),
        vm((L, n_rows), F32),
        vm((L, n_rows), F32),
        vm((JB, n_rows), F32),
        vm((L, L), F32),
        vm((CH, L), F32),
        vm((NP, JT, S, L), F32),
        vm((CH, JT, S, L), F32),
        vm((2, GS, JT, S, L), F32),
        vm((NT, NP, L), F32),
        vm((NT, NP, L), F32),
        vm((NT, NP, L), F32),
        vm((NT, S, L), F32),
        vm((S, L), F32),
        vm((2, NT, S, L), F32),
        vm((2, NT, S, L), F32),
        vm((2, NT, S, L), F32),
        vm((2, NT, S, L), F32),
        vm((NT, S, L), F32),
        vm((3, S, L), F32),
        vm((3, 3, S, L), F32),
        vm((S, L), F32),
        vm((S, L), F32),
        vm((CH, NR, L), F32),
        vm((HB, NR, L), F32),
        vm((4, L, L), F32),
        vm((CH, L), F32),
        vm((2, L), F32),
        vm((L, n_cols // 2), F32),
        dma((NL,)),
        dma((max(plan["waits"], plan0["waits"]),)),
        dma((1,)),
        dma((CS,)),
        pltpu.SemaphoreType.REGULAR,
        dma((2,)),
        dma((2,)),
        dma((2,)),
        dma((2,)),
        dma((2,)),
        dma((2,)),
        dma((2,)),
        dma((3, 3)),
        dma((3, 3)),
        dma((2,)),
        dma((2,)),
        dma((4,)),
        dma((2,)),
    ]
    return kernel, scratch


def solution(mesh):
    chips = mesh.shape["rows"]
    dims = torus_of(chips)
    grid_spec = P(("pairs", "rows"), "cols")

    def local_fn(c1, c2, t0, p, q, eps):
        n_rows, n_cols = p.shape[0] * chips, q.shape[0] * mesh.shape["cols"]
        kernel, scratch = make_kernel(dims, n_rows, n_cols, eps.shape[0], SWEEPS)
        vmem = pl.BlockSpec(memory_space=pltpu.VMEM)
        smem = pl.BlockSpec(memory_space=pltpu.SMEM)
        anywhere = pl.BlockSpec(memory_space=pl.ANY)
        plan, loss = pl.pallas_call(
            kernel,
            name="gromov",
            out_shape=(jax.ShapeDtypeStruct((chips // 2, t0.shape[0], L), F32), jax.ShapeDtypeStruct((1,), F32)),
            in_specs=[smem, smem, vmem, anywhere, vmem, vmem],
            out_specs=(anywhere, smem),
            scratch_shapes=scratch,
            compiler_params=pltpu.CompilerParams(
                collective_id=0, has_side_effects=True, vmem_limit_bytes=60 * 1024 * 1024
            ),
        )(eps, p, c1, c2, t0, q.reshape(chips // 2, L))
        return plan.transpose(1, 0, 2).reshape(t0.shape), loss

    return jax.shard_map(
        local_fn,
        mesh=mesh,
        in_specs=(grid_spec, grid_spec, grid_spec, P(("pairs", "rows")), P(("pairs", "cols")), P("pairs")),
        out_specs=(grid_spec, P("pairs")),
        check_vma=False,
    )
```

```python
import heapq
import itertools
import math

import jax
import jax.numpy as jnp
from jax import lax
from jax.experimental import pallas as pl
from jax.experimental.pallas import tpu as pltpu
from jax.sharding import PartitionSpec as P

SWEEPS = 10
FLAT = pl.DeviceIdType.LOGICAL
L, S = 128, 8
JB = 64
JT = JB // S
F32, BF16 = jnp.float32, jnp.bfloat16
ORDERS = ((0, 1, 2), (1, 2, 0), (2, 0, 1))
TILE_RATE = 11.4
HOP_US = 5.0
AHEAD_US = 3.0
LOG2E = 1.4426950216293335
LOG2E_REST = 1.925963e-8
PARTNER_US = 4.0
LATE = 100


def torus_of(chips):
    return {64: (4, 4, 4), S: (4, 2, 1), 16: (4, 4, 1)}[chips]


def halves(x):
    c = 4097.0 * x
    high = c - (c - x)
    return high, x - high


def quotient(a, b):
    q = a / b
    return q + (a - q * b) / b


def split3(n):
    cuts = [0, (n + 2) // 3, (2 * n + 2) // 3, n]
    return [(cuts[k], cuts[k + 1]) for k in range(3)]


def tree_plan(dims, tiles, rate, lat_us, ahead_us, shared=0):
    rings = {1: (), 2: ((1, "f", 1),), 4: ((1, "f", 1), (3, "f", -1), (2, "a", 1), (2, "b", -1))}
    msgs = []
    for color, order in enumerate(ORDERS):
        lo, hi = split3(tiles)[color]
        for dst in itertools.product(*(range(n) for n in dims)):
            used = [k for k in range(3) if dst[order[k]]]
            if not used or lo == hi:
                continue
            d = order[used[-1]]
            mid = lo + (hi - lo + (sum(dst) + color) % 2) // 2
            for at, part, sign in rings[dims[d]]:
                a, b = {"f": (lo, hi), "a": (lo, mid), "b": (mid, hi)}[part]
                if at != dst[d] or a == b:
                    continue
                src = list(dst)
                src[d] = (src[d] - sign) % dims[d]
                m = dict(id=len(msgs), color=color, src=tuple(src), dst=dst, link=(d, sign), lo=a, hi=b)
                m["us"] = (b - a) / rate
                msgs.append(m)
    into = {}
    for m in msgs:
        into.setdefault((m["color"], m["dst"]), []).append(m)
    users = [[] for _ in msgs]
    missing = []
    for m in msgs:
        deps = [e for e in into.get((m["color"], m["src"]), []) if e["lo"] < m["hi"] and m["lo"] < e["hi"]]
        missing.append(len(deps))
        for e in deps:
            users[e["id"]].append(m)
    sems, waiting = {}, {}
    for m in msgs:
        key = (m["color"] if users[m["id"]] else None, m["dst"])
        m["sem"] = sems.setdefault(key, len(sems))
        waiting.setdefault(m["sem"], []).append(m)
    pending = {k: len(group) for k, group in waiting.items()}
    way = {}

    def way_of(m):
        if m["id"] not in way:
            way[m["id"]] = m["us"] + lat_us + max([way_of(u) for u in users[m["id"]]], default=0.0)
        return way[m["id"]]

    links = sorted({m["link"] for m in msgs})
    queue = {k: [] for k in links}
    idle = dict.fromkeys(links, True)
    ready, events, ops = {}, [], []

    def put(m, now):
        ready[m["id"]] = now
        heapq.heappush(queue[m["link"]], (-way_of(m), m["id"]))

    def start(link, now):
        if idle[link] and queue[link]:
            k = heapq.heappop(queue[link])[1]
            idle[link] = False
            ops.append((max(ready[k], now - ahead_us), 1, "send", msgs[k]))
            heapq.heappush(events, (now + msgs[k]["us"], 0, k))
            heapq.heappush(events, (now + msgs[k]["us"] + lat_us, 1, k))

    for m in msgs:
        if not missing[m["id"]]:
            put(m, 0.0)
    for link in links:
        start(link, 0.0)
    left = {}
    for m in msgs:
        left[m["dst"]] = left.get(m["dst"], 0) + 1
    now = 0.0
    while events:
        now, arrived, k = heapq.heappop(events)
        m = msgs[k]
        if not arrived:
            idle[m["link"]] = True
            start(m["link"], now)
            continue
        pending[m["sem"]] -= 1
        if not pending[m["sem"]]:
            ops.append((now, 0, "wait", waiting[m["sem"]]))
        for u in users[k]:
            missing[u["id"]] -= 1
            if not missing[u["id"]]:
                put(u, now)
                start(u["link"], now)
        left[m["dst"]] -= 1
        if not left[m["dst"]]:
            slot = m["dst"][0] + dims[0] * (m["dst"][1] + dims[1] * m["dst"][2])
            ops.append((now, 0, "slot", slot))
            if slot < shared:
                ops.append((now + PARTNER_US, 0, "partner", slot))
    ops.sort(key=lambda op: op[:2])
    totals = {k: sum(m["hi"] - m["lo"] for m in msgs if m["link"] == k) for k in links}
    return dict(waits=len(sems), ops=[op[2:] for op in ops], links=links, totals=totals, end=now)


def make_kernel(dims, n_rows, n_cols, steps, sweeps):
    X, Y, Z = dims
    CH = X * Y * Z
    NR = n_rows // CH
    G = NR // S
    NT = n_rows // L
    TB = JT * NT
    HB = CH // 2
    JN = n_cols // 2 // L
    JW = JN // 2
    NT0 = G * JW
    TT0 = NT0 + 2 * G
    KJ = CH * JB
    CK = min(1024, KJ)
    CM = min(1024, KJ)
    GS = min(4, CH // 2)
    CS = max(CH * 3 // 8 // GS * GS, GS)
    NP = CH + CS
    NE, NC = (CH - CS) // GS, 2 * CS // GS
    GC = CM // JB // GS
    assert NT == 4 and n_cols == CH * L and JN == HB
    plan0 = tree_plan(dims, TT0, TILE_RATE, HOP_US - 2, AHEAD_US - 1)
    plan = tree_plan(dims, TB, TILE_RATE, HOP_US, AHEAD_US, CS)
    links = plan["links"]
    NL = len(links)
    peers = [(d, k) for d in range(3) for k in range(1, dims[d])]
    strides = (1, X, X * Y)

    def slot_of(offset):
        return offset[0] + X * offset[1] + X * Y * offset[2]

    def kernel(
        eps_ref, p_ref, c1_ref, c2_ref, t0_ref, q_ref,
        out_ref, loss_ref,
        land, kbuf, g0, tt0, tt1, c1f, c1b, c2n, c2p, bacc, lp, lprecv, bp, qf, qrep, vbuf, cbuf,
        mb, sb, fb, ub, ap, xs, xr, mss, msr, pv, ars, arr, arps, arpr, obuf, orecv, trb, loss_rows, loss_two, c2v,
        send_sem, recv_sem, fwd_ssem, fwd_rsem, credit, x_ssem, x_rsem, ms_sem, lp_sem, c1_sem, c2_sem, q_sem, ar_ssem, ar_rsem, arp_sem, o_sem, loss_sem, in_sem,
    ):
        tts = (tt0, tt1)
        chip = lax.axis_index("rows")
        core = lax.axis_index("cols")
        other = 1 - core
        pos = (lax.rem(chip, X), lax.rem(lax.div(chip, X), Y), lax.div(chip, X * Y))

        me = core * CH + chip
        partner = other * CH + chip

        def moved(d, k):
            return me + (lax.rem(pos[d] + k + dims[d], dims[d]) - pos[d]) * strides[d]

        near = {link: moved(*link) for link in links}

        def source_of(slot):
            off = (lax.rem(slot, X), lax.rem(lax.div(slot, X), Y), lax.div(slot, X * Y))
            at = [lax.rem(pos[d] + dims[d] - off[d], dims[d]) for d in range(3)]
            return at[0] + X * at[1] + X * Y * at[2]

        def to_partner(src, dst, ssem, rsem):
            return pltpu.make_async_remote_copy(
                src_ref=src, dst_ref=dst, send_sem=ssem, recv_sem=rsem,
                device_id=partner, device_id_type=FLAT,
            )

        def tree_copy(buf, width, first, m):
            n = m["hi"] - m["lo"]
            return pltpu.make_async_remote_copy(
                src_ref=buf.at[pl.ds((first + slot_of(m["src"])) * width + m["lo"], n)],
                dst_ref=buf.at[pl.ds((first + slot_of(m["dst"])) * width + m["lo"], n)],
                send_sem=send_sem.at[links.index(m["link"])],
                recv_sem=recv_sem.at[m["sem"]],
                device_id=near[m["link"]],
                device_id_type=FLAT,
            )

        def tree(buf, width, first, the_plan, before_send=None, on_slot=None, fillers=()):
            fillers, ready, waits = list(fillers), [], 0
            for op, m in the_plan["ops"]:
                if op == "send":
                    if before_send is not None:
                        before_send(m)
                    tree_copy(buf, width, first, m).start()
                elif op == "wait":
                    while fillers and not fillers[0][0]:
                        fillers.pop(0)[1]()
                    if not ready and fillers and waits >= fillers[0][0]:
                        fillers.pop(0)[1]()
                    while ready:
                        on_slot(*ready.pop(0))
                    n = sum(e["hi"] - e["lo"] for e in m)
                    ref = buf.at[pl.ds((first + slot_of(m[0]["dst"])) * width, n)]
                    pltpu.make_async_copy(ref, ref, recv_sem.at[m[0]["sem"]]).wait()
                    waits += 1
                elif on_slot is not None:
                    ready.append((op, m))
            for at in ready:
                on_slot(*at)
            for _, f in fillers:
                f()

        def tree_sent(buf, the_plan):
            for k, link in enumerate(links):
                n = the_plan["totals"][link]
                ref = buf.at[pl.ds(0, n)]
                pltpu.make_async_copy(ref, ref, send_sem.at[k]).wait()

        def give_credit():
            for d, sign in links:
                pl.semaphore_signal(credit, inc=1, device_id=moved(d, -sign), device_id_type=FLAT)

        def all_sum_send(stage):
            for n, k in enumerate(range(1, dims[stage])):
                pltpu.make_async_remote_copy(
                    src_ref=ars.at[stage], dst_ref=arr.at[stage, n],
                    send_sem=ar_ssem.at[stage, n], recv_sem=ar_rsem.at[stage, n],
                    device_id=moved(stage, k), device_id_type=FLAT,
                ).start()

        def all_sum_get(stage):
            total = ars[stage]
            for n, k in enumerate(range(1, dims[stage])):
                pltpu.make_async_remote_copy(
                    src_ref=ars.at[stage], dst_ref=arr.at[stage, n],
                    send_sem=ar_ssem.at[stage, n], recv_sem=ar_rsem.at[stage, n],
                    device_id=moved(stage, k), device_id_type=FLAT,
                ).wait()
                total = total + arr[stage, n]
            return total

        def all_sum_step(stage):
            total = all_sum_get(stage)
            if stage < 2:
                ars[stage + 1] = total
                all_sum_send(stage + 1)
            else:
                arps[...] = total
                to_partner(arps, arpr, arp_sem.at[0], arp_sem.at[1]).start()

        c2_in = pltpu.make_async_copy(c2_ref, c2v, in_sem.at[0])
        c2_in.start()
        barrier = pltpu.get_barrier_semaphore()
        for d, k in peers:
            pl.semaphore_signal(barrier, inc=1, device_id=moved(d, k), device_id_type=FLAT)
        pl.semaphore_signal(barrier, inc=1, device_id=partner, device_id_type=FLAT)

        row = lax.broadcasted_iota(jnp.int32, (S, L), 0)
        lane = lax.broadcasted_iota(jnp.int32, (S, L), 1)

        for g in range(G):
            rows = slice(g * S, g * S + S)
            pair = jnp.concatenate([c1_ref[rows, :L], c1_ref[rows, L:]], axis=0)
            g0[NT0 + core * G + g] = pair.astype(BF16)
        c1_copy = to_partner(
            g0.at[pl.ds(NT0 + core * G, G)], g0.at[pl.ds(NT0 + core * G, G)], c1_sem.at[0], c1_sem.at[1]
        )
        q_copy = to_partner(q_ref, qf.at[pl.ds(core * HB, HB)], q_sem.at[0], q_sem.at[1])

        tile = jnp.zeros((S, L), F32)
        for t in range(2):
            part = jnp.zeros((1, L), F32)
            for k in range(NR):
                entry = c1_ref[k : k + 1, t * L : t * L + L]
                part = part + entry * entry * p_ref[k]
            tile = jnp.where(row == 2 * core + t, jnp.broadcast_to(part, (S, L)), tile)
        where = (row - 4) * L + lane
        for k in range(NR):
            tile = jnp.where(where == chip * NR + k, p_ref[k], tile)
        ars[0] = tile
        for g in range(G):
            rows = slice(g * S, g * S + S)
            for t in range(JW):
                a, b = t0_ref[rows, (2 * L) * t : (2 * L) * t + L], t0_ref[rows, (2 * L) * t + L : (2 * L) * t + (2 * L)]
                g0[g * JW + t] = jnp.concatenate([a, b], axis=0).astype(BF16)
        qf[pl.ds(core * HB, HB)] = q_ref[...]

        c2_copy = to_partner(c2n.at[pl.ds(core * HB, HB)], c2n.at[pl.ds(core * HB, HB)], c2_sem.at[0], c2_sem.at[1])
        bp[...] = jnp.zeros_like(bp)

        def round_c2(first, last):
            c2_in.wait()
            for t in range(first, last):
                blk = c2v[:, t * L : t * L + L]
                c2n[core * HB + t] = blk.astype(BF16)
                bp[...] += blk * blk * q_ref[t : t + 1, :]

        def finish_b():
            bp[...] = jnp.broadcast_to(jnp.sum(bp[...], axis=1, keepdims=True), (L, L))

        with jax.named_scope("barrier"):
            pl.semaphore_wait(barrier, len(peers) + 1)
        give_credit()
        c1_copy.start()
        q_copy.start()
        all_sum_send(0)

        src = lax.broadcasted_iota(jnp.int32, (L, L), 0)
        dst = lax.broadcasted_iota(jnp.int32, (L, L), 1)
        picks = [
            jnp.where((src - core * JB == dst - h * JB) & (dst >= h * JB) & (dst < h * JB + JB), 1.0, 0.0).astype(BF16)
            for h in range(2)
        ]

        def order_c2(first, last):
            for t in range(first, last):
                a = jnp.dot(c2n[source_of(2 * t)], picks[0], preferred_element_type=F32)
                b = jnp.dot(c2n[source_of(2 * t + 1)], picks[1], preferred_element_type=F32)
                c2p[:, t * L : t * L + L] = (a + b).astype(BF16)

        def order_q(first, last):
            def four(n, carry):
                for k in range(4):
                    p = 4 * n + k
                    shared = p < CS
                    half = jnp.where(shared, other, core)
                    line = jnp.broadcast_to(qf[pl.ds(source_of(jnp.where(shared, p, p - CS)), 1), :], (S, L))
                    for jt in range(JT):
                        own = jnp.where(lane == half * JB + jt * S + row, line, 0.0)
                        qrep[p, jt] = jnp.broadcast_to(jnp.sum(own, axis=1, keepdims=True), (S, L))
                return carry

            lax.fori_loop(first // 4, last // 4, four, 0)

        def span(n, parts, f):
            cuts = [n * k // parts for k in range(parts + 1)]
            return [lambda a=a, b=b: f(a, b) for a, b in zip(cuts, cuts[1:])]

        fillers = [(0, lambda: round_c2(0, HB)), (0, finish_b), (0, lambda: c2_copy.start())]
        fillers += [(0, lambda: q_copy.wait()), (0, lambda: order_q(0, NP)), (LATE // 2, lambda: all_sum_step(0))]
        fillers += [(LATE, lambda: all_sum_step(1))]
        waited = []

        def before_send(m):
            if not waited and m["hi"] > NT0:
                waited.append(1)
                c1_copy.wait()

        def unpack(op, s):
            chip_s = source_of(s)
            for g in range(G):
                tiles = g0[s * TT0 + g * JW : s * TT0 + g * JW + JW].astype(F32).reshape(JN, S, L)
                kbuf[pl.ds((chip_s * G + g) * JN, JN)] = tiles
                at = pl.ds(pl.multiple_of(chip_s * NR + g * S, S), S)
                for h in range(2):
                    pair = g0[s * TT0 + NT0 + h * G + g].astype(F32)
                    c1f[at, 2 * L * h : 2 * L * h + L] = pair[:S]
                    c1f[at, 2 * L * h + L : 2 * L * h + 2 * L] = pair[S:]

        with jax.named_scope("gather0"):
            first = [(0, lambda: unpack("slot", 0))]
            tree(g0, TT0, 0, plan0, before_send=before_send, on_slot=unpack, fillers=first + fillers)
            tree_sent(g0, plan0)
            c1b[...] = c1f[...].astype(BF16)
            all_sum_step(2)

        def finish_lp():
            lp[...] = jnp.concatenate([bp[...]] * NT, axis=1) - 2.0 * bacc[...]

        bacc[...] = jnp.zeros_like(bacc)
        JC = CK // L

        def first_chunk(n, carry):
            cols = []
            for t in range(JC):
                cols.append(kbuf[pl.ds(n * JC + t, CH * G, stride=JN)].reshape(n_rows, L))
            plan_c = jnp.concatenate(cols, axis=1).astype(BF16)
            lead = jnp.dot(c1b[...], plan_c, preferred_element_type=F32).astype(BF16)
            c2c = jnp.concatenate([c2n[core * HB + n * JC + t] for t in range(JC)], axis=1)
            bacc[...] += lax.dot_general(c2c, lead, (((1,), (1,)), ((), ())), preferred_element_type=F32)
            return carry

        with jax.named_scope("firstmm"):
            lax.fori_loop(0, KJ // CK, first_chunk, 0)
            finish_lp()
        to_partner(arps, arpr, arp_sem.at[0], arp_sem.at[1]).wait()
        ap[...] = jnp.where(row < 4, arps[...] + arpr[...], arps[...])
        for t in range(NT):
            pv[t] = jnp.broadcast_to(ap[4 + t : 5 + t, :], (S, L))


        def lead_and_cross(n, plan_c):
            lead = jnp.dot(plan_c[...], c1b[...], preferred_element_type=F32).astype(BF16)
            bacc[...] += jnp.dot(c2p[:, n * CM : n * CM + CM], lead, preferred_element_type=F32)

        def costs():
            copy = to_partner(lp.at[pl.ds(other * JB, JB)], lprecv, lp_sem.at[0], lp_sem.at[1])
            copy.start()
            copy.wait()
            own = lp[pl.ds(pl.multiple_of(core * JB, JB), JB), :] + lprecv[...]
            return own + jnp.concatenate([ap[t : t + 1, :] for t in range(NT)], axis=1)

        def block(s):
            return kbuf[pl.ds(s * TB, TB)].reshape(JT, NT, S, L)

        def weighted(kk, u):
            w = (kk[:, 0] * u[0] + kk[:, 1] * u[1]) + (kk[:, 2] * u[2] + kk[:, 3] * u[3])
            return jnp.sum(w, axis=2, keepdims=True)

        def passes(u, rescale=False, par=0):
            def place(g):
                return g * GS + 2 * CS if not isinstance(g, int) or g < NE else (g - NE) * GS

            def one(at, buf):
                for k in range(GS):
                    p = at + k
                    kk = block(p)
                    if rescale:
                        kk = kk * fb[:, pl.ds(p, 1), :][None]
                        kbuf[pl.ds(p * TB, TB)] = kk.reshape(TB, S, L)
                    cbuf[buf, k] = qrep[p] / jnp.broadcast_to(weighted(kk, u), (JT, S, L))

            def two(at, buf, acc):
                for k in range(GS):
                    p = at + k
                    acc = acc + jnp.sum(block(p) * cbuf[buf, k][:, None], axis=0)
                return acc

            def run(a, b, end):
                shift = place(a) - a * GS
                even, odd = a % 2, (a + 1) % 2
                pairs = max(0, (b - a - 1) // 2)

                def both(n, acc):
                    at = (a + 2 * n) * GS + shift
                    one(at + GS, odd)
                    acc = two(at, even, acc)
                    one(at + 2 * GS, even)
                    return two(at + GS, odd, acc)

                acc = lax.fori_loop(0, pairs, both, jnp.zeros((NT, S, L), F32))
                for g in range(a + 2 * pairs, b):
                    if g + 1 < end:
                        one(place(g + 1), (g + 1) % 2)
                    acc = two(place(g), g % 2, acc)
                return acc

            one(place(0), 0)
            xs[par] = run(0, NE, NE + NC)
            copy = to_partner(xs.at[par], xr.at[par], x_ssem.at[par], x_rsem.at[par])
            copy.start()
            acc = run(NE, NE + NC, NE + NC)
            copy.wait()
            total = jnp.sum((xs[par] + xr[par]) + acc, axis=1, keepdims=True)
            return quotient(pv[...], jnp.broadcast_to(total, (NT, S, L)))

        def plan_chunk(n, dst, u):
            def one(g):
                for k in range(GS):
                    p = CS + (n * GC + g) * GS + k
                    cbuf[g % 2, k] = quotient(qrep[p], jnp.broadcast_to(weighted(block(p), u), (JT, S, L)))

            one(0)
            for g in range(GC):
                if g + 1 < GC:
                    one(g + 1)
                for k in range(GS):
                    s = (n * GC + g) * GS + k
                    v = cbuf[g % 2, k]
                    vbuf[s] = v
                    t = (block(CS + s) * u[None]) * v[:, None]
                    flat = jnp.concatenate([t[:, i].reshape(JB, L) for i in range(NT)], axis=1)
                    at = (g * GS + k) * JB
                    dst[at : at + JB, :] = flat.astype(BF16)

        def outer(r, carry):
            eps = eps_ref[r]
            inv = 1.0 / eps
            inv = inv * (2.0 - eps * inv)
            main = LOG2E * inv
            (e0, e1), (m0, m1) = halves(eps), halves(main)
            prod = eps * main
            low_part = ((e0 * m0 - prod) + (e0 * m1 + e1 * m0)) + e1 * m1
            rest = (((LOG2E - prod) - low_part) + LOG2E_REST) * inv

            def decay(x):
                return jnp.exp2(x * main + x * rest)

            cost = costs()
            for jt in range(JT):
                for t in range(NT):
                    land[CS * TB + jt * NT + t] = cost[jt * S : jt * S + S, t * L : t * L + L]

            def exps(p):
                ll = land[p * TB : p * TB + TB].reshape(JT, NT, S, L)
                low = jnp.min(jnp.min(ll, axis=0), axis=1, keepdims=True)
                kk = decay(low[None] - ll)
                kbuf[p * TB : p * TB + TB] = kk.reshape(TB, S, L)
                mb[:, p : p + 1, :] = low
                sb[:, p : p + 1, :] = jnp.sum(jnp.sum(kk, axis=0), axis=1, keepdims=True)

            def passed_on(s):
                return to_partner(
                    land.at[pl.ds((CS + s) * TB, TB)], land.at[pl.ds(s * TB, TB)], fwd_ssem.at[0], fwd_rsem.at[s]
                )

            def on_slot(op, s):
                if op == "slot":
                    if s < CS:
                        passed_on(s).start()
                    exps(CS + s)
                else:
                    passed_on(s).wait_recv()
                    exps(s)

            def once(n, f):
                @pl.when(r == 0)
                def _():
                    if not n:
                        c2_copy.wait()
                    f()

            with jax.named_scope("gather"):
                pl.semaphore_wait(credit, NL)
                first = [(0, lambda: on_slot("slot", 0)), (plan["waits"] // 4, lambda: on_slot("partner", 0))]
                for n, f in enumerate(span(CH // 2, S, order_c2)):
                    first.append((LATE // 2 + 2 * n, lambda n=n, f=f: once(n, f)))
                tree(land, TB, CS, plan, on_slot=on_slot, fillers=first)
                tree_sent(land, plan)
                ref = land.at[pl.ds(0, CS * TB)]
                pltpu.make_async_copy(ref, ref, fwd_ssem.at[0]).wait()
                give_credit()

            with jax.named_scope("minx"):
                def least_of(a, b):
                    low = jnp.min(mb[:, a:b], axis=1, keepdims=True)
                    part = jnp.sum(sb[:, a:b] * decay(low - mb[:, a:b]), axis=1, keepdims=True)
                    return jnp.broadcast_to(low, (NT, S, L)), jnp.broadcast_to(part, (NT, S, L))

                mss[0], mss[1] = least_of(2 * CS, NP)
                copy = to_partner(mss, msr, ms_sem.at[0], ms_sem.at[1])
                copy.start()
                low, part = least_of(0, 2 * CS)
                copy.wait()
                least = jnp.minimum(jnp.minimum(mss[0], msr[0]), low)
                total = mss[1] * decay(least - mss[0]) + msr[1] * decay(least - msr[0])
                total = total + part * decay(least - low)
                fb[...] = decay(least[:, :1] - mb[...])
                u = quotient(pv[...], total)

            with jax.named_scope("pass1"):
                u = passes(u, rescale=True, par=1)

            def sweep(t, u):
                return passes(u, par=lax.rem(t, 2))

            with jax.named_scope("sweeps"):
                u = lax.fori_loop(2, sweeps, sweep, u)
            ub[...] = u
            bacc[...] = jnp.zeros_like(bacc)
            with jax.named_scope("finish"):
                plan_chunk(0, tts[0], u)
                for n in range(KJ // CM):
                    if n + 1 < KJ // CM:
                        plan_chunk(n + 1, tts[(n + 1) % 2], u)
                    lead_and_cross(n, tts[n % 2])
                finish_lp()
            return carry

        lax.fori_loop(0, steps, outer, 0)

        pl.semaphore_wait(credit, NL)
        u = ub[...]
        v = (vbuf[0], quotient(qrep[0], jnp.broadcast_to(weighted(block(0), u), (JT, S, L))))
        total = jnp.zeros((S, L), F32)
        for own, (p, half) in enumerate(((CS, core), (0, other))):
            plan_b = (block(p) * u[None]) * v[own][:, None]
            part = lp[pl.ds(pl.multiple_of(half * JB, JB), JB), :]
            for jt in range(JT):
                for t in range(NT):
                    cost = part[jt * S : jt * S + S, t * L : t * L + L]
                    total = total + (cost if own else cost + ap[t : t + 1, :]) * plan_b[jt, t]
        loss_rows[0:1] = jnp.sum(total, axis=0, keepdims=True)

        steps_on = [[moved(d, k) - me for k in range(dims[d])] for d in range(3)]
        offsets = sorted(itertools.product(*(range(n) for n in dims)), key=lambda o: -sum(min(k, 4 - k) for k in o))
        for o in offsets[:-1]:
            pltpu.make_async_remote_copy(
                src_ref=loss_rows.at[pl.ds(0, 1)], dst_ref=loss_rows.at[pl.ds(slot_of(o), 1)],
                send_sem=loss_sem.at[0], recv_sem=loss_sem.at[1],
                device_id=me + steps_on[0][o[0]] + steps_on[1][o[1]] + steps_on[2][o[2]], device_id_type=FLAT,
            ).start()

        it = lax.div(chip * NR, L)
        inside = pl.multiple_of(lax.rem(chip * NR, L), S)

        def rows_of(n, carry):
            for k in range(4):
                s = 4 * n + k
                kk = jnp.concatenate([kbuf[(CS + s) * TB + jt * NT + it] for jt in range(JT)], axis=0)
                uu = jnp.concatenate([ub[it]] * JT, axis=0)
                t = (kk * uu) * vbuf[s].reshape(JB, L)
                none = jnp.zeros_like(t)
                both = jnp.where(core == 0, jnp.concatenate([t, none], axis=0), jnp.concatenate([none, t], axis=0))
                trb[k] = both.T
                obuf[source_of(s)] = trb[k, pl.ds(inside, NR), :]
            return carry

        with jax.named_scope("tail"):
            lax.fori_loop(0, CH // 4, rows_of, 0)
            o_copy = to_partner(obuf.at[pl.ds(other * HB, HB)], orecv, o_sem.at[0], o_sem.at[1])
            o_copy.start()
            o_copy.wait()
            orecv[...] = obuf[pl.ds(core * HB, HB)] + orecv[...]
            o_out = pltpu.make_async_copy(orecv, out_ref, in_sem.at[1])
            o_out.start()
            ref = loss_rows.at[pl.ds(1, CH - 1)]
            pltpu.make_async_copy(ref, ref, loss_sem.at[0]).wait()
            pltpu.make_async_copy(ref, ref, loss_sem.at[1]).wait()
            loss_two[0:1] = jnp.sum(loss_rows[...], axis=0, keepdims=True)
            copy = to_partner(loss_two.at[pl.ds(0, 1)], loss_two.at[pl.ds(1, 1)], loss_sem.at[2], loss_sem.at[3])
            copy.start()
            copy.wait()
            loss_ref[0] = jnp.sum(loss_two[...])
            o_out.wait()

    vm = pltpu.VMEM
    dma = pltpu.SemaphoreType.DMA
    scratch = [
        vm((NP * TB, S, L), F32),
        vm((NP * TB, S, L), F32),
        vm((CH * TT0, 16, L), BF16),
        vm((CM, n_rows), BF16),
        vm((CM, n_rows), BF16),
        vm((n_rows, n_rows), F32),
        vm((n_rows, n_rows), BF16),
        vm((CH, L, L), BF16),
        vm((L, KJ), BF16),
        vm((L, n_rows), F32),
        vm((L, n_rows), F32),
        vm((JB, n_rows), F32),
        vm((L, L), F32),
        vm((CH, L), F32),
        vm((NP, JT, S, L), F32),
        vm((CH, JT, S, L), F32),
        vm((2, GS, JT, S, L), F32),
        vm((NT, NP, L), F32),
        vm((NT, NP, L), F32),
        vm((NT, NP, L), F32),
        vm((NT, S, L), F32),
        vm((S, L), F32),
        vm((2, NT, S, L), F32),
        vm((2, NT, S, L), F32),
        vm((2, NT, S, L), F32),
        vm((2, NT, S, L), F32),
        vm((NT, S, L), F32),
        vm((3, S, L), F32),
        vm((3, 3, S, L), F32),
        vm((S, L), F32),
        vm((S, L), F32),
        vm((CH, NR, L), F32),
        vm((HB, NR, L), F32),
        vm((4, L, L), F32),
        vm((CH, L), F32),
        vm((2, L), F32),
        vm((L, n_cols // 2), F32),
        dma((NL,)),
        dma((max(plan["waits"], plan0["waits"]),)),
        dma((1,)),
        dma((CS,)),
        pltpu.SemaphoreType.REGULAR,
        dma((2,)),
        dma((2,)),
        dma((2,)),
        dma((2,)),
        dma((2,)),
        dma((2,)),
        dma((2,)),
        dma((3, 3)),
        dma((3, 3)),
        dma((2,)),
        dma((2,)),
        dma((4,)),
        dma((2,)),
    ]
    return kernel, scratch


def solution(mesh):
    chips = mesh.shape["rows"]
    dims = torus_of(chips)
    grid_spec = P(("pairs", "rows"), "cols")

    def local_fn(c1, c2, t0, p, q, eps):
        n_rows, n_cols = p.shape[0] * chips, q.shape[0] * mesh.shape["cols"]
        kernel, scratch = make_kernel(dims, n_rows, n_cols, eps.shape[0], SWEEPS)
        vmem = pl.BlockSpec(memory_space=pltpu.VMEM)
        smem = pl.BlockSpec(memory_space=pltpu.SMEM)
        anywhere = pl.BlockSpec(memory_space=pl.ANY)
        plan, loss = pl.pallas_call(
            kernel,
            name="gromov",
            out_shape=(jax.ShapeDtypeStruct((chips // 2, t0.shape[0], L), F32), jax.ShapeDtypeStruct((1,), F32)),
            in_specs=[smem, smem, vmem, anywhere, vmem, vmem],
            out_specs=(anywhere, smem),
            scratch_shapes=scratch,
            compiler_params=pltpu.CompilerParams(
                collective_id=0, has_side_effects=True, vmem_limit_bytes=60 * 1024 * 1024
            ),
        )(eps, p, c1, c2, t0, q.reshape(chips // 2, L))
        return plan.transpose(1, 0, 2).reshape(t0.shape), loss

    return jax.shard_map(
        local_fn,
        mesh=mesh,
        in_specs=(grid_spec, grid_spec, grid_spec, P(("pairs", "rows")), P(("pairs", "cols")), P("pairs")),
        out_specs=(grid_spec, P("pairs")),
        check_vma=False,
    )
```

```python
import heapq
import itertools
import math

import jax
import jax.numpy as jnp
from jax import lax
from jax.experimental import pallas as pl
from jax.experimental.pallas import tpu as pltpu
from jax.sharding import PartitionSpec as P

SWEEPS = 10
FLAT = pl.DeviceIdType.LOGICAL
L, S = 128, 8
JB = 64
JT = JB // S
F32, BF16 = jnp.float32, jnp.bfloat16
ORDERS = ((0, 1, 2), (1, 2, 0), (2, 0, 1))
TILE_RATE = 11.4
HOP_US = 5.0
AHEAD_US = 2.0
LOG2E = 1.4426950216293335
LOG2E_REST = 1.925963e-8
PARTNER_US = 4.0
LATE = 100


def torus_of(chips):
    return {64: (4, 4, 4), S: (4, 2, 1), 16: (4, 4, 1)}[chips]


def halves(x):
    c = 4097.0 * x
    high = c - (c - x)
    return high, x - high


def quotient(a, b):
    q = a / b
    return q + (a - q * b) / b


def split3(n):
    cuts = [0, (n + 2) // 3, (2 * n + 2) // 3, n]
    return [(cuts[k], cuts[k + 1]) for k in range(3)]


def tree_plan(dims, tiles, rate, lat_us, ahead_us, shared=0):
    rings = {1: (), 2: ((1, "f", 1),), 4: ((1, "f", 1), (3, "f", -1), (2, "a", 1), (2, "b", -1))}
    msgs = []
    for color, order in enumerate(ORDERS):
        lo, hi = split3(tiles)[color]
        for dst in itertools.product(*(range(n) for n in dims)):
            used = [k for k in range(3) if dst[order[k]]]
            if not used or lo == hi:
                continue
            d = order[used[-1]]
            mid = lo + (hi - lo + (sum(dst) + color) % 2) // 2
            for at, part, sign in rings[dims[d]]:
                a, b = {"f": (lo, hi), "a": (lo, mid), "b": (mid, hi)}[part]
                if at != dst[d] or a == b:
                    continue
                src = list(dst)
                src[d] = (src[d] - sign) % dims[d]
                m = dict(id=len(msgs), color=color, src=tuple(src), dst=dst, link=(d, sign), lo=a, hi=b)
                m["us"] = (b - a) / rate
                msgs.append(m)
    into = {}
    for m in msgs:
        into.setdefault((m["color"], m["dst"]), []).append(m)
    users = [[] for _ in msgs]
    missing = []
    for m in msgs:
        deps = [e for e in into.get((m["color"], m["src"]), []) if e["lo"] < m["hi"] and m["lo"] < e["hi"]]
        missing.append(len(deps))
        for e in deps:
            users[e["id"]].append(m)
    sems, waiting = {}, {}
    for m in msgs:
        key = (m["color"] if users[m["id"]] else None, m["dst"])
        m["sem"] = sems.setdefault(key, len(sems))
        waiting.setdefault(m["sem"], []).append(m)
    pending = {k: len(group) for k, group in waiting.items()}
    way = {}

    def way_of(m):
        if m["id"] not in way:
            way[m["id"]] = m["us"] + lat_us + max([way_of(u) for u in users[m["id"]]], default=0.0)
        return way[m["id"]]

    links = sorted({m["link"] for m in msgs})
    queue = {k: [] for k in links}
    idle = dict.fromkeys(links, True)
    ready, events, ops = {}, [], []

    def put(m, now):
        ready[m["id"]] = now
        heapq.heappush(queue[m["link"]], (-way_of(m), m["id"]))

    def start(link, now):
        if idle[link] and queue[link]:
            k = heapq.heappop(queue[link])[1]
            idle[link] = False
            ops.append((max(ready[k], now - ahead_us), 1, "send", msgs[k]))
            heapq.heappush(events, (now + msgs[k]["us"], 0, k))
            heapq.heappush(events, (now + msgs[k]["us"] + lat_us, 1, k))

    for m in msgs:
        if not missing[m["id"]]:
            put(m, 0.0)
    for link in links:
        start(link, 0.0)
    left = {}
    for m in msgs:
        left[m["dst"]] = left.get(m["dst"], 0) + 1
    now = 0.0
    while events:
        now, arrived, k = heapq.heappop(events)
        m = msgs[k]
        if not arrived:
            idle[m["link"]] = True
            start(m["link"], now)
            continue
        pending[m["sem"]] -= 1
        if not pending[m["sem"]]:
            ops.append((now, 0, "wait", waiting[m["sem"]]))
        for u in users[k]:
            missing[u["id"]] -= 1
            if not missing[u["id"]]:
                put(u, now)
                start(u["link"], now)
        left[m["dst"]] -= 1
        if not left[m["dst"]]:
            slot = m["dst"][0] + dims[0] * (m["dst"][1] + dims[1] * m["dst"][2])
            ops.append((now, 0, "slot", slot))
            if slot < shared:
                ops.append((now + PARTNER_US, 0, "partner", slot))
    ops.sort(key=lambda op: op[:2])
    totals = {k: sum(m["hi"] - m["lo"] for m in msgs if m["link"] == k) for k in links}
    return dict(waits=len(sems), ops=[op[2:] for op in ops], links=links, totals=totals, end=now)


def make_kernel(dims, n_rows, n_cols, steps, sweeps):
    X, Y, Z = dims
    CH = X * Y * Z
    NR = n_rows // CH
    G = NR // S
    NT = n_rows // L
    TB = JT * NT
    HB = CH // 2
    JN = n_cols // 2 // L
    JW = JN // 2
    NT0 = G * JW
    TT0 = NT0 + 2 * G
    KJ = CH * JB
    CK = min(1024, KJ)
    CM = min(1024, KJ)
    GS = min(4, CH // 2)
    CS = max(CH * 3 // 8 // GS * GS, GS)
    NP = CH + CS
    NE, NC = (CH - CS) // GS, 2 * CS // GS
    GC = CM // JB // GS
    assert NT == 4 and n_cols == CH * L and JN == HB
    plan0 = tree_plan(dims, TT0, TILE_RATE, HOP_US - 2, AHEAD_US)
    plan = tree_plan(dims, TB, TILE_RATE, HOP_US, AHEAD_US, CS)
    links = plan["links"]
    NL = len(links)
    peers = [(d, k) for d in range(3) for k in range(1, dims[d])]
    strides = (1, X, X * Y)

    def slot_of(offset):
        return offset[0] + X * offset[1] + X * Y * offset[2]

    def kernel(
        eps_ref, p_ref, c1_ref, c2_ref, t0_ref, q_ref,
        out_ref, loss_ref,
        land, kbuf, g0, tt0, tt1, c1f, c1b, c2n, c2p, bacc, lp, lprecv, bp, qf, qrep, vbuf, cbuf,
        mb, sb, fb, ub, ap, xs, xr, mss, msr, pv, ars, arr, arps, arpr, obuf, orecv, trb, loss_rows, loss_two, c2v,
        send_sem, recv_sem, fwd_ssem, fwd_rsem, credit, x_ssem, x_rsem, ms_sem, lp_sem, c1_sem, c2_sem, q_sem, ar_ssem, ar_rsem, arp_sem, o_sem, loss_sem, in_sem,
    ):
        tts = (tt0, tt1)
        chip = lax.axis_index("rows")
        core = lax.axis_index("cols")
        other = 1 - core
        pos = (lax.rem(chip, X), lax.rem(lax.div(chip, X), Y), lax.div(chip, X * Y))

        me = core * CH + chip
        partner = other * CH + chip

        def moved(d, k):
            return me + (lax.rem(pos[d] + k + dims[d], dims[d]) - pos[d]) * strides[d]

        near = {link: moved(*link) for link in links}

        def source_of(slot):
            off = (lax.rem(slot, X), lax.rem(lax.div(slot, X), Y), lax.div(slot, X * Y))
            at = [lax.rem(pos[d] + dims[d] - off[d], dims[d]) for d in range(3)]
            return at[0] + X * at[1] + X * Y * at[2]

        def to_partner(src, dst, ssem, rsem):
            return pltpu.make_async_remote_copy(
                src_ref=src, dst_ref=dst, send_sem=ssem, recv_sem=rsem,
                device_id=partner, device_id_type=FLAT,
            )

        def tree_copy(buf, width, first, m):
            n = m["hi"] - m["lo"]
            return pltpu.make_async_remote_copy(
                src_ref=buf.at[pl.ds((first + slot_of(m["src"])) * width + m["lo"], n)],
                dst_ref=buf.at[pl.ds((first + slot_of(m["dst"])) * width + m["lo"], n)],
                send_sem=send_sem.at[links.index(m["link"])],
                recv_sem=recv_sem.at[m["sem"]],
                device_id=near[m["link"]],
                device_id_type=FLAT,
            )

        def tree(buf, width, first, the_plan, before_send=None, on_slot=None, fillers=()):
            fillers, ready, waits = list(fillers), [], 0
            for op, m in the_plan["ops"]:
                if op == "send":
                    if before_send is not None:
                        before_send(m)
                    tree_copy(buf, width, first, m).start()
                elif op == "wait":
                    while fillers and not fillers[0][0]:
                        fillers.pop(0)[1]()
                    if not ready and fillers and waits >= fillers[0][0]:
                        fillers.pop(0)[1]()
                    while ready:
                        on_slot(*ready.pop(0))
                    n = sum(e["hi"] - e["lo"] for e in m)
                    ref = buf.at[pl.ds((first + slot_of(m[0]["dst"])) * width, n)]
                    pltpu.make_async_copy(ref, ref, recv_sem.at[m[0]["sem"]]).wait()
                    waits += 1
                elif on_slot is not None:
                    ready.append((op, m))
            for at in ready:
                on_slot(*at)
            for _, f in fillers:
                f()

        def tree_sent(buf, the_plan):
            for k, link in enumerate(links):
                n = the_plan["totals"][link]
                ref = buf.at[pl.ds(0, n)]
                pltpu.make_async_copy(ref, ref, send_sem.at[k]).wait()

        def give_credit():
            for d, sign in links:
                pl.semaphore_signal(credit, inc=1, device_id=moved(d, -sign), device_id_type=FLAT)

        def all_sum_send(stage):
            for n, k in enumerate(range(1, dims[stage])):
                pltpu.make_async_remote_copy(
                    src_ref=ars.at[stage], dst_ref=arr.at[stage, n],
                    send_sem=ar_ssem.at[stage], recv_sem=ar_rsem.at[stage],
                    device_id=moved(stage, k), device_id_type=FLAT,
                ).start()

        def all_sum_get(stage):
            total, n = ars[stage], dims[stage] - 1
            if n:
                ref = arr.at[stage, pl.ds(0, n)]
                pltpu.make_async_copy(ref, ref, ar_ssem.at[stage]).wait()
                pltpu.make_async_copy(ref, ref, ar_rsem.at[stage]).wait()
            for k in range(n):
                total = total + arr[stage, k]
            return total

        def all_sum_step(stage):
            total = all_sum_get(stage)
            if stage < 2:
                ars[stage + 1] = total
                all_sum_send(stage + 1)
            else:
                arps[...] = total
                to_partner(arps, arpr, arp_sem.at[0], arp_sem.at[1]).start()

        c2_in = pltpu.make_async_copy(c2_ref, c2v, in_sem.at[0])
        c2_in.start()
        barrier = pltpu.get_barrier_semaphore()
        for d, k in peers:
            pl.semaphore_signal(barrier, inc=1, device_id=moved(d, k), device_id_type=FLAT)
        pl.semaphore_signal(barrier, inc=1, device_id=partner, device_id_type=FLAT)

        row = lax.broadcasted_iota(jnp.int32, (S, L), 0)
        lane = lax.broadcasted_iota(jnp.int32, (S, L), 1)

        for g in range(G):
            rows = slice(g * S, g * S + S)
            pair = jnp.concatenate([c1_ref[rows, :L], c1_ref[rows, L:]], axis=0)
            g0[NT0 + core * G + g] = pair.astype(BF16)
        c1_copy = to_partner(
            g0.at[pl.ds(NT0 + core * G, G)], g0.at[pl.ds(NT0 + core * G, G)], c1_sem.at[0], c1_sem.at[1]
        )
        q_copy = to_partner(q_ref, qf.at[pl.ds(core * HB, HB)], q_sem.at[0], q_sem.at[1])

        tile = jnp.zeros((S, L), F32)
        for t in range(2):
            part = jnp.zeros((1, L), F32)
            for k in range(NR):
                entry = c1_ref[k : k + 1, t * L : t * L + L]
                part = part + entry * entry * p_ref[k]
            tile = jnp.where(row == 2 * core + t, jnp.broadcast_to(part, (S, L)), tile)
        where = (row - 4) * L + lane
        for k in range(NR):
            tile = jnp.where(where == chip * NR + k, p_ref[k], tile)
        ars[0] = tile
        for g in range(G):
            rows = slice(g * S, g * S + S)
            for t in range(JW):
                a, b = t0_ref[rows, (2 * L) * t : (2 * L) * t + L], t0_ref[rows, (2 * L) * t + L : (2 * L) * t + (2 * L)]
                g0[g * JW + t] = jnp.concatenate([a, b], axis=0).astype(BF16)
        qf[pl.ds(core * HB, HB)] = q_ref[...]

        c2_copy = to_partner(c2n.at[pl.ds(core * HB, HB)], c2n.at[pl.ds(core * HB, HB)], c2_sem.at[0], c2_sem.at[1])
        bp[...] = jnp.zeros_like(bp)

        def round_c2(first, last):
            c2_in.wait()
            for t in range(first, last):
                blk = c2v[:, t * L : t * L + L]
                c2n[core * HB + t] = blk.astype(BF16)
                bp[...] += blk * blk * q_ref[t : t + 1, :]

        def finish_b():
            bp[...] = jnp.broadcast_to(jnp.sum(bp[...], axis=1, keepdims=True), (L, L))

        with jax.named_scope("barrier"):
            pl.semaphore_wait(barrier, len(peers) + 1)
        give_credit()
        c1_copy.start()
        q_copy.start()
        all_sum_send(0)

        src = lax.broadcasted_iota(jnp.int32, (L, L), 0)
        dst = lax.broadcasted_iota(jnp.int32, (L, L), 1)
        picks = [
            jnp.where((src - core * JB == dst - h * JB) & (dst >= h * JB) & (dst < h * JB + JB), 1.0, 0.0).astype(BF16)
            for h in range(2)
        ]

        def order_c2(first, last):
            for t in range(first, last):
                a = jnp.dot(c2n[source_of(2 * t)], picks[0], preferred_element_type=F32)
                b = jnp.dot(c2n[source_of(2 * t + 1)], picks[1], preferred_element_type=F32)
                c2p[:, t * L : t * L + L] = (a + b).astype(BF16)

        def order_q(first, last):
            def four(n, carry):
                for k in range(4):
                    p = 4 * n + k
                    shared = p < CS
                    half = jnp.where(shared, other, core)
                    line = jnp.broadcast_to(qf[pl.ds(source_of(jnp.where(shared, p, p - CS)), 1), :], (S, L))
                    for jt in range(JT):
                        own = jnp.where(lane == half * JB + jt * S + row, line, 0.0)
                        qrep[p, jt] = jnp.broadcast_to(jnp.sum(own, axis=1, keepdims=True), (S, L))
                return carry

            lax.fori_loop(first // 4, last // 4, four, 0)

        def span(n, parts, f):
            cuts = [n * k // parts for k in range(parts + 1)]
            return [lambda a=a, b=b: f(a, b) for a, b in zip(cuts, cuts[1:])]

        fillers = [(0, lambda: round_c2(0, HB)), (0, finish_b), (0, lambda: c2_copy.start())]
        fillers += [(0, lambda: q_copy.wait()), (0, lambda: order_q(0, NP)), (LATE // 2, lambda: all_sum_step(0))]
        fillers += [(LATE, lambda: all_sum_step(1))]
        waited = []

        def before_send(m):
            if not waited and m["hi"] > NT0:
                waited.append(1)
                c1_copy.wait()

        def unpack(op, s):
            chip_s = source_of(s)
            for g in range(G):
                tiles = g0[s * TT0 + g * JW : s * TT0 + g * JW + JW].astype(F32).reshape(JN, S, L)
                kbuf[pl.ds((chip_s * G + g) * JN, JN)] = tiles
                at = pl.ds(pl.multiple_of(chip_s * NR + g * S, S), S)
                for h in range(2):
                    pair = g0[s * TT0 + NT0 + h * G + g].astype(F32)
                    c1f[at, 2 * L * h : 2 * L * h + L] = pair[:S]
                    c1f[at, 2 * L * h + L : 2 * L * h + 2 * L] = pair[S:]

        with jax.named_scope("gather0"):
            first = [(0, lambda: unpack("slot", 0))]
            tree(g0, TT0, 0, plan0, before_send=before_send, on_slot=unpack, fillers=first + fillers)
            tree_sent(g0, plan0)
            c1b[...] = c1f[...].astype(BF16)
            all_sum_step(2)

        def finish_lp():
            lp[...] = jnp.concatenate([bp[...]] * NT, axis=1) - 2.0 * bacc[...]

        bacc[...] = jnp.zeros_like(bacc)
        JC = CK // L

        def first_chunk(n, carry):
            cols = []
            for t in range(JC):
                cols.append(kbuf[pl.ds(n * JC + t, CH * G, stride=JN)].reshape(n_rows, L))
            plan_c = jnp.concatenate(cols, axis=1).astype(BF16)
            lead = jnp.dot(c1b[...], plan_c, preferred_element_type=F32).astype(BF16)
            c2c = jnp.concatenate([c2n[core * HB + n * JC + t] for t in range(JC)], axis=1)
            bacc[...] += lax.dot_general(c2c, lead, (((1,), (1,)), ((), ())), preferred_element_type=F32)
            return carry

        with jax.named_scope("firstmm"):
            lax.fori_loop(0, KJ // CK, first_chunk, 0)
            finish_lp()
        to_partner(arps, arpr, arp_sem.at[0], arp_sem.at[1]).wait()
        ap[...] = jnp.where(row < 4, arps[...] + arpr[...], arps[...])
        for t in range(NT):
            pv[t] = jnp.broadcast_to(ap[4 + t : 5 + t, :], (S, L))


        def lead_and_cross(n, plan_c):
            lead = jnp.dot(plan_c[...], c1b[...], preferred_element_type=F32).astype(BF16)
            bacc[...] += jnp.dot(c2p[:, n * CM : n * CM + CM], lead, preferred_element_type=F32)

        def costs():
            copy = to_partner(lp.at[pl.ds(other * JB, JB)], lprecv, lp_sem.at[0], lp_sem.at[1])
            copy.start()
            copy.wait()
            own = lp[pl.ds(pl.multiple_of(core * JB, JB), JB), :] + lprecv[...]
            return own + jnp.concatenate([ap[t : t + 1, :] for t in range(NT)], axis=1)

        def block(s):
            return kbuf[pl.ds(s * TB, TB)].reshape(JT, NT, S, L)

        def weighted(kk, u):
            w = (kk[:, 0] * u[0] + kk[:, 1] * u[1]) + (kk[:, 2] * u[2] + kk[:, 3] * u[3])
            return jnp.sum(w, axis=2, keepdims=True)

        def passes(u, rescale=False, par=0):
            def place(g):
                return g * GS + 2 * CS if not isinstance(g, int) or g < NE else (g - NE) * GS

            def one(at, buf):
                for k in range(GS):
                    p = at + k
                    kk = block(p)
                    if rescale:
                        kk = kk * fb[:, pl.ds(p, 1), :][None]
                        kbuf[pl.ds(p * TB, TB)] = kk.reshape(TB, S, L)
                    cbuf[buf, k] = qrep[p] / jnp.broadcast_to(weighted(kk, u), (JT, S, L))

            def two(at, buf, acc):
                for k in range(GS):
                    p = at + k
                    acc = acc + jnp.sum(block(p) * cbuf[buf, k][:, None], axis=0)
                return acc

            def run(a, b, end):
                shift = place(a) - a * GS
                even, odd = a % 2, (a + 1) % 2
                pairs = max(0, (b - a - 1) // 2)

                def both(n, acc):
                    at = (a + 2 * n) * GS + shift
                    one(at + GS, odd)
                    acc = two(at, even, acc)
                    one(at + 2 * GS, even)
                    return two(at + GS, odd, acc)

                acc = lax.fori_loop(0, pairs, both, jnp.zeros((NT, S, L), F32))
                for g in range(a + 2 * pairs, b):
                    if g + 1 < end:
                        one(place(g + 1), (g + 1) % 2)
                    acc = two(place(g), g % 2, acc)
                return acc

            one(place(0), 0)
            xs[par] = run(0, NE, NE + NC)
            copy = to_partner(xs.at[par], xr.at[par], x_ssem.at[par], x_rsem.at[par])
            copy.start()
            acc = run(NE, NE + NC, NE + NC)
            copy.wait()
            total = jnp.sum((xs[par] + xr[par]) + acc, axis=1, keepdims=True)
            return quotient(pv[...], jnp.broadcast_to(total, (NT, S, L)))

        def plan_chunk(n, dst, u):
            def one(g):
                for k in range(GS):
                    p = CS + (n * GC + g) * GS + k
                    cbuf[g % 2, k] = quotient(qrep[p], jnp.broadcast_to(weighted(block(p), u), (JT, S, L)))

            one(0)
            for g in range(GC):
                if g + 1 < GC:
                    one(g + 1)
                for k in range(GS):
                    s = (n * GC + g) * GS + k
                    v = cbuf[g % 2, k]
                    vbuf[s] = v
                    t = (block(CS + s) * u[None]) * v[:, None]
                    flat = jnp.concatenate([t[:, i].reshape(JB, L) for i in range(NT)], axis=1)
                    at = (g * GS + k) * JB
                    dst[at : at + JB, :] = flat.astype(BF16)

        def outer(r, carry):
            eps = eps_ref[r]
            inv = 1.0 / eps
            inv = inv * (2.0 - eps * inv)
            main = LOG2E * inv
            (e0, e1), (m0, m1) = halves(eps), halves(main)
            prod = eps * main
            low_part = ((e0 * m0 - prod) + (e0 * m1 + e1 * m0)) + e1 * m1
            rest = (((LOG2E - prod) - low_part) + LOG2E_REST) * inv

            def decay(x):
                return jnp.exp2(x * main + x * rest)

            cost = costs()
            for jt in range(JT):
                for t in range(NT):
                    land[CS * TB + jt * NT + t] = cost[jt * S : jt * S + S, t * L : t * L + L]

            def exps(p):
                ll = land[p * TB : p * TB + TB].reshape(JT, NT, S, L)
                low = jnp.min(jnp.min(ll, axis=0), axis=1, keepdims=True)
                kk = decay(low[None] - ll)
                kbuf[p * TB : p * TB + TB] = kk.reshape(TB, S, L)
                mb[:, p : p + 1, :] = low
                sb[:, p : p + 1, :] = jnp.sum(jnp.sum(kk, axis=0), axis=1, keepdims=True)

            def passed_on(s):
                return to_partner(
                    land.at[pl.ds((CS + s) * TB, TB)], land.at[pl.ds(s * TB, TB)], fwd_ssem.at[0], fwd_rsem.at[s]
                )

            def on_slot(op, s):
                if op == "slot":
                    if s < CS:
                        passed_on(s).start()
                    exps(CS + s)
                else:
                    passed_on(s).wait_recv()
                    exps(s)

            def once(n, f):
                @pl.when(r == 0)
                def _():
                    if not n:
                        c2_copy.wait()
                    f()

            with jax.named_scope("gather"):
                pl.semaphore_wait(credit, NL)
                first = [(0, lambda: on_slot("slot", 0)), (plan["waits"] // 4, lambda: on_slot("partner", 0))]
                for n, f in enumerate(span(CH // 2, S, order_c2)):
                    first.append((LATE // 2 + 2 * n, lambda n=n, f=f: once(n, f)))
                tree(land, TB, CS, plan, on_slot=on_slot, fillers=first)
                tree_sent(land, plan)
                ref = land.at[pl.ds(0, CS * TB)]
                pltpu.make_async_copy(ref, ref, fwd_ssem.at[0]).wait()
                give_credit()

            with jax.named_scope("minx"):
                def least_of(a, b):
                    low = jnp.min(mb[:, a:b], axis=1, keepdims=True)
                    part = jnp.sum(sb[:, a:b] * decay(low - mb[:, a:b]), axis=1, keepdims=True)
                    return jnp.broadcast_to(low, (NT, S, L)), jnp.broadcast_to(part, (NT, S, L))

                mss[0], mss[1] = least_of(2 * CS, NP)
                copy = to_partner(mss, msr, ms_sem.at[0], ms_sem.at[1])
                copy.start()
                low, part = least_of(0, 2 * CS)
                copy.wait()
                least = jnp.minimum(jnp.minimum(mss[0], msr[0]), low)
                total = mss[1] * decay(least - mss[0]) + msr[1] * decay(least - msr[0])
                total = total + part * decay(least - low)
                fb[...] = decay(least[:, :1] - mb[...])
                u = quotient(pv[...], total)

            with jax.named_scope("pass1"):
                u = passes(u, rescale=True, par=1)

            def sweep(t, u):
                return passes(u, par=lax.rem(t, 2))

            with jax.named_scope("sweeps"):
                u = lax.fori_loop(2, sweeps, sweep, u)
            ub[...] = u
            bacc[...] = jnp.zeros_like(bacc)
            with jax.named_scope("finish"):
                plan_chunk(0, tts[0], u)
                for n in range(KJ // CM):
                    if n + 1 < KJ // CM:
                        plan_chunk(n + 1, tts[(n + 1) % 2], u)
                    lead_and_cross(n, tts[n % 2])
                finish_lp()
            return carry

        lax.fori_loop(0, steps, outer, 0)

        pl.semaphore_wait(credit, NL)
        u = ub[...]
        v = (vbuf[0], quotient(qrep[0], jnp.broadcast_to(weighted(block(0), u), (JT, S, L))))
        total = jnp.zeros((S, L), F32)
        for own, (p, half) in enumerate(((CS, core), (0, other))):
            plan_b = (block(p) * u[None]) * v[own][:, None]
            part = lp[pl.ds(pl.multiple_of(half * JB, JB), JB), :]
            for jt in range(JT):
                for t in range(NT):
                    cost = part[jt * S : jt * S + S, t * L : t * L + L]
                    total = total + (cost if own else cost + ap[t : t + 1, :]) * plan_b[jt, t]
        loss_rows[0:1] = jnp.sum(total, axis=0, keepdims=True)

        steps_on = [[moved(d, k) - me for k in range(dims[d])] for d in range(3)]
        offsets = sorted(itertools.product(*(range(n) for n in dims)), key=lambda o: -sum(min(k, 4 - k) for k in o))
        for o in offsets[:-1]:
            pltpu.make_async_remote_copy(
                src_ref=loss_rows.at[pl.ds(0, 1)], dst_ref=loss_rows.at[pl.ds(slot_of(o), 1)],
                send_sem=loss_sem.at[0], recv_sem=loss_sem.at[1],
                device_id=me + steps_on[0][o[0]] + steps_on[1][o[1]] + steps_on[2][o[2]], device_id_type=FLAT,
            ).start()

        it = lax.div(chip * NR, L)
        inside = pl.multiple_of(lax.rem(chip * NR, L), S)

        def rows_of(n, carry):
            for k in range(4):
                s = 4 * n + k
                kk = jnp.concatenate([kbuf[(CS + s) * TB + jt * NT + it] for jt in range(JT)], axis=0)
                uu = jnp.concatenate([ub[it]] * JT, axis=0)
                t = (kk * uu) * vbuf[s].reshape(JB, L)
                none = jnp.zeros_like(t)
                both = jnp.where(core == 0, jnp.concatenate([t, none], axis=0), jnp.concatenate([none, t], axis=0))
                trb[k] = both.T
                obuf[source_of(s)] = trb[k, pl.ds(inside, NR), :]
            return carry

        with jax.named_scope("tail"):
            lax.fori_loop(0, CH // 4, rows_of, 0)
            o_copy = to_partner(obuf.at[pl.ds(other * HB, HB)], orecv, o_sem.at[0], o_sem.at[1])
            o_copy.start()
            o_copy.wait()
            orecv[...] = obuf[pl.ds(core * HB, HB)] + orecv[...]
            o_out = pltpu.make_async_copy(orecv, out_ref, in_sem.at[1])
            o_out.start()
            ref = loss_rows.at[pl.ds(1, CH - 1)]
            pltpu.make_async_copy(ref, ref, loss_sem.at[0]).wait()
            pltpu.make_async_copy(ref, ref, loss_sem.at[1]).wait()
            loss_two[0:1] = jnp.sum(loss_rows[...], axis=0, keepdims=True)
            copy = to_partner(loss_two.at[pl.ds(0, 1)], loss_two.at[pl.ds(1, 1)], loss_sem.at[2], loss_sem.at[3])
            copy.start()
            copy.wait()
            loss_ref[0] = jnp.sum(loss_two[...])
            o_out.wait()

    vm = pltpu.VMEM
    dma = pltpu.SemaphoreType.DMA
    scratch = [
        vm((NP * TB, S, L), F32),
        vm((NP * TB, S, L), F32),
        vm((CH * TT0, 16, L), BF16),
        vm((CM, n_rows), BF16),
        vm((CM, n_rows), BF16),
        vm((n_rows, n_rows), F32),
        vm((n_rows, n_rows), BF16),
        vm((CH, L, L), BF16),
        vm((L, KJ), BF16),
        vm((L, n_rows), F32),
        vm((L, n_rows), F32),
        vm((JB, n_rows), F32),
        vm((L, L), F32),
        vm((CH, L), F32),
        vm((NP, JT, S, L), F32),
        vm((CH, JT, S, L), F32),
        vm((2, GS, JT, S, L), F32),
        vm((NT, NP, L), F32),
        vm((NT, NP, L), F32),
        vm((NT, NP, L), F32),
        vm((NT, S, L), F32),
        vm((S, L), F32),
        vm((2, NT, S, L), F32),
        vm((2, NT, S, L), F32),
        vm((2, NT, S, L), F32),
        vm((2, NT, S, L), F32),
        vm((NT, S, L), F32),
        vm((3, S, L), F32),
        vm((3, 3, S, L), F32),
        vm((S, L), F32),
        vm((S, L), F32),
        vm((CH, NR, L), F32),
        vm((HB, NR, L), F32),
        vm((4, L, L), F32),
        vm((CH, L), F32),
        vm((2, L), F32),
        vm((L, n_cols // 2), F32),
        dma((NL,)),
        dma((max(plan["waits"], plan0["waits"]),)),
        dma((1,)),
        dma((CS,)),
        pltpu.SemaphoreType.REGULAR,
        dma((2,)),
        dma((2,)),
        dma((2,)),
        dma((2,)),
        dma((2,)),
        dma((2,)),
        dma((2,)),
        dma((3,)),
        dma((3,)),
        dma((2,)),
        dma((2,)),
        dma((4,)),
        dma((2,)),
    ]
    return kernel, scratch


def solution(mesh):
    chips = mesh.shape["rows"]
    dims = torus_of(chips)
    grid_spec = P(("pairs", "rows"), "cols")

    def local_fn(c1, c2, t0, p, q, eps):
        n_rows, n_cols = p.shape[0] * chips, q.shape[0] * mesh.shape["cols"]
        kernel, scratch = make_kernel(dims, n_rows, n_cols, eps.shape[0], SWEEPS)
        vmem = pl.BlockSpec(memory_space=pltpu.VMEM)
        smem = pl.BlockSpec(memory_space=pltpu.SMEM)
        anywhere = pl.BlockSpec(memory_space=pl.ANY)
        plan, loss = pl.pallas_call(
            kernel,
            name="gromov",
            out_shape=(jax.ShapeDtypeStruct((chips // 2, t0.shape[0], L), F32), jax.ShapeDtypeStruct((1,), F32)),
            in_specs=[smem, smem, vmem, anywhere, vmem, vmem],
            out_specs=(anywhere, smem),
            scratch_shapes=scratch,
            compiler_params=pltpu.CompilerParams(
                collective_id=0, has_side_effects=True, vmem_limit_bytes=60 * 1024 * 1024
            ),
        )(eps, p, c1, c2, t0, q.reshape(chips // 2, L))
        return plan.transpose(1, 0, 2).reshape(t0.shape), loss

    return jax.shard_map(
        local_fn,
        mesh=mesh,
        in_specs=(grid_spec, grid_spec, grid_spec, P(("pairs", "rows")), P(("pairs", "cols")), P("pairs")),
        out_specs=(grid_spec, P("pairs")),
        check_vma=False,
    )
```
